32 devices in a mesh: data: 1 (over z), tp: 32 (over y, x, core).
Axes of the slice: x: 4, y: 4, z: 1, core: 2. Of those that a mesh axis runs over, the one named last changes fastest.
The devices are a block of a 4x4x8 slice.
Arguments:
- hidden: bfloat16 [2, 768, 4096], P('data')
- seg_ids: int32 [2, 768], P('data')
- grad_out: bfloat16 [2, 768, 4096], P('data')
- gain_attn: float32 [4096], replicated
- gain_mlp: float32 [4096], replicated
- w_q: bfloat16 [4096, 4096], P(None, 'tp')
- w_k: bfloat16 [4096, 1024], replicated
- w_v: bfloat16 [4096, 1024], replicated
- w_o: bfloat16 [4096, 4096], P('tp')
- w_gate: bfloat16 [4096, 14336], P(None, 'tp')
- w_up: bfloat16 [4096, 14336], P(None, 'tp')
- w_down: bfloat16 [14336, 4096], P('tp')
Outputs:
- output 1: bfloat16 [2, 768, 4096], P('data')
- output 2: bfloat16 [2, 768, 4096], P('data')
- output 3: float32 [4096], P('data')
- output 4: float32 [4096], P('data')
- output 5: float32 [4096, 4096], P('data', 'tp')
- output 6: float32 [4096, 1024], P('data')
- output 7: float32 [4096, 1024], P('data')
- output 8: float32 [4096, 4096], P(('data', 'tp'))
- output 9: float32 [4096, 14336], P('data', 'tp')
- output 10: float32 [4096, 14336], P('data', 'tp')
- output 11: float32 [14336, 4096], P(('data', 'tp'))
All inputs are finite; a program needn't handle non-finite values.
Results may differ from the reference program's by a relative error of at most 0.02.
Values are sent between devices in bfloat16 or wider.
A program may use at most 768 MiB of HBM per device.

```python
import jax
import jax.numpy as jnp
from jax import lax

D = 4096
FF = 14336
HEADS = 32
KV_HEADS = 8
HEAD = 128
SEQ = 768
CUTS = 3
EPS = 1e-5


def draw_segments(key):
    cuts = jax.random.randint(key, (2, 1, CUTS), 1, SEQ)
    positions = jnp.arange(SEQ, dtype=jnp.int32)[None, :, None]
    return jnp.sum((positions >= cuts).astype(jnp.int32), axis=-1).astype(jnp.int32)


def draw_weight(key, n_rows, n_cols, scale):
    return (jax.random.normal(key, (n_rows, n_cols), jnp.float32) * scale).astype(jnp.bfloat16)


def setup_inputs(seed: int = 0, part: int = 0) -> dict:
    own_keys = jax.random.split(jax.random.fold_in(jax.random.key(seed), part), 3)
    shared = jax.random.split(jax.random.key(seed + 1), 9)
    qk_scale = 1.5 * D ** -0.5
    return {
        'hidden': jax.random.normal(own_keys[0], (2, SEQ, D), jnp.float32).astype(jnp.bfloat16),
        'seg_ids': draw_segments(own_keys[1]),
        'grad_out': jax.random.normal(own_keys[2], (2, SEQ, D), jnp.float32).astype(jnp.bfloat16),
        'gain_attn': 0.5 + jax.random.uniform(shared[0], (D,), jnp.float32),
        'gain_mlp': 0.5 + jax.random.uniform(shared[1], (D,), jnp.float32),
        'w_q': draw_weight(shared[2], D, HEADS * HEAD, qk_scale),
        'w_k': draw_weight(shared[3], D, KV_HEADS * HEAD, qk_scale),
        'w_v': draw_weight(shared[4], D, KV_HEADS * HEAD, D ** -0.5),
        'w_o': draw_weight(shared[5], HEADS * HEAD, D, (HEADS * HEAD) ** -0.5),
        'w_gate': draw_weight(shared[6], D, FF, D ** -0.5),
        'w_up': draw_weight(shared[7], D, FF, D ** -0.5),
        'w_down': draw_weight(shared[8], FF, D, FF ** -0.5),
    }


def rms_norm(x_in, gain):
    x_float = x_in.astype(jnp.float32)
    inv_rms = lax.rsqrt(jnp.mean(x_float * x_float, axis=-1, keepdims=True) + EPS)
    return (x_float * inv_rms * gain).astype(jnp.bfloat16)


def attention(q_all, k_all, v_all, seg_row):
    group = HEADS // KV_HEADS
    q_heads = q_all.reshape(SEQ, HEADS, HEAD).transpose(1, 0, 2)
    k_heads = jnp.repeat(k_all.reshape(SEQ, KV_HEADS, HEAD).transpose(1, 0, 2), group, axis=0)
    v_heads = jnp.repeat(v_all.reshape(SEQ, KV_HEADS, HEAD).transpose(1, 0, 2), group, axis=0)
    positions = jnp.arange(SEQ)
    allowed = (positions[:, None] >= positions[None, :]) & (seg_row[:, None] == seg_row[None, :])

    def one_head(operands):
        q_head, k_head, v_head = operands
        scores = jnp.dot(q_head.astype(jnp.float32), k_head.astype(jnp.float32).T) * HEAD ** -0.5
        scores = jnp.where(allowed, scores, -1e30)
        probs = jax.nn.softmax(scores, axis=-1).astype(jnp.bfloat16)
        return jnp.dot(probs, v_head, preferred_element_type=jnp.float32)

    ctx = lax.map(jax.checkpoint(one_head), (q_heads, k_heads, v_heads))
    return ctx.transpose(1, 0, 2).reshape(SEQ, HEADS * HEAD).astype(jnp.bfloat16)


def layer(x_half, seg_row, gain_attn, gain_mlp, w_q, w_k, w_v, w_o, w_gate, w_up, w_down):
    normed = rms_norm(x_half, gain_attn)
    q_all = jnp.dot(normed, w_q, preferred_element_type=jnp.float32).astype(jnp.bfloat16)
    k_all = jnp.dot(normed, w_k, preferred_element_type=jnp.float32).astype(jnp.bfloat16)
    v_all = jnp.dot(normed, w_v, preferred_element_type=jnp.float32).astype(jnp.bfloat16)
    ctx = attention(q_all, k_all, v_all, seg_row)
    attn_out = jnp.dot(ctx, w_o, preferred_element_type=jnp.float32).astype(jnp.bfloat16)
    resid = (x_half.astype(jnp.float32) + attn_out.astype(jnp.float32)).astype(jnp.bfloat16)
    mixed = rms_norm(resid, gain_mlp)
    gate = jnp.dot(mixed, w_gate, preferred_element_type=jnp.float32)
    upper = jnp.dot(mixed, w_up, preferred_element_type=jnp.float32)
    act = (jax.nn.silu(gate) * upper).astype(jnp.bfloat16)
    mlp_out = jnp.dot(act, w_down, preferred_element_type=jnp.float32).astype(jnp.bfloat16)
    return (resid.astype(jnp.float32) + mlp_out.astype(jnp.float32)).astype(jnp.bfloat16)


def reference(hidden, seg_ids, grad_out, gain_attn, gain_mlp, w_q, w_k, w_v, w_o, w_gate, w_up, w_down):
    params = (gain_attn, gain_mlp, w_q, w_k, w_v, w_o, w_gate, w_up, w_down)
    y_halves = []
    dx_halves = []
    totals = [jnp.zeros(param.shape, jnp.float32) for param in params]
    for half_idx in range(2):
        seg_row = seg_ids[half_idx]

        def half_layer(x_half, *weights):
            return layer(x_half, seg_row, *weights)

        y_half, pullback = jax.vjp(half_layer, hidden[half_idx], *params)
        cotangents = pullback(grad_out[half_idx])
        y_halves.append(y_half)
        dx_halves.append(cotangents[0])
        totals = [acc_val + cot_val.astype(jnp.float32) for acc_val, cot_val in zip(totals, cotangents[1:])]
    return (jnp.stack(y_halves), jnp.stack(dx_halves), totals[0], totals[1], totals[2], totals[3], totals[4], totals[5], totals[6], totals[7], totals[8])
```

```python
import functools
import math
import jax
import jax.numpy as jnp
from jax import lax
from jax.experimental import pallas as pl
from jax.experimental.pallas import tpu as pltpu
from jax.sharding import PartitionSpec as P

HEAD_DIM = 128
EPS = 1e-5
MESH = pl.DeviceIdType.MESH
F32 = jnp.float32
BF16 = jnp.bfloat16


def dot(lhs, rhs, dims):
    return lax.dot_general(lhs, rhs, (dims, ((), ())), preferred_element_type=F32)


def sum_rows_gather(mode, side, part_ref, refs, outs, scr):
    tp_idx = lax.axis_index('tp')
    core = lax.rem(tp_idx, 2)
    chip = lax.div(tp_idx, 2)
    x_pos = lax.rem(chip, side)
    y_pos = lax.div(chip, side)

    def wrap(pos):
        return lax.rem(pos + 2 * side, side)

    def at_chip(y_at, x_at):
        return {'tp': (y_at * side + x_at) * 2 + core}

    partner = {'tp': chip * 2 + (1 - core)}

    class Colour:
        pass

    colours = []
    for index in range(2):
        col = Colour()
        col.index = index
        col.first = x_pos if index == 0 else y_pos
        col.second = y_pos if index == 0 else x_pos
        colours.append(col)

    def block(col, second, first):
        return (second, first) if col.index == 0 else (first, second)

    def peer1(col, shift):
        return at_chip(*block(col, col.second, wrap(col.first + shift)))

    def peer2(col, shift):
        return at_chip(*block(col, wrap(col.second + shift), col.first))

    part, gat = scr['part'], scr['gat']
    rows, width = part.shape[2], part.shape[3]
    quarter = width // 4

    def cols(col, half):
        return pl.ds((col.index * 2 + half) * quarter, quarter)

    def both_cols(col):
        return pl.ds(col.index * 2 * quarter, 2 * quarter)

    pending = []

    def send(src, dst, sems, index, device):
        copy = pltpu.make_async_remote_copy(src, dst, scr[sems + '_s'].at[index], scr[sems + '_r'].at[index], device_id=device, device_id_type=MESH)
        copy.start()
        pending.append(copy)

    def arrive(dst, sems, index):
        pltpu.make_async_remote_copy(dst, dst, scr[sems + '_s'].at[index], scr[sems + '_r'].at[index], device_id=partner, device_id_type=MESH).wait_recv()

    barrier = pltpu.get_barrier_semaphore()
    peers = [partner]
    if mode == 'da':
        peers += [at_chip(y_pos, wrap(x_pos + shift)) for shift in range(1, side)]
        peers += [at_chip(wrap(y_pos + shift), x_pos) for shift in range(1, side)]
    else:
        peers += [at_chip(y_pos, wrap(x_pos + shift)) for shift in (1, side - 1)]
        peers += [at_chip(wrap(y_pos + shift), x_pos) for shift in (1, side - 1)]

    order = (2, 1, 3, 0)
    loads = {}
    for shift_a in order:
        for shift_b in order:
            y_at, x_at = wrap(y_pos + shift_a), wrap(x_pos + shift_b)
            load = pltpu.make_async_copy(part_ref.at[y_at, x_at], part.at[y_at, x_at], scr['load'].at[shift_a * 4 + shift_b])
            load.start()
            loads[shift_a, shift_b] = load
    for peer in peers:
        pl.semaphore_signal(barrier, inc=1, device_id=peer, device_id_type=MESH)
    pl.semaphore_wait(barrier, len(peers))
    for load in loads.values():
        load.wait()

    signs = (1, -1)

    def add_into(where, at_cols, *terms):
        total = part[(*where, slice(None), at_cols)].astype(F32)
        for term in terms:
            total = total + term[...].astype(F32)
        part[(*where, slice(None), at_cols)] = total.astype(BF16)

    def piece(where, at_cols):
        return part.at[(*where, slice(None), at_cols)]

    shifts = (2, 1, 3, 0)

    def first_far(step):
        for col in colours:
            second = wrap(col.second + shifts[step])
            for way, sign in enumerate(signs):
                src = piece(block(col, second, wrap(col.first + 2)), cols(col, way))
                index = (col.index * 2 + way) * 4 + step
                send(src, scr['r1'].at[index], 'r1', index, peer1(col, sign))

    def first_near(step):
        for col in colours:
            second = wrap(col.second + shifts[step])
            for way, sign in enumerate(signs):
                src = piece(block(col, second, wrap(col.first + sign)), cols(col, 1 - way))
                index = (col.index * 2 + way) * 4 + step
                send(src, scr['r2'].at[index], 'r2', index, peer1(col, sign))

    def first_relay(step):
        for col in colours:
            second = wrap(col.second + shifts[step])
            for way, sign in enumerate(signs):
                where = block(col, second, wrap(col.first + sign))
                index = (col.index * 2 + way) * 4 + step
                arrive(scr['r1'].at[index], 'r1', index)
                add_into(where, cols(col, way), scr['r1'].at[index])
                send(piece(where, cols(col, way)), scr['r3'].at[index], 'r3', index, peer1(col, sign))

    def first_end(step):
        for col in colours:
            where = block(col, wrap(col.second + shifts[step]), col.first)
            for way in range(2):
                index_3 = (col.index * 2 + way) * 4 + step
                index_2 = (col.index * 2 + 1 - way) * 4 + step
                arrive(scr['r2'].at[index_2], 'r2', index_2)
                arrive(scr['r3'].at[index_3], 'r3', index_3)
                add_into(where, cols(col, way), scr['r2'].at[index_2], scr['r3'].at[index_3])

    def second_far():
        for col in colours:
            for way, sign in enumerate(signs):
                index = col.index * 2 + way
                src = piece(block(col, wrap(col.second + 2), col.first), cols(col, way))
                send(src, scr['s1'].at[index], 's1', index, peer2(col, sign))

    def second_near(way):
        sign = signs[way]
        for col in colours:
            index = col.index * 2 + way
            where = block(col, wrap(col.second + sign), col.first)
            send(piece(where, cols(col, 1 - way)), scr['s2'].at[index], 's2', index, peer2(col, sign))

    def second_relay(way):
        sign = signs[way]
        for col in colours:
            index = col.index * 2 + way
            where = block(col, wrap(col.second + sign), col.first)
            arrive(scr['s1'].at[index], 's1', index)
            add_into(where, cols(col, way), scr['s1'].at[index])
            send(piece(where, cols(col, way)), scr['s3'].at[index], 's3', index, peer2(col, sign))

    def second_end():
        for col in colours:
            where = block(col, col.second, col.first)
            for way in range(2):
                index_3 = col.index * 2 + way
                index_2 = col.index * 2 + 1 - way
                arrive(scr['s2'].at[index_2], 's2', index_2)
                arrive(scr['s3'].at[index_3], 's3', index_3)
                add_into(where, cols(col, way), scr['s2'].at[index_2], scr['s3'].at[index_3])

    first_far(0)
    first_near(0)
    first_far(1)
    first_relay(0)
    first_near(1)
    first_far(2)
    first_relay(1)
    first_near(2)
    first_far(3)
    first_end(0)
    second_far()
    first_relay(2)
    first_near(3)
    first_end(1)
    second_near(0)
    second_relay(0)
    first_relay(3)
    first_end(2)
    second_near(1)
    second_relay(1)
    first_end(3)
    second_end()

    own = (y_pos, x_pos)
    row_step(mode, part, gat, own, refs, outs, scr)

    def spread(ref, where, at_cols):
        return ref.at[(*where, slice(None), at_cols)]

    def ring2_own(half_of_way):
        for col in colours:
            where = block(col, col.second, col.first)
            for way, sign in enumerate(signs):
                half = way if half_of_way == 0 else 1 - way
                at = spread(gat, where, cols(col, half))
                send(at, at, 'h1', (col.index * 2 + way) * 2 + half_of_way, peer2(col, sign))

    def ring1_block(step, half_of_way):
        for col in colours:
            where = block(col, wrap(col.second + back[step]), col.first)
            for way, sign in enumerate(signs):
                half = way if half_of_way == 0 else 1 - way
                at = spread(gat, where, cols(col, half))
                send(at, at, 'h2', ((col.index * 2 + way) * 4 + step) * 2 + half_of_way, peer1(col, sign))

    back = (0, side - 1, 1, 2)

    def ring2_arrive(way, half_of_way):
        sign = signs[way]
        half = way if half_of_way == 0 else 1 - way
        for col in colours:
            where = block(col, wrap(col.second - sign), col.first)
            at = spread(gat, where, cols(col, half))
            arrive(at, 'h1', (col.index * 2 + way) * 2 + half_of_way)
            if half_of_way == 0:
                send(at, at, 'f1', col.index * 2 + way, peer2(col, sign))

    def ring2_relayed():
        for col in colours:
            where = block(col, wrap(col.second + 2), col.first)
            for way in range(2):
                arrive(spread(gat, where, cols(col, way)), 'f1', col.index * 2 + way)

    def ring1_arrive(step, half_of_way):
        for col in colours:
            second = wrap(col.second + back[step])
            for way, sign in enumerate(signs):
                half = way if half_of_way == 0 else 1 - way
                at = spread(gat, block(col, second, wrap(col.first - sign)), cols(col, half))
                arrive(at, 'h2', ((col.index * 2 + way) * 4 + step) * 2 + half_of_way)
                if half_of_way == 0:
                    send(at, at, 'f2', (col.index * 2 + way) * 4 + step, peer1(col, sign))

    def ring1_relayed(step):
        for col in colours:
            second = wrap(col.second + back[step])
            for way in range(2):
                at = spread(gat, block(col, second, wrap(col.first + 2)), cols(col, way))
                arrive(at, 'f2', (col.index * 2 + way) * 4 + step)

    stores = []

    def keep(col, where):
        slot = (col.index * side + where[0]) * side + where[1]
        at = spread(gat, where, both_cols(col))
        if 'own' in outs:
            store = pltpu.make_async_copy(at, spread(outs['own'], where, both_cols(col)), scr['own_s'].at[slot])
            store.start()
            stores.append(store)
        target = spread(outs['full'].at[core], where, both_cols(col))
        store = pltpu.make_async_copy(at, target, scr['full_s'].at[slot])
        store.start()
        stores.append(store)
        copy = pltpu.make_async_remote_copy(at, target, scr['d2d_s'].at[slot], scr['d2d_r'].at[slot], device_id=partner, device_id_type=MESH)
        copy.start()
        pending.append(copy)

    def keep_step(step, firsts):
        for col in colours:
            for shift in firsts:
                keep(col, block(col, wrap(col.second + back[step]), wrap(col.first + shift)))

    ring2_own(0)
    ring1_block(0, 0)
    ring2_own(1)
    ring1_block(0, 1)
    keep_step(0, (0,))
    if mode == 'da':
        gain_sum_core(outs, scr, send, arrive, partner)
    ring2_arrive(0, 0)
    ring2_arrive(1, 0)
    ring2_arrive(0, 1)
    ring1_block(1, 0)
    ring1_block(1, 1)
    ring2_arrive(1, 1)
    ring1_block(2, 0)
    ring1_block(2, 1)
    keep_step(1, (0,))
    keep_step(2, (0,))
    ring1_arrive(0, 0)
    if mode == 'da':
        gain_sum_ring(1, scr, send, arrive, [at_chip(wrap(y_pos + shift), x_pos) for shift in range(1, side)])
    ring2_relayed()
    ring1_block(3, 0)
    ring1_block(3, 1)
    keep_step(3, (0,))
    ring1_arrive(0, 1)
    keep_step(0, (1, side - 1))
    ring1_arrive(1, 0)
    if mode == 'da':
        gain_sum_ring(2, scr, send, arrive, [at_chip(y_pos, wrap(x_pos + shift)) for shift in range(1, side)])
        outs['gain'][...] = scr['gain_tot'][...]
    ring1_arrive(2, 0)
    ring1_relayed(0)
    keep_step(0, (2,))
    ring1_arrive(1, 1)
    keep_step(1, (1, side - 1))
    ring1_arrive(2, 1)
    keep_step(2, (1, side - 1))
    ring1_arrive(3, 0)
    ring1_relayed(1)
    keep_step(1, (2,))
    ring1_relayed(2)
    keep_step(2, (2,))
    ring1_arrive(3, 1)
    keep_step(3, (1, side - 1))
    ring1_relayed(3)
    keep_step(3, (2,))

    for store in stores:
        store.wait()
    for copy in pending:
        copy.wait_send()
    for col_index in range(2):
        for y_at in range(side):
            for x_at in range(side):
                slot = (col_index * side + y_at) * side + x_at
                target = spread(outs['full'].at[1 - core], (y_at, x_at), pl.ds(col_index * 2 * quarter, 2 * quarter))
                pltpu.make_async_remote_copy(target, target, scr['d2d_s'].at[slot], scr['d2d_r'].at[slot], device_id=partner, device_id_type=MESH).wait_recv()


def gain_sum_core(outs, scr, send, arrive, partner):
    send(scr['gain_own'], scr['gain_in'].at[0], 'gain', 0, partner)
    arrive(scr['gain_in'].at[0], 'gain', 0)
    scr['gain_tot'][...] = scr['gain_own'][...] + scr['gain_in'][0]


def gain_sum_ring(stage, scr, send, arrive, peers):
    hold = scr['gain_hold'].at[stage - 1]
    hold[...] = scr['gain_tot'][...]
    base = 1 + (stage - 1) * len(peers)
    for index, peer in enumerate(peers):
        send(hold, scr['gain_in'].at[base + index], 'gain', base + index, peer)
    total = hold[...]
    for index in range(len(peers)):
        arrive(scr['gain_in'].at[base + index], 'gain', base + index)
        total = total + scr['gain_in'][base + index]
    scr['gain_tot'][...] = total


def row_step(mode, part, gat, own, refs, outs, scr):
    rows, width = part.shape[2], part.shape[3]
    tile = 16
    if mode != 'o':
        gain_slot = 0 if mode == 'dm' else 1
        gain_out = outs['gain'] if mode == 'dm' else scr['gain_own']
        gain_total = jnp.zeros((1, width), F32)
    for start in range(0, rows, tile):
        at = pl.ds(start, tile)
        summed = part[(*own, at, slice(None))].astype(F32)
        gain = refs['gain'][...]
        if mode == 'o':
            resid = (refs['x_rows'][at, :].astype(F32) + summed).astype(BF16)
            outs['h_rows'][at, :] = resid
            z_in = resid.astype(F32)
            inv = lax.rsqrt(jnp.mean(z_in * z_in, axis=-1, keepdims=True) + EPS)
            gat[(*own, at, slice(None))] = (z_in * inv * gain).astype(BF16)
            continue
        z_in = refs['z_rows'][at, :].astype(F32)
        inv = lax.rsqrt(jnp.mean(z_in * z_in, axis=-1, keepdims=True) + EPS)
        normed = z_in * inv
        gain_total = gain_total + jnp.sum(summed * normed, axis=0, keepdims=True)
        scaled = summed * gain
        back = inv * (scaled - normed * jnp.mean(scaled * normed, axis=-1, keepdims=True))
        total = refs['up_rows'][at, :].astype(F32) + back
        if mode == 'dm':
            outs['d_rows'][at, :] = total
        gat[(*own, at, slice(None))] = total.astype(BF16)
    if mode == 'dm':
        outs['gain'][...] = gain_total
    if mode == 'da':
        scr['gain_own'][0:1, :] = refs['gain_mlp'][...]
        scr['gain_own'][1:2, :] = gain_total


def reduce_gather(mode, side, collective_id, part, *row_args):
    chips = side * side
    seq, width = part.shape
    rows = seq // chips
    part = part.reshape(side, side, rows, width)
    names_in = {'o': ('x_rows', 'gain'), 'dm': ('z_rows', 'up_rows', 'gain'), 'da': ('z_rows', 'up_rows', 'gain', 'gain_mlp')}[mode]
    full = jax.ShapeDtypeStruct((2, side, side, rows, width), BF16)
    own = jax.ShapeDtypeStruct((side, side, rows, width), BF16)
    any_spec = pl.BlockSpec(memory_space=pl.ANY)
    vmem_spec = pl.BlockSpec(memory_space=pltpu.VMEM)
    outs = {'full': (full, any_spec)}
    if mode != 'da':
        outs['own'] = (own, any_spec)
    if mode == 'o':
        outs['h_rows'] = (jax.ShapeDtypeStruct((rows, width), BF16), vmem_spec)
    if mode == 'dm':
        outs['d_rows'] = (jax.ShapeDtypeStruct((rows, width), F32), vmem_spec)
        outs['gain'] = (jax.ShapeDtypeStruct((1, width), F32), vmem_spec)
    if mode == 'da':
        outs['gain'] = (jax.ShapeDtypeStruct((2, width), F32), vmem_spec)
    names_out = tuple(outs)
    quarter = width // 4
    dma = pltpu.SemaphoreType.DMA
    scratch = {
        'part': pltpu.VMEM((side, side, rows, width), BF16),
        'gat': pltpu.VMEM((side, side, rows, width), BF16),
        'load': dma((chips,)),
        'full_s': dma((2 * chips,)),
        'd2d_s': dma((2 * chips,)),
        'd2d_r': dma((2 * chips,)),
    }
    if mode != 'da':
        scratch['own_s'] = dma((2 * chips,))
    for name, count in (('r1', 16), ('r2', 16), ('r3', 16), ('s1', 4), ('s2', 4), ('s3', 4)):
        scratch[name] = pltpu.VMEM((count, rows, quarter), BF16)
    for name, count in (('r1', 16), ('r2', 16), ('r3', 16), ('s1', 4), ('s2', 4), ('s3', 4), ('h1', 8), ('h2', 32), ('f1', 4), ('f2', 16)):
        scratch[name + '_s'] = dma((count,))
        scratch[name + '_r'] = dma((count,))
    if mode == 'da':
        terms = 1 + 2 * (side - 1)
        scratch['gain_own'] = pltpu.VMEM((2, width), F32)
        scratch['gain_tot'] = pltpu.VMEM((2, width), F32)
        scratch['gain_hold'] = pltpu.VMEM((2, 2, width), F32)
        scratch['gain_in'] = pltpu.VMEM((terms, 2, width), F32)
        scratch['gain_s'] = dma((terms,))
        scratch['gain_r'] = dma((terms,))
    names_scr = tuple(scratch)

    def kernel(part_ref, *rest):
        refs = dict(zip(names_in, rest))
        rest = rest[len(names_in):]
        out_refs = dict(zip(names_out, rest))
        scr = dict(zip(names_scr, rest[len(names_out):]))
        sum_rows_gather(mode, side, part_ref, refs, out_refs, scr)

    results = pl.pallas_call(
        kernel,
        name='sum_rows_gather_' + mode,
        out_shape=[outs[name][0] for name in names_out],
        in_specs=[any_spec] + [vmem_spec] * len(names_in),
        out_specs=[outs[name][1] for name in names_out],
        scratch_shapes=[scratch[name] for name in names_scr],
        compiler_params=pltpu.CompilerParams(collective_id=collective_id, has_side_effects=True, vmem_limit_bytes=40 * 2 ** 20),
        cost_estimate=pl.CostEstimate(flops=400_000_000, bytes_accessed=40_000_000, transcendentals=0),
    )(part, *row_args)
    results = dict(zip(names_out, results))
    results['full'] = results['full'].reshape(2, seq, width)
    if 'own' in results:
        results['own'] = results['own'].reshape(seq, width)
    return results


def solution(mesh):
    tp_size = mesh.shape['tp']
    chips = tp_size // 2
    side = math.isqrt(chips)
    swap_pairs = [(index, index ^ 1) for index in range(tp_size)]

    def device_step(hidden, seg_ids, grad_out, gain_attn, gain_mlp, w_q, w_k, w_v, w_o, w_gate, w_up, w_down):
        seq_len, width = hidden.shape[1:]
        hidden_loc = w_gate.shape[1]
        kv_heads = w_k.shape[1] // HEAD_DIM
        per_kv = tp_size // kv_heads
        rows = seq_len // chips
        tp_idx = lax.axis_index('tp')
        core = tp_idx % 2
        chip = tp_idx // 2
        kv_col = (tp_idx // per_kv) * HEAD_DIM
        scale = HEAD_DIM ** -0.5

        def swap(value):
            return lax.ppermute(value, 'tp', swap_pairs)

        def in_order(mine, other):
            return lax.optimization_barrier(jnp.where(core == 0, jnp.stack([mine, other]), jnp.stack([other, mine])))

        def own_rows(value):
            return lax.dynamic_slice_in_dim(value, chip * rows, rows, axis=0)

        gain_attn_row = gain_attn[None, :]
        gain_mlp_row = gain_mlp[None, :]
        x_own = lax.dynamic_index_in_dim(hidden, core, 0, keepdims=False)
        dy_own = lax.dynamic_index_in_dim(grad_out, core, 0, keepdims=False)
        seg_own = lax.dynamic_index_in_dim(seg_ids, core, 0, keepdims=False)

        w_q_2 = swap(w_q)
        w_o_2 = swap(w_o)
        w_gate_2 = swap(w_gate)
        w_up_2 = swap(w_up)
        w_down_2 = swap(w_down)
        w_k_loc = lax.dynamic_slice_in_dim(w_k, kv_col, HEAD_DIM, axis=1)
        w_v_loc = lax.dynamic_slice_in_dim(w_v, kv_col, HEAD_DIM, axis=1)
        w_in = jnp.concatenate([w_q, w_q_2, w_k_loc, w_v_loc], axis=1)
        w_out = jnp.concatenate([w_o, w_o_2], axis=0)

        def rms_forward(x_in):
            x_float = x_in.astype(F32)
            inv_rms = lax.rsqrt(jnp.mean(x_float * x_float, axis=-1, keepdims=True) + EPS)
            return (x_float * inv_rms * gain_attn).astype(BF16)

        normed_own = rms_forward(x_own)
        qkv = dot(normed_own, w_in, ((1,), (0,))).astype(BF16)
        queries = qkv[:, :2 * HEAD_DIM].reshape(seq_len, 2, HEAD_DIM)
        keys = qkv[:, 2 * HEAD_DIM:3 * HEAD_DIM]
        values = qkv[:, 3 * HEAD_DIM:]
        positions = jnp.arange(seq_len)
        allowed = (positions[:, None] >= positions[None, :]) & (seg_own[:, None] == seg_own[None, :])
        scores = jnp.einsum('qhd,kd->hqk', queries, keys, preferred_element_type=F32) * scale
        probs = jax.nn.softmax(jnp.where(allowed[None], scores, -1e30), axis=-1)
        probs_b = probs.astype(BF16)
        ctx = jnp.einsum('hqk,kd->qhd', probs_b, values, preferred_element_type=F32).astype(BF16).reshape(seq_len, 2 * HEAD_DIM)
        ctx_full = in_order(ctx[:, :HEAD_DIM], swap(ctx[:, HEAD_DIM:]))
        attn_part = dot(ctx, w_out, ((1,), (0,))).astype(BF16)
        x_rows = own_rows(x_own)
        dy_rows = own_rows(dy_own)
        first = reduce_gather('o', side, 1, attn_part, x_rows, gain_mlp_row)
        mixed_own, mixed_full, h_rows = first['own'], first['full'], first['h_rows']

        acts, grads_gate, grads_up = [], [], []
        for gate_w, up_w, down_w in ((w_gate, w_up, w_down), (w_gate_2, w_up_2, w_down_2)):
            gate = dot(mixed_own, gate_w, ((1,), (0,)))
            upper = dot(mixed_own, up_w, ((1,), (0,)))
            grad_act = dot(dy_own, down_w, ((1,), (1,)))
            sigmoid_g = jax.nn.sigmoid(gate)
            silu_g = gate * sigmoid_g
            acts.append((silu_g * upper).astype(BF16))
            grads_gate.append((grad_act * upper * sigmoid_g * (1.0 + gate * (1.0 - sigmoid_g))).astype(BF16))
            grads_up.append((grad_act * silu_g).astype(BF16))
        mixed_part = (dot(grads_gate[0], w_gate, ((1,), (1,))) + dot(grads_up[0], w_up, ((1,), (1,)))
                      + dot(grads_gate[1], w_gate_2, ((1,), (1,))) + dot(grads_up[1], w_up_2, ((1,), (1,)))).astype(BF16)
        act_full = in_order(acts[0], swap(acts[1]))
        gate_full = in_order(grads_gate[0], swap(grads_gate[1]))
        up_full = in_order(grads_up[0], swap(grads_up[1]))

        mlp_part = jnp.einsum('bsf,fd->bsd', act_full, w_down, preferred_element_type=F32).astype(BF16).reshape(2 * seq_len, width)
        mlp_rows = lax.psum_scatter(mlp_part, 'tp', scatter_dimension=0, tiled=True)
        h_there = lax.ppermute(h_rows, 'tp', [(index, (index % 2) * chips + index // 2) for index in range(tp_size)])
        y_rows = (h_there.astype(F32) + mlp_rows.astype(F32)).astype(BF16)
        y_out = lax.all_gather(y_rows, 'tp', axis=0, tiled=True).reshape(2, seq_len, width)

        second = reduce_gather('dm', side, 2, mixed_part, h_rows, dy_rows, gain_mlp_row)
        resid_own, resid_full, resid_rows, gain_mlp_part = second['own'], second['full'], second['d_rows'], second['gain']

        grad_ctx = dot(resid_own, w_out, ((1,), (1,))).astype(BF16).reshape(seq_len, 2, HEAD_DIM)
        grad_probs = jnp.einsum('qhd,kd->hqk', grad_ctx, values, preferred_element_type=F32)
        grad_v = jnp.einsum('hqk,qhd->kd', probs_b, grad_ctx, preferred_element_type=F32).astype(BF16)
        grad_scores = (probs * (grad_probs - jnp.sum(grad_probs * probs, axis=-1, keepdims=True)) * scale).astype(BF16)
        grad_q = jnp.einsum('hqk,kd->qhd', grad_scores, keys, preferred_element_type=F32).astype(BF16).reshape(seq_len, 2 * HEAD_DIM)
        grad_k = jnp.einsum('hqk,qhd->kd', grad_scores, queries, preferred_element_type=F32).astype(BF16)
        grad_q_full = in_order(grad_q[:, :HEAD_DIM], swap(grad_q[:, HEAD_DIM:]))

        share = per_kv // 2
        grad_kv = jnp.concatenate([grad_k, grad_v], axis=1).reshape(share, seq_len // share, 2 * HEAD_DIM)
        place = chip % share
        kv_sum = lax.dynamic_index_in_dim(grad_kv, place, 0, keepdims=False).astype(F32)
        for step in range(1, share):
            to_send = lax.dynamic_index_in_dim(grad_kv, (place + step) % share, 0, keepdims=False)
            moves = [(index, (index // per_kv) * per_kv + (index % per_kv + 2 * step) % per_kv) for index in range(tp_size)]
            kv_sum = kv_sum + lax.ppermute(to_send, 'tp', moves).astype(F32)
        kv_all = lax.all_gather(kv_sum.astype(BF16), 'tp', axis=0, tiled=False)
        kv_all = kv_all.reshape(kv_heads, share, 2, seq_len // share, 2 * HEAD_DIM).transpose(2, 1, 3, 0, 4).reshape(2, seq_len, kv_heads, 2 * HEAD_DIM)
        grad_k_all = kv_all[..., :HEAD_DIM].reshape(2, seq_len, kv_heads * HEAD_DIM)
        grad_v_all = kv_all[..., HEAD_DIM:].reshape(2, seq_len, kv_heads * HEAD_DIM)

        normed_part = dot(jnp.concatenate([grad_q, grad_k, grad_v], axis=1), w_in, ((1,), (1,))).astype(BF16)
        third = reduce_gather('da', side, 3, normed_part, x_rows, resid_rows, gain_attn_row, gain_mlp_part)
        grad_in, gain_grads = third['full'], third['gain']

        def weight_grad(lhs, rhs):
            return jnp.einsum('bsd,bse->de', lhs, rhs, preferred_element_type=F32)

        normed_full = rms_forward(hidden)
        grad_w_down = weight_grad(act_full, grad_out)
        grad_w_gate = weight_grad(mixed_full, gate_full)
        grad_w_up = weight_grad(mixed_full, up_full)
        grad_w_o = weight_grad(ctx_full, resid_full)
        grad_w_q = weight_grad(normed_full, grad_q_full)
        grad_w_k = weight_grad(normed_full, grad_k_all)
        grad_w_v = weight_grad(normed_full, grad_v_all)
        return (y_out, grad_in, gain_grads[1], gain_grads[0], grad_w_q, grad_w_k, grad_w_v, grad_w_o, grad_w_gate, grad_w_up, grad_w_down)

    spec_act = P('data', None, None)
    spec_rows = P('data', None)
    spec_gain = P(None)
    spec_cols = P(None, 'tp')
    spec_tprows = P('tp', None)
    spec_whole = P(None, None)
    spec_stack = P(('data', 'tp'), None)
    in_specs = (spec_act, spec_rows, spec_act, spec_gain, spec_gain, spec_cols, spec_whole, spec_whole, spec_tprows, spec_cols, spec_cols, spec_tprows)
    out_specs = (spec_act, spec_act, P('data'), P('data'), P('data', 'tp'), spec_rows, spec_rows, spec_stack, P('data', 'tp'), P('data', 'tp'), spec_stack)
    return jax.shard_map(device_step, mesh=mesh, in_specs=in_specs, out_specs=out_specs, check_vma=False)
```

```python
import functools
import math
import jax
import jax.numpy as jnp
from jax import lax
from jax.experimental import pallas as pl
from jax.experimental.pallas import tpu as pltpu
from jax.sharding import PartitionSpec as P

HEAD_DIM = 128
EPS = 1e-5
MESH = pl.DeviceIdType.MESH
F32 = jnp.float32
BF16 = jnp.bfloat16
MIB = 2 ** 20
ANY = pl.BlockSpec(memory_space=pl.ANY)
VMEM = pl.BlockSpec(memory_space=pltpu.VMEM)


def dot(lhs, rhs, dims):
    return lax.dot_general(lhs, rhs, (dims, ((), ())), preferred_element_type=F32)


NN = ((1,), (0,))
NT = ((1,), (1,))


SIGNS = (1, -1)


class Colour:
    def __init__(self, index, first, second):
        self.index, self.first, self.second = index, first, second


class Torus:
    def __init__(self, side):
        self.side = side
        tp_idx = lax.axis_index('tp')
        self.core = lax.rem(tp_idx, 2)
        self.chip = lax.div(tp_idx, 2)
        self.x = lax.rem(self.chip, side)
        self.y = lax.div(self.chip, side)
        self.partner = {'tp': self.chip * 2 + (1 - self.core)}
        self.colours = (Colour(0, self.x, self.y), Colour(1, self.y, self.x))
        self.pending = []

    def wrap(self, pos):
        return lax.rem(pos + 2 * self.side, self.side)

    def at_chip(self, y_at, x_at):
        return {'tp': (y_at * self.side + x_at) * 2 + self.core}

    def block(self, col, second, first):
        return (second, first) if col.index == 0 else (first, second)

    def peer1(self, col, shift):
        return self.at_chip(*self.block(col, col.second, self.wrap(col.first + shift)))

    def peer2(self, col, shift):
        return self.at_chip(*self.block(col, self.wrap(col.second + shift), col.first))

    def signal_all(self):
        barrier = pltpu.get_barrier_semaphore()
        peers = [self.partner]
        peers += [self.at_chip(self.y, self.wrap(self.x + shift)) for shift in SIGNS]
        peers += [self.at_chip(self.wrap(self.y + shift), self.x) for shift in SIGNS]
        for peer in peers:
            pl.semaphore_signal(barrier, inc=1, device_id=peer, device_id_type=MESH)
        return lambda: pl.semaphore_wait(barrier, len(peers))

    def send(self, src, dst, sems, index, device):
        copy = pltpu.make_async_remote_copy(src, dst, sems[0].at[index], sems[1].at[index], device_id=device, device_id_type=MESH)
        copy.start()
        self.pending.append(copy)

    def arrive(self, dst, sems, index):
        pltpu.make_async_remote_copy(dst, dst, sems[0].at[index], sems[1].at[index], device_id=self.partner, device_id_type=MESH).wait_recv()

    def drain(self):
        for copy in self.pending:
            copy.wait_send()


RS_BUFFERS = (('r1', 16), ('r2', 16), ('r3', 16), ('s1', 4), ('s2', 4), ('s3', 4))
AG_SEMS = (('h1', 8), ('h2', 32), ('f1', 4), ('f2', 16))


class ReduceScatter:
    SHIFTS = (2, 1, 3, 0)

    def __init__(self, torus, part, scr, name):
        self.torus, self.part, self.scr, self.name = torus, part, scr, name
        self.quarter = part.shape[3] // 4

    def buf(self, kind, index):
        return self.scr[self.name + kind].at[index]

    def sems(self, kind):
        return self.scr[self.name + kind + '_s'], self.scr[self.name + kind + '_r']

    def cols(self, col, half):
        return pl.ds((col.index * 2 + half) * self.quarter, self.quarter)

    def piece(self, where, at_cols):
        return self.part.at[(*where, slice(None), at_cols)]

    def send(self, where, at_cols, kind, index, peer):
        self.torus.send(self.piece(where, at_cols), self.buf(kind, index), self.sems(kind), index, peer)

    def add(self, where, at_cols, *kinds):
        total = self.part[(*where, slice(None), at_cols)].astype(F32)
        for kind, index in kinds:
            self.torus.arrive(self.buf(kind, index), self.sems(kind), index)
            total = total + self.buf(kind, index)[...].astype(F32)
        self.part[(*where, slice(None), at_cols)] = total.astype(BF16)

    def each(self, step):
        wrap = self.torus.wrap
        for col in self.torus.colours:
            second = wrap(col.second + self.SHIFTS[step])
            for way, sign in enumerate(SIGNS):
                yield col, second, way, sign, (col.index * 2 + way) * 4 + step

    def far(self, step):
        for col, second, way, sign, index in self.each(step):
            where = self.torus.block(col, second, self.torus.wrap(col.first + 2))
            self.send(where, self.cols(col, way), 'r1', index, self.torus.peer1(col, sign))

    def near(self, step):
        for col, second, way, sign, index in self.each(step):
            where = self.torus.block(col, second, self.torus.wrap(col.first + sign))
            self.send(where, self.cols(col, 1 - way), 'r2', index, self.torus.peer1(col, sign))

    def relay(self, step):
        for col, second, way, sign, index in self.each(step):
            where = self.torus.block(col, second, self.torus.wrap(col.first + sign))
            self.add(where, self.cols(col, way), ('r1', index))
            self.send(where, self.cols(col, way), 'r3', index, self.torus.peer1(col, sign))

    def end(self, step):
        for col, second, way, sign, index in self.each(step):
            where = self.torus.block(col, second, col.first)
            other = (col.index * 2 + 1 - way) * 4 + step
            self.add(where, self.cols(col, way), ('r2', other), ('r3', index))

    def far2(self):
        for col in self.torus.colours:
            for way, sign in enumerate(SIGNS):
                where = self.torus.block(col, self.torus.wrap(col.second + 2), col.first)
                self.send(where, self.cols(col, way), 's1', col.index * 2 + way, self.torus.peer2(col, sign))

    def near2(self, way):
        for col in self.torus.colours:
            where = self.torus.block(col, self.torus.wrap(col.second + SIGNS[way]), col.first)
            self.send(where, self.cols(col, 1 - way), 's2', col.index * 2 + way, self.torus.peer2(col, SIGNS[way]))

    def relay2(self, way):
        for col in self.torus.colours:
            index = col.index * 2 + way
            where = self.torus.block(col, self.torus.wrap(col.second + SIGNS[way]), col.first)
            self.add(where, self.cols(col, way), ('s1', index))
            self.send(where, self.cols(col, way), 's3', index, self.torus.peer2(col, SIGNS[way]))

    def end2(self):
        for col in self.torus.colours:
            where = self.torus.block(col, col.second, col.first)
            for way in range(2):
                self.add(where, self.cols(col, way), ('s2', col.index * 2 + 1 - way), ('s3', col.index * 2 + way))

    def steps(self, fill):
        call = functools.partial
        return [call(fill, 2), call(self.far, 0), call(self.far, 1), call(fill, 1), call(fill, 3),
                call(self.near, 0), call(self.relay, 0), call(self.near, 1), call(self.far, 2), call(self.relay, 1),
                call(fill, 0), call(self.near, 2), call(self.far, 3), call(self.end, 0), call(self.far2),
                call(self.relay, 2), call(self.near, 3), call(self.end, 1), call(self.near2, 0), call(self.relay2, 0),
                call(self.relay, 3), call(self.end, 2), call(self.near2, 1), call(self.relay2, 1), call(self.end, 3),
                call(self.end2)]


class AllGather:
    def __init__(self, torus, gat, scr, name, by_rows, keep):
        self.torus, self.gat, self.scr, self.name, self.by_rows, self.keep_piece = torus, gat, scr, name, by_rows, keep
        self.quarter = gat.shape[2 if by_rows else 3] // 4
        self.back = (0, torus.side - 1, 1, 2)

    def sems(self, kind):
        return self.scr[self.name + kind + '_s'], self.scr[self.name + kind + '_r']

    def piece(self, ref, where, first, count):
        at = pl.ds(first * self.quarter, count * self.quarter)
        return ref.at[(*where, at, slice(None))] if self.by_rows else ref.at[(*where, slice(None), at)]

    def half(self, col, where, half):
        return self.piece(self.gat, where, col.index * 2 + half, 1)

    def own2(self, turn):
        for col in self.torus.colours:
            where = self.torus.block(col, col.second, col.first)
            for way, sign in enumerate(SIGNS):
                at = self.half(col, where, way if turn == 0 else 1 - way)
                self.torus.send(at, at, self.sems('h1'), (col.index * 2 + way) * 2 + turn, self.torus.peer2(col, sign))

    def send1(self, step, turn):
        for col in self.torus.colours:
            where = self.torus.block(col, self.torus.wrap(col.second + self.back[step]), col.first)
            for way, sign in enumerate(SIGNS):
                at = self.half(col, where, way if turn == 0 else 1 - way)
                self.torus.send(at, at, self.sems('h2'), ((col.index * 2 + way) * 4 + step) * 2 + turn, self.torus.peer1(col, sign))

    def arrive2(self, way, turn):
        sign = SIGNS[way]
        for col in self.torus.colours:
            where = self.torus.block(col, self.torus.wrap(col.second - sign), col.first)
            at = self.half(col, where, way if turn == 0 else 1 - way)
            self.torus.arrive(at, self.sems('h1'), (col.index * 2 + way) * 2 + turn)
            if turn == 0:
                self.torus.send(at, at, self.sems('f1'), col.index * 2 + way, self.torus.peer2(col, sign))

    def relayed2(self):
        for col in self.torus.colours:
            where = self.torus.block(col, self.torus.wrap(col.second + 2), col.first)
            for way in range(2):
                self.torus.arrive(self.half(col, where, way), self.sems('f1'), col.index * 2 + way)

    def arrive1(self, step, turn):
        for col in self.torus.colours:
            second = self.torus.wrap(col.second + self.back[step])
            for way, sign in enumerate(SIGNS):
                where = self.torus.block(col, second, self.torus.wrap(col.first - sign))
                at = self.half(col, where, way if turn == 0 else 1 - way)
                self.torus.arrive(at, self.sems('h2'), ((col.index * 2 + way) * 4 + step) * 2 + turn)
                if turn == 0:
                    self.torus.send(at, at, self.sems('f2'), (col.index * 2 + way) * 4 + step, self.torus.peer1(col, sign))

    def relayed1(self, step):
        for col in self.torus.colours:
            second = self.torus.wrap(col.second + self.back[step])
            for way in range(2):
                where = self.torus.block(col, second, self.torus.wrap(col.first + 2))
                self.torus.arrive(self.half(col, where, way), self.sems('f2'), (col.index * 2 + way) * 4 + step)

    def keep(self, step, firsts):
        for col in self.torus.colours:
            for shift in firsts:
                where = self.torus.block(col, self.torus.wrap(col.second + self.back[step]), self.torus.wrap(col.first + shift))
                slot = (col.index * self.torus.side + where[0]) * self.torus.side + where[1]
                self.keep_piece(slot, lambda ref, where=where, col=col: self.piece(ref, where, col.index * 2, 2))

    def steps(self):
        call = functools.partial
        beside = (1, self.torus.side - 1)
        return [call(self.own2, 0), call(self.send1, 0, 0), call(self.own2, 1), call(self.send1, 0, 1), call(self.keep, 0, (0,)),
                call(self.arrive2, 0, 0), call(self.arrive2, 1, 0), call(self.arrive2, 0, 1), call(self.send1, 1, 0), call(self.send1, 1, 1),
                call(self.arrive2, 1, 1), call(self.send1, 2, 0), call(self.send1, 2, 1), call(self.keep, 1, (0,)), call(self.keep, 2, (0,)),
                call(self.arrive1, 0, 0), call(self.relayed2), call(self.send1, 3, 0), call(self.send1, 3, 1), call(self.keep, 3, (0,)),
                call(self.arrive1, 0, 1), call(self.keep, 0, beside), call(self.arrive1, 1, 0), call(self.arrive1, 2, 0),
                call(self.relayed1, 0), call(self.keep, 0, (2,)), call(self.arrive1, 1, 1), call(self.keep, 1, beside),
                call(self.arrive1, 2, 1), call(self.keep, 2, beside), call(self.arrive1, 3, 0), call(self.relayed1, 1), call(self.keep, 1, (2,)),
                call(self.relayed1, 2), call(self.keep, 2, (2,)), call(self.arrive1, 3, 1), call(self.keep, 3, beside),
                call(self.relayed1, 3), call(self.keep, 3, (2,))]


class Store:
    def __init__(self, torus, full, scr, name, own=None):
        self.torus, self.full, self.scr, self.name, self.own = torus, full, scr, name, own
        self.stores = []

    def sem(self, kind, slot):
        return self.scr[self.name + kind].at[slot]

    def keep(self, gat):
        def put(slot, piece):
            pairs = [('full_s', self.full.at[self.torus.core])]
            if self.own is not None:
                pairs.append(('own_s', self.own))
            for kind, ref in pairs:
                store = pltpu.make_async_copy(piece(gat), piece(ref), self.sem(kind, slot))
                store.start()
                self.stores.append(store)
            sems = self.scr[self.name + 'd2d_s'], self.scr[self.name + 'd2d_r']
            self.torus.send(piece(gat), piece(self.full.at[self.torus.core]), sems, slot, self.torus.partner)
        return put

    def drain(self, gather):
        for store in self.stores:
            store.wait()
        side = self.torus.side
        for colour in range(2):
            for y_at in range(side):
                for x_at in range(side):
                    target = gather.piece(self.full.at[1 - self.torus.core], (y_at, x_at), colour * 2, 2)
                    sems = self.scr[self.name + 'd2d_s'], self.scr[self.name + 'd2d_r']
                    self.torus.arrive(target, sems, (colour * side + y_at) * side + x_at)


def rs_scratch(name, side, rows, width):
    dma = pltpu.SemaphoreType.DMA
    scratch = {name + 'part': pltpu.VMEM((side, side, rows, width), BF16)}
    for kind, count in RS_BUFFERS:
        scratch[name + kind] = pltpu.VMEM((count, rows, width // 4), BF16)
        scratch[name + kind + '_s'] = dma((count,))
        scratch[name + kind + '_r'] = dma((count,))
    return scratch


def ag_scratch(name, side, rows, width, own):
    dma = pltpu.SemaphoreType.DMA
    scratch = {name + 'gat': pltpu.VMEM((side, side, rows, width), BF16)}
    for kind, count in AG_SEMS:
        scratch[name + kind + '_s'] = dma((count,))
        scratch[name + kind + '_r'] = dma((count,))
    for kind in ('full_s', 'd2d_s', 'd2d_r') + (('own_s',) if own else ()):
        scratch[name + kind] = dma((2 * side * side,))
    return scratch


class Weights:
    def __init__(self, refs, buf, sem, by_rows):
        self.refs, self.buf, self.sem, self.by_rows = refs, buf, sem, by_rows
        self.copies = [[], []]

    def start(self):
        for colour in range(2):
            for index, ref in enumerate(self.refs):
                if self.by_rows:
                    half, depth = ref.shape[0] // 2, ref.shape[1]
                    rows, cols = pl.ds(colour * half, half), pl.ds(index * depth, depth)
                    copy = pltpu.make_async_copy(ref.at[rows, :], self.buf.at[rows, cols], self.sem.at[colour, index])
                else:
                    half, depth = ref.shape[1] // 2, ref.shape[0]
                    rows, cols = pl.ds(index * depth, depth), pl.ds(colour * half, half)
                    copy = pltpu.make_async_copy(ref.at[:, cols], self.buf.at[rows, cols], self.sem.at[colour, index])
                copy.start()
                self.copies[colour].append(copy)

    def wait(self, colour):
        for copy in self.copies[colour]:
            copy.wait()
        self.copies[colour] = []


def fill_partial(torus, part, lhs, weights):
    rows, width = part.shape[2:]
    tile = min(512, width // 2)

    def fill(shift):
        for col in torus.colours:
            weights.wait(col.index)
            first = torus.wrap(col.first + shift)
            left = []
            for ref in lhs:
                depth = ref.shape[3]
                value = ref[:, first] if col.index == 0 else ref[first]
                left.append((value.reshape(torus.side * rows, depth), depth))

            def body(step, carry, col=col, first=first, left=left):
                at = pl.ds(pl.multiple_of(col.index * (width // 2) + step * tile, tile), tile)
                total = None
                base = 0
                for value, depth in left:
                    if weights.by_rows:
                        term = dot(value, weights.buf[at, base:base + depth], NT)
                    else:
                        term = dot(value, weights.buf[base:base + depth, at], NN)
                    total = term if total is None else total + term
                    base += depth
                total = total.astype(BF16).reshape(torus.side, rows, tile)
                if col.index == 0:
                    part[:, first, :, at] = total
                else:
                    part[first, :, :, at] = total
                return carry

            lax.fori_loop(0, (width // 2) // tile, body, 0)

    return fill


def run(*lists):
    keyed = []
    for order, steps in enumerate(lists):
        keyed += [((index + 0.5) / len(steps), order, step) for index, step in enumerate(steps)]
    for _, _, step in sorted(keyed, key=lambda item: item[:2]):
        step()


def swap_scratch(count):
    return {'swap_s': pltpu.SemaphoreType.DMA((count,)), 'swap_r': pltpu.SemaphoreType.DMA((count,))}


def swap_start(torus, scr, pairs):
    for index, (src, dst) in enumerate(pairs):
        torus.send(src, dst, (scr['swap_s'], scr['swap_r']), index, torus.partner)


def swap_end(torus, scr, pairs):
    for index, (_, dst) in enumerate(pairs):
        torus.arrive(dst, (scr['swap_s'], scr['swap_r']), index)


def row_tiles(rows):
    return [pl.ds(start, 16) for start in range(0, rows, 16)]


def rms_back(z_in, gain, grad):
    inv = lax.rsqrt(jnp.mean(z_in * z_in, axis=-1, keepdims=True) + EPS)
    normed = z_in * inv
    scaled = grad * gain
    back = inv * (scaled - normed * jnp.mean(scaled * normed, axis=-1, keepdims=True))
    return back, jnp.sum(grad * normed, axis=0, keepdims=True)


def call_kernel(name, body, ins, outs, scratch, vmem_mib, flops, collective_id=None):
    names_in, names_out, names_scr = tuple(ins), tuple(outs), tuple(scratch)

    def kernel(*refs):
        refs = list(refs)
        take = lambda names: {key: refs.pop(0) for key in names}
        body(take(names_in), take(names_out), take(names_scr))

    results = pl.pallas_call(
        kernel,
        name=name,
        out_shape=[outs[key][0] for key in names_out],
        in_specs=[ins[key][1] for key in names_in],
        out_specs=[outs[key][1] for key in names_out],
        scratch_shapes=[scratch[key] for key in names_scr],
        compiler_params=pltpu.CompilerParams(collective_id=collective_id, has_side_effects=collective_id is not None, vmem_limit_bytes=int(vmem_mib * MIB)),
        cost_estimate=pl.CostEstimate(flops=int(flops), bytes_accessed=40_000_000, transcendentals=0),
    )(*[ins[key][0] for key in names_in])
    return dict(zip(names_out, results))


def shape(dims, dtype=BF16):
    return jax.ShapeDtypeStruct(dims, dtype)


def sum_attention(side, ctx, normed, w_out, x_rows, gain):
    seq, depth = ctx.shape
    width = gain.shape[1]
    rows = seq // (side * side)
    block = (side, side, rows, width)

    def body(ins, outs, scr):
        torus = Torus(side)
        weights = Weights([ins['w_a'], ins['w_b']], scr['w'], scr['w_s'], False)
        weights.start()
        wait = torus.signal_all()
        part = scr['part']
        fill = fill_partial(torus, part, [ins['ctx']], weights)
        scatter = ReduceScatter(torus, part, scr, '')
        steps = scatter.steps(fill)
        steps[0]()
        wait()
        swaps = [(ins['ctx'].at[:, :, :, pl.ds(depth // 2, depth // 2)], outs['ctx_other']), (ins['normed'], outs['normed_other'])]
        swap_start(torus, scr, swaps)
        run(steps[1:])
        gat = scr['gat']
        own = (torus.y, torus.x)
        for at in row_tiles(rows):
            resid = (ins['x_rows'][at, :].astype(F32) + part[(*own, at, slice(None))].astype(F32)).astype(BF16)
            outs['h_rows'][at, :] = resid
            z_in = resid.astype(F32)
            inv = lax.rsqrt(jnp.mean(z_in * z_in, axis=-1, keepdims=True) + EPS)
            gat[(*own, at, slice(None))] = (z_in * inv * ins['gain'][...]).astype(BF16)
        store = Store(torus, outs['full'], scr, '')
        gather = AllGather(torus, gat, scr, '', False, store.keep(gat))
        run(gather.steps())
        store.drain(gather)
        swap_end(torus, scr, swaps)
        torus.drain()

    ins = {'ctx': (ctx.reshape(side, side, rows, depth), VMEM), 'w_a': (w_out[0], ANY), 'w_b': (w_out[1], ANY), 'x_rows': (x_rows, VMEM), 'gain': (gain, VMEM), 'normed': (normed, ANY)}
    outs = {'full': (shape((2, *block)), ANY), 'h_rows': (shape((rows, width)), VMEM), 'ctx_other': (shape((side, side, rows, depth // 2)), ANY), 'normed_other': (shape((seq, width)), ANY)}
    scratch = {**rs_scratch('', side, rows, width), **ag_scratch('', side, rows, width, False), 'w': pltpu.VMEM((depth, width), BF16), 'w_s': pltpu.SemaphoreType.DMA((2, 2)), **swap_scratch(2)}
    return call_kernel('sum_attention', body, ins, outs, scratch, 36, 4e8, 1)


def sum_mlp(side, grads, acts, w_gates, w_ups, w_downs, h_rows, dy_rows, gain):
    seq, depth = grads[0].shape
    width = gain.shape[1]
    rows = seq // (side * side)
    block = (side, side, rows, width)

    def body(ins, outs, scr):
        torus = Torus(side)
        weights = Weights([ins[f'w_{index}'] for index in range(4)], scr['w'], scr['w_s'], False)
        weights.start()
        weights_p = Weights([ins[f'wd_{index}'] for index in range(2)], scr['wd'], scr['wd_s'], False)
        weights_p.start()
        wait = torus.signal_all()
        scatter = ReduceScatter(torus, scr['part'], scr, '')
        steps = scatter.steps(fill_partial(torus, scr['part'], [ins[f'g_{index}'] for index in range(4)], weights))
        scatter_p = ReduceScatter(torus, scr['p_part'], scr, 'p_')
        fill_p = fill_partial(torus, scr['p_part'], [ins[f'a_{index}'] for index in range(2)], weights_p)
        steps_p = scatter_p.steps(fill_p)
        steps[0]()
        wait()
        swaps = [(ins['g_2'], outs['gate_other']), (ins['g_3'], outs['up_other']), (ins['a_1'], outs['act_other'])]
        swap_start(torus, scr, swaps)
        early = [steps_p[0], steps_p[3], steps_p[4], steps_p[10]]
        rest_p = [step for index, step in enumerate(steps_p) if index not in (0, 3, 4, 10)]
        run(steps[1:22], early)
        for step in rest_p[:3]:
            step()
        run(steps[22:])
        own = (torus.y, torus.x)
        gain_total = jnp.zeros((1, width), F32)
        gat = scr['gat']
        for at in row_tiles(rows):
            back, gain_part = rms_back(ins['h_rows'][at, :].astype(F32), ins['gain'][...], scr['part'][(*own, at, slice(None))].astype(F32))
            gain_total = gain_total + gain_part
            total = ins['dy_rows'][at, :].astype(F32) + back
            outs['d_rows'][at, :] = total
            gat[(*own, at, slice(None))] = total.astype(BF16)
        outs['gain'][...] = gain_total
        store = Store(torus, outs['full'], scr, '', outs['own'])
        gather = AllGather(torus, gat, scr, '', False, store.keep(gat))
        run(gather.steps(), rest_p[3:])
        for at in row_tiles(rows):
            outs['y_rows'][at, :] = (ins['h_rows'][at, :].astype(F32) + scr['p_part'][(*own, at, slice(None))].astype(F32)).astype(BF16)
        store.drain(gather)
        swap_end(torus, scr, swaps)
        torus.drain()

    ins = {}
    for index, grad in enumerate(grads):
        ins[f'g_{index}'] = (grad.reshape(side, side, rows, depth), VMEM)
    for index, act in enumerate(acts):
        ins[f'a_{index}'] = (act.reshape(side, side, rows, depth), VMEM)
    for index, weight in enumerate((w_gates[0], w_ups[0], w_gates[1], w_ups[1])):
        ins[f'w_{index}'] = (weight, ANY)
    for index, weight in enumerate(w_downs):
        ins[f'wd_{index}'] = (weight, ANY)
    ins.update(h_rows=(h_rows, VMEM), dy_rows=(dy_rows, VMEM), gain=(gain, VMEM))
    outs = {'full': (shape((2, *block)), ANY), 'own': (shape(block), ANY), 'd_rows': (shape((rows, width), F32), VMEM), 'gain': (shape((1, width), F32), VMEM), 'y_rows': (shape((rows, width)), VMEM)}
    outs.update({key: (shape((side, side, rows, depth)), ANY) for key in ('gate_other', 'up_other', 'act_other')})
    scratch = {**rs_scratch('', side, rows, width), **rs_scratch('p_', side, rows, width), **ag_scratch('', side, rows, width, True),
               'w': pltpu.VMEM((4 * depth, width), BF16), 'w_s': pltpu.SemaphoreType.DMA((2, 4)), 'wd': pltpu.VMEM((2 * depth, width), BF16), 'wd_s': pltpu.SemaphoreType.DMA((2, 2)), **swap_scratch(3)}
    return call_kernel('sum_mlp', body, ins, outs, scratch, 60, 6e8, 2)


def sum_input(side, dqkv, w_in, dkv, x_rows, d_rows, gain, gain_mlp_part):
    seq, depth = dqkv.shape
    width = gain.shape[1]
    rows = seq // (side * side)
    tokens, pair = dkv.shape[1:]

    def body(ins, outs, scr):
        torus = Torus(side)
        weights = Weights([ins['w_in']], scr['w'], scr['w_s'], True)
        weights.start()
        wait = torus.signal_all()
        part = scr['part']
        scatter = ReduceScatter(torus, part, scr, '')
        steps = scatter.steps(fill_partial(torus, part, [ins['dqkv']], weights))
        own = (torus.y, torus.x)
        gat = scr['k_gat']
        store = Store(torus, outs['kv'], scr, 'k_')
        gather = AllGather(torus, gat, scr, 'k_', True, store.keep(gat))
        place = lax.rem(torus.x, 2)
        mate = torus.at_chip(torus.y, torus.x + 1 - 2 * place)
        mate_sems = scr['mate_s'], scr['mate_r']

        def mate_send():
            torus.send(ins['dkv'].at[1 - place], scr['mate'].at[0], mate_sems, 0, mate)

        def mate_add():
            torus.arrive(scr['mate'].at[0], mate_sems, 0)
            gat[own] = (ins['dkv'][place].astype(F32) + scr['mate'][0].astype(F32)).astype(BF16)

        steps[0]()
        wait()
        swaps = [(ins['dqkv'].at[:, :, :, pl.ds(pair // 2, pair // 2)], outs['q_other'])]
        swap_start(torus, scr, swaps)
        mate_send()
        for step in steps[1:5]:
            step()
        mate_add()
        run(steps[5:], gather.steps())
        gain_total = jnp.zeros((1, width), F32)
        for at in row_tiles(rows):
            back, gain_part = rms_back(ins['x_rows'][at, :].astype(F32), ins['gain'][...], part[(*own, at, slice(None))].astype(F32))
            gain_total = gain_total + gain_part
            outs['rows'][at, :] = (ins['d_rows'][at, :] + back).astype(BF16)
        row = lax.broadcasted_iota(jnp.int32, (16, width), 0)
        extra = jnp.zeros((16, width), F32)
        for index, value in enumerate((gain_total, ins['gain_mlp'][...])):
            for level in range(3):
                rounded = value.astype(BF16).astype(F32)
                extra = jnp.where(row == index * 3 + level, rounded, extra)
                value = value - rounded
        outs['rows'][rows:rows + 16, :] = extra.astype(BF16)
        store.drain(gather)
        swap_end(torus, scr, swaps)
        torus.drain()

    ins = {'dqkv': (dqkv.reshape(side, side, rows, depth), VMEM), 'w_in': (w_in, ANY), 'dkv': (dkv, VMEM), 'x_rows': (x_rows, VMEM), 'd_rows': (d_rows, VMEM), 'gain': (gain, VMEM), 'gain_mlp': (gain_mlp_part, VMEM)}
    outs = {'rows': (shape((rows + 16, width)), VMEM), 'kv': (shape((2, side, side, tokens, pair)), ANY), 'q_other': (shape((side, side, rows, pair // 2)), ANY)}
    dma = pltpu.SemaphoreType.DMA
    scratch = {**rs_scratch('', side, rows, width), **ag_scratch('k_', side, tokens, pair, False), 'w': pltpu.VMEM((width, depth), BF16), 'w_s': dma((2, 1)),
               'mate': pltpu.VMEM((1, tokens, pair), BF16), 'mate_s': dma((1,)), 'mate_r': dma((1,)), **swap_scratch(1)}
    return call_kernel('sum_input', body, ins, outs, scratch, 36, 3e8, 3)


def mlp_grads(mixed_full, grad_out, w_gates, w_ups, w_downs):
    seq, width = grad_out.shape[1:]
    depth = w_gates[0].shape[0]

    def body(ins, outs, scr):
        core = lax.rem(lax.axis_index('tp'), 2)
        copies = {}

        def load(key, src, dst):
            copies[key] = pltpu.make_async_copy(src, dst, scr['sem'].at[len(copies)])
            copies[key].start()

        load('m', ins['m'].at[core], scr['m'])
        load('g0', ins['g0'], scr['w'].at[0])
        load('u0', ins['u0'], scr['w'].at[1])
        load('dy', ins['dy'].at[core], scr['dy'])
        load('d0', ins['d0'], scr['w'].at[2])
        load('g1', ins['g1'], scr['w'].at[3])
        load('u1', ins['u1'], scr['w'].at[4])
        load('d1', ins['d1'], scr['w'].at[5])
        tile = min(256, seq)
        for index in range(2):
            for key in (('m', 'g0', 'u0', 'dy', 'd0') if index == 0 else ('g1', 'u1', 'd1')):
                copies[key].wait()

            def step(tile_index, carry, index=index):
                at = pl.ds(pl.multiple_of(tile_index * tile, tile), tile)
                mixed = scr['m'][at, :]
                gate = dot(mixed, scr['w'][3 * index], NT)
                upper = dot(mixed, scr['w'][3 * index + 1], NT)
                grad_act = dot(scr['dy'][at, :], scr['w'][3 * index + 2], NT)
                sigmoid_g = 1.0 / (1.0 + jnp.exp(-gate))
                silu_g = gate * sigmoid_g
                outs[f'a{index}'][at, :] = (silu_g * upper).astype(BF16)
                outs[f'dg{index}'][at, :] = (grad_act * upper * sigmoid_g * (1.0 + gate * (1.0 - sigmoid_g))).astype(BF16)
                outs[f'du{index}'][at, :] = (grad_act * silu_g).astype(BF16)
                return carry

            lax.fori_loop(0, seq // tile, step, 0)

    ins = {'m': (mixed_full, ANY), 'dy': (grad_out, ANY)}
    for index in range(2):
        ins[f'g{index}'] = (w_gates[index], ANY)
        ins[f'u{index}'] = (w_ups[index], ANY)
        ins[f'd{index}'] = (w_downs[index], ANY)
    outs = {f'{name}{index}': (shape((seq, depth)), VMEM) for index in range(2) for name in ('a', 'dg', 'du')}
    scratch = {'m': pltpu.VMEM((seq, width), BF16), 'dy': pltpu.VMEM((seq, width), BF16), 'w': pltpu.VMEM((6, depth, width), BF16), 'sem': pltpu.SemaphoreType.DMA((8,))}
    return call_kernel('mlp_grads', body, ins, outs, scratch, 58, 17e9)


def weight_grads_mlp(mixed_full, grad_out, resid_full, grads_gate, grads_up, acts, ctxs):
    seq, width = grad_out.shape[1:]
    depth, head = acts[0].shape[1], ctxs[0].shape[1]
    tile = min(512, width)

    def kernel(m_ref, dy_ref, dh_ref, *refs):
        sides = (refs[0:2], refs[2:4], refs[4:6], refs[6:8])
        out_gate, out_up, out_down, out_o, left = refs[8:]
        core = lax.rem(lax.axis_index('tp'), 2)

        @pl.when(pl.program_id(0) == 0)
        def _():
            base = 0
            for pair in sides:
                for half in range(2):
                    left[half, base:base + pair[half].shape[1], :] = pair[half][...].T
                base += pair[0].shape[1]

        def product(base, size, ref):
            return dot(left[0, base:base + size, :], ref[core], NN) + dot(left[1, base:base + size, :], ref[1 - core], NN)

        both = product(0, 2 * depth, m_ref)
        out_gate[...] = both[:depth]
        out_up[...] = both[depth:]
        out_down[...] = product(2 * depth, depth, dy_ref)
        out_o[...] = product(3 * depth, head, dh_ref)

    slab = pl.BlockSpec((2, seq, tile), lambda step: (0, 0, step))
    whole = pl.BlockSpec(memory_space=pltpu.VMEM)
    out = lambda size: pl.BlockSpec((size, tile), lambda step: (0, step))
    return pl.pallas_call(
        kernel,
        name='weight_grads_mlp',
        grid=(width // tile,),
        out_shape=[shape((depth, width), F32)] * 3 + [shape((head, width), F32)],
        in_specs=[slab] * 3 + [whole] * 8,
        out_specs=[out(depth)] * 3 + [out(head)],
        scratch_shapes=[pltpu.VMEM((2, 3 * depth + head, seq), BF16)],
        compiler_params=pltpu.CompilerParams(vmem_limit_bytes=56 * MIB),
        cost_estimate=pl.CostEstimate(flops=18_500_000_000, bytes_accessed=60_000_000, transcendentals=0),
    )(mixed_full, grad_out, resid_full, *grads_gate, *grads_up, *acts, *ctxs)


def weight_grads_qkv(normeds, kv_full, grads_q, kv_heads):
    seq, width = normeds[0].shape
    chips, tokens, pair = kv_full.shape[1:]
    head = pair // 2
    share = seq // tokens
    tile = min(256, width)
    kv_width = kv_heads * head

    def kernel(a_own, a_other, kv_ref, q_own, q_other, out_q, out_k, out_v, right, left):
        core = lax.rem(lax.axis_index('tp'), 2)

        @pl.when(pl.program_id(0) == 0)
        def _():
            for half, q_ref in enumerate((q_own, q_other)):
                right[half, :, 2 * kv_width:] = q_ref[...]
                batch = core if half == 0 else 1 - core
                for chip in range(chips):
                    at = pl.ds((chip % share) * tokens, tokens)
                    base = (chip // share) * head
                    right[half, at, base:base + head] = kv_ref[batch, chip, :, :head]
                    right[half, at, kv_width + base:kv_width + base + head] = kv_ref[batch, chip, :, head:]

        left[0] = a_own[...].T
        left[1] = a_other[...].T

        def product(base, size):
            return dot(left[0], right[0, :, base:base + size], NN) + dot(left[1], right[1, :, base:base + size], NN)

        out_k[...] = product(0, kv_width)
        out_v[...] = product(kv_width, kv_width)
        out_q[...] = product(2 * kv_width, head)

    whole = pl.BlockSpec(memory_space=pltpu.VMEM)
    slab = pl.BlockSpec((seq, tile), lambda step: (0, step))
    out = lambda size: pl.BlockSpec((tile, size), lambda step: (step, 0))
    return pl.pallas_call(
        kernel,
        name='weight_grads_qkv',
        grid=(width // tile,),
        out_shape=[shape((width, head), F32), shape((width, kv_width), F32), shape((width, kv_width), F32)],
        in_specs=[slab, slab, whole, whole, whole],
        out_specs=[out(head), out(kv_width), out(kv_width)],
        scratch_shapes=[pltpu.VMEM((2, seq, 2 * kv_width + head), BF16), pltpu.VMEM((2, tile, seq), BF16)],
        compiler_params=pltpu.CompilerParams(vmem_limit_bytes=56 * MIB),
        cost_estimate=pl.CostEstimate(flops=27_500_000_000, bytes_accessed=60_000_000, transcendentals=0),
    )(*normeds, kv_full, *grads_q)


def in_place(gathered, rows):
    blocks, _, width = gathered.shape
    slots = 8

    def kernel(src, dst, buf, in_sem, out_sem):
        def load(index):
            return pltpu.make_async_copy(src.at[index, pl.ds(0, rows), :], buf.at[index % slots], in_sem.at[index % slots])

        def store(index):
            return pltpu.make_async_copy(buf.at[index % slots], dst.at[index % 2, index // 2], out_sem.at[index % slots])

        ahead = slots // 2
        for index in range(blocks + ahead):
            if index < blocks:
                if index >= slots:
                    store(index - slots).wait()
                load(index).start()
            if index >= ahead:
                load(index - ahead).wait()
                store(index - ahead).start()
        for index in range(blocks - slots, blocks):
            store(index).wait()

    return pl.pallas_call(
        kernel,
        name='in_place',
        out_shape=shape((2, blocks // 2, rows, width)),
        in_specs=[ANY],
        out_specs=ANY,
        scratch_shapes=[pltpu.VMEM((slots, rows, width), BF16), pltpu.SemaphoreType.DMA((slots,)), pltpu.SemaphoreType.DMA((slots,))],
        compiler_params=pltpu.CompilerParams(vmem_limit_bytes=16 * MIB),
        cost_estimate=pl.CostEstimate(flops=20_000_000, bytes_accessed=25_000_000, transcendentals=0),
    )(gathered)


def solution(mesh):
    tp_size = mesh.shape['tp']
    chips = tp_size // 2
    side = math.isqrt(chips)
    swap_pairs = [(index, index ^ 1) for index in range(tp_size)]

    def device_step(hidden, seg_ids, grad_out, gain_attn, gain_mlp, w_q, w_k, w_v, w_o, w_gate, w_up, w_down):
        seq_len, width = hidden.shape[1:]
        kv_heads = w_k.shape[1] // HEAD_DIM
        per_kv = tp_size // kv_heads
        share = per_kv // 2
        rows = seq_len // chips
        tp_idx = lax.axis_index('tp')
        core = tp_idx % 2
        chip = tp_idx // 2
        kv_col = (tp_idx // per_kv) * HEAD_DIM
        scale = HEAD_DIM ** -0.5

        def swap(value):
            return lax.ppermute(value, 'tp', swap_pairs)

        def own_rows(value):
            return lax.dynamic_slice_in_dim(value, chip * rows, rows, axis=0)

        gain_attn_row = gain_attn[None, :]
        gain_mlp_row = gain_mlp[None, :]
        x_own = lax.dynamic_index_in_dim(hidden, core, 0, keepdims=False)
        dy_own = lax.dynamic_index_in_dim(grad_out, core, 0, keepdims=False)
        seg_own = lax.dynamic_index_in_dim(seg_ids, core, 0, keepdims=False)

        w_q_2 = swap(w_q)
        w_outs = (w_o, swap(w_o))
        w_gates = (w_gate.T, swap(w_gate.T))
        w_ups = (w_up.T, swap(w_up.T))
        w_downs = (w_down, swap(w_down))
        w_k_loc = lax.dynamic_slice_in_dim(w_k, kv_col, HEAD_DIM, axis=1)
        w_v_loc = lax.dynamic_slice_in_dim(w_v, kv_col, HEAD_DIM, axis=1)
        w_in = jnp.concatenate([w_q, w_q_2, w_k_loc, w_v_loc], axis=1)

        x_float = x_own.astype(F32)
        inv_own = lax.rsqrt(jnp.mean(x_float * x_float, axis=-1, keepdims=True) + EPS)
        normed_own = lax.optimization_barrier((x_float * inv_own * gain_attn).astype(BF16))
        qkv = dot(normed_own, w_in, NN).astype(BF16)
        queries = qkv[:, :2 * HEAD_DIM].reshape(seq_len, 2, HEAD_DIM)
        keys = qkv[:, 2 * HEAD_DIM:3 * HEAD_DIM]
        values = qkv[:, 3 * HEAD_DIM:]
        positions = jnp.arange(seq_len)
        allowed = (positions[:, None] >= positions[None, :]) & (seg_own[:, None] == seg_own[None, :])
        scores = jnp.einsum('qhd,kd->hqk', queries, keys, preferred_element_type=F32) * scale
        probs = jax.nn.softmax(jnp.where(allowed[None], scores, -1e30), axis=-1)
        probs_b = probs.astype(BF16)
        ctx = jnp.einsum('hqk,kd->qhd', probs_b, values, preferred_element_type=F32).astype(BF16).reshape(seq_len, 2 * HEAD_DIM)
        x_rows = own_rows(x_own)
        dy_rows = own_rows(dy_own)
        first = sum_attention(side, ctx, normed_own, w_outs, x_rows, gain_mlp_row)
        mixed_full = first['full'].reshape(2, seq_len, width)

        mlp = mlp_grads(mixed_full, grad_out, w_gates, w_ups, w_downs)
        second = sum_mlp(side, [mlp['dg0'], mlp['du0'], mlp['dg1'], mlp['du1']], [mlp['a0'], mlp['a1']], w_gates, w_ups, w_downs, first['h_rows'], dy_rows, gain_mlp_row)
        resid_own, resid_full = second['own'].reshape(seq_len, width), second['full'].reshape(2, seq_len, width)

        y_out = in_place(lax.all_gather(second['y_rows'], 'tp'), rows).reshape(2, seq_len, width)

        w_out = jnp.concatenate(w_outs, axis=0)
        grad_ctx = dot(resid_own, w_out, NT).astype(BF16).reshape(seq_len, 2, HEAD_DIM)
        grad_probs = jnp.einsum('qhd,kd->hqk', grad_ctx, values, preferred_element_type=F32)
        grad_v = jnp.einsum('hqk,qhd->kd', probs_b, grad_ctx, preferred_element_type=F32).astype(BF16)
        grad_scores = (probs * (grad_probs - jnp.sum(grad_probs * probs, axis=-1, keepdims=True)) * scale).astype(BF16)
        grad_q = jnp.einsum('hqk,kd->qhd', grad_scores, keys, preferred_element_type=F32).astype(BF16).reshape(seq_len, 2 * HEAD_DIM)
        grad_k = jnp.einsum('hqk,qhd->kd', grad_scores, queries, preferred_element_type=F32).astype(BF16)
        grad_kv = jnp.concatenate([grad_k, grad_v], axis=1)
        third = sum_input(side, jnp.concatenate([grad_q, grad_kv], axis=1), w_in, grad_kv.reshape(share, seq_len // share, 2 * HEAD_DIM), x_rows, second['d_rows'], gain_attn_row, second['gain'])

        gathered = lax.all_gather(third['rows'], 'tp')
        grad_in = in_place(gathered, rows).reshape(2, seq_len, width)
        gain_grads = jnp.sum(gathered[:, rows:].astype(F32), axis=0)
        grad_gain_attn = gain_grads[0] + gain_grads[1] + gain_grads[2]
        grad_gain_mlp = gain_grads[3] + gain_grads[4] + gain_grads[5]

        def flat(value):
            return value.reshape(seq_len, value.shape[-1])

        grad_gate_t, grad_up_t, grad_w_down, grad_w_o = weight_grads_mlp(
            mixed_full, grad_out, resid_full, (mlp['dg0'], flat(second['gate_other'])), (mlp['du0'], flat(second['up_other'])), (mlp['a0'], flat(second['act_other'])),
            (ctx[:, :HEAD_DIM], flat(first['ctx_other'])))
        kv_full = third['kv'].reshape(2, chips, seq_len // share, 2 * HEAD_DIM)
        grad_w_q, grad_w_k, grad_w_v = weight_grads_qkv((normed_own, first['normed_other']), kv_full, (grad_q[:, :HEAD_DIM], flat(third['q_other'])), kv_heads)
        return (y_out, grad_in, grad_gain_attn, grad_gain_mlp, grad_w_q, grad_w_k, grad_w_v, grad_w_o, grad_gate_t.T, grad_up_t.T, grad_w_down)

    spec_act = P('data', None, None)
    spec_rows = P('data', None)
    spec_gain = P(None)
    spec_cols = P(None, 'tp')
    spec_tprows = P('tp', None)
    spec_whole = P(None, None)
    spec_stack = P(('data', 'tp'), None)
    in_specs = (spec_act, spec_rows, spec_act, spec_gain, spec_gain, spec_cols, spec_whole, spec_whole, spec_tprows, spec_cols, spec_cols, spec_tprows)
    out_specs = (spec_act, spec_act, P('data'), P('data'), P('data', 'tp'), spec_rows, spec_rows, spec_stack, P('data', 'tp'), P('data', 'tp'), spec_stack)
    return jax.shard_map(device_step, mesh=mesh, in_specs=in_specs, out_specs=out_specs, check_vma=False)
```

```python
import functools
import math
import types
import jax
import jax.numpy as jnp
from jax import lax
from jax.experimental import pallas as pl
from jax.experimental.pallas import tpu as pltpu
from jax.sharding import PartitionSpec as P

HEAD_DIM = 128
EPS = 1e-5
MESH = pl.DeviceIdType.MESH
F32 = jnp.float32
BF16 = jnp.bfloat16
MIB = 2 ** 20
ANY = pl.BlockSpec(memory_space=pl.ANY)
VMEM = pl.BlockSpec(memory_space=pltpu.VMEM)


def dot(lhs, rhs, dims):
    return lax.dot_general(lhs, rhs, (dims, ((), ())), preferred_element_type=F32)


NN = ((1,), (0,))
NT = ((1,), (1,))


SIGNS = (1, -1)


class Colour:
    def __init__(self, index, first, second):
        self.index, self.first, self.second = index, first, second


class Torus:
    def __init__(self, side):
        self.side = side
        tp_idx = lax.axis_index('tp')
        self.core = lax.rem(tp_idx, 2)
        self.chip = lax.div(tp_idx, 2)
        self.x = lax.rem(self.chip, side)
        self.y = lax.div(self.chip, side)
        self.partner = {'tp': self.chip * 2 + (1 - self.core)}
        self.colours = (Colour(0, self.x, self.y), Colour(1, self.y, self.x))
        self.pending = []

    def wrap(self, pos):
        return lax.rem(pos + 2 * self.side, self.side)

    def at_chip(self, y_at, x_at):
        return {'tp': (y_at * self.side + x_at) * 2 + self.core}

    def block(self, col, second, first):
        return (second, first) if col.index == 0 else (first, second)

    def peer1(self, col, shift):
        return self.at_chip(*self.block(col, col.second, self.wrap(col.first + shift)))

    def peer2(self, col, shift):
        return self.at_chip(*self.block(col, self.wrap(col.second + shift), col.first))

    def signal_all(self):
        barrier = pltpu.get_barrier_semaphore()
        peers = [self.partner]
        peers += [self.at_chip(self.y, self.wrap(self.x + shift)) for shift in SIGNS]
        peers += [self.at_chip(self.wrap(self.y + shift), self.x) for shift in SIGNS]
        for peer in peers:
            pl.semaphore_signal(barrier, inc=1, device_id=peer, device_id_type=MESH)
        return lambda: pl.semaphore_wait(barrier, len(peers))

    def send(self, src, dst, sems, index, device):
        copy = pltpu.make_async_remote_copy(src, dst, sems[0].at[index], sems[1].at[index], device_id=device, device_id_type=MESH)
        copy.start()
        self.pending.append(copy)

    def arrive(self, dst, sems, index):
        pltpu.make_async_remote_copy(dst, dst, sems[0].at[index], sems[1].at[index], device_id=self.partner, device_id_type=MESH).wait_recv()

    def drain(self):
        for copy in self.pending:
            copy.wait_send()


R1, R2, R3, S1, S2, S3 = range(6)
RS_COUNTS = (16, 16, 16, 4, 4, 4)
H1, H2, F1, F2 = range(4)
AG_COUNTS = (8, 32, 4, 16)


class ReduceScatter:
    SHIFTS = (2, 1, 3, 0)

    def __init__(self, torus, scr):
        self.torus, self.part, self.scr = torus, scr.part, scr
        self.quarter = scr.part.shape[3] // 4

    def buf(self, kind, index):
        return self.scr.bufs[kind].at[index]

    def sems(self, kind):
        return self.scr.out_sems[kind], self.scr.in_sems[kind]

    def cols(self, col, half):
        return pl.ds((col.index * 2 + half) * self.quarter, self.quarter)

    def piece(self, where, at_cols):
        return self.part.at[(*where, slice(None), at_cols)]

    def send(self, where, at_cols, kind, index, peer):
        self.torus.send(self.piece(where, at_cols), self.buf(kind, index), self.sems(kind), index, peer)

    def add(self, where, at_cols, *kinds):
        total = self.part[(*where, slice(None), at_cols)].astype(F32)
        for kind, index in kinds:
            self.torus.arrive(self.buf(kind, index), self.sems(kind), index)
            total = total + self.buf(kind, index)[...].astype(F32)
        self.part[(*where, slice(None), at_cols)] = total.astype(BF16)

    def each(self, step):
        wrap = self.torus.wrap
        for col in self.torus.colours:
            second = wrap(col.second + self.SHIFTS[step])
            for way, sign in enumerate(SIGNS):
                yield col, second, way, sign, (col.index * 2 + way) * 4 + step

    def far(self, step):
        for col, second, way, sign, index in self.each(step):
            where = self.torus.block(col, second, self.torus.wrap(col.first + 2))
            self.send(where, self.cols(col, way), R1, index, self.torus.peer1(col, sign))

    def near(self, step):
        for col, second, way, sign, index in self.each(step):
            where = self.torus.block(col, second, self.torus.wrap(col.first + sign))
            self.send(where, self.cols(col, 1 - way), R2, index, self.torus.peer1(col, sign))

    def relay(self, step):
        for col, second, way, sign, index in self.each(step):
            where = self.torus.block(col, second, self.torus.wrap(col.first + sign))
            self.add(where, self.cols(col, way), (R1, index))
            self.send(where, self.cols(col, way), R3, index, self.torus.peer1(col, sign))

    def end(self, step):
        for col, second, way, sign, index in self.each(step):
            where = self.torus.block(col, second, col.first)
            other = (col.index * 2 + 1 - way) * 4 + step
            self.add(where, self.cols(col, way), (R2, other), (R3, index))

    def far2(self):
        for col in self.torus.colours:
            for way, sign in enumerate(SIGNS):
                where = self.torus.block(col, self.torus.wrap(col.second + 2), col.first)
                self.send(where, self.cols(col, way), S1, col.index * 2 + way, self.torus.peer2(col, sign))

    def near2(self, way):
        for col in self.torus.colours:
            where = self.torus.block(col, self.torus.wrap(col.second + SIGNS[way]), col.first)
            self.send(where, self.cols(col, 1 - way), S2, col.index * 2 + way, self.torus.peer2(col, SIGNS[way]))

    def relay2(self, way):
        for col in self.torus.colours:
            index = col.index * 2 + way
            where = self.torus.block(col, self.torus.wrap(col.second + SIGNS[way]), col.first)
            self.add(where, self.cols(col, way), (S1, index))
            self.send(where, self.cols(col, way), S3, index, self.torus.peer2(col, SIGNS[way]))

    def end2(self):
        for col in self.torus.colours:
            where = self.torus.block(col, col.second, col.first)
            for way in range(2):
                self.add(where, self.cols(col, way), (S2, col.index * 2 + 1 - way), (S3, col.index * 2 + way))

    def steps(self, fill):
        call = functools.partial
        return [call(fill, 2), call(self.far, 0), call(self.far, 1), call(fill, 1), call(fill, 3),
                call(self.near, 0), call(self.relay, 0), call(self.near, 1), call(self.far, 2), call(self.relay, 1),
                call(fill, 0), call(self.near, 2), call(self.far, 3), call(self.end, 0), call(self.far2),
                call(self.relay, 2), call(self.near, 3), call(self.end, 1), call(self.near2, 0), call(self.relay2, 0),
                call(self.relay, 3), call(self.end, 2), call(self.near2, 1), call(self.relay2, 1), call(self.end, 3),
                call(self.end2)]


class AllGather:
    def __init__(self, torus, scr, by_rows, keep):
        self.torus, self.gat, self.scr, self.by_rows, self.keep_piece = torus, scr.gat, scr, by_rows, keep
        self.quarter = scr.gat.shape[2 if by_rows else 3] // 4
        self.back = (0, torus.side - 1, 1, 2)

    def sems(self, kind):
        return self.scr.out_sems[kind], self.scr.in_sems[kind]

    def piece(self, ref, where, first, count):
        at = pl.ds(first * self.quarter, count * self.quarter)
        return ref.at[(*where, at, slice(None))] if self.by_rows else ref.at[(*where, slice(None), at)]

    def half(self, col, where, half):
        return self.piece(self.gat, where, col.index * 2 + half, 1)

    def own2(self, turn):
        for col in self.torus.colours:
            where = self.torus.block(col, col.second, col.first)
            for way, sign in enumerate(SIGNS):
                at = self.half(col, where, way if turn == 0 else 1 - way)
                self.torus.send(at, at, self.sems(H1), (col.index * 2 + way) * 2 + turn, self.torus.peer2(col, sign))

    def send1(self, step, turn):
        for col in self.torus.colours:
            where = self.torus.block(col, self.torus.wrap(col.second + self.back[step]), col.first)
            for way, sign in enumerate(SIGNS):
                at = self.half(col, where, way if turn == 0 else 1 - way)
                self.torus.send(at, at, self.sems(H2), ((col.index * 2 + way) * 4 + step) * 2 + turn, self.torus.peer1(col, sign))

    def arrive2(self, way, turn):
        sign = SIGNS[way]
        for col in self.torus.colours:
            where = self.torus.block(col, self.torus.wrap(col.second - sign), col.first)
            at = self.half(col, where, way if turn == 0 else 1 - way)
            self.torus.arrive(at, self.sems(H1), (col.index * 2 + way) * 2 + turn)
            if turn == 0:
                self.torus.send(at, at, self.sems(F1), col.index * 2 + way, self.torus.peer2(col, sign))

    def relayed2(self):
        for col in self.torus.colours:
            where = self.torus.block(col, self.torus.wrap(col.second + 2), col.first)
            for way in range(2):
                self.torus.arrive(self.half(col, where, way), self.sems(F1), col.index * 2 + way)

    def arrive1(self, step, turn):
        for col in self.torus.colours:
            second = self.torus.wrap(col.second + self.back[step])
            for way, sign in enumerate(SIGNS):
                where = self.torus.block(col, second, self.torus.wrap(col.first - sign))
                at = self.half(col, where, way if turn == 0 else 1 - way)
                self.torus.arrive(at, self.sems(H2), ((col.index * 2 + way) * 4 + step) * 2 + turn)
                if turn == 0:
                    self.torus.send(at, at, self.sems(F2), (col.index * 2 + way) * 4 + step, self.torus.peer1(col, sign))

    def relayed1(self, step):
        for col in self.torus.colours:
            second = self.torus.wrap(col.second + self.back[step])
            for way in range(2):
                where = self.torus.block(col, second, self.torus.wrap(col.first + 2))
                self.torus.arrive(self.half(col, where, way), self.sems(F2), (col.index * 2 + way) * 4 + step)

    def keep(self, step, firsts):
        for col in self.torus.colours:
            for shift in firsts:
                where = self.torus.block(col, self.torus.wrap(col.second + self.back[step]), self.torus.wrap(col.first + shift))
                slot = (col.index * self.torus.side + where[0]) * self.torus.side + where[1]
                self.keep_piece(slot, lambda ref, where=where, col=col: self.piece(ref, where, col.index * 2, 2))

    def steps(self):
        call = functools.partial
        beside = (1, self.torus.side - 1)
        return [call(self.own2, 0), call(self.send1, 0, 0), call(self.own2, 1), call(self.send1, 0, 1), call(self.keep, 0, (0,)),
                call(self.arrive2, 0, 0), call(self.arrive2, 1, 0), call(self.arrive2, 0, 1), call(self.send1, 1, 0), call(self.send1, 1, 1),
                call(self.arrive2, 1, 1), call(self.send1, 2, 0), call(self.send1, 2, 1), call(self.keep, 1, (0,)), call(self.keep, 2, (0,)),
                call(self.arrive1, 0, 0), call(self.relayed2), call(self.send1, 3, 0), call(self.send1, 3, 1), call(self.keep, 3, (0,)),
                call(self.arrive1, 0, 1), call(self.keep, 0, beside), call(self.arrive1, 1, 0), call(self.arrive1, 2, 0),
                call(self.relayed1, 0), call(self.keep, 0, (2,)), call(self.arrive1, 1, 1), call(self.keep, 1, beside),
                call(self.arrive1, 2, 1), call(self.keep, 2, beside), call(self.arrive1, 3, 0), call(self.relayed1, 1), call(self.keep, 1, (2,)),
                call(self.relayed1, 2), call(self.keep, 2, (2,)), call(self.arrive1, 3, 1), call(self.keep, 3, beside),
                call(self.relayed1, 3), call(self.keep, 3, (2,))]


class Store:
    def __init__(self, torus, full, scr, own=None):
        self.torus, self.full, self.scr, self.own = torus, full, scr, own
        self.stores = []

    def keep(self, slot, piece):
        pairs = [(self.scr.full_sem, self.full.at[self.torus.core])]
        if self.own is not None:
            pairs.append((self.scr.own_sem, self.own))
        for sem, ref in pairs:
            store = pltpu.make_async_copy(piece(self.scr.gat), piece(ref), sem.at[slot])
            store.start()
            self.stores.append(store)
        self.torus.send(piece(self.scr.gat), piece(self.full.at[self.torus.core]), self.scr.cross_sems, slot, self.torus.partner)

    def drain(self, gather):
        for store in self.stores:
            store.wait()
        side = self.torus.side
        for colour in range(2):
            for y_at in range(side):
                for x_at in range(side):
                    target = gather.piece(self.full.at[1 - self.torus.core], (y_at, x_at), colour * 2, 2)
                    self.torus.arrive(target, self.scr.cross_sems, (colour * side + y_at) * side + x_at)


def rs_scratch(side, rows, width):
    dma = pltpu.SemaphoreType.DMA
    return dict(
        part=pltpu.VMEM((side, side, rows, width), BF16),
        bufs=[pltpu.VMEM((count, rows, width // 4), BF16) for count in RS_COUNTS],
        out_sems=[dma((count,)) for count in RS_COUNTS],
        in_sems=[dma((count,)) for count in RS_COUNTS],
    )


def ag_scratch(side, rows, width):
    dma = pltpu.SemaphoreType.DMA
    blocks = 2 * side * side
    return dict(
        gat=pltpu.VMEM((side, side, rows, width), BF16),
        out_sems=[dma((count,)) for count in AG_COUNTS],
        in_sems=[dma((count,)) for count in AG_COUNTS],
        full_sem=dma((blocks,)),
        own_sem=dma((blocks,)),
        cross_sems=[dma((blocks,)), dma((blocks,))],
    )


class Weights:
    def __init__(self, refs, buf, sem, by_rows):
        self.refs, self.buf, self.sem, self.by_rows = refs, buf, sem, by_rows
        self.copies = [[], []]

    def start(self):
        for colour in range(2):
            for index, ref in enumerate(self.refs):
                if self.by_rows:
                    half, depth = ref.shape[0] // 2, ref.shape[1]
                    rows, cols = pl.ds(colour * half, half), pl.ds(index * depth, depth)
                    copy = pltpu.make_async_copy(ref.at[rows, :], self.buf.at[rows, cols], self.sem.at[colour, index])
                else:
                    half, depth = ref.shape[1] // 2, ref.shape[0]
                    rows, cols = pl.ds(index * depth, depth), pl.ds(colour * half, half)
                    copy = pltpu.make_async_copy(ref.at[:, cols], self.buf.at[rows, cols], self.sem.at[colour, index])
                copy.start()
                self.copies[colour].append(copy)

    def wait(self, colour):
        for copy in self.copies[colour]:
            copy.wait()
        self.copies[colour] = []


def fill_partial(torus, part, lhs, weights):
    rows, width = part.shape[2:]
    tile = min(512, width // 2)

    def fill(shift):
        for col in torus.colours:
            weights.wait(col.index)
            first = torus.wrap(col.first + shift)
            left = []
            for ref in lhs:
                depth = ref.shape[3]
                value = ref[:, first] if col.index == 0 else ref[first]
                left.append((value.reshape(torus.side * rows, depth), depth))

            def body(step, carry, col=col, first=first, left=left):
                at = pl.ds(pl.multiple_of(col.index * (width // 2) + step * tile, tile), tile)
                total = None
                base = 0
                for value, depth in left:
                    if weights.by_rows:
                        term = dot(value, weights.buf[at, base:base + depth], NT)
                    else:
                        term = dot(value, weights.buf[base:base + depth, at], NN)
                    total = term if total is None else total + term
                    base += depth
                total = total.astype(BF16).reshape(torus.side, rows, tile)
                if col.index == 0:
                    part[:, first, :, at] = total
                else:
                    part[first, :, :, at] = total
                return carry

            lax.fori_loop(0, (width // 2) // tile, body, 0)

    return fill


def run(*lists):
    keyed = []
    for order, steps in enumerate(lists):
        keyed += [((index + 0.5) / len(steps), order, step) for index, step in enumerate(steps)]
    for _, _, step in sorted(keyed, key=lambda item: item[:2]):
        step()


def swap_start(torus, sems, pairs):
    for index, (src, dst) in enumerate(pairs):
        torus.send(src, dst, sems, index, torus.partner)


def swap_end(torus, sems, pairs):
    for index, (_, dst) in enumerate(pairs):
        torus.arrive(dst, sems, index)


def row_tiles(rows):
    return [pl.ds(start, 16) for start in range(0, rows, 16)]


def rms_back(z_in, gain, grad):
    inv = lax.rsqrt(jnp.mean(z_in * z_in, axis=-1, keepdims=True) + EPS)
    normed = z_in * inv
    scaled = grad * gain
    back = inv * (scaled - normed * jnp.mean(scaled * normed, axis=-1, keepdims=True))
    return back, jnp.sum(grad * normed, axis=0, keepdims=True)


def bag(tree):
    if isinstance(tree, dict):
        return types.SimpleNamespace(**{key: bag(value) for key, value in tree.items()})
    return [bag(value) for value in tree] if isinstance(tree, list) else tree


def call_kernel(name, body, ins, outs, scratch, flops, collective_id=None):
    is_leaf = lambda value: isinstance(value, tuple)
    in_leaves, in_tree = jax.tree.flatten(ins, is_leaf=is_leaf)
    out_leaves, out_tree = jax.tree.flatten(outs, is_leaf=is_leaf)
    scr_leaves, scr_tree = jax.tree.flatten(scratch)
    first_scr = len(in_leaves) + len(out_leaves)

    def kernel(*refs):
        body(bag(in_tree.unflatten(refs[:len(in_leaves)])), bag(out_tree.unflatten(refs[len(in_leaves):first_scr])), bag(scr_tree.unflatten(refs[first_scr:])))

    results = pl.pallas_call(
        kernel,
        name=name,
        out_shape=[leaf[0] for leaf in out_leaves],
        in_specs=[leaf[1] for leaf in in_leaves],
        out_specs=[leaf[1] for leaf in out_leaves],
        scratch_shapes=scr_leaves,
        compiler_params=pltpu.CompilerParams(collective_id=collective_id, has_side_effects=collective_id is not None, vmem_limit_bytes=60 * MIB),
        cost_estimate=pl.CostEstimate(flops=int(flops), bytes_accessed=40_000_000, transcendentals=0),
    )(*[leaf[0] for leaf in in_leaves])
    return bag(out_tree.unflatten(results))


def shape(dims, dtype=BF16):
    return jax.ShapeDtypeStruct(dims, dtype)


def sum_attention(side, ctx, normed, w_out, x_rows, gain):
    seq, depth = ctx.shape
    width = gain.shape[1]
    rows = seq // (side * side)

    def body(ins, outs, scr):
        torus = Torus(side)
        weights = Weights(ins.w_out, scr.w, scr.w_sem, False)
        weights.start()
        wait = torus.signal_all()
        part = scr.sum.part
        steps = ReduceScatter(torus, scr.sum).steps(fill_partial(torus, part, [ins.ctx], weights))
        steps[0]()
        wait()
        swaps = [(ins.ctx.at[:, :, :, pl.ds(depth // 2, depth // 2)], outs.ctx_other), (ins.normed, outs.normed_other)]
        swap_start(torus, scr.swap_sems, swaps)
        run(steps[1:])
        gat = scr.all.gat
        own = (torus.y, torus.x)
        for at in row_tiles(rows):
            resid = (ins.x_rows[at, :].astype(F32) + part[(*own, at, slice(None))].astype(F32)).astype(BF16)
            outs.h_rows[at, :] = resid
            z_in = resid.astype(F32)
            inv = lax.rsqrt(jnp.mean(z_in * z_in, axis=-1, keepdims=True) + EPS)
            gat[(*own, at, slice(None))] = (z_in * inv * ins.gain[...]).astype(BF16)
        store = Store(torus, outs.full, scr.all)
        gather = AllGather(torus, scr.all, False, store.keep)
        run(gather.steps())
        store.drain(gather)
        swap_end(torus, scr.swap_sems, swaps)
        torus.drain()

    dma = pltpu.SemaphoreType.DMA
    ins = dict(ctx=(ctx.reshape(side, side, rows, depth), VMEM), w_out=[(weight, ANY) for weight in w_out], x_rows=(x_rows, VMEM), gain=(gain, VMEM), normed=(normed, ANY))
    outs = dict(full=(shape((2, side, side, rows, width)), ANY), h_rows=(shape((rows, width)), VMEM), ctx_other=(shape((side, side, rows, depth // 2)), ANY), normed_other=(shape((seq, width)), ANY))
    scratch = dict(sum=rs_scratch(side, rows, width), all=ag_scratch(side, rows, width), w=pltpu.VMEM((depth, width), BF16), w_sem=dma((2, 2)), swap_sems=[dma((2,)), dma((2,))])
    return call_kernel('sum_attention', body, ins, outs, scratch, 4e8, 1)


def sum_mlp(side, grads, acts, w_gates, w_ups, w_downs, h_rows, dy_rows, gain):
    seq, depth = grads[0].shape
    width = gain.shape[1]
    rows = seq // (side * side)
    block = (side, side, rows, width)

    def body(ins, outs, scr):
        torus = Torus(side)
        weights = Weights(ins.w_in, scr.w, scr.w_sem, False)
        weights.start()
        weights_p = Weights(ins.w_downs, scr.wd, scr.wd_sem, False)
        weights_p.start()
        wait = torus.signal_all()
        steps = ReduceScatter(torus, scr.sum).steps(fill_partial(torus, scr.sum.part, ins.grads, weights))
        steps_p = ReduceScatter(torus, scr.sum_p).steps(fill_partial(torus, scr.sum_p.part, ins.acts, weights_p))
        steps[0]()
        wait()
        swaps = [(ins.grads[2], outs.gate_other), (ins.grads[3], outs.up_other), (ins.acts[1], outs.act_other)]
        swap_start(torus, scr.swap_sems, swaps)
        early = [steps_p[0], steps_p[3], steps_p[4], steps_p[10]]
        rest_p = [step for index, step in enumerate(steps_p) if index not in (0, 3, 4, 10)]
        run(steps[1:22], early)
        for step in rest_p[:3]:
            step()
        run(steps[22:])
        own = (torus.y, torus.x)
        gain_total = jnp.zeros((1, width), F32)
        gat = scr.all.gat
        for at in row_tiles(rows):
            back, gain_part = rms_back(ins.h_rows[at, :].astype(F32), ins.gain[...], scr.sum.part[(*own, at, slice(None))].astype(F32))
            gain_total = gain_total + gain_part
            total = ins.dy_rows[at, :].astype(F32) + back
            outs.d_rows[at, :] = total
            gat[(*own, at, slice(None))] = total.astype(BF16)
        outs.gain[...] = gain_total
        store = Store(torus, outs.full, scr.all, outs.own)
        gather = AllGather(torus, scr.all, False, store.keep)
        run(gather.steps(), rest_p[3:])
        for at in row_tiles(rows):
            outs.y_rows[at, :] = (ins.h_rows[at, :].astype(F32) + scr.sum_p.part[(*own, at, slice(None))].astype(F32)).astype(BF16)
        store.drain(gather)
        swap_end(torus, scr.swap_sems, swaps)
        torus.drain()

    blocked = lambda value: (value.reshape(side, side, rows, depth), VMEM)
    dma = pltpu.SemaphoreType.DMA
    ins = dict(grads=[blocked(grad) for grad in grads], acts=[blocked(act) for act in acts], w_in=[(weight, ANY) for weight in (w_gates[0], w_ups[0], w_gates[1], w_ups[1])],
               w_downs=[(weight, ANY) for weight in w_downs], h_rows=(h_rows, VMEM), dy_rows=(dy_rows, VMEM), gain=(gain, VMEM))
    other = (shape((side, side, rows, depth)), ANY)
    outs = dict(full=(shape((2, *block)), ANY), own=(shape(block), ANY), d_rows=(shape((rows, width), F32), VMEM), gain=(shape((1, width), F32), VMEM), y_rows=(shape((rows, width)), VMEM),
                gate_other=other, up_other=other, act_other=other)
    scratch = dict(sum=rs_scratch(side, rows, width), sum_p=rs_scratch(side, rows, width), all=ag_scratch(side, rows, width),
                   w=pltpu.VMEM((4 * depth, width), BF16), w_sem=dma((2, 4)), wd=pltpu.VMEM((2 * depth, width), BF16), wd_sem=dma((2, 2)), swap_sems=[dma((3,)), dma((3,))])
    return call_kernel('sum_mlp', body, ins, outs, scratch, 6e8, 2)


def sum_input(side, dqkv, w_qs, w_k, w_v, x_rows, d_rows, gain, gain_mlp_part):
    seq, depth = dqkv.shape
    width = gain.shape[1]
    rows = seq // (side * side)
    head = depth // 4
    half_side = side // 2
    tokens = seq // 2
    per_kv = 2 * side * side // (w_k.shape[1] // head)

    def body(ins, outs, scr):
        torus = Torus(side)
        kv_col = pl.multiple_of(lax.div(torus.chip * 2, per_kv) * head, head)
        weights = Weights([*ins.w_qs, ins.w_k.at[:, pl.ds(kv_col, head)], ins.w_v.at[:, pl.ds(kv_col, head)]], scr.w, scr.w_sem, True)
        weights.start()
        wait = torus.signal_all()
        part = scr.sum.part
        steps = ReduceScatter(torus, scr.sum).steps(fill_partial(torus, part, [ins.dqkv], weights))
        own = (torus.y, torus.x)
        gat = scr.all.gat
        store = Store(torus, outs.kv, scr.all)
        gather = AllGather(torus, scr.all, True, store.keep)
        place = lax.rem(torus.x, 2)
        mate = torus.at_chip(torus.y, torus.x + 1 - 2 * place)
        kv_cols = pl.ds(2 * head, 2 * head)

        def mate_add():
            torus.arrive(scr.mate, scr.mate_sems, 0)
            mine = ins.dqkv[pl.ds(place * half_side, half_side), :, :, kv_cols]
            gat[own] = (mine.astype(F32) + scr.mate[...].astype(F32)).astype(BF16).reshape(tokens, 2 * head)

        steps[0]()
        wait()
        swaps = [(ins.dqkv.at[:, :, :, pl.ds(head, head)], outs.q_other)]
        swap_start(torus, scr.swap_sems, swaps)
        torus.send(ins.dqkv.at[pl.ds((1 - place) * half_side, half_side), :, :, kv_cols], scr.mate, scr.mate_sems, 0, mate)
        for step in steps[1:5]:
            step()
        mate_add()
        run(steps[5:], gather.steps())
        gain_total = jnp.zeros((1, width), F32)
        for at in row_tiles(rows):
            back, gain_part = rms_back(ins.x_rows[at, :].astype(F32), ins.gain[...], part[(*own, at, slice(None))].astype(F32))
            gain_total = gain_total + gain_part
            outs.rows[at, :] = (ins.d_rows[at, :] + back).astype(BF16)
        row = lax.broadcasted_iota(jnp.int32, (8, width), 0)
        extra = jnp.zeros((8, width), F32)
        for index, value in enumerate((gain_total, ins.gain_mlp[...])):
            for level in range(3):
                rounded = value.astype(BF16).astype(F32)
                extra = jnp.where(row == index * 3 + level, rounded, extra)
                value = value - rounded
        outs.rows[rows:rows + 8, :] = extra.astype(BF16)
        store.drain(gather)
        swap_end(torus, scr.swap_sems, swaps)
        torus.drain()

    dma = pltpu.SemaphoreType.DMA
    ins = dict(dqkv=(dqkv.reshape(side, side, rows, depth), VMEM), w_qs=[(weight, ANY) for weight in w_qs], w_k=(w_k, ANY), w_v=(w_v, ANY), x_rows=(x_rows, VMEM), d_rows=(d_rows, VMEM),
               gain=(gain, VMEM), gain_mlp=(gain_mlp_part, VMEM))
    outs = dict(rows=(shape((rows + 8, width)), VMEM), kv=(shape((2, side, side, tokens, 2 * head)), ANY), q_other=(shape((side, side, rows, head)), ANY))
    scratch = dict(sum=rs_scratch(side, rows, width), all=ag_scratch(side, tokens, 2 * head), w=pltpu.VMEM((width, depth), BF16), w_sem=dma((2, 4)),
                   mate=pltpu.VMEM((half_side, side, rows, 2 * head), BF16), mate_sems=[dma((1,)), dma((1,))], swap_sems=[dma((1,)), dma((1,))])
    return call_kernel('sum_input', body, ins, outs, scratch, 3e8, 3)


def scores_softmax(qkv, seg_row, seg_col, head_index, tile_index, tile):
    reach = (tile_index + 1) * tile
    queries = qkv[tile_index * tile:reach, head_index * HEAD_DIM:(head_index + 1) * HEAD_DIM]
    scores = dot(qkv[:reach, 2 * HEAD_DIM:3 * HEAD_DIM], queries, NT) * HEAD_DIM ** -0.5
    key_at = lax.broadcasted_iota(jnp.int32, (reach, tile), 0)
    query_at = lax.broadcasted_iota(jnp.int32, (reach, tile), 1) + tile_index * tile
    allowed = (key_at <= query_at) & (seg_col[:reach, :] == seg_row[:, tile_index * tile:reach])
    scores = jnp.where(allowed, scores, -1e30)
    weights = jnp.exp(scores - jnp.max(scores, axis=0, keepdims=True))
    return weights * (1.0 / jnp.sum(weights, axis=0, keepdims=True)), queries


def segments(seg_ref):
    core = lax.rem(lax.axis_index('tp'), 2)
    seg_row = seg_ref[pl.ds(core, 1), :].astype(F32)
    return seg_row, jnp.broadcast_to(seg_row, (8, seg_row.shape[1])).T[:, :1]


def attention_forward(hidden, seg_ids, gain, w_qs, w_k, w_v, per_kv):
    seq, width = hidden.shape[1:]
    chunk = seq // 4
    tile = min(256, seq)
    depth = 4 * HEAD_DIM

    def body(ins, outs, scr):
        tp_idx = lax.axis_index('tp')
        kv_col = pl.multiple_of(lax.div(tp_idx, per_kv) * HEAD_DIM, HEAD_DIM)
        loads = []
        for index in range(4):
            at = pl.ds(index * chunk, chunk)
            loads.append(pltpu.make_async_copy(ins.hidden.at[lax.rem(tp_idx, 2), at, :], scr.x.at[at, :], scr.x_sem.at[index]))
        cols = [ins.w_qs[0], ins.w_qs[1], ins.w_k.at[:, pl.ds(kv_col, HEAD_DIM)], ins.w_v.at[:, pl.ds(kv_col, HEAD_DIM)]]
        for index, ref in enumerate(cols):
            loads.append(pltpu.make_async_copy(ref, scr.w.at[:, pl.ds(index * HEAD_DIM, HEAD_DIM)], scr.w_sem.at[index]))
        for load in loads:
            load.start()
        stores = []
        for index in range(4):
            loads[index].wait()

            def normalize(step, carry, index=index):
                at = pl.ds(pl.multiple_of(index * chunk + step * 16, 16), 16)
                x_float = scr.x[at, :].astype(F32)
                inv = lax.rsqrt(jnp.mean(x_float * x_float, axis=-1, keepdims=True) + EPS)
                scr.normed[at, :] = (x_float * inv * ins.gain[...]).astype(BF16)
                return carry

            lax.fori_loop(0, chunk // 16, normalize, 0)
            at = pl.ds(index * chunk, chunk)
            store = pltpu.make_async_copy(scr.normed.at[at, :], outs.normed.at[at, :], scr.out_sem.at[index])
            store.start()
            stores.append(store)
            if index == 0:
                for load in loads[4:]:
                    load.wait()
            outs.qkv[at, :] = dot(scr.normed[at, :], scr.w[...], NN).astype(BF16)
        seg_row, seg_col = segments(ins.seg)
        values_t = outs.qkv[:, 3 * HEAD_DIM:].T
        for head_index in range(2):
            for tile_index in range(seq // tile):
                probs, _ = scores_softmax(outs.qkv, seg_row, seg_col, head_index, tile_index, tile)
                ctx_t = dot(values_t[:, :(tile_index + 1) * tile], probs.astype(BF16), NN)
                outs.ctx[tile_index * tile:(tile_index + 1) * tile, head_index * HEAD_DIM:(head_index + 1) * HEAD_DIM] = ctx_t.T.astype(BF16)
        for store in stores:
            store.wait()

    dma = pltpu.SemaphoreType.DMA
    ins = dict(hidden=(hidden, ANY), seg=(seg_ids, VMEM), gain=(gain, VMEM), w_qs=[(weight, ANY) for weight in w_qs], w_k=(w_k, ANY), w_v=(w_v, ANY))
    outs = dict(normed=(shape((seq, width)), ANY), qkv=(shape((seq, depth)), VMEM), ctx=(shape((seq, 2 * HEAD_DIM)), VMEM))
    scratch = dict(x=pltpu.VMEM((seq, width), BF16), normed=pltpu.VMEM((seq, width), BF16), w=pltpu.VMEM((width, depth), BF16), x_sem=dma((4,)), w_sem=dma((4,)), out_sem=dma((4,)))
    return call_kernel('attention_forward', body, ins, outs, scratch, 5e9)


def attention_backward(resid, seg_ids, w_outs, qkv, token):
    seq, width = resid.shape
    chunk = seq // 4
    tile = min(256, seq)
    depth = 4 * HEAD_DIM

    def body(ins, outs, scr):
        loads = []
        for index in range(2):
            at = pl.ds(index * HEAD_DIM, HEAD_DIM)
            loads.append(pltpu.make_async_copy(ins.w_outs[index], scr.w.at[at, :], scr.w_sem.at[index]))
        for index in range(4):
            at = pl.ds(index * chunk, chunk)
            loads.append(pltpu.make_async_copy(ins.resid.at[at, :], scr.resid.at[at, :], scr.in_sem.at[index]))
        for load in loads:
            load.start()
        for load in loads[:2]:
            load.wait()
        for index in range(4):
            loads[2 + index].wait()
            at = pl.ds(index * chunk, chunk)
            scr.grad_ctx[at, :] = dot(scr.resid[at, :], scr.w[...], NT).astype(BF16)
        seg_row, seg_col = segments(ins.seg)
        keys_t = ins.qkv[:, 2 * HEAD_DIM:3 * HEAD_DIM].T
        scr.grad_k[...] = jnp.zeros_like(scr.grad_k)
        scr.grad_v[...] = jnp.zeros_like(scr.grad_v)
        for head_index in range(2):
            cols = slice(head_index * HEAD_DIM, (head_index + 1) * HEAD_DIM)
            for tile_index in range(seq // tile):
                reach = (tile_index + 1) * tile
                rows = slice(tile_index * tile, reach)
                probs, queries = scores_softmax(ins.qkv, seg_row, seg_col, head_index, tile_index, tile)
                grad_ctx = scr.grad_ctx[rows, cols]
                grad_probs = dot(ins.qkv[:reach, 3 * HEAD_DIM:], grad_ctx, NT)
                centre = jnp.sum(grad_probs * probs, axis=0, keepdims=True)
                grad_scores = (probs * (grad_probs - centre) * HEAD_DIM ** -0.5).astype(BF16)
                scr.grad_v[:reach, :] += dot(probs.astype(BF16), grad_ctx, NN)
                scr.grad_k[:reach, :] += dot(grad_scores, queries, NN)
                outs.dqkv[rows, cols] = dot(keys_t[:, :reach], grad_scores, NN).T.astype(BF16)
        outs.dqkv[:, 2 * HEAD_DIM:3 * HEAD_DIM] = scr.grad_k[...].astype(BF16)
        outs.dqkv[:, 3 * HEAD_DIM:] = scr.grad_v[...].astype(BF16)

    dma = pltpu.SemaphoreType.DMA
    ins = dict(resid=(resid, ANY), seg=(seg_ids, VMEM), w_outs=[(weight, ANY) for weight in w_outs], qkv=(qkv, VMEM), token=(token, ANY))
    outs = dict(dqkv=(shape((seq, depth)), VMEM))
    scratch = dict(resid=pltpu.VMEM((seq, width), BF16), w=pltpu.VMEM((2 * HEAD_DIM, width), BF16), grad_ctx=pltpu.VMEM((seq, 2 * HEAD_DIM), BF16),
                   grad_k=pltpu.VMEM((seq, HEAD_DIM), F32), grad_v=pltpu.VMEM((seq, HEAD_DIM), F32), w_sem=dma((2,)), in_sem=dma((4,)))
    return call_kernel('attention_backward', body, ins, outs, scratch, 4e9).dqkv


def mlp_grads(mixed_full, grad_out, w_gates, w_ups, w_downs):
    seq, width = grad_out.shape[1:]
    depth = w_gates[0].shape[0]
    tile = min(256, seq)

    def body(ins, outs, scr):
        core = lax.rem(lax.axis_index('tp'), 2)
        loads = []

        def load(src, dst):
            loads.append(pltpu.make_async_copy(src, dst, scr.sem.at[len(loads)]))
            loads[-1].start()

        load(ins.mixed.at[core], scr.mixed)
        load(ins.w_gates[0], scr.w.at[0])
        load(ins.w_ups[0], scr.w.at[1])
        load(ins.grad_out.at[core], scr.grad_out)
        load(ins.w_downs[0], scr.w.at[2])
        load(ins.w_gates[1], scr.w.at[3])
        load(ins.w_ups[1], scr.w.at[4])
        load(ins.w_downs[1], scr.w.at[5])
        for index in range(2):
            for copy in loads[:5] if index == 0 else loads[5:]:
                copy.wait()

            def step(tile_index, carry, index=index):
                at = pl.ds(pl.multiple_of(tile_index * tile, tile), tile)
                mixed = scr.mixed[at, :]
                gate = dot(mixed, scr.w[3 * index], NT)
                upper = dot(mixed, scr.w[3 * index + 1], NT)
                grad_act = dot(scr.grad_out[at, :], scr.w[3 * index + 2], NT)
                sigmoid_g = 1.0 / (1.0 + jnp.exp(-gate))
                silu_g = gate * sigmoid_g
                outs.acts[index][at, :] = (silu_g * upper).astype(BF16)
                outs.gates[index][at, :] = (grad_act * upper * sigmoid_g * (1.0 + gate * (1.0 - sigmoid_g))).astype(BF16)
                outs.ups[index][at, :] = (grad_act * silu_g).astype(BF16)
                return carry

            lax.fori_loop(0, seq // tile, step, 0)

    whole = lambda values: [(value, ANY) for value in values]
    ins = dict(mixed=(mixed_full, ANY), grad_out=(grad_out, ANY), w_gates=whole(w_gates), w_ups=whole(w_ups), w_downs=whole(w_downs))
    out = (shape((seq, depth)), VMEM)
    outs = dict(acts=[out, out], gates=[out, out], ups=[out, out])
    scratch = dict(mixed=pltpu.VMEM((seq, width), BF16), grad_out=pltpu.VMEM((seq, width), BF16), w=pltpu.VMEM((6, depth, width), BF16), sem=pltpu.SemaphoreType.DMA((8,)))
    return call_kernel('mlp_grads', body, ins, outs, scratch, 17e9)


def weight_grads_mlp(mixed_full, grad_out, resid_full, grads_gate, grads_up, acts, ctxs):
    seq, width = grad_out.shape[1:]
    depth, head = acts[0].shape[1], ctxs[1].shape[1]
    tile = min(512, width)

    def kernel(m_ref, dy_ref, dh_ref, *refs):
        sides = (refs[0:2], refs[2:4], refs[4:6], refs[6:8])
        out_gate, out_up, out_down, out_o, token, left = refs[8:]
        core = lax.rem(lax.axis_index('tp'), 2)

        @pl.when(pl.program_id(0) == 0)
        def _():
            base = 0
            for pair in sides:
                size = pair[1].shape[1]
                for half in range(2):
                    left[half, base:base + size, :] = pair[half][:, :size].T
                base += size

        def product(base, size, ref):
            return dot(left[0, base:base + size, :], ref[core], NN) + dot(left[1, base:base + size, :], ref[1 - core], NN)

        token[...] = jnp.zeros_like(token)
        both = product(0, 2 * depth, m_ref)
        out_gate[...] = both[:depth]
        out_up[...] = both[depth:]
        out_down[...] = product(2 * depth, depth, dy_ref)
        out_o[...] = product(3 * depth, head, dh_ref)

    slab = pl.BlockSpec((2, seq, tile), lambda step: (0, 0, step))
    whole = pl.BlockSpec(memory_space=pltpu.VMEM)
    out = lambda size: pl.BlockSpec((size, tile), lambda step: (0, step))
    return pl.pallas_call(
        kernel,
        name='weight_grads_mlp',
        grid=(width // tile,),
        out_shape=[shape((depth, width), F32)] * 3 + [shape((head, width), F32), shape((8, 128), F32)],
        in_specs=[slab] * 3 + [whole] * 8,
        out_specs=[out(depth)] * 3 + [out(head), pl.BlockSpec((8, 128), lambda step: (0, 0))],
        scratch_shapes=[pltpu.VMEM((2, 3 * depth + head, seq), BF16)],
        compiler_params=pltpu.CompilerParams(vmem_limit_bytes=60 * MIB),
        cost_estimate=pl.CostEstimate(flops=18_500_000_000, bytes_accessed=60_000_000, transcendentals=0),
    )(mixed_full, grad_out, resid_full, *grads_gate, *grads_up, *acts, *ctxs)


def weight_grads_qkv(normeds, kv_full, grads_q, kv_heads):
    seq, width = normeds[0].shape
    chips, tokens, pair = kv_full.shape[1:]
    head = pair // 2
    share = seq // tokens
    tile = min(256, width)
    kv_width = kv_heads * head

    def kernel(a_own, a_other, kv_ref, q_own, q_other, out_q, out_k, out_v, right, left):
        core = lax.rem(lax.axis_index('tp'), 2)

        @pl.when(pl.program_id(0) == 0)
        def _():
            for half, q_ref in enumerate((q_own, q_other)):
                right[half, :, 2 * kv_width:] = q_ref[:, :head]
                batch = core if half == 0 else 1 - core
                for chip in range(chips):
                    at = pl.ds((chip % share) * tokens, tokens)
                    base = (chip // share) * head
                    right[half, at, base:base + head] = kv_ref[batch, chip, :, :head]
                    right[half, at, kv_width + base:kv_width + base + head] = kv_ref[batch, chip, :, head:]

        left[0] = a_own[...].T
        left[1] = a_other[...].T

        def product(base, size):
            return dot(left[0], right[0, :, base:base + size], NN) + dot(left[1], right[1, :, base:base + size], NN)

        out_k[...] = product(0, kv_width)
        out_v[...] = product(kv_width, kv_width)
        out_q[...] = product(2 * kv_width, head)

    whole = pl.BlockSpec(memory_space=pltpu.VMEM)
    slab = pl.BlockSpec((seq, tile), lambda step: (0, step))
    out = lambda size: pl.BlockSpec((tile, size), lambda step: (step, 0))
    return pl.pallas_call(
        kernel,
        name='weight_grads_qkv',
        grid=(width // tile,),
        out_shape=[shape((width, head), F32), shape((width, kv_width), F32), shape((width, kv_width), F32)],
        in_specs=[slab, slab, whole, whole, whole],
        out_specs=[out(head), out(kv_width), out(kv_width)],
        scratch_shapes=[pltpu.VMEM((2, seq, 2 * kv_width + head), BF16), pltpu.VMEM((2, tile, seq), BF16)],
        compiler_params=pltpu.CompilerParams(vmem_limit_bytes=60 * MIB),
        cost_estimate=pl.CostEstimate(flops=27_500_000_000, bytes_accessed=60_000_000, transcendentals=0),
    )(*normeds, kv_full, *grads_q)


def in_place(gathered, rows):
    blocks, _, width = gathered.shape
    slots = 8

    def kernel(src, dst, buf, in_sem, out_sem):
        def load(index):
            return pltpu.make_async_copy(src.at[index, pl.ds(0, rows), :], buf.at[index % slots], in_sem.at[index % slots])

        def store(index):
            return pltpu.make_async_copy(buf.at[index % slots], dst.at[index % 2, index // 2], out_sem.at[index % slots])

        ahead = slots // 2
        for index in range(blocks + ahead):
            if index < blocks:
                if index >= slots:
                    store(index - slots).wait()
                load(index).start()
            if index >= ahead:
                load(index - ahead).wait()
                store(index - ahead).start()
        for index in range(blocks - slots, blocks):
            store(index).wait()

    return pl.pallas_call(
        kernel,
        name='in_place',
        out_shape=shape((2, blocks // 2, rows, width)),
        in_specs=[ANY],
        out_specs=ANY,
        scratch_shapes=[pltpu.VMEM((slots, rows, width), BF16), pltpu.SemaphoreType.DMA((slots,)), pltpu.SemaphoreType.DMA((slots,))],
        compiler_params=pltpu.CompilerParams(vmem_limit_bytes=60 * MIB),
        cost_estimate=pl.CostEstimate(flops=20_000_000, bytes_accessed=25_000_000, transcendentals=0),
    )(gathered)


def solution(mesh):
    tp_size = mesh.shape['tp']
    chips = tp_size // 2
    side = math.isqrt(chips)
    swap_pairs = [(index, index ^ 1) for index in range(tp_size)]

    def device_step(hidden, seg_ids, grad_out, gain_attn, gain_mlp, w_q, w_k, w_v, w_o, w_gate, w_up, w_down):
        seq_len, width = hidden.shape[1:]
        kv_heads = w_k.shape[1] // HEAD_DIM
        per_kv = tp_size // kv_heads
        share = per_kv // 2
        rows = seq_len // chips
        tp_idx = lax.axis_index('tp')

        def swap(value):
            return lax.ppermute(value, 'tp', swap_pairs)

        def own_rows(value):
            return lax.dynamic_slice(value, (tp_idx % 2, tp_idx // 2 * rows, 0), (1, rows, width))[0]

        def flat(value):
            return value.reshape(seq_len, value.shape[-1])

        gain_attn_row = gain_attn[None, :]
        gain_mlp_row = gain_mlp[None, :]
        x_rows = own_rows(hidden)

        w_qs = (w_q, swap(w_q))
        w_outs = (w_o, swap(w_o))
        w_gates = (w_gate.T, swap(w_gate.T))
        w_ups = (w_up.T, swap(w_up.T))
        w_downs = (w_down, swap(w_down))

        attn = attention_forward(hidden, seg_ids, gain_attn_row, w_qs, w_k, w_v, per_kv)
        first = sum_attention(side, attn.ctx, attn.normed, w_outs, x_rows, gain_mlp_row)
        mixed_full = first.full.reshape(2, seq_len, width)
        mlp = mlp_grads(mixed_full, grad_out, w_gates, w_ups, w_downs)
        second = sum_mlp(side, [mlp.gates[0], mlp.ups[0], mlp.gates[1], mlp.ups[1]], mlp.acts, w_gates, w_ups, w_downs, first.h_rows, own_rows(grad_out), gain_mlp_row)
        resid_full = second.full.reshape(2, seq_len, width)

        y_out = in_place(lax.all_gather(second.y_rows, 'tp'), rows).reshape(2, seq_len, width)
        grad_gate_t, grad_up_t, grad_w_down, grad_w_o, token = weight_grads_mlp(
            mixed_full, grad_out, resid_full, (mlp.gates[0], flat(second.gate_other)), (mlp.ups[0], flat(second.up_other)), (mlp.acts[0], flat(second.act_other)),
            (attn.ctx, flat(first.ctx_other)))
        dqkv = attention_backward(flat(second.own), seg_ids, w_outs, attn.qkv, token)
        third = sum_input(side, dqkv, w_qs, w_k, w_v, x_rows, second.d_rows, gain_attn_row, second.gain)

        gathered = lax.all_gather(third.rows, 'tp')
        grad_in = in_place(gathered, rows).reshape(2, seq_len, width)
        gain_grads = jnp.sum(gathered[:, rows:].astype(F32), axis=0)
        grad_gain_attn = gain_grads[0] + gain_grads[1] + gain_grads[2]
        grad_gain_mlp = gain_grads[3] + gain_grads[4] + gain_grads[5]
        kv_full = third.kv.reshape(2, chips, seq_len // share, 2 * HEAD_DIM)
        grad_w_q, grad_w_k, grad_w_v = weight_grads_qkv((attn.normed, first.normed_other), kv_full, (dqkv, flat(third.q_other)), kv_heads)
        return (y_out, grad_in, grad_gain_attn, grad_gain_mlp, grad_w_q, grad_w_k, grad_w_v, grad_w_o, grad_gate_t.T, grad_up_t.T, grad_w_down)

    spec_act = P('data', None, None)
    spec_rows = P('data', None)
    spec_gain = P(None)
    spec_cols = P(None, 'tp')
    spec_tprows = P('tp', None)
    spec_whole = P(None, None)
    spec_stack = P(('data', 'tp'), None)
    in_specs = (spec_act, spec_rows, spec_act, spec_gain, spec_gain, spec_cols, spec_whole, spec_whole, spec_tprows, spec_cols, spec_cols, spec_tprows)
    out_specs = (spec_act, spec_act, P('data'), P('data'), P('data', 'tp'), spec_rows, spec_rows, spec_stack, P('data', 'tp'), P('data', 'tp'), spec_stack)
    return jax.shard_map(device_step, mesh=mesh, in_specs=in_specs, out_specs=out_specs, check_vma=False)
```

```python
import functools
import math
import types
import jax
import jax.numpy as jnp
from jax import lax
from jax.experimental import pallas as pl
from jax.experimental.pallas import tpu as pltpu
from jax.sharding import PartitionSpec as P

HEAD_DIM = 128
EPS = 1e-5
MESH = pl.DeviceIdType.MESH
F32 = jnp.float32
BF16 = jnp.bfloat16
LIMIT = 63 * 2 ** 20
K0, K1, K2, K3 = range(4)
PAIR = range(2)
ANY = pl.BlockSpec(memory_space=pl.ANY)
VMEM = pl.BlockSpec(memory_space=pltpu.VMEM)


def dot(lhs, rhs, dims):
    return lax.dot_general(lhs, rhs, (dims, ((), ())), preferred_element_type=F32)


NN = ((1,), (0,))
NT = ((1,), (1,))


SIGNS = (1, -1)


class Colour:
    def __init__(self, index, first, second):
        self.index, self.first, self.second = index, first, second


class Torus:
    def __init__(self, side):
        self.side = side
        tp_idx = lax.axis_index('tp')
        self.core = lax.rem(tp_idx, 2)
        self.chip = lax.div(tp_idx, 2)
        self.x = lax.rem(self.chip, side)
        self.y = lax.div(self.chip, side)
        self.partner = {'tp': self.chip * 2 + (1 - self.core)}
        self.colours = (Colour(0, self.x, self.y), Colour(1, self.y, self.x))
        self.pending = []

    def wrap(self, pos):
        return lax.rem(pos + 2 * self.side, self.side)

    def at_chip(self, y_at, x_at):
        return {'tp': (y_at * self.side + x_at) * 2 + self.core}

    def block(self, col, second, first):
        return (second, first) if col.index == 0 else (first, second)

    def peer1(self, col, shift):
        return self.at_chip(*self.block(col, col.second, self.wrap(col.first + shift)))

    def peer2(self, col, shift):
        return self.at_chip(*self.block(col, self.wrap(col.second + shift), col.first))

    def signal_all(self):
        barrier = pltpu.get_barrier_semaphore()
        peers = [self.partner]
        peers += [self.at_chip(self.y, self.wrap(self.x + shift)) for shift in SIGNS]
        peers += [self.at_chip(self.wrap(self.y + shift), self.x) for shift in SIGNS]
        for peer in peers:
            pl.semaphore_signal(barrier, inc=1, device_id=peer, device_id_type=MESH)
        return lambda: pl.semaphore_wait(barrier, len(peers))

    def send(self, src, dst, sems, index, device):
        copy = pltpu.make_async_remote_copy(src, dst, sems[K0].at[index], sems[K1].at[index], device_id=device, device_id_type=MESH)
        copy.start()
        self.pending.append(copy)

    def arrive(self, dst, sems, index):
        pltpu.make_async_remote_copy(dst, dst, sems[K0].at[index], sems[K1].at[index], device_id=self.partner, device_id_type=MESH).wait_recv()

    def drain(self):
        for copy in self.pending:
            copy.wait_send()


R1, R2, R3, S1, S2, S3 = range(6)
RS_COUNTS = (16, 16, 16, 4, 4, 4)
H1, H2, F1, F2 = range(4)
AG_COUNTS = (8, 32, 4, 16)


class ReduceScatter:
    SHIFTS = (2, 1, 3, 0)

    def __init__(self, torus, scr):
        self.torus, self.part, self.scr = torus, scr.part, scr
        self.quarter = scr.part.shape[K3] // 4

    def buf(self, kind, index):
        return self.scr.bufs[kind].at[index]

    def sems(self, kind):
        return self.scr.out_sems[kind], self.scr.in_sems[kind]

    def cols(self, col, half):
        return pl.ds((col.index * 2 + half) * self.quarter, self.quarter)

    def piece(self, where, at_cols):
        return self.part.at[(*where, slice(None), at_cols)]

    def send(self, where, at_cols, kind, index, peer):
        self.torus.send(self.piece(where, at_cols), self.buf(kind, index), self.sems(kind), index, peer)

    def add(self, where, at_cols, *kinds):
        total = self.part[(*where, slice(None), at_cols)].astype(F32)
        for kind, index in kinds:
            self.torus.arrive(self.buf(kind, index), self.sems(kind), index)
            total = total + self.buf(kind, index)[...].astype(F32)
        self.part[(*where, slice(None), at_cols)] = total.astype(BF16)

    def each(self, step):
        wrap = self.torus.wrap
        for col in self.torus.colours:
            second = wrap(col.second + self.SHIFTS[step])
            for way, sign in enumerate(SIGNS):
                yield col, second, way, sign, (col.index * 2 + way) * 4 + step

    def far(self, step):
        for col, second, way, sign, index in self.each(step):
            where = self.torus.block(col, second, self.torus.wrap(col.first + 2))
            self.send(where, self.cols(col, way), R1, index, self.torus.peer1(col, sign))

    def near(self, step):
        for col, second, way, sign, index in self.each(step):
            where = self.torus.block(col, second, self.torus.wrap(col.first + sign))
            self.send(where, self.cols(col, 1 - way), R2, index, self.torus.peer1(col, sign))

    def relay(self, step):
        for col, second, way, sign, index in self.each(step):
            where = self.torus.block(col, second, self.torus.wrap(col.first + sign))
            self.add(where, self.cols(col, way), (R1, index))
            self.send(where, self.cols(col, way), R3, index, self.torus.peer1(col, sign))

    def end(self, step):
        for col, second, way, sign, index in self.each(step):
            where = self.torus.block(col, second, col.first)
            other = (col.index * 2 + 1 - way) * 4 + step
            self.add(where, self.cols(col, way), (R2, other), (R3, index))

    def far2(self):
        for col in self.torus.colours:
            for way, sign in enumerate(SIGNS):
                where = self.torus.block(col, self.torus.wrap(col.second + 2), col.first)
                self.send(where, self.cols(col, way), S1, col.index * 2 + way, self.torus.peer2(col, sign))

    def near2(self, way):
        for col in self.torus.colours:
            where = self.torus.block(col, self.torus.wrap(col.second + SIGNS[way]), col.first)
            self.send(where, self.cols(col, 1 - way), S2, col.index * 2 + way, self.torus.peer2(col, SIGNS[way]))

    def relay2(self, way):
        for col in self.torus.colours:
            index = col.index * 2 + way
            where = self.torus.block(col, self.torus.wrap(col.second + SIGNS[way]), col.first)
            self.add(where, self.cols(col, way), (S1, index))
            self.send(where, self.cols(col, way), S3, index, self.torus.peer2(col, SIGNS[way]))

    def end2(self):
        for col in self.torus.colours:
            where = self.torus.block(col, col.second, col.first)
            for way in PAIR:
                self.add(where, self.cols(col, way), (S2, col.index * 2 + 1 - way), (S3, col.index * 2 + way))

    def steps(self, fill):
        call = functools.partial
        return [call(fill, K2), call(self.far, K0), call(self.far, K1), call(fill, K1), call(fill, K3),
                call(self.near, K0), call(self.relay, K0), call(self.near, K1), call(self.far, K2), call(self.relay, K1),
                call(fill, K0), call(self.near, K2), call(self.far, K3), call(self.end, K0), self.far2,
                call(self.relay, K2), call(self.near, K3), call(self.end, K1), call(self.near2, K0), call(self.relay2, K0),
                call(self.relay, K3), call(self.end, K2), call(self.near2, K1), call(self.relay2, K1), call(self.end, K3),
                self.end2]


class AllGather:
    def __init__(self, torus, scr, by_rows):
        self.torus, self.gat, self.scr, self.by_rows, self.store = torus, scr.gat, scr, by_rows, None
        self.quarter = scr.gat.shape[2 if by_rows else 3] // 4
        self.back = (0, torus.side - 1, 1, 2)

    def sems(self, kind):
        return self.scr.out_sems[kind], self.scr.in_sems[kind]

    def piece(self, ref, where, first, count):
        at = pl.ds(first * self.quarter, count * self.quarter)
        return ref.at[(*where, at, slice(None))] if self.by_rows else ref.at[(*where, slice(None), at)]

    def half(self, col, where, half):
        return self.piece(self.gat, where, col.index * 2 + half, 1)

    def own2(self, turn):
        for col in self.torus.colours:
            where = self.torus.block(col, col.second, col.first)
            for way, sign in enumerate(SIGNS):
                at = self.half(col, where, way if turn == 0 else 1 - way)
                self.torus.send(at, at, self.sems(H1), (col.index * 2 + way) * 2 + turn, self.torus.peer2(col, sign))

    def send1(self, step, turn):
        for col in self.torus.colours:
            where = self.torus.block(col, self.torus.wrap(col.second + self.back[step]), col.first)
            for way, sign in enumerate(SIGNS):
                at = self.half(col, where, way if turn == 0 else 1 - way)
                self.torus.send(at, at, self.sems(H2), ((col.index * 2 + way) * 4 + step) * 2 + turn, self.torus.peer1(col, sign))

    def arrive2(self, way, turn):
        sign = SIGNS[way]
        for col in self.torus.colours:
            where = self.torus.block(col, self.torus.wrap(col.second - sign), col.first)
            at = self.half(col, where, way if turn == 0 else 1 - way)
            self.torus.arrive(at, self.sems(H1), (col.index * 2 + way) * 2 + turn)
            if turn == 0:
                self.torus.send(at, at, self.sems(F1), col.index * 2 + way, self.torus.peer2(col, sign))

    def relayed2(self):
        for col in self.torus.colours:
            where = self.torus.block(col, self.torus.wrap(col.second + 2), col.first)
            for way in PAIR:
                self.torus.arrive(self.half(col, where, way), self.sems(F1), col.index * 2 + way)

    def arrive1(self, step, turn):
        for col in self.torus.colours:
            second = self.torus.wrap(col.second + self.back[step])
            for way, sign in enumerate(SIGNS):
                where = self.torus.block(col, second, self.torus.wrap(col.first - sign))
                at = self.half(col, where, way if turn == 0 else 1 - way)
                self.torus.arrive(at, self.sems(H2), ((col.index * 2 + way) * 4 + step) * 2 + turn)
                if turn == 0:
                    self.torus.send(at, at, self.sems(F2), (col.index * 2 + way) * 4 + step, self.torus.peer1(col, sign))

    def relayed1(self, step):
        for col in self.torus.colours:
            second = self.torus.wrap(col.second + self.back[step])
            for way in PAIR:
                where = self.torus.block(col, second, self.torus.wrap(col.first + 2))
                self.torus.arrive(self.half(col, where, way), self.sems(F2), (col.index * 2 + way) * 4 + step)

    def keep(self, step, firsts):
        for col in self.torus.colours:
            for shift in firsts:
                where = self.torus.block(col, self.torus.wrap(col.second + self.back[step]), self.torus.wrap(col.first + shift))
                self.store.keep(where, col.index, lambda ref, where=where, col=col: self.piece(ref, where, col.index * 2, 2))

    def steps(self, whole=None):
        call = functools.partial
        whole = whole or (lambda step: None)
        here, beside, across = (K0,), (K1, self.torus.side - 1), (K2,)
        result = []
        for turn in PAIR:
            result += [call(self.own2, turn), call(self.send1, K0, turn)]
        result += [call(self.keep, K0, here), call(self.arrive2, K0, K0), call(self.arrive2, K1, K0)]
        for way in PAIR:
            step = way + K1
            result += [call(self.arrive2, way, K1), call(self.send1, step, K0), call(self.send1, step, K1), call(self.keep, step, here)]
        result += [call(self.arrive1, K0, K0), self.relayed2, call(self.send1, K3, K0), call(self.send1, K3, K1), call(self.keep, K3, here),
                   call(self.arrive1, K0, K1), call(self.keep, K0, beside), call(self.arrive1, K1, K0), call(self.arrive1, K2, K0),
                   call(self.relayed1, K0), call(self.keep, K0, across), call(whole, K0)]
        for step in (K1, K2):
            result += [call(self.arrive1, step, K1), call(self.keep, step, beside)]
        result += [call(self.arrive1, K3, K0)]
        for step in (K1, K2):
            result += [call(self.relayed1, step), call(self.keep, step, across), call(whole, step)]
        return result + [call(self.arrive1, K3, K1), call(self.keep, K3, beside), call(self.relayed1, K3), call(self.keep, K3, across), call(whole, K3)]


class Store:
    def __init__(self, torus, scr, places, own=None):
        self.torus, self.scr, self.places, self.own = torus, scr, places, own
        self.stores = []

    def slot(self, where, colour, index):
        return ((index * 2 + colour) * self.torus.side + where[K0]) * self.torus.side + where[K1]

    def keep(self, where, colour, piece):
        for index, (src, dst) in enumerate(self.places(where, colour, self.torus.core)):
            slot = self.slot(where, colour, index)
            pairs = [(self.scr.full_sem, dst)]
            if self.own is not None:
                pairs.append((self.scr.own_sem, piece(self.own)))
            for sem, ref in pairs:
                store = pltpu.make_async_copy(src, ref, sem.at[slot])
                store.start()
                self.stores.append(store)
            self.torus.send(src, dst, self.scr.cross_sems, slot, self.torus.partner)

    def drain(self):
        for store in self.stores:
            store.wait()
        side = self.torus.side
        for colour in PAIR:
            for y_at in range(side):
                for x_at in range(side):
                    for index, (_, dst) in enumerate(self.places((y_at, x_at), colour, 1 - self.torus.core)):
                        self.torus.arrive(dst, self.scr.cross_sems, self.slot((y_at, x_at), colour, index))


def plain_places(gather, full):
    return lambda where, colour, half: [(gather.piece(gather.gat, where, colour * 2, 2), gather.piece(full.at[half], where, colour * 2, 2))]


def rs_scratch(side, rows, width):
    dma = pltpu.SemaphoreType.DMA
    return dict(
        part=pltpu.VMEM((side, side, rows, width), BF16),
        bufs=[pltpu.VMEM((count, rows, width // 4), BF16) for count in RS_COUNTS],
        out_sems=[dma((count,)) for count in RS_COUNTS],
        in_sems=[dma((count,)) for count in RS_COUNTS],
    )


def ag_scratch(side, rows, width, places=1):
    dma = pltpu.SemaphoreType.DMA
    blocks = 2 * side * side * places
    return dict(
        gat=pltpu.VMEM((side, side, rows, width), BF16),
        out_sems=[dma((count,)) for count in AG_COUNTS],
        in_sems=[dma((count,)) for count in AG_COUNTS],
        full_sem=dma((blocks,)),
        own_sem=dma((blocks,)),
        cross_sems=[dma((blocks,)), dma((blocks,))],
    )


class Weights:
    def __init__(self, refs, buf, sem, by_rows):
        self.refs, self.buf, self.sem, self.by_rows = refs, buf, sem, by_rows
        self.copies = [[], []]

    def start(self):
        for colour in PAIR:
            for index, ref in enumerate(self.refs):
                if self.by_rows:
                    half, depth = ref.shape[K0] // 2, ref.shape[K1]
                    rows, cols = pl.ds(colour * half, half), pl.ds(index * depth, depth)
                    copy = pltpu.make_async_copy(ref.at[rows, :], self.buf.at[rows, cols], self.sem.at[colour, index])
                else:
                    half, depth = ref.shape[K1] // 2, ref.shape[K0]
                    rows, cols = pl.ds(index * depth, depth), pl.ds(colour * half, half)
                    copy = pltpu.make_async_copy(ref.at[:, cols], self.buf.at[rows, cols], self.sem.at[colour, index])
                copy.start()
                self.copies[colour].append(copy)

    def wait(self, colour):
        for copy in self.copies[colour]:
            copy.wait()
        self.copies[colour] = []


def fill_partial(torus, part, lhs, weights):
    rows, width = part.shape[2:]
    tile = min(512, width // 2)

    def fill(shift):
        for col in torus.colours:
            weights.wait(col.index)
            first = torus.wrap(col.first + shift)
            left = []
            for ref in lhs:
                depth = ref.shape[K3]
                value = ref[:, first] if col.index == 0 else ref[first]
                left.append((value.reshape(torus.side * rows, depth), depth))

            def body(step, carry, col=col, first=first, left=left):
                at = pl.ds(pl.multiple_of(col.index * (width // 2) + step * tile, tile), tile)
                total = None
                base = 0
                for value, depth in left:
                    if weights.by_rows:
                        term = dot(value, weights.buf[at, base:base + depth], NT)
                    else:
                        term = dot(value, weights.buf[base:base + depth, at], NN)
                    total = term if total is None else total + term
                    base += depth
                total = total.astype(BF16).reshape(torus.side, rows, tile)
                if col.index == 0:
                    part[:, first, :, at] = total
                else:
                    part[first, :, :, at] = total
                return carry

            lax.fori_loop(0, (width // 2) // tile, body, 0)

    return fill


def run(*lists):
    keyed = []
    for order, steps in enumerate(lists):
        keyed += [((index + 0.5) / len(steps), order, step) for index, step in enumerate(steps)]
    for _, _, step in sorted(keyed, key=lambda item: item[:2]):
        step()


def swap_start(torus, sems, pairs):
    for index, (src, dst) in enumerate(pairs):
        torus.send(src, dst, sems, index, torus.partner)


def swap_end(torus, sems, pairs, first=0):
    for index, (_, dst) in enumerate(pairs):
        if index >= first:
            torus.arrive(dst, sems, index)


class Turner:
    def __init__(self, src, dst, scr):
        self.src, self.dst, self.scr = src, dst, scr
        self.unit = scr.turn_in.shape[K2]
        self.count = src.shape[K1] // self.unit

    def load(self, index):
        at = pl.ds(pl.multiple_of(index * self.unit, self.unit), self.unit)
        slot = lax.rem(index, 2)
        return pltpu.make_async_copy(self.src.at[:, at], self.scr.turn_in.at[slot], self.scr.turn_in_sem.at[slot])

    def save(self, index):
        at = pl.ds(pl.multiple_of(index * self.unit, self.unit), self.unit)
        slot = lax.rem(index, 2)
        return pltpu.make_async_copy(self.scr.turn_out.at[slot], self.dst.at[at, :], self.scr.turn_out_sem.at[slot])

    def steps(self, parts):
        each = self.count // parts

        def step(part):
            if part == 0:
                self.load(0).start()

            def body(index, carry):
                @pl.when(index + 1 < self.count)
                def _():
                    self.load(index + 1).start()

                self.load(index).wait()

                @pl.when(index >= 2)
                def _():
                    self.save(index - 2).wait()

                self.scr.turn_out[lax.rem(index, 2)] = self.scr.turn_in[lax.rem(index, 2)].T
                self.save(index).start()
                return carry

            lax.fori_loop(part * each, (part + 1) * each, body, 0)
            if part == parts - 1:
                self.save(self.count - 2).wait()
                self.save(self.count - 1).wait()

        return [functools.partial(step, part) for part in range(parts)]


def turner_scratch(rows, unit):
    dma = pltpu.SemaphoreType.DMA
    return dict(turn_in=pltpu.VMEM((2, rows, unit), BF16), turn_out=pltpu.VMEM((2, unit, rows), BF16), turn_in_sem=dma((K2,)), turn_out_sem=dma((K2,)))


def row_tiles(rows):
    return [pl.ds(start, 16) for start in range(0, rows, 16)]


def rms_back(z_in, gain, grad):
    inv = lax.rsqrt(jnp.mean(z_in * z_in, axis=-1, keepdims=True) + EPS)
    normed = z_in * inv
    scaled = grad * gain
    back = inv * (scaled - normed * jnp.mean(scaled * normed, axis=-1, keepdims=True))
    return back, jnp.sum(grad * normed, axis=0, keepdims=True)


def bag(tree):
    if isinstance(tree, dict):
        return types.SimpleNamespace(**{key: bag(value) for key, value in tree.items()})
    return [bag(value) for value in tree] if isinstance(tree, list) else tree


def call_kernel(name, body, ins, outs, scratch, flops, collective_id=None):
    is_leaf = lambda value: isinstance(value, tuple)
    in_leaves, in_tree = jax.tree.flatten(ins, is_leaf=is_leaf)
    out_leaves, out_tree = jax.tree.flatten(outs, is_leaf=is_leaf)
    scr_leaves, scr_tree = jax.tree.flatten(scratch)
    first_scr = len(in_leaves) + len(out_leaves)

    def kernel(*refs):
        body(bag(in_tree.unflatten(refs[:len(in_leaves)])), bag(out_tree.unflatten(refs[len(in_leaves):first_scr])), bag(scr_tree.unflatten(refs[first_scr:])))

    results = pl.pallas_call(
        kernel,
        name=name,
        out_shape=[leaf[K0] for leaf in out_leaves],
        in_specs=[leaf[K1] for leaf in in_leaves],
        out_specs=[leaf[K1] for leaf in out_leaves],
        scratch_shapes=scr_leaves,
        compiler_params=pltpu.CompilerParams(collective_id=collective_id, has_side_effects=collective_id is not None, vmem_limit_bytes=LIMIT),
        cost_estimate=pl.CostEstimate(flops=int(flops), bytes_accessed=int(4e7), transcendentals=0),
    )(*[leaf[K0] for leaf in in_leaves])
    return bag(out_tree.unflatten(results))


def shape(dims, dtype=BF16):
    return jax.ShapeDtypeStruct(dims, dtype)


def sum_attention(side, attn, w_outs, hidden, grad_out, gain, w_gate, w_up, w_down):
    seq, depth = attn.ctx.shape
    width = gain.shape[K1]
    hidden_loc = w_gate.shape[K0]
    rows = seq // (side * side)

    def body(ins, outs, scr):
        torus = Torus(side)
        weights = Weights(ins.w_outs, scr.w, scr.w_sem, False)
        weights.start()
        rows_at = pl.ds(pl.multiple_of(torus.chip * rows, rows), rows)
        x_load = pltpu.make_async_copy(ins.hidden.at[torus.core, rows_at, :], scr.x_rows, scr.x_sem.at[K0])
        x_load.start()

        def load_weight(src, slot):
            load = pltpu.make_async_copy(src, scr.w_mlp.at[slot], scr.w_mlp_sem.at[slot])
            load.start()
            return load

        loads = {slot: load_weight(src, slot) for slot, src in ((K0, ins.w_down), (K2, ins.w_gate), (K3, ins.w_up))}
        wait = torus.signal_all()
        part = scr.sum.part
        steps = ReduceScatter(torus, scr.sum).steps(fill_partial(torus, part, [ins.ctx], weights))
        steps[K0]()
        wait()
        other_ctx = ins.ctx.at[:, :, :, pl.ds(depth // 2, depth // 2)]
        swaps = [(ins.w_down, outs.w_down), (ins.w_gate, outs.w_gate), (ins.w_up, outs.w_up), (other_ctx, outs.ctx_other), (ins.normed, outs.normed_other)]
        swap_start(torus, scr.swap_sems, swaps)

        def dy_load(group):
            at = pl.ds(group * side * rows, side * rows)
            return pltpu.make_async_copy(ins.grad_out.at[torus.core, at, :], scr.dy.at[group % 2], scr.dy_sem.at[group % 2])

        def grad_act(group):
            if group == 0:
                torus.arrive(outs.w_down, scr.swap_sems, 0)
                loads[K1] = load_weight(outs.w_down, K1)
                for slot in PAIR:
                    loads[slot].wait()
            dy_load(group).wait()
            for slot in PAIR:
                product = dot(scr.dy[group % 2], scr.w_mlp[slot], NT)
                scr.grad_act[slot, group] = product.reshape(side, rows, hidden_loc)
            if group + 2 < side:
                dy_load(group + 2).start()

        dy_load(0).start()
        dy_load(1).start()
        half = len(steps) // 3
        run(steps[1:half])
        run(steps[half:], [functools.partial(grad_act, group) for group in range(side)])
        for index, (slot, out) in enumerate(((K0, outs.w_gate), (K1, outs.w_up))):
            torus.arrive(out, scr.swap_sems, index + 1)
            loads[slot] = load_weight(out, slot)
        scr.pre[...] = jnp.zeros_like(scr.pre)
        gat = scr.all.gat
        own = (torus.y, torus.x)
        x_load.wait()
        for at in row_tiles(rows):
            resid = (scr.x_rows[at, :].astype(F32) + part[(*own, at, slice(None))].astype(F32)).astype(BF16)
            outs.h_rows[at, :] = resid
            z_in = resid.astype(F32)
            inv = lax.rsqrt(jnp.mean(z_in * z_in, axis=-1, keepdims=True) + EPS)
            gat[(*own, at, slice(None))] = (z_in * inv * ins.gain[...]).astype(BF16)
        gather = AllGather(torus, scr.all, False)
        gather.store = Store(torus, scr.all, plain_places(gather, outs.full))

        def products(step):
            if step == 0:
                for load in (loads[slot] for slot in (K0, K1, K2, K3)):
                    load.wait()
            for col in torus.colours:
                second = torus.wrap(col.second + gather.back[step])
                at_cols = pl.ds(col.index * (width // 2), width // 2)
                mixed = gat[second, :, :, at_cols] if col.index == 0 else gat[:, second, :, at_cols]
                mixed = mixed.reshape(side * rows, width // 2)

                def body(slot, carry, col=col, second=second, at_cols=at_cols, mixed=mixed):
                    term = dot(mixed, scr.w_mlp[slot, :, at_cols], NT).reshape(side, rows, hidden_loc)
                    if col.index == 0:
                        scr.pre[slot, second] += term
                    else:
                        scr.pre[slot, :, second] += term
                    return carry

                lax.fori_loop(0, 4, body, 0)
            for inner, count in ((0, step + 1), (1, step)):

                def block(index, carry, inner=inner):
                    shift = lax.rem(3 * index + 3 * lax.div(index * (index - 1), 2), side)
                    pair = (gather.back[step], shift) if inner == 0 else (shift, gather.back[step])
                    y_at, x_at = torus.wrap(torus.y + pair[K0]), torus.wrap(torus.x + pair[K1])
                    for core in PAIR:
                        gate, upper = scr.pre[2 - 2 * core, y_at, x_at], scr.pre[3 - 2 * core, y_at, x_at]
                        grad = scr.grad_act[core, y_at, x_at]
                        sigmoid_g = 1.0 / (1.0 + jnp.exp(-gate))
                        silu_g = gate * sigmoid_g
                        outs.acts[core][y_at, x_at] = (silu_g * upper).astype(BF16)
                        outs.gates[core][y_at, x_at] = (grad * upper * sigmoid_g * (1.0 + gate * (1.0 - sigmoid_g))).astype(BF16)
                        outs.ups[core][y_at, x_at] = (grad * silu_g).astype(BF16)
                    return carry

                lax.fori_loop(0, count, block, 0)

        run(gather.steps(products))
        gather.store.drain()
        swap_end(torus, scr.swap_sems, swaps, 3)
        torus.drain()

    dma = pltpu.SemaphoreType.DMA
    block = (side, side, rows, hidden_loc)
    ins = dict(ctx=(attn.ctx.reshape(side, side, rows, depth), VMEM), w_outs=[(weight, ANY) for weight in w_outs], hidden=(hidden, ANY), grad_out=(grad_out, ANY), gain=(gain, VMEM),
               normed=(attn.normed, ANY), w_gate=(w_gate, ANY), w_up=(w_up, ANY), w_down=(w_down, ANY))
    out, weight = (shape(block), VMEM), (shape((hidden_loc, width)), ANY)
    outs = dict(full=(shape((2, side, side, rows, width)), ANY), h_rows=(shape((rows, width)), VMEM), ctx_other=(shape((side, side, rows, depth // 2)), ANY), normed_other=(shape((seq, width)), ANY),
                w_gate=weight, w_up=weight, w_down=weight, acts=[out, out], gates=[out, out], ups=[out, out])
    scratch = dict(sum=rs_scratch(side, rows, width), all=ag_scratch(side, rows, width), w=pltpu.VMEM((depth, width), BF16), w_sem=dma((K2, K2)), swap_sems=[dma((5,)), dma((5,))],
                   x_rows=pltpu.VMEM((rows, width), BF16), x_sem=dma((K1,)), w_mlp=pltpu.VMEM((4, hidden_loc, width), BF16), w_mlp_sem=dma((4,)),
                   dy=pltpu.VMEM((2, side * rows, width), BF16), dy_sem=dma((K2,)), pre=pltpu.VMEM((4, *block), F32), grad_act=pltpu.VMEM((2, *block), F32))
    return call_kernel('sum_attention', body, ins, outs, scratch, 4e8, 1)


def sum_mlp(side, mlp, w_gates, w_ups, w_downs, grad_out, gain):
    depth = w_gates[K0].shape[K0]
    width = gain.shape[K1]
    rows = mlp.h_rows.shape[K0]
    seq = rows * side * side
    block = (side, side, rows, width)

    def body(ins, outs, scr):
        torus = Torus(side)
        weights = Weights(ins.w_in, scr.w, scr.w_sem, False)
        weights.start()
        weights_p = Weights(ins.w_downs, scr.wd, scr.wd_sem, False)
        weights_p.start()
        rows_at = pl.ds(pl.multiple_of(torus.chip * rows, rows), rows)
        dy_load = pltpu.make_async_copy(ins.grad_out.at[torus.core, rows_at, :], scr.dy_rows, scr.dy_sem.at[K0])
        dy_load.start()
        wait = torus.signal_all()
        steps = ReduceScatter(torus, scr.sum).steps(fill_partial(torus, scr.sum.part, ins.grads, weights))
        steps_p = ReduceScatter(torus, scr.sum_p).steps(fill_partial(torus, scr.sum_p.part, ins.acts, weights_p))
        steps[K0]()
        wait()

        turned = []

        def turn(index):
            kind, core = index // 2, index % 2
            src = (ins.grads[2 * core], ins.grads[2 * core + 1], ins.acts[core])[kind]
            slot = index % 2
            if index >= 2:
                turned[index - 2]()
            scr.turn[slot] = src[...].reshape(seq, depth).T
            at = pl.ds(kind * depth, depth)
            if core == 0:
                save = pltpu.make_async_copy(scr.turn.at[slot], outs.left.at[at, :], scr.turn_sem.at[kind])
                save.start()
                turned.append(save.wait)
            else:
                torus.send(scr.turn.at[slot], outs.left_other.at[at, :], scr.swap_sems, kind, torus.partner)
                turned.append(torus.pending.pop().wait_send)

        turns = [functools.partial(turn, index) for index in range(6)]
        fills = (K0, K3, 4, 10)
        early = [steps_p[index] for index in fills]
        rest_p = [step for index, step in enumerate(steps_p) if index not in fills]
        late = 22
        run(steps[1:late], early)
        for step in rest_p[:3]:
            step()
        run(steps[late:])
        own = (torus.y, torus.x)
        gain_total = jnp.zeros((1, width), F32)
        gat = scr.all.gat
        dy_load.wait()
        for at in row_tiles(rows):
            back, gain_part = rms_back(ins.h_rows[at, :].astype(F32), ins.gain[...], scr.sum.part[(*own, at, slice(None))].astype(F32))
            gain_total = gain_total + gain_part
            total = scr.dy_rows[at, :].astype(F32) + back
            outs.d_rows[at, :] = total
            gat[(*own, at, slice(None))] = total.astype(BF16)
        outs.gain[...] = gain_total
        gather = AllGather(torus, scr.all, False)
        gather.store = Store(torus, scr.all, plain_places(gather, outs.full), outs.own)
        run(gather.steps(), rest_p[3:], turns)
        for at in row_tiles(rows):
            outs.y_rows[at, :] = (ins.h_rows[at, :].astype(F32) + scr.sum_p.part[(*own, at, slice(None))].astype(F32)).astype(BF16)
        turned[4]()
        turned[5]()
        for kind in range(3):
            torus.arrive(outs.left_other.at[pl.ds(kind * depth, depth), :], scr.swap_sems, kind)
        gather.store.drain()
        torus.drain()

    dma = pltpu.SemaphoreType.DMA
    ins = dict(grads=[(grad, VMEM) for grad in (mlp.gates[K0], mlp.ups[K0], mlp.gates[K1], mlp.ups[K1])], acts=[(act, VMEM) for act in mlp.acts],
               w_in=[(weight, ANY) for weight in (w_gates[K0], w_ups[K0], w_gates[K1], w_ups[K1])], w_downs=[(weight, ANY) for weight in w_downs],
               h_rows=(mlp.h_rows, VMEM), grad_out=(grad_out, ANY), gain=(gain, VMEM))
    left = (shape((3 * depth, seq)), ANY)
    outs = dict(full=(shape((2, *block)), ANY), own=(shape(block), ANY), d_rows=(shape((rows, width), F32), VMEM), gain=(shape((1, width), F32), VMEM), y_rows=(shape((rows, width)), VMEM), left=left, left_other=left)
    scratch = dict(sum=rs_scratch(side, rows, width), sum_p=rs_scratch(side, rows, width), all=ag_scratch(side, rows, width), dy_rows=pltpu.VMEM((rows, width), BF16), dy_sem=dma((K1,)),
                   w=pltpu.VMEM((4 * depth, width), BF16), w_sem=dma((K2, 4)), wd=pltpu.VMEM((2 * depth, width), BF16), wd_sem=dma((K2, K2)),
                   turn=pltpu.VMEM((2, depth, seq), BF16), turn_sem=dma((K3,)), swap_sems=[dma((K3,)), dma((K3,))])
    return call_kernel('sum_mlp', body, ins, outs, scratch, 6e8, 2)


def sum_input(side, dqkv, w_qs, w_k, w_v, hidden, d_rows, gain, gain_mlp_part, normeds):
    seq, depth = dqkv.shape
    width = gain.shape[K1]
    rows = seq // (side * side)
    head = depth // 4
    half_side = side // 2
    tokens = seq // 2
    kv_width = w_k.shape[K1]
    per_kv = 2 * side * side * head // kv_width

    def body(ins, outs, scr):
        torus = Torus(side)
        kv_col = pl.multiple_of(lax.div(torus.chip * 2, per_kv) * head, head)
        weights = Weights([*ins.w_qs, ins.w_k.at[:, pl.ds(kv_col, head)], ins.w_v.at[:, pl.ds(kv_col, head)]], scr.w, scr.w_sem, True)
        weights.start()
        wait = torus.signal_all()
        part = scr.sum.part
        steps = ReduceScatter(torus, scr.sum).steps(fill_partial(torus, part, [ins.dqkv], weights))
        own = (torus.y, torus.x)
        gat = scr.all.gat
        gather = AllGather(torus, scr.all, True)

        def places(where, colour, half):
            chip = where[K0] * side + where[K1]
            tokens_at = pl.ds(pl.multiple_of(lax.rem(chip, 2) * tokens + colour * (tokens // 2), tokens // 2), tokens // 2)
            at = lax.div(chip, 2) * head
            src = gather.piece(gat, where, colour * 2, 2)
            return [(src.at[:, pl.ds(index * head, head)], outs.kv.at[half, tokens_at, pl.ds(pl.multiple_of(at + index * kv_width, head), head)]) for index in PAIR]

        gather.store = Store(torus, scr.all, places)
        rows_at = pl.ds(pl.multiple_of(torus.chip * rows, rows), rows)
        x_load = pltpu.make_async_copy(ins.hidden.at[torus.core, rows_at, :], scr.x_rows, scr.x_sem.at[K0])
        x_load.start()
        turns = Turner(ins.normeds[K0], outs.lefts[K0], scr).steps(8) + Turner(ins.normeds[K1], outs.lefts[K1], scr).steps(8)
        place = lax.rem(torus.x, 2)
        mate = torus.at_chip(torus.y, torus.x + 1 - 2 * place)
        kv_cols = pl.ds(2 * head, 2 * head)

        def mate_add():
            torus.arrive(scr.mate, scr.mate_sems, 0)
            mine = ins.dqkv[pl.ds(place * half_side, half_side), :, :, kv_cols]
            gat[own] = (mine.astype(F32) + scr.mate[...].astype(F32)).astype(BF16).reshape(tokens, 2 * head)

        steps[K0]()
        wait()
        swaps = [(ins.dqkv.at[:, :, :, pl.ds(head, head)], outs.q_other)]
        swap_start(torus, scr.swap_sems, swaps)
        torus.send(ins.dqkv.at[pl.ds((1 - place) * half_side, half_side), :, :, kv_cols], scr.mate, scr.mate_sems, 0, mate)
        for step in steps[1:5]:
            step()
        mate_add()
        run(steps[5:], gather.steps(), turns)
        x_load.wait()
        gain_total = jnp.zeros((1, width), F32)
        for at in row_tiles(rows):
            back, gain_part = rms_back(scr.x_rows[at, :].astype(F32), ins.gain[...], part[(*own, at, slice(None))].astype(F32))
            gain_total = gain_total + gain_part
            outs.rows[at, :] = (ins.d_rows[at, :] + back).astype(BF16)
        row = lax.broadcasted_iota(jnp.int32, (8, width), 0)
        extra = jnp.zeros((8, width), F32)
        for index, value in enumerate((gain_total, ins.gain_mlp[...])):
            for level in range(3):
                rounded = value.astype(BF16).astype(F32)
                extra = jnp.where(row == index * 3 + level, rounded, extra)
                value = value - rounded
        outs.rows[rows:rows + 8, :] = extra.astype(BF16)
        gather.store.drain()
        swap_end(torus, scr.swap_sems, swaps)
        torus.drain()

    dma = pltpu.SemaphoreType.DMA
    ins = dict(dqkv=(dqkv.reshape(side, side, rows, depth), VMEM), w_qs=[(weight, ANY) for weight in w_qs], w_k=(w_k, ANY), w_v=(w_v, ANY), hidden=(hidden, ANY), d_rows=(d_rows, VMEM), normeds=[(normed, ANY) for normed in normeds],
               gain=(gain, VMEM), gain_mlp=(gain_mlp_part, VMEM))
    outs = dict(rows=(shape((rows + 8, width)), VMEM), kv=(shape((2, seq, 2 * kv_width)), ANY), lefts=[(shape((width, seq)), ANY)] * 2, q_other=(shape((side, side, rows, head)), ANY))
    scratch = dict(sum=rs_scratch(side, rows, width), all=ag_scratch(side, tokens, 2 * head, 2), x_rows=pltpu.VMEM((rows, width), BF16), x_sem=dma((K1,)), **turner_scratch(seq, min(256, width // 8)), w=pltpu.VMEM((width, depth), BF16), w_sem=dma((K2, 4)),
                   mate=pltpu.VMEM((half_side, side, rows, 2 * head), BF16), mate_sems=[dma((K1,)), dma((K1,))], swap_sems=[dma((K1,)), dma((K1,))])
    return call_kernel('sum_input', body, ins, outs, scratch, 3e8, 3)


def scores_softmax(qkv, seg_row, seg_col, head_index, tile_index, tile):
    reach = (tile_index + 1) * tile
    queries = qkv[tile_index * tile:reach, head_index * HEAD_DIM:(head_index + 1) * HEAD_DIM]
    scores = dot(qkv[:reach, 2 * HEAD_DIM:3 * HEAD_DIM], queries, NT) * HEAD_DIM ** -0.5
    key_at = lax.broadcasted_iota(jnp.int32, (reach, tile), 0)
    query_at = lax.broadcasted_iota(jnp.int32, (reach, tile), 1) + tile_index * tile
    allowed = (key_at <= query_at) & (seg_col[:reach, :] == seg_row[:, tile_index * tile:reach])
    scores = jnp.where(allowed, scores, -1e30)
    weights = jnp.exp(scores - jnp.max(scores, axis=0, keepdims=True))
    return weights * (1.0 / jnp.sum(weights, axis=0, keepdims=True)), queries


def segments(seg_ref):
    core = lax.rem(lax.axis_index('tp'), 2)
    seg_row = seg_ref[pl.ds(core, 1), :].astype(F32)
    return seg_row, jnp.broadcast_to(seg_row, (8, seg_row.shape[K1])).T[:, :1]


def attention_forward(hidden, seg_ids, gain, w_q, w_k, w_v, w_o, per_kv):
    seq, width = hidden.shape[1:]
    chunk = seq // 4
    tile = min(256, seq)
    depth = 4 * HEAD_DIM

    def body(ins, outs, scr):
        tp_idx = lax.axis_index('tp')
        core = lax.rem(tp_idx, 2)
        kv_col = pl.multiple_of(lax.div(tp_idx, per_kv) * HEAD_DIM, HEAD_DIM)
        partner = dict(tp=tp_idx + 1 - 2 * core)
        barrier = pltpu.get_barrier_semaphore()
        pl.semaphore_signal(barrier, inc=1, device_id=partner, device_id_type=MESH)
        loads = []
        for index in range(4):
            at = pl.ds(index * chunk, chunk)
            loads.append(pltpu.make_async_copy(ins.hidden.at[core, at, :], scr.x.at[at, :], scr.x_sem.at[index]))

        def w_cols(index):
            return scr.w.at[:, pl.ds(index * HEAD_DIM, HEAD_DIM)]

        for index, ref in ((0, ins.w_q), (2, ins.w_k.at[:, pl.ds(kv_col, HEAD_DIM)]), (3, ins.w_v.at[:, pl.ds(kv_col, HEAD_DIM)])):
            loads.append(pltpu.make_async_copy(ref, w_cols(index), scr.w_sem.at[index]))
        for load in loads:
            load.start()
        pl.semaphore_wait(barrier, 1)
        swaps = [(ins.w_q, w_cols(1)), (ins.w_o, outs.w_o), (ins.w_q, outs.w_q)]
        copies = []
        for index, (src, dst) in enumerate(swaps):
            copies.append(pltpu.make_async_remote_copy(src, dst, scr.swap_sems[K0].at[index], scr.swap_sems[K1].at[index], device_id=partner, device_id_type=MESH))
            copies[index].start()
        stores = []
        for index in range(4):
            loads[index].wait()

            def normalize(step, carry, index=index):
                at = pl.ds(pl.multiple_of(index * chunk + step * 16, 16), 16)
                x_float = scr.x[at, :].astype(F32)
                inv = lax.rsqrt(jnp.mean(x_float * x_float, axis=-1, keepdims=True) + EPS)
                scr.normed[at, :] = (x_float * inv * ins.gain[...]).astype(BF16)
                return carry

            lax.fori_loop(0, chunk // 16, normalize, 0)
            at = pl.ds(index * chunk, chunk)
            store = pltpu.make_async_copy(scr.normed.at[at, :], outs.normed.at[at, :], scr.out_sem.at[index])
            store.start()
            stores.append(store)
            if index == 0:
                for load in loads[4:]:
                    load.wait()
                copies[K0].wait_recv()
            outs.qkv[at, :] = dot(scr.normed[at, :], scr.w[...], NN).astype(BF16)
        seg_row, seg_col = segments(ins.seg)
        values_t = outs.qkv[:, 3 * HEAD_DIM:].T
        for head_index in PAIR:
            for tile_index in range(seq // tile):
                probs, _ = scores_softmax(outs.qkv, seg_row, seg_col, head_index, tile_index, tile)
                ctx_t = dot(values_t[:, :(tile_index + 1) * tile], probs.astype(BF16), NN)
                outs.ctx[tile_index * tile:(tile_index + 1) * tile, head_index * HEAD_DIM:(head_index + 1) * HEAD_DIM] = ctx_t.T.astype(BF16)
        for store in stores:
            store.wait()
        copies[K0].wait_send()
        copies[K1].wait()
        copies[K2].wait()

    dma = pltpu.SemaphoreType.DMA
    ins = dict(hidden=(hidden, ANY), seg=(seg_ids, VMEM), gain=(gain, VMEM), w_q=(w_q, ANY), w_o=(w_o, ANY), w_k=(w_k, ANY), w_v=(w_v, ANY))
    outs = dict(normed=(shape((seq, width)), ANY), qkv=(shape((seq, depth)), VMEM), ctx=(shape((seq, 2 * HEAD_DIM)), VMEM), w_q=(shape(w_q.shape), ANY), w_o=(shape(w_o.shape), ANY))
    scratch = dict(swap_sems=[dma((K3,)), dma((K3,))], x=pltpu.VMEM((seq, width), BF16), normed=pltpu.VMEM((seq, width), BF16), w=pltpu.VMEM((width, depth), BF16), x_sem=dma((4,)), w_sem=dma((4,)), out_sem=dma((4,)))
    return call_kernel('attention_forward', body, ins, outs, scratch, 5e9, 4)


def attention_backward(resid, seg_ids, w_outs, qkv, token):
    seq, width = resid.shape
    chunk = seq // 4
    tile = min(256, seq)
    depth = 4 * HEAD_DIM

    def body(ins, outs, scr):
        loads = []
        for index in PAIR:
            at = pl.ds(index * HEAD_DIM, HEAD_DIM)
            loads.append(pltpu.make_async_copy(ins.w_outs[index], scr.w.at[at, :], scr.w_sem.at[index]))
        for index in range(4):
            at = pl.ds(index * chunk, chunk)
            loads.append(pltpu.make_async_copy(ins.resid.at[at, :], scr.resid.at[at, :], scr.in_sem.at[index]))
        for load in loads:
            load.start()
        for load in loads[:2]:
            load.wait()
        for index in range(4):
            loads[2 + index].wait()
            at = pl.ds(index * chunk, chunk)
            scr.grad_ctx[at, :] = dot(scr.resid[at, :], scr.w[...], NT).astype(BF16)
        seg_row, seg_col = segments(ins.seg)
        keys_t = ins.qkv[:, 2 * HEAD_DIM:3 * HEAD_DIM].T
        scr.grad_k[...] = jnp.zeros_like(scr.grad_k)
        scr.grad_v[...] = jnp.zeros_like(scr.grad_v)
        for head_index in PAIR:
            cols = slice(head_index * HEAD_DIM, (head_index + 1) * HEAD_DIM)
            for tile_index in range(seq // tile):
                reach = (tile_index + 1) * tile
                rows = slice(tile_index * tile, reach)
                probs, queries = scores_softmax(ins.qkv, seg_row, seg_col, head_index, tile_index, tile)
                grad_ctx = scr.grad_ctx[rows, cols]
                grad_probs = dot(ins.qkv[:reach, 3 * HEAD_DIM:], grad_ctx, NT)
                centre = jnp.sum(grad_probs * probs, axis=0, keepdims=True)
                grad_scores = (probs * (grad_probs - centre) * HEAD_DIM ** -0.5).astype(BF16)
                scr.grad_v[:reach, :] += dot(probs.astype(BF16), grad_ctx, NN)
                scr.grad_k[:reach, :] += dot(grad_scores, queries, NN)
                outs.dqkv[rows, cols] = dot(keys_t[:, :reach], grad_scores, NN).T.astype(BF16)
        outs.dqkv[:, 2 * HEAD_DIM:3 * HEAD_DIM] = scr.grad_k[...].astype(BF16)
        outs.dqkv[:, 3 * HEAD_DIM:] = scr.grad_v[...].astype(BF16)

    dma = pltpu.SemaphoreType.DMA
    ins = dict(resid=(resid, ANY), seg=(seg_ids, VMEM), w_outs=[(weight, ANY) for weight in w_outs], qkv=(qkv, VMEM), token=(token, ANY))
    outs = dict(dqkv=(shape((seq, depth)), VMEM))
    scratch = dict(resid=pltpu.VMEM((seq, width), BF16), w=pltpu.VMEM((2 * HEAD_DIM, width), BF16), grad_ctx=pltpu.VMEM((seq, 2 * HEAD_DIM), BF16),
                   grad_k=pltpu.VMEM((seq, HEAD_DIM), F32), grad_v=pltpu.VMEM((seq, HEAD_DIM), F32), w_sem=dma((K2,)), in_sem=dma((4,)))
    return call_kernel('attention_backward', body, ins, outs, scratch, 4e9).dqkv


def weight_grads_mlp(mixed_full, grad_out, resid_full, lefts, ctxs):
    seq, width = grad_out.shape[1:]
    depth, head = lefts[K0].shape[K0] // 3, ctxs[K1].shape[K1]
    tile = min(512, width)

    def kernel(m_ref, dy_ref, dh_ref, left_own, left_other, ctx_own, ctx_other, out_gate, out_up, out_down, out_o, token, ctx_t):
        core = lax.rem(lax.axis_index('tp'), 2)

        @pl.when(pl.program_id(0) == 0)
        def _():
            for half, ref in enumerate((ctx_own, ctx_other)):
                ctx_t[half] = ref[:, :head].T

        token[...] = jnp.zeros_like(token)
        halves = (core, 1 - core)
        lefts = (left_own, left_other)

        def product(base, size, ref):
            own, other = (dot(left[base:base + size, :], ref[half], NN) for left, half in zip(lefts, halves))
            return own + other

        both = product(0, 2 * depth, m_ref)
        out_gate[...] = both[:depth]
        out_up[...] = both[depth:]
        out_down[...] = product(2 * depth, depth, dy_ref)
        out_o[...] = dot(ctx_t[K0], dh_ref[core], NN) + dot(ctx_t[K1], dh_ref[1 - core], NN)

    slab = pl.BlockSpec((2, seq, tile), lambda step: (0, 0, step))
    out = lambda size: pl.BlockSpec((size, tile), lambda step: (0, step))
    token = (8, HEAD_DIM)
    return pl.pallas_call(
        kernel,
        name='weight_grads_mlp',
        grid=(width // tile,),
        out_shape=[shape((depth, width), F32)] * 3 + [shape((head, width), F32), shape(token, F32)],
        in_specs=[slab] * 3 + [VMEM] * 4,
        out_specs=[out(depth)] * 3 + [out(head), pl.BlockSpec(token, lambda step: (0, 0))],
        scratch_shapes=[pltpu.VMEM((2, head, seq), BF16)],
        compiler_params=pltpu.CompilerParams(vmem_limit_bytes=LIMIT),
        cost_estimate=pl.CostEstimate(flops=int(18e9), bytes_accessed=int(6e7), transcendentals=0),
    )(mixed_full, grad_out, resid_full, *lefts, *ctxs)


def weight_grads_qkv(lefts, kv_full, grads_q):
    width, seq = lefts[K0].shape
    head = grads_q[K1].shape[K1]
    kv_width = kv_full.shape[K2] // 2
    tile = min(256, width)

    def kernel(a_own, a_other, kv_ref, q_own, q_other, out_q, out_k, out_v):
        core = lax.rem(lax.axis_index('tp'), 2)
        for index, out in enumerate((out_k, out_v)):
            at = pl.ds(index * kv_width, kv_width)
            out[...] = dot(a_own[...], kv_ref[core, :, at], NN) + dot(a_other[...], kv_ref[1 - core, :, at], NN)
        out_q[...] = dot(a_own[...], q_own[:, :head], NN) + dot(a_other[...], q_other[...], NN)

    slab = pl.BlockSpec((tile, seq), lambda step: (step, 0))
    out = lambda size: pl.BlockSpec((tile, size), lambda step: (step, 0))
    return pl.pallas_call(
        kernel,
        name='weight_grads_qkv',
        grid=(width // tile,),
        out_shape=[shape((width, size), F32) for size in (head, kv_width, kv_width)],
        in_specs=[slab] * 2 + [VMEM] * 3,
        out_specs=[out(size) for size in (head, kv_width, kv_width)],
        compiler_params=pltpu.CompilerParams(vmem_limit_bytes=LIMIT),
        cost_estimate=pl.CostEstimate(flops=int(27e9), bytes_accessed=int(6e7), transcendentals=0),
    )(*lefts, kv_full, *grads_q)


def in_place(gathered, rows):
    blocks, _, width = gathered.shape
    slots = 8

    def kernel(src, dst, buf, in_sem, out_sem):
        def load(index):
            return pltpu.make_async_copy(src.at[index, pl.ds(0, rows), :], buf.at[index % slots], in_sem.at[index % slots])

        def store(index):
            return pltpu.make_async_copy(buf.at[index % slots], dst.at[index % 2, index // 2], out_sem.at[index % slots])

        ahead = slots // 2
        for index in range(blocks + ahead):
            if index < blocks:
                if index >= slots:
                    store(index - slots).wait()
                load(index).start()
            if index >= ahead:
                load(index - ahead).wait()
                store(index - ahead).start()
        for index in range(blocks - slots, blocks):
            store(index).wait()

    return pl.pallas_call(
        kernel,
        name='in_place',
        out_shape=shape((2, blocks // 2, rows, width)),
        in_specs=[ANY],
        out_specs=ANY,
        scratch_shapes=[pltpu.VMEM((slots, rows, width), BF16), pltpu.SemaphoreType.DMA((slots,)), pltpu.SemaphoreType.DMA((slots,))],
        compiler_params=pltpu.CompilerParams(vmem_limit_bytes=LIMIT),
        cost_estimate=pl.CostEstimate(flops=int(2e7), bytes_accessed=int(2e7), transcendentals=0),
    )(gathered)


def solution(mesh):
    tp_size = mesh.shape['tp']
    chips = tp_size // 2
    side = math.isqrt(chips)

    def device_step(hidden, seg_ids, grad_out, gain_attn, gain_mlp, w_q, w_k, w_v, w_o, w_gate, w_up, w_down):
        seq_len, width = hidden.shape[1:]
        kv_heads = w_k.shape[K1] // HEAD_DIM
        per_kv = tp_size // kv_heads
        rows = seq_len // chips

        def flat(value):
            return value.reshape(seq_len, value.shape[-1])

        gain_attn_row = gain_attn[None, :]
        gain_mlp_row = gain_mlp[None, :]

        attn = attention_forward(hidden, seg_ids, gain_attn_row, w_q, w_k, w_v, w_o, per_kv)
        w_qs, w_outs = (w_q, attn.w_q), (w_o, attn.w_o)
        mlp = sum_attention(side, attn, w_outs, hidden, grad_out, gain_mlp_row, w_gate.T, w_up.T, w_down)
        mixed_full = mlp.full.reshape(2, seq_len, width)
        second = sum_mlp(side, mlp, (w_gate.T, mlp.w_gate), (w_up.T, mlp.w_up), (w_down, mlp.w_down), grad_out, gain_mlp_row)
        resid_full = second.full.reshape(2, seq_len, width)

        y_out = in_place(lax.all_gather(second.y_rows, 'tp'), rows).reshape(2, seq_len, width)
        grad_gate_t, grad_up_t, grad_w_down, grad_w_o, token = weight_grads_mlp(mixed_full, grad_out, resid_full, (second.left, second.left_other), (attn.ctx, flat(mlp.ctx_other)))
        dqkv = attention_backward(flat(second.own), seg_ids, w_outs, attn.qkv, token)
        third = sum_input(side, dqkv, w_qs, w_k, w_v, hidden, second.d_rows, gain_attn_row, second.gain, (attn.normed, mlp.normed_other))

        gathered = lax.all_gather(third.rows, 'tp')
        grad_in = in_place(gathered, rows).reshape(2, seq_len, width)
        gain_grads = jnp.sum(gathered[:, rows:].astype(F32), axis=0)
        grad_gain_attn = gain_grads[K0] + gain_grads[K1] + gain_grads[K2]
        grad_gain_mlp = gain_grads[K3] + gain_grads[4] + gain_grads[5]
        grad_w_q, grad_w_k, grad_w_v = weight_grads_qkv(third.lefts, third.kv, (dqkv, flat(third.q_other)))
        return (y_out, grad_in, grad_gain_attn, grad_gain_mlp, grad_w_q, grad_w_k, grad_w_v, grad_w_o, grad_gate_t.T, grad_up_t.T, grad_w_down)

    spec_act = P('data', None, None)
    spec_rows = P('data', None)
    spec_gain = P(None)
    spec_cols = P(None, 'tp')
    spec_tprows = P('tp', None)
    spec_whole = P(None, None)
    spec_stack = P(('data', 'tp'), None)
    in_specs = (spec_act, spec_rows, spec_act, spec_gain, spec_gain, spec_cols, spec_whole, spec_whole, spec_tprows, spec_cols, spec_cols, spec_tprows)
    out_specs = (spec_act, spec_act, P('data'), P('data'), P('data', 'tp'), spec_rows, spec_rows, spec_stack, P('data', 'tp'), P('data', 'tp'), spec_stack)
    return jax.shard_map(device_step, mesh=mesh, in_specs=in_specs, out_specs=out_specs, check_vma=False)
```

```python
import functools
import math
import types
import jax
import jax.numpy as jnp
from jax import lax
from jax.experimental import pallas as pl
from jax.experimental.pallas import tpu as pltpu
from jax.sharding import PartitionSpec as P

HEAD_DIM = 128
EPS = 1e-5
MESH = pl.DeviceIdType.MESH
F32 = jnp.float32
BF16 = jnp.bfloat16
LIMIT = 63 * 2 ** 20
K0, K1, K2, K3 = range(4)
PAIR = range(2)
ANY = pl.BlockSpec(memory_space=pl.ANY)
VMEM = pl.BlockSpec(memory_space=pltpu.VMEM)


def dot(lhs, rhs, dims):
    return lax.dot_general(lhs, rhs, (dims, ((), ())), preferred_element_type=F32)


NN = ((1,), (0,))
NT = ((1,), (1,))


SIGNS = (1, -1)


class Colour:
    def __init__(self, index, first, second):
        self.index, self.first, self.second = index, first, second


class Torus:
    def __init__(self, side):
        self.side = side
        tp_idx = lax.axis_index('tp')
        self.core = lax.rem(tp_idx, 2)
        self.chip = lax.div(tp_idx, 2)
        self.x = lax.rem(self.chip, side)
        self.y = lax.div(self.chip, side)
        self.partner = {'tp': self.chip * 2 + (1 - self.core)}
        self.colours = (Colour(0, self.x, self.y), Colour(1, self.y, self.x))
        self.pending = []

    def wrap(self, pos):
        return lax.rem(pos + 2 * self.side, self.side)

    def at_chip(self, y_at, x_at):
        return {'tp': (y_at * self.side + x_at) * 2 + self.core}

    def block(self, col, second, first):
        return (second, first) if col.index == 0 else (first, second)

    def peer1(self, col, shift):
        return self.at_chip(*self.block(col, col.second, self.wrap(col.first + shift)))

    def peer2(self, col, shift):
        return self.at_chip(*self.block(col, self.wrap(col.second + shift), col.first))

    def signal_all(self):
        barrier = pltpu.get_barrier_semaphore()
        peers = [self.partner]
        peers += [self.at_chip(self.y, self.wrap(self.x + shift)) for shift in SIGNS]
        peers += [self.at_chip(self.wrap(self.y + shift), self.x) for shift in SIGNS]
        for peer in peers:
            pl.semaphore_signal(barrier, inc=1, device_id=peer, device_id_type=MESH)
        return lambda: pl.semaphore_wait(barrier, len(peers))

    def send(self, src, dst, sems, index, device):
        copy = pltpu.make_async_remote_copy(src, dst, sems[K0].at[index], sems[K1].at[index], device_id=device, device_id_type=MESH)
        copy.start()
        self.pending.append(copy)

    def arrive(self, dst, sems, index):
        pltpu.make_async_remote_copy(dst, dst, sems[K0].at[index], sems[K1].at[index], device_id=self.partner, device_id_type=MESH).wait_recv()

    def drain(self):
        for copy in self.pending:
            copy.wait_send()


R1, R2, R3, S1, S2, S3 = range(6)
RS_COUNTS = (16, 16, 16, 4, 4, 4)
H1, H2, F1, F2 = range(4)
AG_COUNTS = (8, 32, 4, 16)


class ReduceScatter:
    SHIFTS = (2, 1, 3, 0)

    def __init__(self, torus, scr):
        self.torus, self.part, self.scr = torus, scr.part, scr
        self.quarter = scr.part.shape[K3] // 4

    def buf(self, kind, index):
        return self.scr.bufs[kind].at[index]

    def sems(self, kind):
        return self.scr.out_sems[kind], self.scr.in_sems[kind]

    def cols(self, col, half):
        return pl.ds((col.index * 2 + half) * self.quarter, self.quarter)

    def piece(self, where, at_cols):
        return self.part.at[(*where, slice(None), at_cols)]

    def send(self, where, at_cols, kind, index, peer):
        self.torus.send(self.piece(where, at_cols), self.buf(kind, index), self.sems(kind), index, peer)

    def add(self, where, at_cols, *kinds):
        total = self.part[(*where, slice(None), at_cols)].astype(F32)
        for kind, index in kinds:
            self.torus.arrive(self.buf(kind, index), self.sems(kind), index)
            total = total + self.buf(kind, index)[...].astype(F32)
        self.part[(*where, slice(None), at_cols)] = total.astype(BF16)

    def each(self, step):
        wrap = self.torus.wrap
        for col in self.torus.colours:
            second = wrap(col.second + self.SHIFTS[step])
            for way, sign in enumerate(SIGNS):
                yield col, second, way, sign, (col.index * 2 + way) * 4 + step

    def far(self, step):
        for col, second, way, sign, index in self.each(step):
            where = self.torus.block(col, second, self.torus.wrap(col.first + 2))
            self.send(where, self.cols(col, way), R1, index, self.torus.peer1(col, sign))

    def near(self, step):
        for col, second, way, sign, index in self.each(step):
            where = self.torus.block(col, second, self.torus.wrap(col.first + sign))
            self.send(where, self.cols(col, 1 - way), R2, index, self.torus.peer1(col, sign))

    def relay(self, step):
        for col, second, way, sign, index in self.each(step):
            where = self.torus.block(col, second, self.torus.wrap(col.first + sign))
            self.add(where, self.cols(col, way), (R1, index))
            self.send(where, self.cols(col, way), R3, index, self.torus.peer1(col, sign))

    def end(self, step):
        for col, second, way, sign, index in self.each(step):
            where = self.torus.block(col, second, col.first)
            other = (col.index * 2 + 1 - way) * 4 + step
            self.add(where, self.cols(col, way), (R2, other), (R3, index))

    def far2(self):
        for col in self.torus.colours:
            for way, sign in enumerate(SIGNS):
                where = self.torus.block(col, self.torus.wrap(col.second + 2), col.first)
                self.send(where, self.cols(col, way), S1, col.index * 2 + way, self.torus.peer2(col, sign))

    def near2(self, way):
        for col in self.torus.colours:
            where = self.torus.block(col, self.torus.wrap(col.second + SIGNS[way]), col.first)
            self.send(where, self.cols(col, 1 - way), S2, col.index * 2 + way, self.torus.peer2(col, SIGNS[way]))

    def relay2(self, way):
        for col in self.torus.colours:
            index = col.index * 2 + way
            where = self.torus.block(col, self.torus.wrap(col.second + SIGNS[way]), col.first)
            self.add(where, self.cols(col, way), (S1, index))
            self.send(where, self.cols(col, way), S3, index, self.torus.peer2(col, SIGNS[way]))

    def end2(self):
        for col in self.torus.colours:
            where = self.torus.block(col, col.second, col.first)
            for way in PAIR:
                self.add(where, self.cols(col, way), (S2, col.index * 2 + 1 - way), (S3, col.index * 2 + way))

    def steps(self, fill):
        call = functools.partial
        return [call(fill, K2), call(self.far, K0), call(self.far, K1), call(fill, K1), call(fill, K3),
                call(self.near, K0), call(self.relay, K0), call(self.near, K1), call(self.far, K2), call(self.relay, K1),
                call(fill, K0), call(self.near, K2), call(self.far, K3), call(self.end, K0), self.far2,
                call(self.relay, K2), call(self.near, K3), call(self.end, K1), call(self.near2, K0), call(self.relay2, K0),
                call(self.relay, K3), call(self.end, K2), call(self.near2, K1), call(self.relay2, K1), call(self.end, K3),
                self.end2]


class AllGather:
    def __init__(self, torus, scr, by_rows):
        self.torus, self.gat, self.scr, self.by_rows, self.store = torus, scr.gat, scr, by_rows, None
        self.quarter = scr.gat.shape[2 if by_rows else 3] // 4
        self.back = (0, torus.side - 1, 1, 2)

    def sems(self, kind):
        return self.scr.out_sems[kind], self.scr.in_sems[kind]

    def piece(self, ref, where, first, count):
        at = pl.ds(first * self.quarter, count * self.quarter)
        return ref.at[(*where, at, slice(None))] if self.by_rows else ref.at[(*where, slice(None), at)]

    def half(self, col, where, half):
        return self.piece(self.gat, where, col.index * 2 + half, 1)

    def own2(self, turn):
        for col in self.torus.colours:
            where = self.torus.block(col, col.second, col.first)
            for way, sign in enumerate(SIGNS):
                at = self.half(col, where, way if turn == 0 else 1 - way)
                self.torus.send(at, at, self.sems(H1), (col.index * 2 + way) * 2 + turn, self.torus.peer2(col, sign))

    def send1(self, step, turn):
        for col in self.torus.colours:
            where = self.torus.block(col, self.torus.wrap(col.second + self.back[step]), col.first)
            for way, sign in enumerate(SIGNS):
                at = self.half(col, where, way if turn == 0 else 1 - way)
                self.torus.send(at, at, self.sems(H2), ((col.index * 2 + way) * 4 + step) * 2 + turn, self.torus.peer1(col, sign))

    def arrive2(self, way, turn):
        sign = SIGNS[way]
        for col in self.torus.colours:
            where = self.torus.block(col, self.torus.wrap(col.second - sign), col.first)
            at = self.half(col, where, way if turn == 0 else 1 - way)
            self.torus.arrive(at, self.sems(H1), (col.index * 2 + way) * 2 + turn)
            if turn == 0:
                self.torus.send(at, at, self.sems(F1), col.index * 2 + way, self.torus.peer2(col, sign))

    def relayed2(self):
        for col in self.torus.colours:
            where = self.torus.block(col, self.torus.wrap(col.second + 2), col.first)
            for way in PAIR:
                self.torus.arrive(self.half(col, where, way), self.sems(F1), col.index * 2 + way)

    def arrive1(self, step, turn):
        for col in self.torus.colours:
            second = self.torus.wrap(col.second + self.back[step])
            for way, sign in enumerate(SIGNS):
                where = self.torus.block(col, second, self.torus.wrap(col.first - sign))
                at = self.half(col, where, way if turn == 0 else 1 - way)
                self.torus.arrive(at, self.sems(H2), ((col.index * 2 + way) * 4 + step) * 2 + turn)
                if turn == 0:
                    self.torus.send(at, at, self.sems(F2), (col.index * 2 + way) * 4 + step, self.torus.peer1(col, sign))

    def relayed1(self, step):
        for col in self.torus.colours:
            second = self.torus.wrap(col.second + self.back[step])
            for way in PAIR:
                where = self.torus.block(col, second, self.torus.wrap(col.first + 2))
                self.torus.arrive(self.half(col, where, way), self.sems(F2), (col.index * 2 + way) * 4 + step)

    def keep(self, step, firsts):
        for col in self.torus.colours:
            for shift in firsts:
                where = self.torus.block(col, self.torus.wrap(col.second + self.back[step]), self.torus.wrap(col.first + shift))
                self.store.keep(where, col.index, lambda ref, where=where, col=col: self.piece(ref, where, col.index * 2, 2))

    def steps(self, whole=None):
        call = functools.partial
        whole = whole or (lambda step: None)
        here, beside, across = (K0,), (K1, self.torus.side - 1), (K2,)
        result = []
        for turn in PAIR:
            result += [call(self.own2, turn), call(self.send1, K0, turn)]
        result += [call(self.keep, K0, here), call(self.arrive2, K0, K0), call(self.arrive2, K1, K0)]
        for way in PAIR:
            step = way + K1
            result += [call(self.arrive2, way, K1), call(self.send1, step, K0), call(self.send1, step, K1), call(self.keep, step, here)]
        result += [call(self.arrive1, K0, K0), self.relayed2, call(self.send1, K3, K0), call(self.send1, K3, K1), call(self.keep, K3, here),
                   call(self.arrive1, K0, K1), call(self.keep, K0, beside), call(self.arrive1, K1, K0), call(self.arrive1, K2, K0),
                   call(self.relayed1, K0), call(self.keep, K0, across), call(whole, K0)]
        for step in (K1, K2):
            result += [call(self.arrive1, step, K1), call(self.keep, step, beside)]
        result += [call(self.arrive1, K3, K0)]
        for step in (K1, K2):
            result += [call(self.relayed1, step), call(self.keep, step, across), call(whole, step)]
        return result + [call(self.arrive1, K3, K1), call(self.keep, K3, beside), call(self.relayed1, K3), call(self.keep, K3, across), call(whole, K3)]


class Store:
    def __init__(self, torus, scr, places, own=None):
        self.torus, self.scr, self.places, self.own = torus, scr, places, own
        self.stores = []

    def slot(self, where, colour, index):
        return ((index * 2 + colour) * self.torus.side + where[K0]) * self.torus.side + where[K1]

    def keep(self, where, colour, piece):
        for index, (src, dst) in enumerate(self.places(where, colour, self.torus.core)):
            slot = self.slot(where, colour, index)
            pairs = [(self.scr.full_sem, dst)]
            if self.own is not None:
                pairs.append((self.scr.own_sem, piece(self.own)))
            for sem, ref in pairs:
                store = pltpu.make_async_copy(src, ref, sem.at[slot])
                store.start()
                self.stores.append(store)
            self.torus.send(src, dst, self.scr.cross_sems, slot, self.torus.partner)

    def drain(self):
        for store in self.stores:
            store.wait()
        side = self.torus.side
        for colour in PAIR:
            for y_at in range(side):
                for x_at in range(side):
                    for index, (_, dst) in enumerate(self.places((y_at, x_at), colour, 1 - self.torus.core)):
                        self.torus.arrive(dst, self.scr.cross_sems, self.slot((y_at, x_at), colour, index))


def plain_places(gather, full):
    return lambda where, colour, half: [(gather.piece(gather.gat, where, colour * 2, 2), gather.piece(full.at[half], where, colour * 2, 2))]


def rs_scratch(side, rows, width):
    dma = pltpu.SemaphoreType.DMA
    return dict(
        part=pltpu.VMEM((side, side, rows, width), BF16),
        bufs=[pltpu.VMEM((count, rows, width // 4), BF16) for count in RS_COUNTS],
        out_sems=[dma((count,)) for count in RS_COUNTS],
        in_sems=[dma((count,)) for count in RS_COUNTS],
    )


def ag_scratch(side, rows, width, places=1):
    dma = pltpu.SemaphoreType.DMA
    blocks = 2 * side * side * places
    return dict(
        gat=pltpu.VMEM((side, side, rows, width), BF16),
        out_sems=[dma((count,)) for count in AG_COUNTS],
        in_sems=[dma((count,)) for count in AG_COUNTS],
        full_sem=dma((blocks,)),
        own_sem=dma((blocks,)),
        cross_sems=[dma((blocks,)), dma((blocks,))],
    )


class Weights:
    def __init__(self, refs, buf, sem, by_rows):
        self.refs, self.buf, self.sem, self.by_rows = refs, buf, sem, by_rows
        self.copies = [[], []]

    def start(self):
        for colour in PAIR:
            for index, ref in enumerate(self.refs):
                if self.by_rows:
                    half, depth = ref.shape[K0] // 2, ref.shape[K1]
                    rows, cols = pl.ds(colour * half, half), pl.ds(index * depth, depth)
                    copy = pltpu.make_async_copy(ref.at[rows, :], self.buf.at[rows, cols], self.sem.at[colour, index])
                else:
                    half, depth = ref.shape[K1] // 2, ref.shape[K0]
                    rows, cols = pl.ds(index * depth, depth), pl.ds(colour * half, half)
                    copy = pltpu.make_async_copy(ref.at[:, cols], self.buf.at[rows, cols], self.sem.at[colour, index])
                copy.start()
                self.copies[colour].append(copy)

    def wait(self, colour):
        for copy in self.copies[colour]:
            copy.wait()
        self.copies[colour] = []


def fill_partial(torus, part, lhs, weights):
    rows, width = part.shape[2:]
    tile = min(512, width // 2)

    def fill(shift):
        for col in torus.colours:
            weights.wait(col.index)
            first = torus.wrap(col.first + shift)
            left = []
            for ref in lhs:
                depth = ref.shape[K3]
                value = ref[:, first] if col.index == 0 else ref[first]
                left.append((value.reshape(torus.side * rows, depth), depth))

            def body(step, carry, col=col, first=first, left=left):
                at = pl.ds(pl.multiple_of(col.index * (width // 2) + step * tile, tile), tile)
                total = None
                base = 0
                for value, depth in left:
                    if weights.by_rows:
                        term = dot(value, weights.buf[at, base:base + depth], NT)
                    else:
                        term = dot(value, weights.buf[base:base + depth, at], NN)
                    total = term if total is None else total + term
                    base += depth
                total = total.astype(BF16).reshape(torus.side, rows, tile)
                if col.index == 0:
                    part[:, first, :, at] = total
                else:
                    part[first, :, :, at] = total
                return carry

            lax.fori_loop(0, (width // 2) // tile, body, 0)

    return fill


def run(*lists):
    keyed = []
    for order, steps in enumerate(lists):
        keyed += [((index + 0.5) / len(steps), order, step) for index, step in enumerate(steps)]
    for _, _, step in sorted(keyed, key=lambda item: item[:2]):
        step()


def swap_start(torus, sems, pairs):
    for index, (src, dst) in enumerate(pairs):
        torus.send(src, dst, sems, index, torus.partner)


def swap_end(torus, sems, pairs, first=0):
    for index, (_, dst) in enumerate(pairs):
        if index >= first:
            torus.arrive(dst, sems, index)


class Turner:
    def __init__(self, src, dst, scr):
        self.src, self.dst, self.scr = src, dst, scr
        self.unit = scr.turn_in.shape[K2]
        self.count = src.shape[K1] // self.unit

    def load(self, index):
        at = pl.ds(pl.multiple_of(index * self.unit, self.unit), self.unit)
        slot = lax.rem(index, 2)
        return pltpu.make_async_copy(self.src.at[:, at], self.scr.turn_in.at[slot], self.scr.turn_in_sem.at[slot])

    def save(self, index):
        at = pl.ds(pl.multiple_of(index * self.unit, self.unit), self.unit)
        slot = lax.rem(index, 2)
        return pltpu.make_async_copy(self.scr.turn_out.at[slot], self.dst.at[at, :], self.scr.turn_out_sem.at[slot])

    def steps(self, parts):
        each = self.count // parts

        def step(part):
            if part == 0:
                self.load(0).start()

            def body(index, carry):
                @pl.when(index + 1 < self.count)
                def _():
                    self.load(index + 1).start()

                self.load(index).wait()

                @pl.when(index >= 2)
                def _():
                    self.save(index - 2).wait()

                self.scr.turn_out[lax.rem(index, 2)] = self.scr.turn_in[lax.rem(index, 2)].T
                self.save(index).start()
                return carry

            lax.fori_loop(part * each, (part + 1) * each, body, 0)
            if part == parts - 1:
                self.save(self.count - 2).wait()
                self.save(self.count - 1).wait()

        return [functools.partial(step, part) for part in range(parts)]


def turner_scratch(rows, unit):
    dma = pltpu.SemaphoreType.DMA
    return dict(turn_in=pltpu.VMEM((2, rows, unit), BF16), turn_out=pltpu.VMEM((2, unit, rows), BF16), turn_in_sem=dma((K2,)), turn_out_sem=dma((K2,)))


def row_tiles(rows):
    return [pl.ds(start, 16) for start in range(0, rows, 16)]


def rms_back(z_in, gain, grad):
    inv = lax.rsqrt(jnp.mean(z_in * z_in, axis=-1, keepdims=True) + EPS)
    normed = z_in * inv
    scaled = grad * gain
    back = inv * (scaled - normed * jnp.mean(scaled * normed, axis=-1, keepdims=True))
    return back, jnp.sum(grad * normed, axis=0, keepdims=True)


def bag(tree):
    if isinstance(tree, dict):
        return types.SimpleNamespace(**{key: bag(value) for key, value in tree.items()})
    return [bag(value) for value in tree] if isinstance(tree, list) else tree


def call_kernel(name, body, ins, outs, scratch, flops, collective_id=None):
    is_leaf = lambda value: isinstance(value, tuple)
    in_leaves, in_tree = jax.tree.flatten(ins, is_leaf=is_leaf)
    out_leaves, out_tree = jax.tree.flatten(outs, is_leaf=is_leaf)
    scr_leaves, scr_tree = jax.tree.flatten(scratch)
    first_scr = len(in_leaves) + len(out_leaves)

    def kernel(*refs):
        body(bag(in_tree.unflatten(refs[:len(in_leaves)])), bag(out_tree.unflatten(refs[len(in_leaves):first_scr])), bag(scr_tree.unflatten(refs[first_scr:])))

    results = pl.pallas_call(
        kernel,
        name=name,
        out_shape=[leaf[K0] for leaf in out_leaves],
        in_specs=[leaf[K1] for leaf in in_leaves],
        out_specs=[leaf[K1] for leaf in out_leaves],
        scratch_shapes=scr_leaves,
        compiler_params=pltpu.CompilerParams(collective_id=collective_id, has_side_effects=collective_id is not None, vmem_limit_bytes=LIMIT),
        cost_estimate=pl.CostEstimate(flops=int(flops), bytes_accessed=int(4e7), transcendentals=0),
    )(*[leaf[K0] for leaf in in_leaves])
    return bag(out_tree.unflatten(results))


def shape(dims, dtype=BF16):
    return jax.ShapeDtypeStruct(dims, dtype)


def sum_attention(side, attn, w_outs, hidden, grad_out, gain, w_gate, w_up, w_down):
    seq, depth = attn.ctx.shape
    width = gain.shape[K1]
    hidden_loc = w_gate.shape[K0]
    rows = seq // (side * side)

    def body(ins, outs, scr):
        torus = Torus(side)
        weights = Weights(ins.w_outs, scr.w, scr.w_sem, False)
        weights.start()
        rows_at = pl.ds(pl.multiple_of(torus.chip * rows, rows), rows)
        x_load = pltpu.make_async_copy(ins.hidden.at[torus.core, rows_at, :], scr.x_rows, scr.x_sem.at[K0])
        x_load.start()

        def load_weight(src, slot):
            load = pltpu.make_async_copy(src, scr.w_mlp.at[slot], scr.w_mlp_sem.at[slot])
            load.start()
            return load

        loads = {slot: load_weight(src, slot) for slot, src in ((K0, ins.w_down), (K2, ins.w_gate), (K3, ins.w_up))}
        wait = torus.signal_all()
        part = scr.sum.part
        steps = ReduceScatter(torus, scr.sum).steps(fill_partial(torus, part, [ins.ctx], weights))
        steps[K0]()
        wait()
        other_ctx = ins.ctx.at[:, :, :, pl.ds(depth // 2, depth // 2)]
        swaps = [(ins.w_down, outs.w_down), (ins.w_gate, outs.w_gate), (ins.w_up, outs.w_up), (other_ctx, outs.ctx_other), (ins.normed, outs.normed_other)]
        swap_start(torus, scr.swap_sems, swaps)

        def dy_load(group):
            at = pl.ds(group * side * rows, side * rows)
            return pltpu.make_async_copy(ins.grad_out.at[torus.core, at, :], scr.dy.at[group % 2], scr.dy_sem.at[group % 2])

        def grad_act(group):
            if group == 0:
                torus.arrive(outs.w_down, scr.swap_sems, 0)
                loads[K1] = load_weight(outs.w_down, K1)
                for slot in PAIR:
                    loads[slot].wait()
            dy_load(group).wait()
            for slot in PAIR:
                product = dot(scr.dy[group % 2], scr.w_mlp[slot], NT)
                scr.grad_act[slot, group] = product.reshape(side, rows, hidden_loc)
            if group + 2 < side:
                dy_load(group + 2).start()

        dy_load(0).start()
        dy_load(1).start()
        half = len(steps) // 3
        run(steps[1:half])
        run(steps[half:], [functools.partial(grad_act, group) for group in range(side)])
        for index, (slot, out) in enumerate(((K0, outs.w_gate), (K1, outs.w_up))):
            torus.arrive(out, scr.swap_sems, index + 1)
            loads[slot] = load_weight(out, slot)
        scr.pre[...] = jnp.zeros_like(scr.pre)
        gat = scr.all.gat
        own = (torus.y, torus.x)
        x_load.wait()
        for at in row_tiles(rows):
            resid = (scr.x_rows[at, :].astype(F32) + part[(*own, at, slice(None))].astype(F32)).astype(BF16)
            outs.h_rows[at, :] = resid
            z_in = resid.astype(F32)
            inv = lax.rsqrt(jnp.mean(z_in * z_in, axis=-1, keepdims=True) + EPS)
            gat[(*own, at, slice(None))] = (z_in * inv * ins.gain[...]).astype(BF16)
        gather = AllGather(torus, scr.all, False)
        gather.store = Store(torus, scr.all, plain_places(gather, outs.full))

        def products(step):
            if step == 0:
                for load in (loads[slot] for slot in (K0, K1, K2, K3)):
                    load.wait()
            for col in torus.colours:
                second = torus.wrap(col.second + gather.back[step])
                at_cols = pl.ds(col.index * (width // 2), width // 2)
                mixed = gat[second, :, :, at_cols] if col.index == 0 else gat[:, second, :, at_cols]
                mixed = mixed.reshape(side * rows, width // 2)

                def body(slot, carry, col=col, second=second, at_cols=at_cols, mixed=mixed):
                    term = dot(mixed, scr.w_mlp[slot, :, at_cols], NT).reshape(side, rows, hidden_loc)
                    if col.index == 0:
                        scr.pre[slot, second] += term
                    else:
                        scr.pre[slot, :, second] += term
                    return carry

                lax.fori_loop(0, 4, body, 0)
            for inner, count in ((0, step + 1), (1, step)):

                def block(index, carry, inner=inner):
                    shift = lax.rem(3 * index + 3 * lax.div(index * (index - 1), 2), side)
                    pair = (gather.back[step], shift) if inner == 0 else (shift, gather.back[step])
                    y_at, x_at = torus.wrap(torus.y + pair[K0]), torus.wrap(torus.x + pair[K1])
                    for core in PAIR:
                        gate, upper = scr.pre[2 - 2 * core, y_at, x_at], scr.pre[3 - 2 * core, y_at, x_at]
                        grad = scr.grad_act[core, y_at, x_at]
                        sigmoid_g = 1.0 / (1.0 + jnp.exp(-gate))
                        silu_g = gate * sigmoid_g
                        outs.acts[core][y_at, x_at] = (silu_g * upper).astype(BF16)
                        outs.gates[core][y_at, x_at] = (grad * upper * sigmoid_g * (1.0 + gate * (1.0 - sigmoid_g))).astype(BF16)
                        outs.ups[core][y_at, x_at] = (grad * silu_g).astype(BF16)
                    return carry

                lax.fori_loop(0, count, block, 0)

        run(gather.steps(products))
        gather.store.drain()
        swap_end(torus, scr.swap_sems, swaps, 3)
        torus.drain()

    dma = pltpu.SemaphoreType.DMA
    block = (side, side, rows, hidden_loc)
    ins = dict(ctx=(attn.ctx.reshape(side, side, rows, depth), VMEM), w_outs=[(weight, ANY) for weight in w_outs], hidden=(hidden, ANY), grad_out=(grad_out, ANY), gain=(gain, VMEM),
               normed=(attn.normed, ANY), w_gate=(w_gate, ANY), w_up=(w_up, ANY), w_down=(w_down, ANY))
    out, weight = (shape(block), VMEM), (shape((hidden_loc, width)), ANY)
    outs = dict(full=(shape((2, side, side, rows, width)), ANY), h_rows=(shape((rows, width)), VMEM), ctx_other=(shape((side, side, rows, depth // 2)), ANY), normed_other=(shape((seq, width)), ANY),
                w_gate=weight, w_up=weight, w_down=weight, acts=[out, out], gates=[out, out], ups=[out, out])
    scratch = dict(sum=rs_scratch(side, rows, width), all=ag_scratch(side, rows, width), w=pltpu.VMEM((depth, width), BF16), w_sem=dma((K2, K2)), swap_sems=[dma((5,)), dma((5,))],
                   x_rows=pltpu.VMEM((rows, width), BF16), x_sem=dma((K1,)), w_mlp=pltpu.VMEM((4, hidden_loc, width), BF16), w_mlp_sem=dma((4,)),
                   dy=pltpu.VMEM((2, side * rows, width), BF16), dy_sem=dma((K2,)), pre=pltpu.VMEM((4, *block), F32), grad_act=pltpu.VMEM((2, *block), F32))
    return call_kernel('sum_attention', body, ins, outs, scratch, 4e8, 1)


def sum_mlp(side, mlp, w_gates, w_ups, w_downs, grad_out, gain):
    depth = w_gates[K0].shape[K0]
    width = gain.shape[K1]
    rows = mlp.h_rows.shape[K0]
    seq = rows * side * side
    block = (side, side, rows, width)

    def body(ins, outs, scr):
        torus = Torus(side)
        weights = Weights(ins.w_in, scr.w, scr.w_sem, False)
        weights.start()
        weights_p = Weights(ins.w_downs, scr.wd, scr.wd_sem, False)
        weights_p.start()
        rows_at = pl.ds(pl.multiple_of(torus.chip * rows, rows), rows)
        dy_load = pltpu.make_async_copy(ins.grad_out.at[torus.core, rows_at, :], scr.dy_rows, scr.dy_sem.at[K0])
        dy_load.start()
        wait = torus.signal_all()
        steps = ReduceScatter(torus, scr.sum).steps(fill_partial(torus, scr.sum.part, ins.grads, weights))
        steps_p = ReduceScatter(torus, scr.sum_p).steps(fill_partial(torus, scr.sum_p.part, ins.acts, weights_p))
        steps[K0]()
        wait()

        turned = []

        def turn(index):
            kind, core = index // 2, index % 2
            src = (ins.grads[2 * core], ins.grads[2 * core + 1], ins.acts[core])[kind]
            slot = index % 2
            if index >= 2:
                turned[index - 2]()
            scr.turn[slot] = src[...].reshape(seq, depth).T
            at = pl.ds(kind * depth, depth)
            if core == 0:
                save = pltpu.make_async_copy(scr.turn.at[slot], outs.left.at[at, :], scr.turn_sem.at[kind])
                save.start()
                turned.append(save.wait)
            else:
                torus.send(scr.turn.at[slot], outs.left_other.at[at, :], scr.swap_sems, kind, torus.partner)
                turned.append(torus.pending.pop().wait_send)

        turns = [functools.partial(turn, index) for index in range(6)]
        fills = (K0, K3, 4, 10)
        early = [steps_p[index] for index in fills]
        rest_p = [step for index, step in enumerate(steps_p) if index not in fills]
        late = 22
        run(steps[1:late], early)
        for step in rest_p[:3]:
            step()
        run(steps[late:])
        own = (torus.y, torus.x)
        gain_total = jnp.zeros((1, width), F32)
        gat = scr.all.gat
        dy_load.wait()
        for at in row_tiles(rows):
            back, gain_part = rms_back(ins.h_rows[at, :].astype(F32), ins.gain[...], scr.sum.part[(*own, at, slice(None))].astype(F32))
            gain_total = gain_total + gain_part
            total = scr.dy_rows[at, :].astype(F32) + back
            outs.d_rows[at, :] = total
            gat[(*own, at, slice(None))] = total.astype(BF16)
        outs.gain[...] = gain_total
        gather = AllGather(torus, scr.all, False)
        gather.store = Store(torus, scr.all, plain_places(gather, outs.full), outs.own)
        run(gather.steps(), rest_p[3:], turns)
        for at in row_tiles(rows):
            outs.y_rows[at, :] = (ins.h_rows[at, :].astype(F32) + scr.sum_p.part[(*own, at, slice(None))].astype(F32)).astype(BF16)
        turned[4]()
        turned[5]()
        for kind in range(3):
            torus.arrive(outs.left_other.at[pl.ds(kind * depth, depth), :], scr.swap_sems, kind)
        gather.store.drain()
        torus.drain()

    dma = pltpu.SemaphoreType.DMA
    ins = dict(grads=[(grad, VMEM) for grad in (mlp.gates[K0], mlp.ups[K0], mlp.gates[K1], mlp.ups[K1])], acts=[(act, VMEM) for act in mlp.acts],
               w_in=[(weight, ANY) for weight in (w_gates[K0], w_ups[K0], w_gates[K1], w_ups[K1])], w_downs=[(weight, ANY) for weight in w_downs],
               h_rows=(mlp.h_rows, VMEM), grad_out=(grad_out, ANY), gain=(gain, VMEM))
    left = (shape((3 * depth, seq)), ANY)
    outs = dict(full=(shape((2, *block)), ANY), own=(shape(block), ANY), d_rows=(shape((rows, width), F32), VMEM), gain=(shape((1, width), F32), VMEM), y_rows=(shape((rows, width)), VMEM), left=left, left_other=left)
    scratch = dict(sum=rs_scratch(side, rows, width), sum_p=rs_scratch(side, rows, width), all=ag_scratch(side, rows, width), dy_rows=pltpu.VMEM((rows, width), BF16), dy_sem=dma((K1,)),
                   w=pltpu.VMEM((4 * depth, width), BF16), w_sem=dma((K2, 4)), wd=pltpu.VMEM((2 * depth, width), BF16), wd_sem=dma((K2, K2)),
                   turn=pltpu.VMEM((2, depth, seq), BF16), turn_sem=dma((K3,)), swap_sems=[dma((K3,)), dma((K3,))])
    return call_kernel('sum_mlp', body, ins, outs, scratch, 6e8, 2)


def sum_input(side, dqkv, w_qs, w_k, w_v, hidden, second, gain, normeds):
    seq, depth = dqkv.shape
    width = gain.shape[K1]
    rows = seq // (side * side)
    head = depth // 4
    half_side = side // 2
    tokens = seq // 2
    kv_width = w_k.shape[K1]
    per_kv = 2 * side * side * head // kv_width

    def body(ins, outs, scr):
        torus = Torus(side)
        kv_col = pl.multiple_of(lax.div(torus.chip * 2, per_kv) * head, head)
        weights = Weights([*ins.w_qs, ins.w_k.at[:, pl.ds(kv_col, head)], ins.w_v.at[:, pl.ds(kv_col, head)]], scr.w, scr.w_sem, True)
        weights.start()
        wait = torus.signal_all()
        part = scr.sum.part
        steps = ReduceScatter(torus, scr.sum).steps(fill_partial(torus, part, [ins.dqkv], weights))
        own = (torus.y, torus.x)
        gat = scr.all.gat
        gather = AllGather(torus, scr.all, True)

        def places(where, colour, half):
            chip = where[K0] * side + where[K1]
            tokens_at = pl.ds(pl.multiple_of(lax.rem(chip, 2) * tokens + colour * (tokens // 2), tokens // 2), tokens // 2)
            at = lax.div(chip, 2) * head
            src = gather.piece(gat, where, colour * 2, 2)
            return [(src.at[:, pl.ds(index * head, head)], outs.kv.at[half, tokens_at, pl.ds(pl.multiple_of(at + index * kv_width, head), head)]) for index in PAIR]

        gather.store = Store(torus, scr.all, places)
        rows_at = pl.ds(pl.multiple_of(torus.chip * rows, rows), rows)
        x_load = pltpu.make_async_copy(ins.hidden.at[torus.core, rows_at, :], scr.x_rows, scr.x_sem.at[K0])
        x_load.start()
        turns = Turner(ins.normeds[K0], outs.lefts[K0], scr).steps(8) + Turner(ins.normeds[K1], outs.lefts[K1], scr).steps(8)
        place = lax.rem(torus.x, 2)
        mate = torus.at_chip(torus.y, torus.x + 1 - 2 * place)
        kv_cols = pl.ds(2 * head, 2 * head)

        def mate_add():
            torus.arrive(scr.mate, scr.mate_sems, 0)
            mine = ins.dqkv[pl.ds(place * half_side, half_side), :, :, kv_cols]
            gat[own] = (mine.astype(F32) + scr.mate[...].astype(F32)).astype(BF16).reshape(tokens, 2 * head)

        steps[K0]()
        wait()
        swaps = [(ins.dqkv.at[:, :, :, pl.ds(head, head)], outs.q_other)]
        swap_start(torus, scr.swap_sems, swaps)
        torus.send(ins.dqkv.at[pl.ds((1 - place) * half_side, half_side), :, :, kv_cols], scr.mate, scr.mate_sems, 0, mate)
        for step in steps[1:5]:
            step()
        mate_add()
        run(steps[5:], gather.steps(), turns)
        x_load.wait()
        gain_total = jnp.zeros((1, width), F32)
        for at in row_tiles(rows):
            back, gain_part = rms_back(scr.x_rows[at, :].astype(F32), ins.gain[...], part[(*own, at, slice(None))].astype(F32))
            gain_total = gain_total + gain_part
            outs.rows[at, :] = (ins.d_rows[at, :] + back).astype(BF16)
            outs.rows[pl.ds(rows + at.start, at.size), :] = ins.y_rows[at, :]
        row = lax.broadcasted_iota(jnp.int32, (8, width), 0)
        extra = jnp.zeros((8, width), F32)
        for index, value in enumerate((gain_total, ins.gain_mlp[...])):
            for level in range(3):
                rounded = value.astype(BF16).astype(F32)
                extra = jnp.where(row == index * 3 + level, rounded, extra)
                value = value - rounded
        outs.rows[2 * rows:2 * rows + 8, :] = extra.astype(BF16)
        gather.store.drain()
        swap_end(torus, scr.swap_sems, swaps)
        torus.drain()

    dma = pltpu.SemaphoreType.DMA
    ins = dict(dqkv=(dqkv.reshape(side, side, rows, depth), VMEM), w_qs=[(weight, ANY) for weight in w_qs], w_k=(w_k, ANY), w_v=(w_v, ANY), hidden=(hidden, ANY), d_rows=(second.d_rows, VMEM), y_rows=(second.y_rows, VMEM), normeds=[(normed, ANY) for normed in normeds],
               gain=(gain, VMEM), gain_mlp=(second.gain, VMEM))
    outs = dict(rows=(shape((2 * rows + 8, width)), VMEM), kv=(shape((2, seq, 2 * kv_width)), ANY), lefts=[(shape((width, seq)), ANY)] * 2, q_other=(shape((side, side, rows, head)), ANY))
    scratch = dict(sum=rs_scratch(side, rows, width), all=ag_scratch(side, tokens, 2 * head, 2), x_rows=pltpu.VMEM((rows, width), BF16), x_sem=dma((K1,)), **turner_scratch(seq, min(256, width // 8)), w=pltpu.VMEM((width, depth), BF16), w_sem=dma((K2, 4)),
                   mate=pltpu.VMEM((half_side, side, rows, 2 * head), BF16), mate_sems=[dma((K1,)), dma((K1,))], swap_sems=[dma((K1,)), dma((K1,))])
    return call_kernel('sum_input', body, ins, outs, scratch, 3e8, 3)


def scores_softmax(qkv, seg_row, seg_col, head_index, tile_index, tile):
    reach = (tile_index + 1) * tile
    queries = qkv[tile_index * tile:reach, head_index * HEAD_DIM:(head_index + 1) * HEAD_DIM]
    scores = dot(qkv[:reach, 2 * HEAD_DIM:3 * HEAD_DIM], queries, NT) * HEAD_DIM ** -0.5
    key_at = lax.broadcasted_iota(jnp.int32, (reach, tile), 0)
    query_at = lax.broadcasted_iota(jnp.int32, (reach, tile), 1) + tile_index * tile
    allowed = (key_at <= query_at) & (seg_col[:reach, :] == seg_row[:, tile_index * tile:reach])
    scores = jnp.where(allowed, scores, -1e30)
    weights = jnp.exp(scores - jnp.max(scores, axis=0, keepdims=True))
    return weights * (1.0 / jnp.sum(weights, axis=0, keepdims=True)), queries


def segments(seg_ref):
    core = lax.rem(lax.axis_index('tp'), 2)
    seg_row = seg_ref[pl.ds(core, 1), :].astype(F32)
    return seg_row, jnp.broadcast_to(seg_row, (8, seg_row.shape[K1])).T[:, :1]


def attention_forward(hidden, seg_ids, gain, w_q, w_k, w_v, w_o, per_kv):
    seq, width = hidden.shape[1:]
    chunk = seq // 4
    tile = min(256, seq)
    depth = 4 * HEAD_DIM

    def body(ins, outs, scr):
        tp_idx = lax.axis_index('tp')
        core = lax.rem(tp_idx, 2)
        kv_col = pl.multiple_of(lax.div(tp_idx, per_kv) * HEAD_DIM, HEAD_DIM)
        partner = dict(tp=tp_idx + 1 - 2 * core)
        barrier = pltpu.get_barrier_semaphore()
        pl.semaphore_signal(barrier, inc=1, device_id=partner, device_id_type=MESH)
        loads = []
        for index in range(4):
            at = pl.ds(index * chunk, chunk)
            loads.append(pltpu.make_async_copy(ins.hidden.at[core, at, :], scr.x.at[at, :], scr.x_sem.at[index]))

        def w_cols(index):
            return scr.w.at[:, pl.ds(index * HEAD_DIM, HEAD_DIM)]

        for index, ref in ((0, ins.w_q), (2, ins.w_k.at[:, pl.ds(kv_col, HEAD_DIM)]), (3, ins.w_v.at[:, pl.ds(kv_col, HEAD_DIM)])):
            loads.append(pltpu.make_async_copy(ref, w_cols(index), scr.w_sem.at[index]))
        for load in loads:
            load.start()
        pl.semaphore_wait(barrier, 1)
        swaps = [(ins.w_q, w_cols(1)), (ins.w_o, outs.w_o), (ins.w_q, outs.w_q)]
        copies = []
        for index, (src, dst) in enumerate(swaps):
            copies.append(pltpu.make_async_remote_copy(src, dst, scr.swap_sems[K0].at[index], scr.swap_sems[K1].at[index], device_id=partner, device_id_type=MESH))
            copies[index].start()
        stores = []
        for index in range(4):
            loads[index].wait()

            def normalize(step, carry, index=index):
                at = pl.ds(pl.multiple_of(index * chunk + step * 16, 16), 16)
                x_float = scr.x[at, :].astype(F32)
                inv = lax.rsqrt(jnp.mean(x_float * x_float, axis=-1, keepdims=True) + EPS)
                scr.normed[at, :] = (x_float * inv * ins.gain[...]).astype(BF16)
                return carry

            lax.fori_loop(0, chunk // 16, normalize, 0)
            at = pl.ds(index * chunk, chunk)
            store = pltpu.make_async_copy(scr.normed.at[at, :], outs.normed.at[at, :], scr.out_sem.at[index])
            store.start()
            stores.append(store)
            if index == 0:
                for load in loads[4:]:
                    load.wait()
                copies[K0].wait_recv()
            outs.qkv[at, :] = dot(scr.normed[at, :], scr.w[...], NN).astype(BF16)
        seg_row, seg_col = segments(ins.seg)
        values_t = outs.qkv[:, 3 * HEAD_DIM:].T
        for head_index in PAIR:
            for tile_index in range(seq // tile):
                probs, _ = scores_softmax(outs.qkv, seg_row, seg_col, head_index, tile_index, tile)
                ctx_t = dot(values_t[:, :(tile_index + 1) * tile], probs.astype(BF16), NN)
                outs.ctx[tile_index * tile:(tile_index + 1) * tile, head_index * HEAD_DIM:(head_index + 1) * HEAD_DIM] = ctx_t.T.astype(BF16)
        for store in stores:
            store.wait()
        copies[K0].wait_send()
        copies[K1].wait()
        copies[K2].wait()

    dma = pltpu.SemaphoreType.DMA
    ins = dict(hidden=(hidden, ANY), seg=(seg_ids, VMEM), gain=(gain, VMEM), w_q=(w_q, ANY), w_o=(w_o, ANY), w_k=(w_k, ANY), w_v=(w_v, ANY))
    outs = dict(normed=(shape((seq, width)), ANY), qkv=(shape((seq, depth)), VMEM), ctx=(shape((seq, 2 * HEAD_DIM)), VMEM), w_q=(shape(w_q.shape), ANY), w_o=(shape(w_o.shape), ANY))
    scratch = dict(swap_sems=[dma((K3,)), dma((K3,))], x=pltpu.VMEM((seq, width), BF16), normed=pltpu.VMEM((seq, width), BF16), w=pltpu.VMEM((width, depth), BF16), x_sem=dma((4,)), w_sem=dma((4,)), out_sem=dma((4,)))
    return call_kernel('attention_forward', body, ins, outs, scratch, 5e9, 4)


def attention_backward(resid, seg_ids, w_outs, qkv):
    seq, width = resid.shape
    chunk = seq // 4
    tile = min(256, seq)
    depth = 4 * HEAD_DIM

    def body(ins, outs, scr):
        loads = []
        for index in PAIR:
            at = pl.ds(index * HEAD_DIM, HEAD_DIM)
            loads.append(pltpu.make_async_copy(ins.w_outs[index], scr.w.at[at, :], scr.w_sem.at[index]))
        for index in range(4):
            at = pl.ds(index * chunk, chunk)
            loads.append(pltpu.make_async_copy(ins.resid.at[at, :], scr.resid.at[at, :], scr.in_sem.at[index]))
        for load in loads:
            load.start()
        for load in loads[:2]:
            load.wait()
        for index in range(4):
            loads[2 + index].wait()
            at = pl.ds(index * chunk, chunk)
            scr.grad_ctx[at, :] = dot(scr.resid[at, :], scr.w[...], NT).astype(BF16)
        seg_row, seg_col = segments(ins.seg)
        keys_t = ins.qkv[:, 2 * HEAD_DIM:3 * HEAD_DIM].T
        scr.grad_k[...] = jnp.zeros_like(scr.grad_k)
        scr.grad_v[...] = jnp.zeros_like(scr.grad_v)
        for head_index in PAIR:
            cols = slice(head_index * HEAD_DIM, (head_index + 1) * HEAD_DIM)
            for tile_index in range(seq // tile):
                reach = (tile_index + 1) * tile
                rows = slice(tile_index * tile, reach)
                probs, queries = scores_softmax(ins.qkv, seg_row, seg_col, head_index, tile_index, tile)
                grad_ctx = scr.grad_ctx[rows, cols]
                grad_probs = dot(ins.qkv[:reach, 3 * HEAD_DIM:], grad_ctx, NT)
                centre = jnp.sum(grad_probs * probs, axis=0, keepdims=True)
                grad_scores = (probs * (grad_probs - centre) * HEAD_DIM ** -0.5).astype(BF16)
                scr.grad_v[:reach, :] += dot(probs.astype(BF16), grad_ctx, NN)
                scr.grad_k[:reach, :] += dot(grad_scores, queries, NN)
                outs.dqkv[rows, cols] = dot(keys_t[:, :reach], grad_scores, NN).T.astype(BF16)
        outs.dqkv[:, 2 * HEAD_DIM:3 * HEAD_DIM] = scr.grad_k[...].astype(BF16)
        outs.dqkv[:, 3 * HEAD_DIM:] = scr.grad_v[...].astype(BF16)

    dma = pltpu.SemaphoreType.DMA
    ins = dict(resid=(resid, ANY), seg=(seg_ids, VMEM), w_outs=[(weight, ANY) for weight in w_outs], qkv=(qkv, VMEM))
    outs = dict(dqkv=(shape((seq, depth)), VMEM))
    scratch = dict(resid=pltpu.VMEM((seq, width), BF16), w=pltpu.VMEM((2 * HEAD_DIM, width), BF16), grad_ctx=pltpu.VMEM((seq, 2 * HEAD_DIM), BF16),
                   grad_k=pltpu.VMEM((seq, HEAD_DIM), F32), grad_v=pltpu.VMEM((seq, HEAD_DIM), F32), w_sem=dma((K2,)), in_sem=dma((4,)))
    return call_kernel('attention_backward', body, ins, outs, scratch, 4e9).dqkv


def weight_grads_mlp(mixed_full, grad_out, resid_full, lefts, ctxs, token):
    seq, width = grad_out.shape[1:]
    depth, head = lefts[K0].shape[K0] // 3, ctxs[K1].shape[K1]
    tile = min(512, width)

    def kernel(m_ref, dy_ref, dh_ref, left_own, left_other, ctx_own, ctx_other, _, out_gate, out_up, out_down, out_o, ctx_t):
        core = lax.rem(lax.axis_index('tp'), 2)

        @pl.when(pl.program_id(0) == 0)
        def _():
            for half, ref in enumerate((ctx_own, ctx_other)):
                ctx_t[half] = ref[:, :head].T

        halves = (core, 1 - core)
        lefts = (left_own, left_other)

        def product(base, size, ref):
            own, other = (dot(left[base:base + size, :], ref[half], NN) for left, half in zip(lefts, halves))
            return own + other

        both = product(0, 2 * depth, m_ref)
        out_gate[...] = both[:depth]
        out_up[...] = both[depth:]
        out_down[...] = product(2 * depth, depth, dy_ref)
        out_o[...] = dot(ctx_t[K0], dh_ref[core], NN) + dot(ctx_t[K1], dh_ref[1 - core], NN)

    slab = pl.BlockSpec((2, seq, tile), lambda step: (0, 0, step))
    out = lambda size: pl.BlockSpec((size, tile), lambda step: (0, step))
    return pl.pallas_call(
        kernel,
        name='weight_grads_mlp',
        grid=(width // tile,),
        out_shape=[shape((depth, width), F32)] * 3 + [shape((head, width), F32)],
        in_specs=[slab] * 3 + [VMEM] * 4 + [ANY],
        out_specs=[out(depth)] * 3 + [out(head)],
        scratch_shapes=[pltpu.VMEM((2, head, seq), BF16)],
        compiler_params=pltpu.CompilerParams(vmem_limit_bytes=LIMIT),
        cost_estimate=pl.CostEstimate(flops=int(18e9), bytes_accessed=int(6e7), transcendentals=0),
    )(mixed_full, grad_out, resid_full, *lefts, *ctxs, token)


def weight_grads_qkv(lefts, kv_full, grads_q):
    width, seq = lefts[K0].shape
    head = grads_q[K1].shape[K1]
    kv_width = kv_full.shape[K2] // 2
    tile = min(512, width)

    def kernel(a_own, a_other, kv_ref, q_own, q_other, out_q, out_k, out_v):
        core = lax.rem(lax.axis_index('tp'), 2)
        for index, out in enumerate((out_k, out_v)):
            at = pl.ds(index * kv_width, kv_width)
            out[...] = dot(a_own[...], kv_ref[core, :, at], NN) + dot(a_other[...], kv_ref[1 - core, :, at], NN)
        out_q[...] = dot(a_own[...], q_own[:, :head], NN) + dot(a_other[...], q_other[...], NN)

    slab = pl.BlockSpec((tile, seq), lambda step: (step, 0))
    out = lambda size: pl.BlockSpec((tile, size), lambda step: (step, 0))
    return pl.pallas_call(
        kernel,
        name='weight_grads_qkv',
        grid=(width // tile,),
        out_shape=[shape((width, size), F32) for size in (head, kv_width, kv_width)],
        in_specs=[slab] * 2 + [VMEM] * 3,
        out_specs=[out(size) for size in (head, kv_width, kv_width)],
        compiler_params=pltpu.CompilerParams(vmem_limit_bytes=LIMIT),
        cost_estimate=pl.CostEstimate(flops=int(27e9), bytes_accessed=int(6e7), transcendentals=0),
    )(*lefts, kv_full, *grads_q)


def in_place(gathered, rows):
    blocks, _, width = gathered.shape
    slots = 24
    pieces = 2 * blocks

    def kernel(src, dx_ref, y_ref, gain_attn, gain_mlp, buf, extra, in_sem, out_sem, extra_sem):
        gains = pltpu.make_async_copy(src.at[:, pl.ds(2 * rows, 8), :], extra, extra_sem.at[K0])

        def load(index):
            at = pl.ds(index // blocks * rows, rows)
            return pltpu.make_async_copy(src.at[index % blocks, at, :], buf.at[index % slots], in_sem.at[index % slots])

        def store(index):
            dst, block = (dx_ref, y_ref)[index // blocks], index % blocks
            return pltpu.make_async_copy(buf.at[index % slots], dst.at[block % 2, block // 2], out_sem.at[index % slots])

        ahead = slots // 2
        for index in range(pieces + ahead):
            if index < pieces:
                if index >= slots:
                    store(index - slots).wait()
                load(index).start()
            if index == ahead:
                gains.start()
            if index >= ahead:
                load(index - ahead).wait()
                store(index - ahead).start()
        gains.wait()
        total = jnp.sum(extra[...].astype(F32), axis=0)
        for first, ref in ((0, gain_attn), (3, gain_mlp)):
            ref[...] = total[first:first + 1] + total[first + 1:first + 2] + total[first + 2:first + 3]
        for index in range(pieces - slots, pieces):
            store(index).wait()

    dma = pltpu.SemaphoreType.DMA
    whole = shape((2, blocks // 2, rows, width))
    return pl.pallas_call(
        kernel,
        name='in_place',
        out_shape=[whole, whole, shape((1, width), F32), shape((1, width), F32)],
        in_specs=[ANY],
        out_specs=[ANY, ANY, VMEM, VMEM],
        scratch_shapes=[pltpu.VMEM((slots, rows, width), BF16), pltpu.VMEM((blocks, 8, width), BF16), dma((slots,)), dma((slots,)), dma((K1,))],
        compiler_params=pltpu.CompilerParams(vmem_limit_bytes=LIMIT),
        cost_estimate=pl.CostEstimate(flops=int(2e7), bytes_accessed=int(2e7), transcendentals=0),
    )(gathered)


def solution(mesh):
    tp_size = mesh.shape['tp']
    chips = tp_size // 2
    side = math.isqrt(chips)

    def device_step(hidden, seg_ids, grad_out, gain_attn, gain_mlp, w_q, w_k, w_v, w_o, w_gate, w_up, w_down):
        seq_len, width = hidden.shape[1:]
        kv_heads = w_k.shape[K1] // HEAD_DIM
        per_kv = tp_size // kv_heads
        rows = seq_len // chips

        def flat(value):
            return value.reshape(seq_len, value.shape[-1])

        gain_attn_row = gain_attn[None, :]
        gain_mlp_row = gain_mlp[None, :]

        attn = attention_forward(hidden, seg_ids, gain_attn_row, w_q, w_k, w_v, w_o, per_kv)
        w_qs, w_outs = (w_q, attn.w_q), (w_o, attn.w_o)
        mlp = sum_attention(side, attn, w_outs, hidden, grad_out, gain_mlp_row, w_gate.T, w_up.T, w_down)
        mixed_full = mlp.full.reshape(2, seq_len, width)
        second = sum_mlp(side, mlp, (w_gate.T, mlp.w_gate), (w_up.T, mlp.w_up), (w_down, mlp.w_down), grad_out, gain_mlp_row)
        resid_full = second.full.reshape(2, seq_len, width)

        dqkv = attention_backward(flat(second.own), seg_ids, w_outs, attn.qkv)
        third = sum_input(side, dqkv, w_qs, w_k, w_v, hidden, second, gain_attn_row, (attn.normed, mlp.normed_other))

        grad_in, y_out, grad_gain_attn, grad_gain_mlp = in_place(lax.all_gather(third.rows, 'tp'), rows)
        grad_gate_t, grad_up_t, grad_w_down, grad_w_o = weight_grads_mlp(
            mixed_full, grad_out, resid_full, (second.left, second.left_other), (attn.ctx, flat(mlp.ctx_other)), third.q_other)
        grad_w_q, grad_w_k, grad_w_v = weight_grads_qkv(third.lefts, third.kv, (dqkv, flat(third.q_other)))
        return (y_out.reshape(hidden.shape), grad_in.reshape(hidden.shape), grad_gain_attn[K0], grad_gain_mlp[K0], grad_w_q, grad_w_k, grad_w_v, grad_w_o, grad_gate_t.T, grad_up_t.T, grad_w_down)

    spec_act = P('data', None, None)
    spec_rows = P('data', None)
    spec_gain = P(None)
    spec_cols = P(None, 'tp')
    spec_tprows = P('tp', None)
    spec_whole = P(None, None)
    spec_stack = P(('data', 'tp'), None)
    in_specs = (spec_act, spec_rows, spec_act, spec_gain, spec_gain, spec_cols, spec_whole, spec_whole, spec_tprows, spec_cols, spec_cols, spec_tprows)
    out_specs = (spec_act, spec_act, P('data'), P('data'), P('data', 'tp'), spec_rows, spec_rows, spec_stack, P('data', 'tp'), P('data', 'tp'), spec_stack)
    return jax.shard_map(device_step, mesh=mesh, in_specs=in_specs, out_specs=out_specs, check_vma=False)
```

```python
import functools
import math
import types
import jax
import jax.numpy as jnp
from jax import lax
from jax.experimental import pallas as pl
from jax.experimental.pallas import tpu as pltpu
from jax.sharding import PartitionSpec as P

HEAD_DIM = 128
EPS = 1e-5
MESH = pl.DeviceIdType.MESH
F32 = jnp.float32
BF16 = jnp.bfloat16
LIMIT = 63 * 2 ** 20
K0, K1, K2, K3 = range(4)
PAIR = range(2)
ANY = pl.BlockSpec(memory_space=pl.ANY)
VMEM = pl.BlockSpec(memory_space=pltpu.VMEM)


def dot(lhs, rhs, dims):
    return lax.dot_general(lhs, rhs, (dims, ((), ())), preferred_element_type=F32)


NN = ((1,), (0,))
NT = ((1,), (1,))


SIGNS = (1, -1)


class Colour:
    def __init__(self, index, first, second):
        self.index, self.first, self.second = index, first, second


class Torus:
    def __init__(self, side):
        self.side = side
        tp_idx = lax.axis_index('tp')
        self.core = lax.rem(tp_idx, 2)
        self.chip = lax.div(tp_idx, 2)
        self.x = lax.rem(self.chip, side)
        self.y = lax.div(self.chip, side)
        self.partner = {'tp': self.chip * 2 + (1 - self.core)}
        self.colours = (Colour(0, self.x, self.y), Colour(1, self.y, self.x))
        self.pending = []

    def wrap(self, pos):
        return lax.rem(pos + 2 * self.side, self.side)

    def at_chip(self, y_at, x_at):
        return {'tp': (y_at * self.side + x_at) * 2 + self.core}

    def block(self, col, second, first):
        return (second, first) if col.index == 0 else (first, second)

    def peer1(self, col, shift):
        return self.at_chip(*self.block(col, col.second, self.wrap(col.first + shift)))

    def peer2(self, col, shift):
        return self.at_chip(*self.block(col, self.wrap(col.second + shift), col.first))

    def signal_all(self):
        barrier = pltpu.get_barrier_semaphore()
        peers = [self.partner]
        peers += [self.at_chip(self.y, self.wrap(self.x + shift)) for shift in SIGNS]
        peers += [self.at_chip(self.wrap(self.y + shift), self.x) for shift in SIGNS]
        for peer in peers:
            pl.semaphore_signal(barrier, inc=1, device_id=peer, device_id_type=MESH)
        return lambda: pl.semaphore_wait(barrier, len(peers))

    def send(self, src, dst, sems, index, device):
        copy = pltpu.make_async_remote_copy(src, dst, sems[K0].at[index], sems[K1].at[index], device_id=device, device_id_type=MESH)
        copy.start()
        self.pending.append(copy)

    def arrive(self, dst, sems, index):
        pltpu.make_async_remote_copy(dst, dst, sems[K0].at[index], sems[K1].at[index], device_id=self.partner, device_id_type=MESH).wait_recv()

    def drain(self):
        for copy in self.pending:
            copy.wait_send()


R1, R2, R3, S1, S2, S3 = range(6)
RS_COUNTS = (16, 16, 16, 4, 4, 4)
H1, H2, F1, F2 = range(4)
AG_COUNTS = (8, 32, 4, 16)


class ReduceScatter:
    SHIFTS = (2, 1, 3, 0)

    def __init__(self, torus, scr):
        self.torus, self.part, self.scr = torus, scr.part, scr
        self.quarter = scr.part.shape[K3] // 4

    def buf(self, kind, index):
        return self.scr.bufs[kind].at[index]

    def sems(self, kind):
        return self.scr.out_sems[kind], self.scr.in_sems[kind]

    def cols(self, col, half):
        return pl.ds((col.index * 2 + half) * self.quarter, self.quarter)

    def piece(self, where, at_cols):
        return self.part.at[(*where, slice(None), at_cols)]

    def send(self, where, at_cols, kind, index, peer):
        self.torus.send(self.piece(where, at_cols), self.buf(kind, index), self.sems(kind), index, peer)

    def add(self, where, at_cols, *kinds):
        total = self.part[(*where, slice(None), at_cols)].astype(F32)
        for kind, index in kinds:
            self.torus.arrive(self.buf(kind, index), self.sems(kind), index)
            total = total + self.buf(kind, index)[...].astype(F32)
        self.part[(*where, slice(None), at_cols)] = total.astype(BF16)

    def each(self, step):
        wrap = self.torus.wrap
        for col in self.torus.colours:
            second = wrap(col.second + self.SHIFTS[step])
            for way, sign in enumerate(SIGNS):
                yield col, second, way, sign, (col.index * 2 + way) * 4 + step

    def far(self, step):
        for col, second, way, sign, index in self.each(step):
            where = self.torus.block(col, second, self.torus.wrap(col.first + 2))
            self.send(where, self.cols(col, way), R1, index, self.torus.peer1(col, sign))

    def near(self, step):
        for col, second, way, sign, index in self.each(step):
            where = self.torus.block(col, second, self.torus.wrap(col.first + sign))
            self.send(where, self.cols(col, 1 - way), R2, index, self.torus.peer1(col, sign))

    def relay(self, step):
        for col, second, way, sign, index in self.each(step):
            where = self.torus.block(col, second, self.torus.wrap(col.first + sign))
            self.add(where, self.cols(col, way), (R1, index))
            self.send(where, self.cols(col, way), R3, index, self.torus.peer1(col, sign))

    def end(self, step):
        for col, second, way, sign, index in self.each(step):
            where = self.torus.block(col, second, col.first)
            other = (col.index * 2 + 1 - way) * 4 + step
            self.add(where, self.cols(col, way), (R2, other), (R3, index))

    def far2(self):
        for col in self.torus.colours:
            for way, sign in enumerate(SIGNS):
                where = self.torus.block(col, self.torus.wrap(col.second + 2), col.first)
                self.send(where, self.cols(col, way), S1, col.index * 2 + way, self.torus.peer2(col, sign))

    def near2(self, way):
        for col in self.torus.colours:
            where = self.torus.block(col, self.torus.wrap(col.second + SIGNS[way]), col.first)
            self.send(where, self.cols(col, 1 - way), S2, col.index * 2 + way, self.torus.peer2(col, SIGNS[way]))

    def relay2(self, way):
        for col in self.torus.colours:
            index = col.index * 2 + way
            where = self.torus.block(col, self.torus.wrap(col.second + SIGNS[way]), col.first)
            self.add(where, self.cols(col, way), (S1, index))
            self.send(where, self.cols(col, way), S3, index, self.torus.peer2(col, SIGNS[way]))

    def end2(self):
        for col in self.torus.colours:
            where = self.torus.block(col, col.second, col.first)
            for way in PAIR:
                self.add(where, self.cols(col, way), (S2, col.index * 2 + 1 - way), (S3, col.index * 2 + way))

    def steps(self, fill):
        call = functools.partial
        return [call(fill, K2), call(self.far, K0), call(self.far, K1), call(fill, K1), call(fill, K3),
                call(self.near, K0), call(self.relay, K0), call(self.near, K1), call(self.far, K2), call(self.relay, K1),
                call(fill, K0), call(self.near, K2), call(self.far, K3), call(self.end, K0), self.far2,
                call(self.relay, K2), call(self.near, K3), call(self.end, K1), call(self.near2, K0), call(self.relay2, K0),
                call(self.relay, K3), call(self.end, K2), call(self.near2, K1), call(self.relay2, K1), call(self.end, K3),
                self.end2]


class AllGather:
    def __init__(self, torus, scr, by_rows):
        self.torus, self.gat, self.scr, self.by_rows, self.store = torus, scr.gat, scr, by_rows, None
        self.quarter = scr.gat.shape[2 if by_rows else 3] // 4
        self.back = (0, torus.side - 1, 1, 2)

    def sems(self, kind):
        return self.scr.out_sems[kind], self.scr.in_sems[kind]

    def piece(self, ref, where, first, count):
        at = pl.ds(first * self.quarter, count * self.quarter)
        return ref.at[(*where, at, slice(None))] if self.by_rows else ref.at[(*where, slice(None), at)]

    def half(self, col, where, half):
        return self.piece(self.gat, where, col.index * 2 + half, 1)

    def own2(self, turn):
        for col in self.torus.colours:
            where = self.torus.block(col, col.second, col.first)
            for way, sign in enumerate(SIGNS):
                at = self.half(col, where, way if turn == 0 else 1 - way)
                self.torus.send(at, at, self.sems(H1), (col.index * 2 + way) * 2 + turn, self.torus.peer2(col, sign))

    def send1(self, step, turn):
        for col in self.torus.colours:
            where = self.torus.block(col, self.torus.wrap(col.second + self.back[step]), col.first)
            for way, sign in enumerate(SIGNS):
                at = self.half(col, where, way if turn == 0 else 1 - way)
                self.torus.send(at, at, self.sems(H2), ((col.index * 2 + way) * 4 + step) * 2 + turn, self.torus.peer1(col, sign))

    def arrive2(self, way, turn):
        sign = SIGNS[way]
        for col in self.torus.colours:
            where = self.torus.block(col, self.torus.wrap(col.second - sign), col.first)
            at = self.half(col, where, way if turn == 0 else 1 - way)
            self.torus.arrive(at, self.sems(H1), (col.index * 2 + way) * 2 + turn)
            if turn == 0:
                self.torus.send(at, at, self.sems(F1), col.index * 2 + way, self.torus.peer2(col, sign))

    def relayed2(self):
        for col in self.torus.colours:
            where = self.torus.block(col, self.torus.wrap(col.second + 2), col.first)
            for way in PAIR:
                self.torus.arrive(self.half(col, where, way), self.sems(F1), col.index * 2 + way)

    def arrive1(self, step, turn):
        for col in self.torus.colours:
            second = self.torus.wrap(col.second + self.back[step])
            for way, sign in enumerate(SIGNS):
                where = self.torus.block(col, second, self.torus.wrap(col.first - sign))
                at = self.half(col, where, way if turn == 0 else 1 - way)
                self.torus.arrive(at, self.sems(H2), ((col.index * 2 + way) * 4 + step) * 2 + turn)
                if turn == 0:
                    self.torus.send(at, at, self.sems(F2), (col.index * 2 + way) * 4 + step, self.torus.peer1(col, sign))

    def relayed1(self, step):
        for col in self.torus.colours:
            second = self.torus.wrap(col.second + self.back[step])
            for way in PAIR:
                where = self.torus.block(col, second, self.torus.wrap(col.first + 2))
                self.torus.arrive(self.half(col, where, way), self.sems(F2), (col.index * 2 + way) * 4 + step)

    def keep(self, step, firsts):
        for col in self.torus.colours:
            for shift in firsts:
                where = self.torus.block(col, self.torus.wrap(col.second + self.back[step]), self.torus.wrap(col.first + shift))
                self.store.keep(where, col.index, lambda ref, where=where, col=col: self.piece(ref, where, col.index * 2, 2))

    def steps(self, whole=None):
        call = functools.partial
        whole = whole or (lambda step: None)
        here, beside, across = (K0,), (K1, self.torus.side - 1), (K2,)
        result = []
        for turn in PAIR:
            result += [call(self.own2, turn), call(self.send1, K0, turn)]
        result += [call(self.keep, K0, here), call(self.arrive2, K0, K0), call(self.arrive2, K1, K0)]
        for way in PAIR:
            step = way + K1
            result += [call(self.arrive2, way, K1), call(self.send1, step, K0), call(self.send1, step, K1), call(self.keep, step, here)]
        result += [call(self.arrive1, K0, K0), self.relayed2, call(self.send1, K3, K0), call(self.send1, K3, K1), call(self.keep, K3, here),
                   call(self.arrive1, K0, K1), call(self.keep, K0, beside), call(self.arrive1, K1, K0), call(self.arrive1, K2, K0),
                   call(self.relayed1, K0), call(self.keep, K0, across), call(whole, K0)]
        for step in (K1, K2):
            result += [call(self.arrive1, step, K1), call(self.keep, step, beside)]
        result += [call(self.arrive1, K3, K0)]
        for step in (K1, K2):
            result += [call(self.relayed1, step), call(self.keep, step, across), call(whole, step)]
        return result + [call(self.arrive1, K3, K1), call(self.keep, K3, beside), call(self.relayed1, K3), call(self.keep, K3, across), call(whole, K3)]


class Store:
    def __init__(self, torus, scr, places, own=None):
        self.torus, self.scr, self.places, self.own = torus, scr, places, own
        self.stores = []

    def slot(self, where, colour, index):
        return ((index * 2 + colour) * self.torus.side + where[K0]) * self.torus.side + where[K1]

    def keep(self, where, colour, piece):
        for index, (src, dst) in enumerate(self.places(where, colour, self.torus.core)):
            slot = self.slot(where, colour, index)
            pairs = [(self.scr.full_sem, dst)]
            if self.own is not None:
                pairs.append((self.scr.own_sem, piece(self.own)))
            for sem, ref in pairs:
                store = pltpu.make_async_copy(src, ref, sem.at[slot])
                store.start()
                self.stores.append(store)
            self.torus.send(src, dst, self.scr.cross_sems, slot, self.torus.partner)

    def drain(self):
        for store in self.stores:
            store.wait()
        side = self.torus.side
        for colour in PAIR:
            for y_at in range(side):
                for x_at in range(side):
                    for index, (_, dst) in enumerate(self.places((y_at, x_at), colour, 1 - self.torus.core)):
                        self.torus.arrive(dst, self.scr.cross_sems, self.slot((y_at, x_at), colour, index))


def plain_places(gather, full):
    return lambda where, colour, half: [(gather.piece(gather.gat, where, colour * 2, 2), gather.piece(full.at[half], where, colour * 2, 2))]


def rs_scratch(side, rows, width):
    dma = pltpu.SemaphoreType.DMA
    return dict(
        part=pltpu.VMEM((side, side, rows, width), BF16),
        bufs=[pltpu.VMEM((count, rows, width // 4), BF16) for count in RS_COUNTS],
        out_sems=[dma((count,)) for count in RS_COUNTS],
        in_sems=[dma((count,)) for count in RS_COUNTS],
    )


def ag_scratch(side, rows, width, places=1):
    dma = pltpu.SemaphoreType.DMA
    blocks = 2 * side * side * places
    return dict(
        gat=pltpu.VMEM((side, side, rows, width), BF16),
        out_sems=[dma((count,)) for count in AG_COUNTS],
        in_sems=[dma((count,)) for count in AG_COUNTS],
        full_sem=dma((blocks,)),
        own_sem=dma((blocks,)),
        cross_sems=[dma((blocks,)), dma((blocks,))],
    )


class Weights:
    def __init__(self, refs, buf, sem, by_rows):
        self.refs, self.buf, self.sem, self.by_rows = refs, buf, sem, by_rows
        self.copies = [[], []]

    def start(self):
        for colour in PAIR:
            for index, ref in enumerate(self.refs):
                if self.by_rows:
                    half, depth = ref.shape[K0] // 2, ref.shape[K1]
                    rows, cols = pl.ds(colour * half, half), pl.ds(index * depth, depth)
                    copy = pltpu.make_async_copy(ref.at[rows, :], self.buf.at[rows, cols], self.sem.at[colour, index])
                else:
                    half, depth = ref.shape[K1] // 2, ref.shape[K0]
                    rows, cols = pl.ds(index * depth, depth), pl.ds(colour * half, half)
                    copy = pltpu.make_async_copy(ref.at[:, cols], self.buf.at[rows, cols], self.sem.at[colour, index])
                copy.start()
                self.copies[colour].append(copy)

    def wait(self, colour):
        for copy in self.copies[colour]:
            copy.wait()
        self.copies[colour] = []


def fill_partial(torus, part, lhs, weights):
    rows, width = part.shape[2:]
    tile = min(512, width // 2)

    def fill(shift):
        for col in torus.colours:
            weights.wait(col.index)
            first = torus.wrap(col.first + shift)
            left = []
            for ref in lhs:
                depth = ref.shape[K3]
                value = ref[:, first] if col.index == 0 else ref[first]
                left.append((value.reshape(torus.side * rows, depth), depth))

            def body(step, carry, col=col, first=first, left=left):
                at = pl.ds(pl.multiple_of(col.index * (width // 2) + step * tile, tile), tile)
                total = None
                base = 0
                for value, depth in left:
                    if weights.by_rows:
                        term = dot(value, weights.buf[at, base:base + depth], NT)
                    else:
                        term = dot(value, weights.buf[base:base + depth, at], NN)
                    total = term if total is None else total + term
                    base += depth
                total = total.astype(BF16).reshape(torus.side, rows, tile)
                if col.index == 0:
                    part[:, first, :, at] = total
                else:
                    part[first, :, :, at] = total
                return carry

            lax.fori_loop(0, (width // 2) // tile, body, 0)

    return fill


def run(*lists):
    keyed = []
    for order, steps in enumerate(lists):
        keyed += [((index + 0.5) / len(steps), order, step) for index, step in enumerate(steps)]
    for _, _, step in sorted(keyed, key=lambda item: item[:2]):
        step()


def swap_start(torus, sems, pairs):
    for index, (src, dst) in enumerate(pairs):
        torus.send(src, dst, sems, index, torus.partner)


def swap_end(torus, sems, pairs, first=0):
    for index, (_, dst) in enumerate(pairs):
        if index >= first:
            torus.arrive(dst, sems, index)


def row_tiles(rows):
    return [pl.ds(start, 16) for start in range(0, rows, 16)]


def rms_back(z_in, gain, grad):
    inv = lax.rsqrt(jnp.mean(z_in * z_in, axis=-1, keepdims=True) + EPS)
    normed = z_in * inv
    scaled = grad * gain
    back = inv * (scaled - normed * jnp.mean(scaled * normed, axis=-1, keepdims=True))
    return back, jnp.sum(grad * normed, axis=0, keepdims=True)


def bag(tree):
    if isinstance(tree, dict):
        return types.SimpleNamespace(**{key: bag(value) for key, value in tree.items()})
    return [bag(value) for value in tree] if isinstance(tree, list) else tree


def call_kernel(name, body, ins, outs, scratch, flops, collective_id=None):
    is_leaf = lambda value: isinstance(value, tuple)
    in_leaves, in_tree = jax.tree.flatten(ins, is_leaf=is_leaf)
    out_leaves, out_tree = jax.tree.flatten(outs, is_leaf=is_leaf)
    scr_leaves, scr_tree = jax.tree.flatten(scratch)
    first_scr = len(in_leaves) + len(out_leaves)

    def kernel(*refs):
        body(bag(in_tree.unflatten(refs[:len(in_leaves)])), bag(out_tree.unflatten(refs[len(in_leaves):first_scr])), bag(scr_tree.unflatten(refs[first_scr:])))

    results = pl.pallas_call(
        kernel,
        name=name,
        out_shape=[leaf[K0] for leaf in out_leaves],
        in_specs=[leaf[K1] for leaf in in_leaves],
        out_specs=[leaf[K1] for leaf in out_leaves],
        scratch_shapes=scr_leaves,
        compiler_params=pltpu.CompilerParams(collective_id=collective_id, has_side_effects=collective_id is not None, vmem_limit_bytes=LIMIT),
        cost_estimate=pl.CostEstimate(flops=int(flops), bytes_accessed=int(4e7), transcendentals=0),
    )(*[leaf[K0] for leaf in in_leaves])
    return bag(out_tree.unflatten(results))


def shape(dims, dtype=BF16):
    return jax.ShapeDtypeStruct(dims, dtype)


def sum_attention(side, attn, w_outs, hidden, grad_out, gain, w_gate, w_up, w_down):
    seq, depth = attn.ctx.shape
    width = gain.shape[K1]
    hidden_loc = w_gate.shape[K0]
    rows = seq // (side * side)

    def body(ins, outs, scr):
        torus = Torus(side)
        weights = Weights(ins.w_outs, scr.w, scr.w_sem, False)
        weights.start()
        rows_at = pl.ds(pl.multiple_of(torus.chip * rows, rows), rows)
        x_load = pltpu.make_async_copy(ins.hidden.at[torus.core, rows_at, :], scr.x_rows, scr.x_sem.at[K0])
        x_load.start()

        def load_weight(src, slot):
            load = pltpu.make_async_copy(src, scr.w_mlp.at[slot], scr.w_mlp_sem.at[slot])
            load.start()
            return load

        loads = {slot: load_weight(src, slot) for slot, src in ((K0, ins.w_down), (K2, ins.w_gate), (K3, ins.w_up))}
        wait = torus.signal_all()
        part = scr.sum.part
        steps = ReduceScatter(torus, scr.sum).steps(fill_partial(torus, part, [ins.ctx], weights))
        steps[K0]()
        wait()
        other_ctx = ins.ctx.at[:, :, :, pl.ds(depth // 2, depth // 2)]
        swaps = [(ins.w_down, outs.w_down), (ins.w_gate, outs.w_gate), (ins.w_up, outs.w_up), (other_ctx, outs.ctx_other), (ins.normed, outs.normed_other)]
        swap_start(torus, scr.swap_sems, swaps)

        def dy_load(group):
            at = pl.ds(group * side * rows, side * rows)
            return pltpu.make_async_copy(ins.grad_out.at[torus.core, at, :], scr.dy.at[group % 2], scr.dy_sem.at[group % 2])

        def grad_act(group):
            if group == 0:
                torus.arrive(outs.w_down, scr.swap_sems, 0)
                loads[K1] = load_weight(outs.w_down, K1)
                for slot in PAIR:
                    loads[slot].wait()
            dy_load(group).wait()
            for slot in PAIR:
                product = dot(scr.dy[group % 2], scr.w_mlp[slot], NT)
                scr.grad_act[slot, group] = product.reshape(side, rows, hidden_loc)
            if group + 2 < side:
                dy_load(group + 2).start()

        dy_load(0).start()
        dy_load(1).start()
        half = len(steps) // 3
        run(steps[1:half])
        run(steps[half:], [functools.partial(grad_act, group) for group in range(side)])
        for index, (slot, out) in enumerate(((K0, outs.w_gate), (K1, outs.w_up))):
            torus.arrive(out, scr.swap_sems, index + 1)
            loads[slot] = load_weight(out, slot)
        scr.pre[...] = jnp.zeros_like(scr.pre)
        gat = scr.all.gat
        own = (torus.y, torus.x)
        x_load.wait()
        for at in row_tiles(rows):
            resid = (scr.x_rows[at, :].astype(F32) + part[(*own, at, slice(None))].astype(F32)).astype(BF16)
            outs.h_rows[at, :] = resid
            z_in = resid.astype(F32)
            inv = lax.rsqrt(jnp.mean(z_in * z_in, axis=-1, keepdims=True) + EPS)
            gat[(*own, at, slice(None))] = (z_in * inv * ins.gain[...]).astype(BF16)
        gather = AllGather(torus, scr.all, False)
        gather.store = Store(torus, scr.all, plain_places(gather, outs.full))

        def products(step):
            if step == 0:
                for load in (loads[slot] for slot in (K0, K1, K2, K3)):
                    load.wait()
            for col in torus.colours:
                second = torus.wrap(col.second + gather.back[step])
                at_cols = pl.ds(col.index * (width // 2), width // 2)
                mixed = gat[second, :, :, at_cols] if col.index == 0 else gat[:, second, :, at_cols]
                mixed = mixed.reshape(side * rows, width // 2)

                def body(slot, carry, col=col, second=second, at_cols=at_cols, mixed=mixed):
                    term = dot(mixed, scr.w_mlp[slot, :, at_cols], NT).reshape(side, rows, hidden_loc)
                    if col.index == 0:
                        scr.pre[slot, second] += term
                    else:
                        scr.pre[slot, :, second] += term
                    return carry

                lax.fori_loop(0, 4, body, 0)
            for inner, count in ((0, step + 1), (1, step)):

                def block(index, carry, inner=inner):
                    shift = lax.rem(3 * index + 3 * lax.div(index * (index - 1), 2), side)
                    pair = (gather.back[step], shift) if inner == 0 else (shift, gather.back[step])
                    y_at, x_at = torus.wrap(torus.y + pair[K0]), torus.wrap(torus.x + pair[K1])
                    for core in PAIR:
                        gate, upper = scr.pre[2 - 2 * core, y_at, x_at], scr.pre[3 - 2 * core, y_at, x_at]
                        grad = scr.grad_act[core, y_at, x_at]
                        sigmoid_g = 1.0 / (1.0 + jnp.exp(-gate))
                        silu_g = gate * sigmoid_g
                        outs.acts[core][y_at, x_at] = (silu_g * upper).astype(BF16)
                        outs.gates[core][y_at, x_at] = (grad * upper * sigmoid_g * (1.0 + gate * (1.0 - sigmoid_g))).astype(BF16)
                        outs.ups[core][y_at, x_at] = (grad * silu_g).astype(BF16)
                    return carry

                lax.fori_loop(0, count, block, 0)

        run(gather.steps(products))
        gather.store.drain()
        swap_end(torus, scr.swap_sems, swaps, 3)
        torus.drain()

    dma = pltpu.SemaphoreType.DMA
    block = (side, side, rows, hidden_loc)
    ins = dict(ctx=(attn.ctx.reshape(side, side, rows, depth), VMEM), w_outs=[(weight, ANY) for weight in w_outs], hidden=(hidden, ANY), grad_out=(grad_out, ANY), gain=(gain, VMEM),
               normed=(attn.normed, ANY), w_gate=(w_gate, ANY), w_up=(w_up, ANY), w_down=(w_down, ANY))
    out, weight = (shape(block), VMEM), (shape((hidden_loc, width)), ANY)
    outs = dict(full=(shape((2, side, side, rows, width)), ANY), h_rows=(shape((rows, width)), VMEM), ctx_other=(shape((side, side, rows, depth // 2)), ANY), normed_other=(shape((seq, width)), ANY),
                w_gate=weight, w_up=weight, w_down=weight, acts=[out, out], gates=[out, out], ups=[out, out])
    scratch = dict(sum=rs_scratch(side, rows, width), all=ag_scratch(side, rows, width), w=pltpu.VMEM((depth, width), BF16), w_sem=dma((K2, K2)), swap_sems=[dma((5,)), dma((5,))],
                   x_rows=pltpu.VMEM((rows, width), BF16), x_sem=dma((K1,)), w_mlp=pltpu.VMEM((4, hidden_loc, width), BF16), w_mlp_sem=dma((4,)),
                   dy=pltpu.VMEM((2, side * rows, width), BF16), dy_sem=dma((K2,)), pre=pltpu.VMEM((4, *block), F32), grad_act=pltpu.VMEM((2, *block), F32))
    return call_kernel('sum_attention', body, ins, outs, scratch, 4e8, 1)


def sum_mlp(side, mlp, w_gates, w_ups, w_downs, grad_out, gain):
    depth = w_gates[K0].shape[K0]
    width = gain.shape[K1]
    rows = mlp.h_rows.shape[K0]
    seq = rows * side * side
    block = (side, side, rows, width)

    def body(ins, outs, scr):
        torus = Torus(side)
        weights = Weights(ins.w_in, scr.w, scr.w_sem, False)
        weights.start()
        weights_p = Weights(ins.w_downs, scr.wd, scr.wd_sem, False)
        weights_p.start()
        rows_at = pl.ds(pl.multiple_of(torus.chip * rows, rows), rows)
        dy_load = pltpu.make_async_copy(ins.grad_out.at[torus.core, rows_at, :], scr.dy_rows, scr.dy_sem.at[K0])
        dy_load.start()
        wait = torus.signal_all()
        steps = ReduceScatter(torus, scr.sum).steps(fill_partial(torus, scr.sum.part, ins.grads, weights))
        steps_p = ReduceScatter(torus, scr.sum_p).steps(fill_partial(torus, scr.sum_p.part, ins.acts, weights_p))
        steps[K0]()
        wait()

        turned = []

        def half_at(half):
            return pl.ds(pl.multiple_of(half * seq, seq), seq)

        def turn(index):
            kind, core = index // 2, index % 2
            src = (ins.grads[2 * core], ins.grads[2 * core + 1], ins.acts[core])[kind]
            slot = index % 2
            if index >= 2:
                turned[index - 2]()
            scr.turn[slot] = src[...].reshape(seq, depth).T
            at = pl.ds(kind * depth, depth), half_at(torus.core)
            if core == 0:
                save = pltpu.make_async_copy(scr.turn.at[slot], outs.left.at[at], scr.turn_sem.at[kind])
                save.start()
                turned.append(save.wait)
            else:
                torus.send(scr.turn.at[slot], outs.left.at[at], scr.swap_sems, kind, torus.partner)
                turned.append(torus.pending.pop().wait_send)

        turns = [functools.partial(turn, index) for index in range(6)]
        fills = (K0, K3, 4, 10)
        early = [steps_p[index] for index in fills]
        rest_p = [step for index, step in enumerate(steps_p) if index not in fills]
        late = 22
        run(steps[1:late], early)
        for step in rest_p[:3]:
            step()
        run(steps[late:])
        own = (torus.y, torus.x)
        gain_total = jnp.zeros((1, width), F32)
        gat = scr.all.gat
        dy_load.wait()
        for at in row_tiles(rows):
            back, gain_part = rms_back(ins.h_rows[at, :].astype(F32), ins.gain[...], scr.sum.part[(*own, at, slice(None))].astype(F32))
            gain_total = gain_total + gain_part
            total = scr.dy_rows[at, :].astype(F32) + back
            outs.d_rows[at, :] = total
            gat[(*own, at, slice(None))] = total.astype(BF16)
        outs.gain[...] = gain_total
        gather = AllGather(torus, scr.all, False)
        gather.store = Store(torus, scr.all, plain_places(gather, outs.full), outs.own)
        run(gather.steps(), rest_p[3:], turns)
        for at in row_tiles(rows):
            outs.y_rows[at, :] = (ins.h_rows[at, :].astype(F32) + scr.sum_p.part[(*own, at, slice(None))].astype(F32)).astype(BF16)
        turned[4]()
        turned[5]()
        for kind in range(3):
            torus.arrive(outs.left.at[pl.ds(kind * depth, depth), half_at(1 - torus.core)], scr.swap_sems, kind)
        gather.store.drain()
        torus.drain()

    dma = pltpu.SemaphoreType.DMA
    ins = dict(grads=[(grad, VMEM) for grad in (mlp.gates[K0], mlp.ups[K0], mlp.gates[K1], mlp.ups[K1])], acts=[(act, VMEM) for act in mlp.acts],
               w_in=[(weight, ANY) for weight in (w_gates[K0], w_ups[K0], w_gates[K1], w_ups[K1])], w_downs=[(weight, ANY) for weight in w_downs],
               h_rows=(mlp.h_rows, VMEM), grad_out=(grad_out, ANY), gain=(gain, VMEM))
    outs = dict(full=(shape((2, *block)), ANY), own=(shape(block), ANY), d_rows=(shape((rows, width), F32), VMEM), gain=(shape((1, width), F32), VMEM), y_rows=(shape((rows, width)), VMEM), left=(shape((3 * depth, 2 * seq)), ANY))
    scratch = dict(sum=rs_scratch(side, rows, width), sum_p=rs_scratch(side, rows, width), all=ag_scratch(side, rows, width), dy_rows=pltpu.VMEM((rows, width), BF16), dy_sem=dma((K1,)),
                   w=pltpu.VMEM((4 * depth, width), BF16), w_sem=dma((K2, 4)), wd=pltpu.VMEM((2 * depth, width), BF16), wd_sem=dma((K2, K2)),
                   turn=pltpu.VMEM((2, depth, seq), BF16), turn_sem=dma((K3,)), swap_sems=[dma((K3,)), dma((K3,))])
    return call_kernel('sum_mlp', body, ins, outs, scratch, 6e8, 2)


def sum_input(side, dqkv, w_qs, w_k, w_v, hidden, second, gain):
    seq, depth = dqkv.shape
    width = gain.shape[K1]
    rows = seq // (side * side)
    head = depth // 4
    half_side = side // 2
    tokens = seq // 2
    kv_width = w_k.shape[K1]
    per_kv = 2 * side * side * head // kv_width

    def body(ins, outs, scr):
        torus = Torus(side)
        kv_col = pl.multiple_of(lax.div(torus.chip * 2, per_kv) * head, head)
        weights = Weights([*ins.w_qs, ins.w_k.at[:, pl.ds(kv_col, head)], ins.w_v.at[:, pl.ds(kv_col, head)]], scr.w, scr.w_sem, True)
        weights.start()
        wait = torus.signal_all()
        part = scr.sum.part
        steps = ReduceScatter(torus, scr.sum).steps(fill_partial(torus, part, [ins.dqkv], weights))
        own = (torus.y, torus.x)
        gat = scr.all.gat
        gather = AllGather(torus, scr.all, True)

        def places(where, colour, half):
            chip = where[K0] * side + where[K1]
            tokens_at = pl.ds(pl.multiple_of(lax.rem(chip, 2) * tokens + colour * (tokens // 2), tokens // 2), tokens // 2)
            at = lax.div(chip, 2) * head
            src = gather.piece(gat, where, colour * 2, 2)
            return [(src.at[:, pl.ds(index * head, head)], outs.kv.at[half, tokens_at, pl.ds(pl.multiple_of(at + index * kv_width, head), head)]) for index in PAIR]

        gather.store = Store(torus, scr.all, places)
        rows_at = pl.ds(pl.multiple_of(torus.chip * rows, rows), rows)
        x_load = pltpu.make_async_copy(ins.hidden.at[torus.core, rows_at, :], scr.x_rows, scr.x_sem.at[K0])
        x_load.start()
        place = lax.rem(torus.x, 2)
        mate = torus.at_chip(torus.y, torus.x + 1 - 2 * place)
        kv_cols = pl.ds(2 * head, 2 * head)

        def mate_add():
            torus.arrive(scr.mate, scr.mate_sems, 0)
            mine = ins.dqkv[pl.ds(place * half_side, half_side), :, :, kv_cols]
            gat[own] = (mine.astype(F32) + scr.mate[...].astype(F32)).astype(BF16).reshape(tokens, 2 * head)

        steps[K0]()
        wait()
        swaps = [(ins.dqkv.at[:, :, :, pl.ds(head, head)], outs.q_other)]
        swap_start(torus, scr.swap_sems, swaps)
        torus.send(ins.dqkv.at[pl.ds((1 - place) * half_side, half_side), :, :, kv_cols], scr.mate, scr.mate_sems, 0, mate)
        for step in steps[1:5]:
            step()
        mate_add()
        run(steps[5:], gather.steps())
        x_load.wait()
        gain_total = jnp.zeros((1, width), F32)
        for at in row_tiles(rows):
            back, gain_part = rms_back(scr.x_rows[at, :].astype(F32), ins.gain[...], part[(*own, at, slice(None))].astype(F32))
            gain_total = gain_total + gain_part
            outs.rows[at, :] = (ins.d_rows[at, :] + back).astype(BF16)
        row = lax.broadcasted_iota(jnp.int32, (8, width), 0)
        extra = jnp.zeros((8, width), F32)
        for index, value in enumerate((gain_total, ins.gain_mlp[...])):
            for level in range(3):
                rounded = value.astype(BF16).astype(F32)
                extra = jnp.where(row == index * 3 + level, rounded, extra)
                value = value - rounded
        outs.rows[rows:rows + 8, :] = extra.astype(BF16)
        gather.store.drain()
        swap_end(torus, scr.swap_sems, swaps)
        torus.drain()

    dma = pltpu.SemaphoreType.DMA
    ins = dict(dqkv=(dqkv.reshape(side, side, rows, depth), VMEM), w_qs=[(weight, ANY) for weight in w_qs], w_k=(w_k, ANY), w_v=(w_v, ANY), hidden=(hidden, ANY), d_rows=(second.d_rows, VMEM),
               gain=(gain, VMEM), gain_mlp=(second.gain, VMEM))
    outs = dict(rows=(shape((rows + 8, width)), VMEM), kv=(shape((2, seq, 2 * kv_width)), ANY), q_other=(shape((side, side, rows, head)), ANY))
    scratch = dict(sum=rs_scratch(side, rows, width), all=ag_scratch(side, tokens, 2 * head, 2), x_rows=pltpu.VMEM((rows, width), BF16), x_sem=dma((K1,)), w=pltpu.VMEM((width, depth), BF16), w_sem=dma((K2, 4)),
                   mate=pltpu.VMEM((half_side, side, rows, 2 * head), BF16), mate_sems=[dma((K1,)), dma((K1,))], swap_sems=[dma((K1,)), dma((K1,))])
    return call_kernel('sum_input', body, ins, outs, scratch, 3e8, 3)


def scores_softmax(qkv, seg_row, seg_col, head_index, tile_index, tile):
    reach = (tile_index + 1) * tile
    queries = qkv[tile_index * tile:reach, head_index * HEAD_DIM:(head_index + 1) * HEAD_DIM]
    scores = dot(qkv[:reach, 2 * HEAD_DIM:3 * HEAD_DIM], queries, NT) * HEAD_DIM ** -0.5
    key_at = lax.broadcasted_iota(jnp.int32, (reach, tile), 0)
    query_at = lax.broadcasted_iota(jnp.int32, (reach, tile), 1) + tile_index * tile
    allowed = (key_at <= query_at) & (seg_col[:reach, :] == seg_row[:, tile_index * tile:reach])
    scores = jnp.where(allowed, scores, -1e30)
    weights = jnp.exp(scores - jnp.max(scores, axis=0, keepdims=True))
    return weights * (1.0 / jnp.sum(weights, axis=0, keepdims=True)), queries


def segments(seg_ref):
    core = lax.rem(lax.axis_index('tp'), 2)
    seg_row = seg_ref[pl.ds(core, 1), :].astype(F32)
    return seg_row, jnp.broadcast_to(seg_row, (8, seg_row.shape[K1])).T[:, :1]


def attention_forward(hidden, seg_ids, gain, w_q, w_k, w_v, w_o, per_kv):
    seq, width = hidden.shape[1:]
    chunk = seq // 4
    tile = min(256, seq)
    depth = 4 * HEAD_DIM

    def body(ins, outs, scr):
        tp_idx = lax.axis_index('tp')
        core = lax.rem(tp_idx, 2)
        kv_col = pl.multiple_of(lax.div(tp_idx, per_kv) * HEAD_DIM, HEAD_DIM)
        partner = dict(tp=tp_idx + 1 - 2 * core)
        barrier = pltpu.get_barrier_semaphore()
        pl.semaphore_signal(barrier, inc=1, device_id=partner, device_id_type=MESH)
        loads = []
        for index in range(4):
            at = pl.ds(index * chunk, chunk)
            loads.append(pltpu.make_async_copy(ins.hidden.at[core, at, :], scr.x.at[at, :], scr.x_sem.at[index]))

        def w_cols(index):
            return scr.w.at[:, pl.ds(index * HEAD_DIM, HEAD_DIM)]

        for index, ref in ((0, ins.w_q), (2, ins.w_k.at[:, pl.ds(kv_col, HEAD_DIM)]), (3, ins.w_v.at[:, pl.ds(kv_col, HEAD_DIM)])):
            loads.append(pltpu.make_async_copy(ref, w_cols(index), scr.w_sem.at[index]))
        for load in loads:
            load.start()
        pl.semaphore_wait(barrier, 1)
        swaps = [(ins.w_q, w_cols(1)), (ins.w_o, outs.w_o), (ins.w_q, outs.w_q)]
        copies = []
        for index, (src, dst) in enumerate(swaps):
            copies.append(pltpu.make_async_remote_copy(src, dst, scr.swap_sems[K0].at[index], scr.swap_sems[K1].at[index], device_id=partner, device_id_type=MESH))
            copies[index].start()
        stores = []
        for index in range(4):
            loads[index].wait()

            def normalize(step, carry, index=index):
                at = pl.ds(pl.multiple_of(index * chunk + step * 16, 16), 16)
                x_float = scr.x[at, :].astype(F32)
                inv = lax.rsqrt(jnp.mean(x_float * x_float, axis=-1, keepdims=True) + EPS)
                scr.normed[at, :] = (x_float * inv * ins.gain[...]).astype(BF16)
                return carry

            lax.fori_loop(0, chunk // 16, normalize, 0)
            at = pl.ds(index * chunk, chunk)
            store = pltpu.make_async_copy(scr.normed.at[at, :], outs.normed.at[at, :], scr.out_sem.at[index])
            store.start()
            stores.append(store)
            if index == 0:
                for load in loads[4:]:
                    load.wait()
                copies[K0].wait_recv()
            outs.qkv[at, :] = dot(scr.normed[at, :], scr.w[...], NN).astype(BF16)
        seg_row, seg_col = segments(ins.seg)
        values_t = outs.qkv[:, 3 * HEAD_DIM:].T
        for head_index in PAIR:
            for tile_index in range(seq // tile):
                probs, _ = scores_softmax(outs.qkv, seg_row, seg_col, head_index, tile_index, tile)
                ctx_t = dot(values_t[:, :(tile_index + 1) * tile], probs.astype(BF16), NN)
                outs.ctx[tile_index * tile:(tile_index + 1) * tile, head_index * HEAD_DIM:(head_index + 1) * HEAD_DIM] = ctx_t.T.astype(BF16)
        for store in stores:
            store.wait()
        copies[K0].wait_send()
        copies[K1].wait()
        copies[K2].wait()

    dma = pltpu.SemaphoreType.DMA
    ins = dict(hidden=(hidden, ANY), seg=(seg_ids, VMEM), gain=(gain, VMEM), w_q=(w_q, ANY), w_o=(w_o, ANY), w_k=(w_k, ANY), w_v=(w_v, ANY))
    outs = dict(normed=(shape((seq, width)), ANY), qkv=(shape((seq, depth)), VMEM), ctx=(shape((seq, 2 * HEAD_DIM)), VMEM), w_q=(shape(w_q.shape), ANY), w_o=(shape(w_o.shape), ANY))
    scratch = dict(swap_sems=[dma((K3,)), dma((K3,))], x=pltpu.VMEM((seq, width), BF16), normed=pltpu.VMEM((seq, width), BF16), w=pltpu.VMEM((width, depth), BF16), x_sem=dma((4,)), w_sem=dma((4,)), out_sem=dma((4,)))
    return call_kernel('attention_forward', body, ins, outs, scratch, 5e9, 4)


def attention_backward(resid, seg_ids, w_outs, qkv):
    seq, width = resid.shape
    chunk = seq // 4
    tile = min(256, seq)
    depth = 4 * HEAD_DIM

    def body(ins, outs, scr):
        loads = []
        for index in PAIR:
            at = pl.ds(index * HEAD_DIM, HEAD_DIM)
            loads.append(pltpu.make_async_copy(ins.w_outs[index], scr.w.at[at, :], scr.w_sem.at[index]))
        for index in range(4):
            at = pl.ds(index * chunk, chunk)
            loads.append(pltpu.make_async_copy(ins.resid.at[at, :], scr.resid.at[at, :], scr.in_sem.at[index]))
        for load in loads:
            load.start()
        for load in loads[:2]:
            load.wait()
        for index in range(4):
            loads[2 + index].wait()
            at = pl.ds(index * chunk, chunk)
            scr.grad_ctx[at, :] = dot(scr.resid[at, :], scr.w[...], NT).astype(BF16)
        seg_row, seg_col = segments(ins.seg)
        keys_t = ins.qkv[:, 2 * HEAD_DIM:3 * HEAD_DIM].T
        scr.grad_k[...] = jnp.zeros_like(scr.grad_k)
        scr.grad_v[...] = jnp.zeros_like(scr.grad_v)
        for head_index in PAIR:
            cols = slice(head_index * HEAD_DIM, (head_index + 1) * HEAD_DIM)
            for tile_index in range(seq // tile):
                reach = (tile_index + 1) * tile
                rows = slice(tile_index * tile, reach)
                probs, queries = scores_softmax(ins.qkv, seg_row, seg_col, head_index, tile_index, tile)
                grad_ctx = scr.grad_ctx[rows, cols]
                grad_probs = dot(ins.qkv[:reach, 3 * HEAD_DIM:], grad_ctx, NT)
                centre = jnp.sum(grad_probs * probs, axis=0, keepdims=True)
                grad_scores = (probs * (grad_probs - centre) * HEAD_DIM ** -0.5).astype(BF16)
                scr.grad_v[:reach, :] += dot(probs.astype(BF16), grad_ctx, NN)
                scr.grad_k[:reach, :] += dot(grad_scores, queries, NN)
                outs.dqkv[rows, cols] = dot(keys_t[:, :reach], grad_scores, NN).T.astype(BF16)
        outs.dqkv[:, 2 * HEAD_DIM:3 * HEAD_DIM] = scr.grad_k[...].astype(BF16)
        outs.dqkv[:, 3 * HEAD_DIM:] = scr.grad_v[...].astype(BF16)

    dma = pltpu.SemaphoreType.DMA
    ins = dict(resid=(resid, ANY), seg=(seg_ids, VMEM), w_outs=[(weight, ANY) for weight in w_outs], qkv=(qkv, VMEM))
    outs = dict(dqkv=(shape((seq, depth)), VMEM))
    scratch = dict(resid=pltpu.VMEM((seq, width), BF16), w=pltpu.VMEM((2 * HEAD_DIM, width), BF16), grad_ctx=pltpu.VMEM((seq, 2 * HEAD_DIM), BF16),
                   grad_k=pltpu.VMEM((seq, HEAD_DIM), F32), grad_v=pltpu.VMEM((seq, HEAD_DIM), F32), w_sem=dma((K2,)), in_sem=dma((4,)))
    return call_kernel('attention_backward', body, ins, outs, scratch, 4e9).dqkv


def weight_grads_mlp(mixed_full, grad_out, resid_full, left, ctxs, token):
    seq, width = grad_out.shape[1:]
    depth, head = left.shape[K0] // 3, ctxs[K1].shape[K1]
    tile = min(512, width)

    def kernel(m_ref, dy_ref, dh_ref, left_ref, ctx_own, ctx_other, _, out_gate, out_up, out_down, out_o, ctx_t):
        core = lax.rem(lax.axis_index('tp'), 2)

        @pl.when(pl.program_id(0) == 0)
        def _():
            for half, ref in ((core, ctx_own), (1 - core, ctx_other)):
                ctx_t[:, pl.ds(pl.multiple_of(half * seq, seq), seq)] = ref[:, :head].T

        def both(ref):
            return ref[...].reshape(2 * seq, tile)

        out_gate[...] = dot(left_ref[:depth, :], both(m_ref), NN)
        out_up[...] = dot(left_ref[depth:2 * depth, :], both(m_ref), NN)
        out_down[...] = dot(left_ref[2 * depth:, :], both(dy_ref), NN)
        out_o[...] = dot(ctx_t[...], both(dh_ref), NN)

    slab = pl.BlockSpec((2, seq, tile), lambda step: (0, 0, step))
    out = lambda size: pl.BlockSpec((size, tile), lambda step: (0, step))
    return pl.pallas_call(
        kernel,
        name='weight_grads_mlp',
        grid=(width // tile,),
        out_shape=[shape((depth, width), F32)] * 3 + [shape((head, width), F32)],
        in_specs=[slab] * 3 + [VMEM] * 3 + [ANY],
        out_specs=[out(depth)] * 3 + [out(head)],
        scratch_shapes=[pltpu.VMEM((head, 2 * seq), BF16)],
        compiler_params=pltpu.CompilerParams(vmem_limit_bytes=LIMIT),
        cost_estimate=pl.CostEstimate(flops=int(18e9), bytes_accessed=int(6e7), transcendentals=0),
    )(mixed_full, grad_out, resid_full, left, *ctxs, token)


def weight_grads_qkv(normeds, kv_full, grads_q):
    seq, width = normeds[K0].shape
    head = grads_q[K1].shape[K1]
    kv_width = kv_full.shape[K2] // 2
    tile = min(512, width)

    def kernel(a_own, a_other, kv_ref, q_own, q_other, out_q, out_k, out_v, left, q_both):
        core = lax.rem(lax.axis_index('tp'), 2)
        halves = [pl.ds(pl.multiple_of(half * seq, seq), seq) for half in (core, 1 - core)]

        @pl.when(pl.program_id(0) == 0)
        def _():
            q_both[halves[K0], :] = q_own[:, :head]
            q_both[halves[K1], :] = q_other[...]

        left[:, halves[K0]] = a_own[...].T
        left[:, halves[K1]] = a_other[...].T
        out_q[...] = dot(left[...], q_both[...], NN)
        for index, out in enumerate((out_k, out_v)):
            right = kv_ref[:, :, pl.ds(index * kv_width, kv_width)].reshape(2 * seq, kv_width)
            out[...] = dot(left[...], right, NN)

    slab = pl.BlockSpec((seq, tile), lambda step: (0, step))
    out = lambda size: pl.BlockSpec((tile, size), lambda step: (step, 0))
    return pl.pallas_call(
        kernel,
        name='weight_grads_qkv',
        grid=(width // tile,),
        out_shape=[shape((width, size), F32) for size in (head, kv_width, kv_width)],
        in_specs=[slab] * 2 + [VMEM] * 3,
        out_specs=[out(size) for size in (head, kv_width, kv_width)],
        scratch_shapes=[pltpu.VMEM((tile, 2 * seq), BF16), pltpu.VMEM((2 * seq, head), BF16)],
        compiler_params=pltpu.CompilerParams(vmem_limit_bytes=LIMIT),
        cost_estimate=pl.CostEstimate(flops=int(27e9), bytes_accessed=int(6e7), transcendentals=0),
    )(*normeds, kv_full, *grads_q)


def in_place(gathered, rows):
    blocks, held, width = gathered.shape
    slots = 24
    gains = 2 if held > rows else 0

    def kernel(src, dst, *refs):
        buf, extra, in_sem, out_sem, extra_sem = refs[gains:]

        def load(index):
            return pltpu.make_async_copy(src.at[index, pl.ds(0, rows), :], buf.at[index % slots], in_sem.at[index % slots])

        def store(index):
            return pltpu.make_async_copy(buf.at[index % slots], dst.at[index % 2, index // 2], out_sem.at[index % slots])

        ahead = slots // 2
        for index in range(blocks + ahead):
            if index < blocks:
                if index >= slots:
                    store(index - slots).wait()
                load(index).start()
            if index == ahead and gains:
                last = pltpu.make_async_copy(src.at[:, pl.ds(held - 8, 8), :], extra, extra_sem.at[K0])
                last.start()
            if index >= ahead:
                load(index - ahead).wait()
                store(index - ahead).start()
        if gains:
            last.wait()
            total = jnp.sum(extra[...].astype(F32), axis=0)
            for first, ref in zip((0, 3), refs):
                ref[...] = total[first:first + 1] + total[first + 1:first + 2] + total[first + 2:first + 3]
        for index in range(blocks - slots, blocks):
            store(index).wait()

    dma = pltpu.SemaphoreType.DMA
    return pl.pallas_call(
        kernel,
        name='in_place',
        out_shape=[shape((2, blocks // 2, rows, width))] + [shape((1, width), F32)] * gains,
        in_specs=[ANY],
        out_specs=[ANY] + [VMEM] * gains,
        scratch_shapes=[pltpu.VMEM((slots, rows, width), BF16), pltpu.VMEM((blocks, 8, width), BF16), dma((slots,)), dma((slots,)), dma((K1,))],
        compiler_params=pltpu.CompilerParams(vmem_limit_bytes=LIMIT),
        cost_estimate=pl.CostEstimate(flops=int(2e7), bytes_accessed=int(2e7), transcendentals=0),
    )(gathered)


def solution(mesh):
    tp_size = mesh.shape['tp']
    chips = tp_size // 2
    side = math.isqrt(chips)

    def device_step(hidden, seg_ids, grad_out, gain_attn, gain_mlp, w_q, w_k, w_v, w_o, w_gate, w_up, w_down):
        seq_len, width = hidden.shape[1:]
        kv_heads = w_k.shape[K1] // HEAD_DIM
        per_kv = tp_size // kv_heads
        rows = seq_len // chips

        def flat(value):
            return value.reshape(seq_len, value.shape[-1])

        gain_attn_row = gain_attn[None, :]
        gain_mlp_row = gain_mlp[None, :]

        attn = attention_forward(hidden, seg_ids, gain_attn_row, w_q, w_k, w_v, w_o, per_kv)
        w_qs, w_outs = (w_q, attn.w_q), (w_o, attn.w_o)
        mlp = sum_attention(side, attn, w_outs, hidden, grad_out, gain_mlp_row, w_gate.T, w_up.T, w_down)
        mixed_full = mlp.full.reshape(2, seq_len, width)
        second = sum_mlp(side, mlp, (w_gate.T, mlp.w_gate), (w_up.T, mlp.w_up), (w_down, mlp.w_down), grad_out, gain_mlp_row)
        resid_full = second.full.reshape(2, seq_len, width)

        (y_out,) = in_place(lax.all_gather(second.y_rows, 'tp'), rows)
        dqkv = attention_backward(flat(second.own), seg_ids, w_outs, attn.qkv)
        third = sum_input(side, dqkv, w_qs, w_k, w_v, hidden, second, gain_attn_row)
        grad_in, grad_gain_attn, grad_gain_mlp = in_place(lax.all_gather(third.rows, 'tp'), rows)
        grad_gate_t, grad_up_t, grad_w_down, grad_w_o = weight_grads_mlp(mixed_full, grad_out, resid_full, second.left, (attn.ctx, flat(mlp.ctx_other)), third.q_other)
        grad_w_q, grad_w_k, grad_w_v = weight_grads_qkv((attn.normed, mlp.normed_other), third.kv, (dqkv, flat(third.q_other)))
        return (y_out.reshape(hidden.shape), grad_in.reshape(hidden.shape), grad_gain_attn[K0], grad_gain_mlp[K0], grad_w_q, grad_w_k, grad_w_v, grad_w_o, grad_gate_t.T, grad_up_t.T, grad_w_down)

    spec_act = P('data', None, None)
    spec_rows = P('data', None)
    spec_gain = P(None)
    spec_cols = P(None, 'tp')
    spec_tprows = P('tp', None)
    spec_whole = P(None, None)
    spec_stack = P(('data', 'tp'), None)
    in_specs = (spec_act, spec_rows, spec_act, spec_gain, spec_gain, spec_cols, spec_whole, spec_whole, spec_tprows, spec_cols, spec_cols, spec_tprows)
    out_specs = (spec_act, spec_act, P('data'), P('data'), P('data', 'tp'), spec_rows, spec_rows, spec_stack, P('data', 'tp'), P('data', 'tp'), spec_stack)
    return jax.shard_map(device_step, mesh=mesh, in_specs=in_specs, out_specs=out_specs, check_vma=False)
```

```python
import functools
import math
import types
import jax
import jax.numpy as jnp
from jax import lax
from jax.experimental import pallas as pl
from jax.experimental.pallas import tpu as pltpu
from jax.sharding import PartitionSpec as P

HEAD_DIM = 128
EPS = 1e-5
MESH = pl.DeviceIdType.MESH
F32 = jnp.float32
BF16 = jnp.bfloat16
LIMIT = 63 * 2 ** 20
K0, K1, K2, K3 = range(4)
PAIR = range(2)
ANY = pl.BlockSpec(memory_space=pl.ANY)
VMEM = pl.BlockSpec(memory_space=pltpu.VMEM)


def dot(lhs, rhs, dims):
    return lax.dot_general(lhs, rhs, (dims, ((), ())), preferred_element_type=F32)


NN = ((1,), (0,))
NT = ((1,), (1,))


SIGNS = (1, -1)


class Colour:
    def __init__(self, index, first, second):
        self.index, self.first, self.second = index, first, second


class Torus:
    def __init__(self, side):
        self.side = side
        tp_idx = lax.axis_index('tp')
        self.core = lax.rem(tp_idx, 2)
        self.chip = lax.div(tp_idx, 2)
        self.x = lax.rem(self.chip, side)
        self.y = lax.div(self.chip, side)
        self.partner = {'tp': self.chip * 2 + (1 - self.core)}
        self.colours = (Colour(0, self.x, self.y), Colour(1, self.y, self.x))
        self.pending = []

    def wrap(self, pos):
        return lax.rem(pos + 2 * self.side, self.side)

    def at_chip(self, y_at, x_at):
        return {'tp': (y_at * self.side + x_at) * 2 + self.core}

    def block(self, col, second, first):
        return (second, first) if col.index == 0 else (first, second)

    def peer1(self, col, shift):
        return self.at_chip(*self.block(col, col.second, self.wrap(col.first + shift)))

    def peer2(self, col, shift):
        return self.at_chip(*self.block(col, self.wrap(col.second + shift), col.first))

    def signal_all(self):
        barrier = pltpu.get_barrier_semaphore()
        peers = [self.partner]
        peers += [self.at_chip(self.y, self.wrap(self.x + shift)) for shift in SIGNS]
        peers += [self.at_chip(self.wrap(self.y + shift), self.x) for shift in SIGNS]
        for peer in peers:
            pl.semaphore_signal(barrier, inc=1, device_id=peer, device_id_type=MESH)
        return lambda: pl.semaphore_wait(barrier, len(peers))

    def send(self, src, dst, sems, index, device):
        copy = pltpu.make_async_remote_copy(src, dst, sems[K0].at[index], sems[K1].at[index], device_id=device, device_id_type=MESH)
        copy.start()
        self.pending.append(copy)

    def arrive(self, dst, sems, index):
        pltpu.make_async_remote_copy(dst, dst, sems[K0].at[index], sems[K1].at[index], device_id=self.partner, device_id_type=MESH).wait_recv()

    def drain(self):
        for copy in self.pending:
            copy.wait_send()


R1, R2, R3, S1, S2, S3 = range(6)
RS_COUNTS = (16, 16, 16, 4, 4, 4)
H1, H2, F1, F2 = range(4)
AG_COUNTS = (8, 32, 4, 16)


class ReduceScatter:
    SHIFTS = (2, 1, 3, 0)

    def __init__(self, torus, scr):
        self.torus, self.part, self.scr = torus, scr.part, scr
        self.quarter = scr.part.shape[K3] // 4

    def buf(self, kind, index):
        return self.scr.bufs[kind].at[index]

    def sems(self, kind):
        return self.scr.out_sems[kind], self.scr.in_sems[kind]

    def cols(self, col, half):
        return pl.ds((col.index * 2 + half) * self.quarter, self.quarter)

    def piece(self, where, at_cols):
        return self.part.at[(*where, slice(None), at_cols)]

    def send(self, where, at_cols, kind, index, peer):
        self.torus.send(self.piece(where, at_cols), self.buf(kind, index), self.sems(kind), index, peer)

    def add(self, where, at_cols, *kinds):
        total = self.part[(*where, slice(None), at_cols)].astype(F32)
        for kind, index in kinds:
            self.torus.arrive(self.buf(kind, index), self.sems(kind), index)
            total = total + self.buf(kind, index)[...].astype(F32)
        self.part[(*where, slice(None), at_cols)] = total.astype(BF16)

    def each(self, step):
        wrap = self.torus.wrap
        for col in self.torus.colours:
            second = wrap(col.second + self.SHIFTS[step])
            for way, sign in enumerate(SIGNS):
                yield col, second, way, sign, (col.index * 2 + way) * 4 + step

    def far(self, step):
        for col, second, way, sign, index in self.each(step):
            where = self.torus.block(col, second, self.torus.wrap(col.first + 2))
            self.send(where, self.cols(col, way), R1, index, self.torus.peer1(col, sign))

    def near(self, step):
        for col, second, way, sign, index in self.each(step):
            where = self.torus.block(col, second, self.torus.wrap(col.first + sign))
            self.send(where, self.cols(col, 1 - way), R2, index, self.torus.peer1(col, sign))

    def relay(self, step):
        for col, second, way, sign, index in self.each(step):
            where = self.torus.block(col, second, self.torus.wrap(col.first + sign))
            self.add(where, self.cols(col, way), (R1, index))
            self.send(where, self.cols(col, way), R3, index, self.torus.peer1(col, sign))

    def end(self, step):
        for col, second, way, sign, index in self.each(step):
            where = self.torus.block(col, second, col.first)
            other = (col.index * 2 + 1 - way) * 4 + step
            self.add(where, self.cols(col, way), (R2, other), (R3, index))

    def far2(self):
        for col in self.torus.colours:
            for way, sign in enumerate(SIGNS):
                where = self.torus.block(col, self.torus.wrap(col.second + 2), col.first)
                self.send(where, self.cols(col, way), S1, col.index * 2 + way, self.torus.peer2(col, sign))

    def near2(self, way):
        for col in self.torus.colours:
            where = self.torus.block(col, self.torus.wrap(col.second + SIGNS[way]), col.first)
            self.send(where, self.cols(col, 1 - way), S2, col.index * 2 + way, self.torus.peer2(col, SIGNS[way]))

    def relay2(self, way):
        for col in self.torus.colours:
            index = col.index * 2 + way
            where = self.torus.block(col, self.torus.wrap(col.second + SIGNS[way]), col.first)
            self.add(where, self.cols(col, way), (S1, index))
            self.send(where, self.cols(col, way), S3, index, self.torus.peer2(col, SIGNS[way]))

    def end2(self):
        for col in self.torus.colours:
            where = self.torus.block(col, col.second, col.first)
            for way in PAIR:
                self.add(where, self.cols(col, way), (S2, col.index * 2 + 1 - way), (S3, col.index * 2 + way))

    def steps(self, fill):
        call = functools.partial
        return [call(fill, K2), call(self.far, K0), call(self.far, K1), call(fill, K1), call(fill, K3),
                call(self.near, K0), call(self.relay, K0), call(self.near, K1), call(self.far, K2), call(self.relay, K1),
                call(fill, K0), call(self.near, K2), call(self.far, K3), call(self.end, K0), self.far2,
                call(self.relay, K2), call(self.near, K3), call(self.end, K1), call(self.near2, K0), call(self.relay2, K0),
                call(self.relay, K3), call(self.end, K2), call(self.near2, K1), call(self.relay2, K1), call(self.end, K3),
                self.end2]


class AllGather:
    def __init__(self, torus, scr, by_rows):
        self.torus, self.gat, self.scr, self.by_rows, self.store = torus, scr.gat, scr, by_rows, None
        self.quarter = scr.gat.shape[2 if by_rows else 3] // 4
        self.back = (0, torus.side - 1, 1, 2)

    def sems(self, kind):
        return self.scr.out_sems[kind], self.scr.in_sems[kind]

    def piece(self, ref, where, first, count):
        at = pl.ds(first * self.quarter, count * self.quarter)
        return ref.at[(*where, at, slice(None))] if self.by_rows else ref.at[(*where, slice(None), at)]

    def half(self, col, where, half):
        return self.piece(self.gat, where, col.index * 2 + half, 1)

    def own2(self, turn):
        for col in self.torus.colours:
            where = self.torus.block(col, col.second, col.first)
            for way, sign in enumerate(SIGNS):
                at = self.half(col, where, way if turn == 0 else 1 - way)
                self.torus.send(at, at, self.sems(H1), (col.index * 2 + way) * 2 + turn, self.torus.peer2(col, sign))

    def send1(self, step, turn):
        for col in self.torus.colours:
            where = self.torus.block(col, self.torus.wrap(col.second + self.back[step]), col.first)
            for way, sign in enumerate(SIGNS):
                at = self.half(col, where, way if turn == 0 else 1 - way)
                self.torus.send(at, at, self.sems(H2), ((col.index * 2 + way) * 4 + step) * 2 + turn, self.torus.peer1(col, sign))

    def arrive2(self, way, turn):
        sign = SIGNS[way]
        for col in self.torus.colours:
            where = self.torus.block(col, self.torus.wrap(col.second - sign), col.first)
            at = self.half(col, where, way if turn == 0 else 1 - way)
            self.torus.arrive(at, self.sems(H1), (col.index * 2 + way) * 2 + turn)
            if turn == 0:
                self.torus.send(at, at, self.sems(F1), col.index * 2 + way, self.torus.peer2(col, sign))

    def relayed2(self):
        for col in self.torus.colours:
            where = self.torus.block(col, self.torus.wrap(col.second + 2), col.first)
            for way in PAIR:
                self.torus.arrive(self.half(col, where, way), self.sems(F1), col.index * 2 + way)

    def arrive1(self, step, turn):
        for col in self.torus.colours:
            second = self.torus.wrap(col.second + self.back[step])
            for way, sign in enumerate(SIGNS):
                where = self.torus.block(col, second, self.torus.wrap(col.first - sign))
                at = self.half(col, where, way if turn == 0 else 1 - way)
                self.torus.arrive(at, self.sems(H2), ((col.index * 2 + way) * 4 + step) * 2 + turn)
                if turn == 0:
                    self.torus.send(at, at, self.sems(F2), (col.index * 2 + way) * 4 + step, self.torus.peer1(col, sign))

    def relayed1(self, step):
        for col in self.torus.colours:
            second = self.torus.wrap(col.second + self.back[step])
            for way in PAIR:
                where = self.torus.block(col, second, self.torus.wrap(col.first + 2))
                self.torus.arrive(self.half(col, where, way), self.sems(F2), (col.index * 2 + way) * 4 + step)

    def keep(self, step, firsts):
        for col in self.torus.colours:
            for shift in firsts:
                where = self.torus.block(col, self.torus.wrap(col.second + self.back[step]), self.torus.wrap(col.first + shift))
                self.store.keep(where, col.index, lambda ref, where=where, col=col: self.piece(ref, where, col.index * 2, 2))

    def steps(self, whole=None):
        call = functools.partial
        whole = whole or (lambda step: None)
        here, beside, across = (K0,), (K1, self.torus.side - 1), (K2,)
        result = []
        for turn in PAIR:
            result += [call(self.own2, turn), call(self.send1, K0, turn)]
        result += [call(self.keep, K0, here), call(self.arrive2, K0, K0), call(self.arrive2, K1, K0)]
        for way in PAIR:
            step = way + K1
            result += [call(self.arrive2, way, K1), call(self.send1, step, K0), call(self.send1, step, K1), call(self.keep, step, here)]
        result += [call(self.arrive1, K0, K0), self.relayed2, call(self.send1, K3, K0), call(self.send1, K3, K1), call(self.keep, K3, here),
                   call(self.arrive1, K0, K1), call(self.keep, K0, beside), call(self.arrive1, K1, K0), call(self.arrive1, K2, K0),
                   call(self.relayed1, K0), call(self.keep, K0, across), call(whole, K0)]
        for step in (K1, K2):
            result += [call(self.arrive1, step, K1), call(self.keep, step, beside)]
        result += [call(self.arrive1, K3, K0)]
        for step in (K1, K2):
            result += [call(self.relayed1, step), call(self.keep, step, across), call(whole, step)]
        return result + [call(self.arrive1, K3, K1), call(self.keep, K3, beside), call(self.relayed1, K3), call(self.keep, K3, across), call(whole, K3)]


class Store:
    def __init__(self, torus, scr, places, own=None):
        self.torus, self.scr, self.places, self.own = torus, scr, places, own
        self.stores = []

    def slot(self, where, colour, index):
        return ((index * 2 + colour) * self.torus.side + where[K0]) * self.torus.side + where[K1]

    def keep(self, where, colour, piece):
        for index, (src, dst) in enumerate(self.places(where, colour, self.torus.core)):
            slot = self.slot(where, colour, index)
            pairs = [(self.scr.full_sem, dst)]
            if self.own is not None:
                pairs.append((self.scr.own_sem, piece(self.own)))
            for sem, ref in pairs:
                store = pltpu.make_async_copy(src, ref, sem.at[slot])
                store.start()
                self.stores.append(store)
            self.torus.send(src, dst, self.scr.cross_sems, slot, self.torus.partner)

    def drain(self):
        for store in self.stores:
            store.wait()
        side = self.torus.side
        for colour in PAIR:
            for y_at in range(side):
                for x_at in range(side):
                    for index, (_, dst) in enumerate(self.places((y_at, x_at), colour, 1 - self.torus.core)):
                        self.torus.arrive(dst, self.scr.cross_sems, self.slot((y_at, x_at), colour, index))


def plain_places(gather, full):
    return lambda where, colour, half: [(gather.piece(gather.gat, where, colour * 2, 2), gather.piece(full.at[half], where, colour * 2, 2))]


def rs_scratch(side, rows, width):
    dma = pltpu.SemaphoreType.DMA
    return dict(
        part=pltpu.VMEM((side, side, rows, width), BF16),
        bufs=[pltpu.VMEM((count, rows, width // 4), BF16) for count in RS_COUNTS],
        out_sems=[dma((count,)) for count in RS_COUNTS],
        in_sems=[dma((count,)) for count in RS_COUNTS],
    )


def ag_scratch(side, rows, width, places=1):
    dma = pltpu.SemaphoreType.DMA
    blocks = 2 * side * side * places
    return dict(
        gat=pltpu.VMEM((side, side, rows, width), BF16),
        out_sems=[dma((count,)) for count in AG_COUNTS],
        in_sems=[dma((count,)) for count in AG_COUNTS],
        full_sem=dma((blocks,)),
        own_sem=dma((blocks,)),
        cross_sems=[dma((blocks,)), dma((blocks,))],
    )


class Weights:
    def __init__(self, refs, buf, sem, by_rows):
        self.refs, self.buf, self.sem, self.by_rows = refs, buf, sem, by_rows
        self.copies = [[], []]

    def start(self):
        for colour in PAIR:
            for index, ref in enumerate(self.refs):
                if self.by_rows:
                    half, depth = ref.shape[K0] // 2, ref.shape[K1]
                    rows, cols = pl.ds(colour * half, half), pl.ds(index * depth, depth)
                    copy = pltpu.make_async_copy(ref.at[rows, :], self.buf.at[rows, cols], self.sem.at[colour, index])
                else:
                    half, depth = ref.shape[K1] // 2, ref.shape[K0]
                    rows, cols = pl.ds(index * depth, depth), pl.ds(colour * half, half)
                    copy = pltpu.make_async_copy(ref.at[:, cols], self.buf.at[rows, cols], self.sem.at[colour, index])
                copy.start()
                self.copies[colour].append(copy)

    def wait(self, colour):
        for copy in self.copies[colour]:
            copy.wait()
        self.copies[colour] = []


def fill_partial(torus, part, lhs, weights):
    rows, width = part.shape[2:]
    tile = min(512, width // 2)

    def fill(shift):
        for col in torus.colours:
            weights.wait(col.index)
            first = torus.wrap(col.first + shift)
            left = []
            for ref in lhs:
                depth = ref.shape[K3]
                value = ref[:, first] if col.index == 0 else ref[first]
                left.append((value.reshape(torus.side * rows, depth), depth))

            def body(step, carry, col=col, first=first, left=left):
                at = pl.ds(pl.multiple_of(col.index * (width // 2) + step * tile, tile), tile)
                total = None
                base = 0
                for value, depth in left:
                    if weights.by_rows:
                        term = dot(value, weights.buf[at, base:base + depth], NT)
                    else:
                        term = dot(value, weights.buf[base:base + depth, at], NN)
                    total = term if total is None else total + term
                    base += depth
                total = total.astype(BF16).reshape(torus.side, rows, tile)
                if col.index == 0:
                    part[:, first, :, at] = total
                else:
                    part[first, :, :, at] = total
                return carry

            lax.fori_loop(0, (width // 2) // tile, body, 0)

    return fill


def run(*lists):
    keyed = []
    for order, steps in enumerate(lists):
        keyed += [((index + 0.5) / len(steps), order, step) for index, step in enumerate(steps)]
    for _, _, step in sorted(keyed, key=lambda item: item[:2]):
        step()


def swap_start(torus, sems, pairs):
    for index, (src, dst) in enumerate(pairs):
        torus.send(src, dst, sems, index, torus.partner)


def swap_end(torus, sems, pairs, first=0):
    for index, (_, dst) in enumerate(pairs):
        if index >= first:
            torus.arrive(dst, sems, index)


def row_tiles(rows):
    return [pl.ds(start, 16) for start in range(0, rows, 16)]


def rms_back(z_in, gain, grad):
    inv = lax.rsqrt(jnp.mean(z_in * z_in, axis=-1, keepdims=True) + EPS)
    normed = z_in * inv
    scaled = grad * gain
    back = inv * (scaled - normed * jnp.mean(scaled * normed, axis=-1, keepdims=True))
    return back, jnp.sum(grad * normed, axis=0, keepdims=True)


def bag(tree):
    if isinstance(tree, dict):
        return types.SimpleNamespace(**{key: bag(value) for key, value in tree.items()})
    return [bag(value) for value in tree] if isinstance(tree, list) else tree


class Staging:
    def __init__(self, loads, saves):
        self.loads, self.saves, self.left = loads, saves, {}

    def start(self):
        for load in self.loads:
            load.start()

    def wait(self):
        for load in self.loads:
            load.wait()

    def save(self, *refs):
        for ref, save in self.saves:
            if any(ref is one for one in refs):
                save.start()
                self.left[id(ref)] = save

    def finish(self):
        self.save(*[ref for ref, _ in self.saves if id(ref) not in self.left])
        for save in self.left.values():
            save.wait()


def call_kernel(name, body, ins, outs, scratch, flops, collective_id=None):
    is_leaf = lambda value: isinstance(value, tuple)
    in_leaves, in_tree = jax.tree.flatten(ins, is_leaf=is_leaf)
    out_leaves, out_tree = jax.tree.flatten(outs, is_leaf=is_leaf)
    scr_leaves, scr_tree = jax.tree.flatten(scratch)
    first_scr = len(in_leaves) + len(out_leaves)
    staged = [index for index, leaf in enumerate(in_leaves + out_leaves) if leaf[K1] is VMEM]
    stages = []
    for index in staged:
        leaf = (in_leaves + out_leaves)[index][K0]
        stages.append(pltpu.VMEM(leaf.shape, leaf.dtype))

    def kernel(*refs):
        refs = list(refs)
        own = refs[first_scr + len(scr_leaves):]
        sem = own.pop()
        loads, saves = [], []
        for slot, (index, ref) in enumerate(zip(staged, own)):
            if index < len(in_leaves):
                loads.append(pltpu.make_async_copy(refs[index], ref, sem.at[slot]))
            else:
                saves.append((ref, pltpu.make_async_copy(ref, refs[index], sem.at[slot])))
            refs[index] = ref
        staging = Staging(loads, saves)
        staging.start()
        body(bag(in_tree.unflatten(refs[:len(in_leaves)])), bag(out_tree.unflatten(refs[len(in_leaves):first_scr])), bag(scr_tree.unflatten(refs[first_scr:first_scr + len(scr_leaves)])), staging)
        staging.finish()

    results = pl.pallas_call(
        kernel,
        name=name,
        out_shape=[leaf[K0] for leaf in out_leaves],
        in_specs=[ANY] * len(in_leaves),
        out_specs=[ANY] * len(out_leaves),
        scratch_shapes=scr_leaves + stages + [pltpu.SemaphoreType.DMA((len(staged),))],
        compiler_params=pltpu.CompilerParams(collective_id=collective_id, has_side_effects=collective_id is not None, vmem_limit_bytes=LIMIT),
        cost_estimate=pl.CostEstimate(flops=int(flops), bytes_accessed=int(4e7), transcendentals=0),
    )(*[leaf[K0] for leaf in in_leaves])
    return bag(out_tree.unflatten(results))


def shape(dims, dtype=BF16):
    return jax.ShapeDtypeStruct(dims, dtype)


def sum_attention(side, attn, w_outs, hidden, grad_out, gain, w_gate, w_up, w_down):
    seq, depth = attn.ctx.shape
    width = gain.shape[K1]
    hidden_loc = w_gate.shape[K0]
    rows = seq // (side * side)

    def body(ins, outs, scr, staging):
        torus = Torus(side)
        weights = Weights(ins.w_outs, scr.w, scr.w_sem, False)
        weights.start()
        rows_at = pl.ds(pl.multiple_of(torus.chip * rows, rows), rows)
        x_load = pltpu.make_async_copy(ins.hidden.at[torus.core, rows_at, :], scr.x_rows, scr.x_sem.at[K0])
        x_load.start()

        def load_weight(src, slot):
            load = pltpu.make_async_copy(src, scr.w_mlp.at[slot], scr.w_mlp_sem.at[slot])
            load.start()
            return load

        loads = {slot: load_weight(src, slot) for slot, src in ((K0, ins.w_down), (K2, ins.w_gate), (K3, ins.w_up))}
        wait = torus.signal_all()
        part = scr.sum.part
        steps = ReduceScatter(torus, scr.sum).steps(fill_partial(torus, part, [ins.ctx], weights))
        staging.wait()
        steps[K0]()
        wait()
        other_ctx = ins.ctx.at[:, :, :, pl.ds(depth // 2, depth // 2)]
        swaps = [(ins.w_down, outs.w_down), (ins.w_gate, outs.w_gate), (ins.w_up, outs.w_up), (other_ctx, outs.ctx_other), (ins.normed, outs.normed_other)]
        swap_start(torus, scr.swap_sems, swaps)

        def dy_load(group):
            at = pl.ds(group * side * rows, side * rows)
            return pltpu.make_async_copy(ins.grad_out.at[torus.core, at, :], scr.dy.at[group % 2], scr.dy_sem.at[group % 2])

        def grad_act(group):
            if group == 0:
                torus.arrive(outs.w_down, scr.swap_sems, 0)
                loads[K1] = load_weight(outs.w_down, K1)
                for slot in PAIR:
                    loads[slot].wait()
            dy_load(group).wait()
            for slot in PAIR:
                product = dot(scr.dy[group % 2], scr.w_mlp[slot], NT)
                scr.grad_act[slot, group] = product.reshape(side, rows, hidden_loc)
            if group + 2 < side:
                dy_load(group + 2).start()

        dy_load(0).start()
        dy_load(1).start()
        half = len(steps) // 3
        run(steps[1:half])
        run(steps[half:], [functools.partial(grad_act, group) for group in range(side)])
        for index, (slot, out) in enumerate(((K0, outs.w_gate), (K1, outs.w_up))):
            torus.arrive(out, scr.swap_sems, index + 1)
            loads[slot] = load_weight(out, slot)
        scr.pre[...] = jnp.zeros_like(scr.pre)
        gat = scr.all.gat
        own = (torus.y, torus.x)
        x_load.wait()
        for at in row_tiles(rows):
            resid = (scr.x_rows[at, :].astype(F32) + part[(*own, at, slice(None))].astype(F32)).astype(BF16)
            outs.h_rows[at, :] = resid
            z_in = resid.astype(F32)
            inv = lax.rsqrt(jnp.mean(z_in * z_in, axis=-1, keepdims=True) + EPS)
            gat[(*own, at, slice(None))] = (z_in * inv * ins.gain[...]).astype(BF16)
        staging.save(outs.h_rows)
        gather = AllGather(torus, scr.all, False)
        gather.store = Store(torus, scr.all, plain_places(gather, outs.full))

        def products(step):
            if step == 0:
                for load in (loads[slot] for slot in (K0, K1, K2, K3)):
                    load.wait()
            for col in torus.colours:
                second = torus.wrap(col.second + gather.back[step])
                at_cols = pl.ds(col.index * (width // 2), width // 2)
                mixed = gat[second, :, :, at_cols] if col.index == 0 else gat[:, second, :, at_cols]
                mixed = mixed.reshape(side * rows, width // 2)

                def body(slot, carry, col=col, second=second, at_cols=at_cols, mixed=mixed):
                    term = dot(mixed, scr.w_mlp[slot, :, at_cols], NT).reshape(side, rows, hidden_loc)
                    if col.index == 0:
                        scr.pre[slot, second] += term
                    else:
                        scr.pre[slot, :, second] += term
                    return carry

                lax.fori_loop(0, 4, body, 0)
            for inner, count in ((0, step + 1), (1, step)):

                def block(index, carry, inner=inner):
                    shift = lax.rem(3 * index + 3 * lax.div(index * (index - 1), 2), side)
                    pair = (gather.back[step], shift) if inner == 0 else (shift, gather.back[step])
                    y_at, x_at = torus.wrap(torus.y + pair[K0]), torus.wrap(torus.x + pair[K1])
                    for core in PAIR:
                        gate, upper = scr.pre[2 - 2 * core, y_at, x_at], scr.pre[3 - 2 * core, y_at, x_at]
                        grad = scr.grad_act[core, y_at, x_at]
                        sigmoid_g = 1.0 / (1.0 + jnp.exp(-gate))
                        silu_g = gate * sigmoid_g
                        scr.results[core, y_at, x_at] = (silu_g * upper).astype(BF16)
                        scr.results[2 + core, y_at, x_at] = (grad * upper * sigmoid_g * (1.0 + gate * (1.0 - sigmoid_g))).astype(BF16)
                        scr.results[4 + core, y_at, x_at] = (grad * silu_g).astype(BF16)
                    for kind, out in enumerate(outs.acts + outs.gates + outs.ups):
                        pltpu.make_async_copy(scr.results.at[kind, y_at, x_at], out.at[y_at, x_at], scr.result_sem.at[kind]).start()
                    return carry

                lax.fori_loop(0, count, block, 0)

        run(gather.steps(products))
        for kind, out in enumerate(outs.acts + outs.gates + outs.ups):
            pltpu.make_async_copy(scr.results.at[kind], out, scr.result_sem.at[kind]).wait()
        gather.store.drain()
        swap_end(torus, scr.swap_sems, swaps, 3)
        torus.drain()

    dma = pltpu.SemaphoreType.DMA
    block = (side, side, rows, hidden_loc)
    ins = dict(ctx=(attn.ctx.reshape(side, side, rows, depth), VMEM), w_outs=[(weight, ANY) for weight in w_outs], hidden=(hidden, ANY), grad_out=(grad_out, ANY), gain=(gain, VMEM),
               normed=(attn.normed, ANY), w_gate=(w_gate, ANY), w_up=(w_up, ANY), w_down=(w_down, ANY))
    out, weight = (shape(block), ANY), (shape((hidden_loc, width)), ANY)
    outs = dict(full=(shape((2, side, side, rows, width)), ANY), h_rows=(shape((rows, width)), VMEM), ctx_other=(shape((side, side, rows, depth // 2)), ANY), normed_other=(shape((seq, width)), ANY),
                w_gate=weight, w_up=weight, w_down=weight, acts=[out, out], gates=[out, out], ups=[out, out])
    scratch = dict(sum=rs_scratch(side, rows, width), all=ag_scratch(side, rows, width), w=pltpu.VMEM((depth, width), BF16), w_sem=dma((K2, K2)), swap_sems=[dma((5,)), dma((5,))],
                   x_rows=pltpu.VMEM((rows, width), BF16), x_sem=dma((K1,)), w_mlp=pltpu.VMEM((4, hidden_loc, width), BF16), w_mlp_sem=dma((4,)),
                   dy=pltpu.VMEM((2, side * rows, width), BF16), dy_sem=dma((K2,)), pre=pltpu.VMEM((4, *block), F32), grad_act=pltpu.VMEM((2, *block), F32), results=pltpu.VMEM((6, *block), BF16), result_sem=dma((6,)))
    return call_kernel('sum_attention', body, ins, outs, scratch, 4e8, 1)


def sum_mlp(side, mlp, w_gates, w_ups, w_downs, grad_out, gain):
    depth = w_gates[K0].shape[K0]
    width = gain.shape[K1]
    rows = mlp.h_rows.shape[K0]
    seq = rows * side * side
    block = (side, side, rows, width)

    def body(ins, outs, scr, staging):
        torus = Torus(side)
        weights = Weights(ins.w_in, scr.w, scr.w_sem, False)
        weights.start()
        weights_p = Weights(ins.w_downs, scr.wd, scr.wd_sem, False)
        weights_p.start()
        rows_at = pl.ds(pl.multiple_of(torus.chip * rows, rows), rows)
        dy_load = pltpu.make_async_copy(ins.grad_out.at[torus.core, rows_at, :], scr.dy_rows, scr.dy_sem.at[K0])
        dy_load.start()
        wait = torus.signal_all()
        steps = ReduceScatter(torus, scr.sum).steps(fill_partial(torus, scr.sum.part, ins.grads, weights))
        steps_p = ReduceScatter(torus, scr.sum_p).steps(fill_partial(torus, scr.sum_p.part, ins.acts, weights_p))
        staging.wait()
        steps[K0]()
        wait()

        turned = []

        def half_at(half):
            return pl.ds(pl.multiple_of(half * seq, seq), seq)

        def turn(index):
            kind, core = index // 2, index % 2
            src = (ins.grads[2 * core], ins.grads[2 * core + 1], ins.acts[core])[kind]
            slot = index % 2
            if index >= 2:
                turned[index - 2]()
            scr.turn[slot] = src[...].reshape(seq, depth).T
            at = slice(None), half_at(torus.core)
            if core == 0:
                save = pltpu.make_async_copy(scr.turn.at[slot], outs.lefts[kind].at[at], scr.turn_sem.at[kind])
                save.start()
                turned.append(save.wait)
            else:
                torus.send(scr.turn.at[slot], outs.lefts[kind].at[at], scr.swap_sems, kind, torus.partner)
                turned.append(torus.pending.pop().wait_send)

        turns = [functools.partial(turn, index) for index in range(6)]
        fills = (K0, K3, 4, 10)
        early = [steps_p[index] for index in fills]
        rest_p = [step for index, step in enumerate(steps_p) if index not in fills]
        late = 22
        run(steps[1:late], early)
        for step in rest_p[:3]:
            step()
        run(steps[late:])
        own = (torus.y, torus.x)
        gain_total = jnp.zeros((1, width), F32)
        gat = scr.all.gat
        dy_load.wait()
        for at in row_tiles(rows):
            back, gain_part = rms_back(ins.h_rows[at, :].astype(F32), ins.gain[...], scr.sum.part[(*own, at, slice(None))].astype(F32))
            gain_total = gain_total + gain_part
            total = scr.dy_rows[at, :].astype(F32) + back
            outs.d_rows[at, :] = total
            gat[(*own, at, slice(None))] = total.astype(BF16)
        outs.gain[...] = gain_total
        staging.save(outs.d_rows, outs.gain)
        gather = AllGather(torus, scr.all, False)
        gather.store = Store(torus, scr.all, plain_places(gather, outs.full), outs.own)
        run(gather.steps(), rest_p[3:], turns)
        for at in row_tiles(rows):
            outs.y_rows[at, :] = (ins.h_rows[at, :].astype(F32) + scr.sum_p.part[(*own, at, slice(None))].astype(F32)).astype(BF16)
        staging.save(outs.y_rows)
        turned[4]()
        turned[5]()
        for kind in range(3):
            torus.arrive(outs.lefts[kind].at[:, half_at(1 - torus.core)], scr.swap_sems, kind)
        gather.store.drain()
        torus.drain()

    dma = pltpu.SemaphoreType.DMA
    ins = dict(grads=[(grad, VMEM) for grad in (mlp.gates[K0], mlp.ups[K0], mlp.gates[K1], mlp.ups[K1])], acts=[(act, VMEM) for act in mlp.acts],
               w_in=[(weight, ANY) for weight in (w_gates[K0], w_ups[K0], w_gates[K1], w_ups[K1])], w_downs=[(weight, ANY) for weight in w_downs],
               h_rows=(mlp.h_rows, VMEM), grad_out=(grad_out, ANY), gain=(gain, VMEM))
    outs = dict(full=(shape((2, *block)), ANY), own=(shape(block), ANY), d_rows=(shape((rows, width), F32), VMEM), gain=(shape((1, width), F32), VMEM), y_rows=(shape((rows, width)), VMEM), lefts=[(shape((depth, 2 * seq)), ANY)] * 3)
    scratch = dict(sum=rs_scratch(side, rows, width), sum_p=rs_scratch(side, rows, width), all=ag_scratch(side, rows, width), dy_rows=pltpu.VMEM((rows, width), BF16), dy_sem=dma((K1,)),
                   w=pltpu.VMEM((4 * depth, width), BF16), w_sem=dma((K2, 4)), wd=pltpu.VMEM((2 * depth, width), BF16), wd_sem=dma((K2, K2)),
                   turn=pltpu.VMEM((2, depth, seq), BF16), turn_sem=dma((K3,)), swap_sems=[dma((K3,)), dma((K3,))])
    return call_kernel('sum_mlp', body, ins, outs, scratch, 6e8, 2)


def sum_input(side, dqkv, w_qs, w_k, w_v, hidden, second, gain):
    seq, depth = dqkv.shape
    width = gain.shape[K1]
    rows = seq // (side * side)
    head = depth // 4
    half_side = side // 2
    tokens = seq // 2
    kv_width = w_k.shape[K1]
    per_kv = 2 * side * side * head // kv_width

    def body(ins, outs, scr, staging):
        torus = Torus(side)
        kv_col = pl.multiple_of(lax.div(torus.chip * 2, per_kv) * head, head)
        weights = Weights([*ins.w_qs, ins.w_k.at[:, pl.ds(kv_col, head)], ins.w_v.at[:, pl.ds(kv_col, head)]], scr.w, scr.w_sem, True)
        weights.start()
        wait = torus.signal_all()
        part = scr.sum.part
        steps = ReduceScatter(torus, scr.sum).steps(fill_partial(torus, part, [ins.dqkv], weights))
        own = (torus.y, torus.x)
        gat = scr.all.gat
        gather = AllGather(torus, scr.all, True)

        def places(where, colour, half):
            chip = where[K0] * side + where[K1]
            tokens_at = pl.ds(pl.multiple_of(lax.rem(chip, 2) * tokens + colour * (tokens // 2), tokens // 2), tokens // 2)
            at = lax.div(chip, 2) * head
            src = gather.piece(gat, where, colour * 2, 2)
            return [(src.at[:, pl.ds(index * head, head)], outs.kv.at[half, tokens_at, pl.ds(pl.multiple_of(at + index * kv_width, head), head)]) for index in PAIR]

        gather.store = Store(torus, scr.all, places)
        rows_at = pl.ds(pl.multiple_of(torus.chip * rows, rows), rows)
        x_load = pltpu.make_async_copy(ins.hidden.at[torus.core, rows_at, :], scr.x_rows, scr.x_sem.at[K0])
        x_load.start()
        place = lax.rem(torus.x, 2)
        mate = torus.at_chip(torus.y, torus.x + 1 - 2 * place)
        kv_cols = pl.ds(2 * head, 2 * head)

        def mate_add():
            torus.arrive(scr.mate, scr.mate_sems, 0)
            mine = ins.dqkv[pl.ds(place * half_side, half_side), :, :, kv_cols]
            gat[own] = (mine.astype(F32) + scr.mate[...].astype(F32)).astype(BF16).reshape(tokens, 2 * head)

        staging.wait()
        steps[K0]()
        wait()
        swaps = [(ins.dqkv.at[:, :, :, pl.ds(head, head)], outs.q_other)]
        swap_start(torus, scr.swap_sems, swaps)
        torus.send(ins.dqkv.at[pl.ds((1 - place) * half_side, half_side), :, :, kv_cols], scr.mate, scr.mate_sems, 0, mate)
        for step in steps[1:5]:
            step()
        mate_add()
        run(steps[5:], gather.steps())
        x_load.wait()
        gain_total = jnp.zeros((1, width), F32)
        for at in row_tiles(rows):
            back, gain_part = rms_back(scr.x_rows[at, :].astype(F32), ins.gain[...], part[(*own, at, slice(None))].astype(F32))
            gain_total = gain_total + gain_part
            outs.rows[at, :] = (ins.d_rows[at, :] + back).astype(BF16)
        row = lax.broadcasted_iota(jnp.int32, (8, width), 0)
        extra = jnp.zeros((8, width), F32)
        for index, value in enumerate((gain_total, ins.gain_mlp[...])):
            for level in range(3):
                rounded = value.astype(BF16).astype(F32)
                extra = jnp.where(row == index * 3 + level, rounded, extra)
                value = value - rounded
        outs.rows[rows:rows + 8, :] = extra.astype(BF16)
        staging.save(outs.rows)
        gather.store.drain()
        swap_end(torus, scr.swap_sems, swaps)
        torus.drain()

    dma = pltpu.SemaphoreType.DMA
    ins = dict(dqkv=(dqkv.reshape(side, side, rows, depth), VMEM), w_qs=[(weight, ANY) for weight in w_qs], w_k=(w_k, ANY), w_v=(w_v, ANY), hidden=(hidden, ANY), d_rows=(second.d_rows, VMEM),
               gain=(gain, VMEM), gain_mlp=(second.gain, VMEM))
    outs = dict(rows=(shape((rows + 8, width)), VMEM), kv=(shape((2, seq, 2 * kv_width)), ANY), q_other=(shape((side, side, rows, head)), ANY))
    scratch = dict(sum=rs_scratch(side, rows, width), all=ag_scratch(side, tokens, 2 * head, 2), x_rows=pltpu.VMEM((rows, width), BF16), x_sem=dma((K1,)), w=pltpu.VMEM((width, depth), BF16), w_sem=dma((K2, 4)),
                   mate=pltpu.VMEM((half_side, side, rows, 2 * head), BF16), mate_sems=[dma((K1,)), dma((K1,))], swap_sems=[dma((K1,)), dma((K1,))])
    return call_kernel('sum_input', body, ins, outs, scratch, 3e8, 3)


def scores_softmax(qkv, seg_row, seg_col, head_index, tile_index, tile):
    reach = (tile_index + 1) * tile
    queries = qkv[tile_index * tile:reach, head_index * HEAD_DIM:(head_index + 1) * HEAD_DIM]
    scores = dot(qkv[:reach, 2 * HEAD_DIM:3 * HEAD_DIM], queries, NT) * HEAD_DIM ** -0.5
    key_at = lax.broadcasted_iota(jnp.int32, (reach, tile), 0)
    query_at = lax.broadcasted_iota(jnp.int32, (reach, tile), 1) + tile_index * tile
    allowed = (key_at <= query_at) & (seg_col[:reach, :] == seg_row[:, tile_index * tile:reach])
    scores = jnp.where(allowed, scores, -1e30)
    weights = jnp.exp(scores - jnp.max(scores, axis=0, keepdims=True))
    return weights * (1.0 / jnp.sum(weights, axis=0, keepdims=True)), queries


def segments(seg_ref):
    core = lax.rem(lax.axis_index('tp'), 2)
    seg_row = seg_ref[pl.ds(core, 1), :].astype(F32)
    return seg_row, jnp.broadcast_to(seg_row, (8, seg_row.shape[K1])).T[:, :1]


def attention_forward(hidden, seg_ids, gain, w_q, w_k, w_v, w_o, per_kv):
    seq, width = hidden.shape[1:]
    chunk = seq // 4
    tile = min(256, seq)
    depth = 4 * HEAD_DIM

    def body(ins, outs, scr, staging):
        tp_idx = lax.axis_index('tp')
        core = lax.rem(tp_idx, 2)
        kv_col = pl.multiple_of(lax.div(tp_idx, per_kv) * HEAD_DIM, HEAD_DIM)
        partner = dict(tp=tp_idx + 1 - 2 * core)
        barrier = pltpu.get_barrier_semaphore()
        pl.semaphore_signal(barrier, inc=1, device_id=partner, device_id_type=MESH)
        loads = []
        for index in range(4):
            at = pl.ds(index * chunk, chunk)
            loads.append(pltpu.make_async_copy(ins.hidden.at[core, at, :], scr.x.at[at, :], scr.x_sem.at[index]))

        def w_cols(index):
            return scr.w.at[:, pl.ds(index * HEAD_DIM, HEAD_DIM)]

        for index, ref in ((0, ins.w_q), (2, ins.w_k.at[:, pl.ds(kv_col, HEAD_DIM)]), (3, ins.w_v.at[:, pl.ds(kv_col, HEAD_DIM)])):
            loads.append(pltpu.make_async_copy(ref, w_cols(index), scr.w_sem.at[index]))
        for load in loads:
            load.start()
        pl.semaphore_wait(barrier, 1)
        swaps = [(ins.w_q, w_cols(1)), (ins.w_o, outs.w_o), (ins.w_q, outs.w_q)]
        copies = []
        for index, (src, dst) in enumerate(swaps):
            copies.append(pltpu.make_async_remote_copy(src, dst, scr.swap_sems[K0].at[index], scr.swap_sems[K1].at[index], device_id=partner, device_id_type=MESH))
            copies[index].start()
        stores = []
        for index in range(4):
            loads[index].wait()

            if index == 0:
                staging.wait()

            def square(step, carry, index=index):
                at = pl.ds(pl.multiple_of(index * chunk + step * 16, 16), 16)
                total = jnp.zeros((16, HEAD_DIM), F32)
                for lane in range(0, width, HEAD_DIM):
                    value = scr.x[at, lane:lane + HEAD_DIM].astype(F32)
                    total = total + value * value
                scr.squares[pl.ds(pl.multiple_of(step * 16, 16), 16), :] = total
                return carry

            lax.fori_loop(0, chunk // 16, square, 0)
            inv = lax.rsqrt(jnp.sum(scr.squares[...], axis=-1, keepdims=True) / width + EPS)
            scr.squares[...] = jnp.broadcast_to(inv, scr.squares.shape)

            def normalize(step, carry, index=index):
                at = pl.ds(pl.multiple_of(index * chunk + step * 16, 16), 16)
                scale = scr.squares[pl.ds(pl.multiple_of(step * 16, 16), 16), :]
                for lane in range(0, width, HEAD_DIM):
                    cols = slice(lane, lane + HEAD_DIM)
                    scr.normed[at, cols] = (scr.x[at, cols].astype(F32) * scale * ins.gain[:, cols]).astype(BF16)
                return carry

            lax.fori_loop(0, chunk // 16, normalize, 0)
            at = pl.ds(index * chunk, chunk)
            store = pltpu.make_async_copy(scr.normed.at[at, :], outs.normed.at[at, :], scr.out_sem.at[index])
            store.start()
            stores.append(store)
            if index == 0:
                for load in loads[4:]:
                    load.wait()
                copies[K0].wait_recv()
            outs.qkv[at, :] = dot(scr.normed[at, :], scr.w[...], NN).astype(BF16)
        staging.save(outs.qkv)
        seg_row, seg_col = segments(ins.seg)
        values_t = outs.qkv[:, 3 * HEAD_DIM:].T
        for head_index in PAIR:
            for tile_index in range(seq // tile):
                probs, _ = scores_softmax(outs.qkv, seg_row, seg_col, head_index, tile_index, tile)
                ctx_t = dot(values_t[:, :(tile_index + 1) * tile], probs.astype(BF16), NN)
                outs.ctx[tile_index * tile:(tile_index + 1) * tile, head_index * HEAD_DIM:(head_index + 1) * HEAD_DIM] = ctx_t.T.astype(BF16)
        for store in stores:
            store.wait()
        copies[K0].wait_send()
        copies[K1].wait()
        copies[K2].wait()

    dma = pltpu.SemaphoreType.DMA
    ins = dict(hidden=(hidden, ANY), seg=(seg_ids, VMEM), gain=(gain, VMEM), w_q=(w_q, ANY), w_o=(w_o, ANY), w_k=(w_k, ANY), w_v=(w_v, ANY))
    outs = dict(normed=(shape((seq, width)), ANY), qkv=(shape((seq, depth)), VMEM), ctx=(shape((seq, 2 * HEAD_DIM)), VMEM), w_q=(shape(w_q.shape), ANY), w_o=(shape(w_o.shape), ANY))
    scratch = dict(squares=pltpu.VMEM((chunk, HEAD_DIM), F32), swap_sems=[dma((K3,)), dma((K3,))], x=pltpu.VMEM((seq, width), BF16), normed=pltpu.VMEM((seq, width), BF16), w=pltpu.VMEM((width, depth), BF16), x_sem=dma((4,)), w_sem=dma((4,)), out_sem=dma((4,)))
    return call_kernel('attention_forward', body, ins, outs, scratch, 5e9, 4)


def attention_backward(resid, seg_ids, w_outs, qkv, token):
    seq, width = resid.shape
    chunk = seq // 4
    tile = min(256, seq)
    depth = 4 * HEAD_DIM

    def body(ins, outs, scr, staging):
        loads = []
        for index in PAIR:
            at = pl.ds(index * HEAD_DIM, HEAD_DIM)
            loads.append(pltpu.make_async_copy(ins.w_outs[index], scr.w.at[at, :], scr.w_sem.at[index]))
        for index in range(4):
            at = pl.ds(index * chunk, chunk)
            loads.append(pltpu.make_async_copy(ins.resid.at[at, :], scr.resid.at[at, :], scr.in_sem.at[index]))
        for load in loads:
            load.start()
        for load in loads[:2]:
            load.wait()
        staging.wait()
        for index in range(4):
            loads[2 + index].wait()
            at = pl.ds(index * chunk, chunk)
            scr.grad_ctx[at, :] = dot(scr.resid[at, :], scr.w[...], NT).astype(BF16)
        seg_row, seg_col = segments(ins.seg)
        keys_t = ins.qkv[:, 2 * HEAD_DIM:3 * HEAD_DIM].T
        scr.grad_k[...] = jnp.zeros_like(scr.grad_k)
        scr.grad_v[...] = jnp.zeros_like(scr.grad_v)
        for head_index in PAIR:
            cols = slice(head_index * HEAD_DIM, (head_index + 1) * HEAD_DIM)
            for tile_index in range(seq // tile):
                reach = (tile_index + 1) * tile
                rows = slice(tile_index * tile, reach)
                probs, queries = scores_softmax(ins.qkv, seg_row, seg_col, head_index, tile_index, tile)
                grad_ctx = scr.grad_ctx[rows, cols]
                grad_probs = dot(ins.qkv[:reach, 3 * HEAD_DIM:], grad_ctx, NT)
                centre = jnp.sum(grad_probs * probs, axis=0, keepdims=True)
                grad_scores = (probs * (grad_probs - centre) * HEAD_DIM ** -0.5).astype(BF16)
                scr.grad_v[:reach, :] += dot(probs.astype(BF16), grad_ctx, NN)
                scr.grad_k[:reach, :] += dot(grad_scores, queries, NN)
                outs.dqkv[rows, cols] = dot(keys_t[:, :reach], grad_scores, NN).T.astype(BF16)
        outs.dqkv[:, 2 * HEAD_DIM:3 * HEAD_DIM] = scr.grad_k[...].astype(BF16)
        outs.dqkv[:, 3 * HEAD_DIM:] = scr.grad_v[...].astype(BF16)

    dma = pltpu.SemaphoreType.DMA
    ins = dict(resid=(resid, ANY), seg=(seg_ids, VMEM), w_outs=[(weight, ANY) for weight in w_outs], qkv=(qkv, VMEM), token=(token, ANY))
    outs = dict(dqkv=(shape((seq, depth)), VMEM))
    scratch = dict(resid=pltpu.VMEM((seq, width), BF16), w=pltpu.VMEM((2 * HEAD_DIM, width), BF16), grad_ctx=pltpu.VMEM((seq, 2 * HEAD_DIM), BF16),
                   grad_k=pltpu.VMEM((seq, HEAD_DIM), F32), grad_v=pltpu.VMEM((seq, HEAD_DIM), F32), w_sem=dma((K2,)), in_sem=dma((4,)))
    return call_kernel('attention_backward', body, ins, outs, scratch, 4e9).dqkv


def weight_grads(name, groups, ctxs, tokens=()):
    seq, width = groups[K0][K1].shape[1:]
    head = ctxs[K1].shape[K1] if ctxs else 0
    tile = min(512, width)
    lefts = [left for left, _ in groups if left is not None]
    sizes = [head if left is None else left.shape[K0] for left, _ in groups]
    given = len(groups) + len(lefts) + len(ctxs)

    def kernel(*refs):
        rights, left_refs = refs[:len(groups)], list(refs[len(groups):len(groups) + len(lefts)])
        outs = refs[given + len(tokens):given + len(tokens) + len(groups)]
        if ctxs:
            core = lax.rem(lax.axis_index('tp'), 2)
            ctx_t = refs[-1]

            @pl.when(pl.program_id(0) == 0)
            def _():
                for half, ref in zip((core, 1 - core), refs[given - 2:given]):
                    ctx_t[:, pl.ds(pl.multiple_of(half * seq, seq), seq)] = ref[:, :head].T

        for (left, _), right, out in zip(groups, rights, outs):
            ref = ctx_t if left is None else left_refs.pop(0)
            out[...] = dot(ref[...], right[...].reshape(2 * seq, tile), NN)

    slab = pl.BlockSpec((2, seq, tile), lambda step: (0, 0, step))
    return pl.pallas_call(
        kernel,
        name=name,
        grid=(width // tile,),
        out_shape=[shape((size, width), F32) for size in sizes],
        in_specs=[slab] * len(groups) + [VMEM] * (len(lefts) + len(ctxs)) + [ANY] * len(tokens),
        out_specs=[pl.BlockSpec((size, tile), lambda step: (0, step)) for size in sizes],
        scratch_shapes=[pltpu.VMEM((head, 2 * seq), BF16)] if ctxs else [],
        compiler_params=pltpu.CompilerParams(vmem_limit_bytes=LIMIT),
        cost_estimate=pl.CostEstimate(flops=int(1e10), bytes_accessed=int(4e7), transcendentals=0),
    )(*[right for _, right in groups], *lefts, *ctxs, *tokens)


def weight_grads_pair(left_gate, left_up, mixed_full):
    seq, width = mixed_full.shape[1:]
    depth = left_gate.shape[K0]
    tile = min(512, width)

    def kernel(m_ref, gate_ref, up_ref, out_gate, out_up):
        mixed = m_ref[...].reshape(2 * seq, tile)
        out_gate[...] = dot(gate_ref[...], mixed, NN)
        out_up[...] = dot(up_ref[...], mixed, NN)

    out = pl.BlockSpec((depth, tile), lambda step: (0, step))
    return pl.pallas_call(
        kernel,
        name='weight_grads_pair',
        grid=(width // tile,),
        out_shape=[shape((depth, width), F32)] * 2,
        in_specs=[pl.BlockSpec((2, seq, tile), lambda step: (0, 0, step)), VMEM, VMEM],
        out_specs=[out, out],
        compiler_params=pltpu.CompilerParams(vmem_limit_bytes=LIMIT),
        cost_estimate=pl.CostEstimate(flops=int(1e10), bytes_accessed=int(4e7), transcendentals=0),
    )(mixed_full, left_gate, left_up)


def weight_grads_qkv(normeds, kv_full, grads_q):
    seq, width = normeds[K0].shape
    head = grads_q[K1].shape[K1]
    kv_width = kv_full.shape[K2] // 2
    tile = min(512, width)

    def kernel(a_own, a_other, kv_ref, q_own, q_other, out_q, out_k, out_v, left, q_both):
        core = lax.rem(lax.axis_index('tp'), 2)
        halves = [pl.ds(pl.multiple_of(half * seq, seq), seq) for half in (core, 1 - core)]

        @pl.when(pl.program_id(0) == 0)
        def _():
            q_both[halves[K0], :] = q_own[:, :head]
            q_both[halves[K1], :] = q_other[...]

        left[:, halves[K0]] = a_own[...].T
        left[:, halves[K1]] = a_other[...].T
        out_q[...] = dot(left[...], q_both[...], NN)
        for index, out in enumerate((out_k, out_v)):
            right = kv_ref[:, :, pl.ds(index * kv_width, kv_width)].reshape(2 * seq, kv_width)
            out[...] = dot(left[...], right, NN)

    slab = pl.BlockSpec((seq, tile), lambda step: (0, step))
    out = lambda size: pl.BlockSpec((tile, size), lambda step: (step, 0))
    return pl.pallas_call(
        kernel,
        name='weight_grads_qkv',
        grid=(width // tile,),
        out_shape=[shape((width, size), F32) for size in (head, kv_width, kv_width)],
        in_specs=[slab] * 2 + [VMEM] * 3,
        out_specs=[out(size) for size in (head, kv_width, kv_width)],
        scratch_shapes=[pltpu.VMEM((tile, 2 * seq), BF16), pltpu.VMEM((2 * seq, head), BF16)],
        compiler_params=pltpu.CompilerParams(vmem_limit_bytes=LIMIT),
        cost_estimate=pl.CostEstimate(flops=int(27e9), bytes_accessed=int(6e7), transcendentals=0),
    )(*normeds, kv_full, *grads_q)


def in_place(gathered, rows):
    blocks, held, width = gathered.shape
    slots = 24
    gains = 2 if held > rows else 0

    def kernel(src, dst, *refs):
        buf, extra, in_sem, out_sem, extra_sem = refs[gains:]

        def load(index):
            return pltpu.make_async_copy(src.at[index, pl.ds(0, rows), :], buf.at[index % slots], in_sem.at[index % slots])

        def store(index):
            return pltpu.make_async_copy(buf.at[index % slots], dst.at[index % 2, index // 2], out_sem.at[index % slots])

        ahead = slots // 2
        for index in range(blocks + ahead):
            if index < blocks:
                if index >= slots:
                    store(index - slots).wait()
                load(index).start()
            if index == ahead and gains:
                last = pltpu.make_async_copy(src.at[:, pl.ds(held - 8, 8), :], extra, extra_sem.at[K0])
                last.start()
            if index >= ahead:
                load(index - ahead).wait()
                store(index - ahead).start()
        if gains:
            last.wait()
            total = jnp.sum(extra[...].astype(F32), axis=0)
            for first, ref in zip((0, 3), refs):
                ref[...] = total[first:first + 1] + total[first + 1:first + 2] + total[first + 2:first + 3]
        for index in range(blocks - slots, blocks):
            store(index).wait()

    dma = pltpu.SemaphoreType.DMA
    return pl.pallas_call(
        kernel,
        name='in_place',
        out_shape=[shape((2, blocks // 2, rows, width))] + [shape((1, width), F32)] * gains,
        in_specs=[ANY],
        out_specs=[ANY] + [VMEM] * gains,
        scratch_shapes=[pltpu.VMEM((slots, rows, width), BF16), pltpu.VMEM((blocks, 8, width), BF16), dma((slots,)), dma((slots,)), dma((K1,))],
        compiler_params=pltpu.CompilerParams(vmem_limit_bytes=LIMIT),
        cost_estimate=pl.CostEstimate(flops=int(2e7), bytes_accessed=int(2e7), transcendentals=0),
    )(gathered)


def solution(mesh):
    tp_size = mesh.shape['tp']
    chips = tp_size // 2
    side = math.isqrt(chips)

    def device_step(hidden, seg_ids, grad_out, gain_attn, gain_mlp, w_q, w_k, w_v, w_o, w_gate, w_up, w_down):
        seq_len, width = hidden.shape[1:]
        kv_heads = w_k.shape[K1] // HEAD_DIM
        per_kv = tp_size // kv_heads
        rows = seq_len // chips

        def flat(value):
            return value.reshape(seq_len, value.shape[-1])

        gain_attn_row = gain_attn[None, :]
        gain_mlp_row = gain_mlp[None, :]

        attn = attention_forward(hidden, seg_ids, gain_attn_row, w_q, w_k, w_v, w_o, per_kv)
        w_qs, w_outs = (w_q, attn.w_q), (w_o, attn.w_o)
        mlp = sum_attention(side, attn, w_outs, hidden, grad_out, gain_mlp_row, w_gate.T, w_up.T, w_down)
        mixed_full = mlp.full.reshape(2, seq_len, width)
        second = sum_mlp(side, mlp, (w_gate.T, mlp.w_gate), (w_up.T, mlp.w_up), (w_down, mlp.w_down), grad_out, gain_mlp_row)
        resid_full = second.full.reshape(2, seq_len, width)

        (y_out,) = in_place(lax.all_gather(second.y_rows, 'tp'), rows)
        left_gate, left_up, left_act = second.lefts
        grad_gate_t, grad_up_t = weight_grads_pair(left_gate, left_up, mixed_full)
        dqkv = attention_backward(flat(second.own), seg_ids, w_outs, attn.qkv, grad_up_t)
        third = sum_input(side, dqkv, w_qs, w_k, w_v, hidden, second, gain_attn_row)
        grad_in, grad_gain_attn, grad_gain_mlp = in_place(lax.all_gather(third.rows, 'tp'), rows)
        grad_w_down, grad_w_o = weight_grads('weight_grads_down', [(left_act, grad_out), (None, resid_full)], (attn.ctx, flat(mlp.ctx_other)), (third.q_other,))
        grad_w_q, grad_w_k, grad_w_v = weight_grads_qkv((attn.normed, mlp.normed_other), third.kv, (dqkv, flat(third.q_other)))
        return (y_out.reshape(hidden.shape), grad_in.reshape(hidden.shape), grad_gain_attn[K0], grad_gain_mlp[K0], grad_w_q, grad_w_k, grad_w_v, grad_w_o, grad_gate_t.T, grad_up_t.T, grad_w_down)

    spec_act = P('data', None, None)
    spec_rows = P('data', None)
    spec_gain = P(None)
    spec_cols = P(None, 'tp')
    spec_tprows = P('tp', None)
    spec_whole = P(None, None)
    spec_stack = P(('data', 'tp'), None)
    in_specs = (spec_act, spec_rows, spec_act, spec_gain, spec_gain, spec_cols, spec_whole, spec_whole, spec_tprows, spec_cols, spec_cols, spec_tprows)
    out_specs = (spec_act, spec_act, P('data'), P('data'), P('data', 'tp'), spec_rows, spec_rows, spec_stack, P('data', 'tp'), P('data', 'tp'), spec_stack)
    return jax.shard_map(device_step, mesh=mesh, in_specs=in_specs, out_specs=out_specs, check_vma=False)
```

```python
import functools
import math
import types
import jax
import jax.numpy as jnp
from jax import lax
from jax.experimental import pallas as pl
from jax.experimental.pallas import tpu as pltpu
from jax.sharding import PartitionSpec as P

HEAD_DIM = 128
EPS = 1e-5
MESH = pl.DeviceIdType.MESH
F32 = jnp.float32
BF16 = jnp.bfloat16
LIMIT = 63 * 2 ** 20
K0, K1, K2, K3 = range(4)
PAIR = range(2)
ANY = pl.BlockSpec(memory_space=pl.ANY)
VMEM = pl.BlockSpec(memory_space=pltpu.VMEM)


def dot(lhs, rhs, dims):
    return lax.dot_general(lhs, rhs, (dims, ((), ())), preferred_element_type=F32)


NN = ((1,), (0,))
NT = ((1,), (1,))


SIGNS = (1, -1)


class Colour:
    def __init__(self, index, first, second):
        self.index, self.first, self.second = index, first, second


class Torus:
    def __init__(self, side):
        self.side = side
        tp_idx = lax.axis_index('tp')
        self.core = lax.rem(tp_idx, 2)
        self.chip = lax.div(tp_idx, 2)
        self.x = lax.rem(self.chip, side)
        self.y = lax.div(self.chip, side)
        self.partner = {'tp': self.chip * 2 + (1 - self.core)}
        self.colours = (Colour(0, self.x, self.y), Colour(1, self.y, self.x))
        self.pending = []

    def wrap(self, pos):
        return lax.rem(pos + 2 * self.side, self.side)

    def at_chip(self, y_at, x_at):
        return {'tp': (y_at * self.side + x_at) * 2 + self.core}

    def block(self, col, second, first):
        return (second, first) if col.index == 0 else (first, second)

    def peer1(self, col, shift):
        return self.at_chip(*self.block(col, col.second, self.wrap(col.first + shift)))

    def peer2(self, col, shift):
        return self.at_chip(*self.block(col, self.wrap(col.second + shift), col.first))

    def signal_all(self):
        barrier = pltpu.get_barrier_semaphore()
        peers = [self.partner]
        peers += [self.at_chip(self.y, self.wrap(self.x + shift)) for shift in SIGNS]
        peers += [self.at_chip(self.wrap(self.y + shift), self.x) for shift in SIGNS]
        for peer in peers:
            pl.semaphore_signal(barrier, inc=1, device_id=peer, device_id_type=MESH)
        return lambda: pl.semaphore_wait(barrier, len(peers))

    def send(self, src, dst, sems, index, device):
        copy = pltpu.make_async_remote_copy(src, dst, sems[K0].at[index], sems[K1].at[index], device_id=device, device_id_type=MESH)
        copy.start()
        self.pending.append(copy)

    def arrive(self, dst, sems, index):
        pltpu.make_async_remote_copy(dst, dst, sems[K0].at[index], sems[K1].at[index], device_id=self.partner, device_id_type=MESH).wait_recv()

    def drain(self):
        for copy in self.pending:
            copy.wait_send()


R1, R2, R3, S1, S2, S3 = range(6)
RS_COUNTS = (16, 16, 16, 4, 4, 4)
H1, H2, F1, F2 = range(4)
AG_COUNTS = (8, 32, 4, 16)


class ReduceScatter:
    SHIFTS = (2, 1, 3, 0)

    def __init__(self, torus, scr):
        self.torus, self.part, self.scr = torus, scr.part, scr
        self.quarter = scr.part.shape[K3] // 4

    def buf(self, kind, index):
        return self.scr.bufs[kind].at[index]

    def sems(self, kind):
        return self.scr.out_sems[kind], self.scr.in_sems[kind]

    def cols(self, col, half):
        return pl.ds((col.index * 2 + half) * self.quarter, self.quarter)

    def piece(self, where, at_cols):
        return self.part.at[(*where, slice(None), at_cols)]

    def send(self, where, at_cols, kind, index, peer):
        self.torus.send(self.piece(where, at_cols), self.buf(kind, index), self.sems(kind), index, peer)

    def add(self, where, at_cols, *kinds):
        total = self.part[(*where, slice(None), at_cols)].astype(F32)
        for kind, index in kinds:
            self.torus.arrive(self.buf(kind, index), self.sems(kind), index)
            total = total + self.buf(kind, index)[...].astype(F32)
        self.part[(*where, slice(None), at_cols)] = total.astype(BF16)

    def each(self, step):
        wrap = self.torus.wrap
        for col in self.torus.colours:
            second = wrap(col.second + self.SHIFTS[step])
            for way, sign in enumerate(SIGNS):
                yield col, second, way, sign, (col.index * 2 + way) * 4 + step

    def far(self, step):
        for col, second, way, sign, index in self.each(step):
            where = self.torus.block(col, second, self.torus.wrap(col.first + 2))
            self.send(where, self.cols(col, way), R1, index, self.torus.peer1(col, sign))

    def near(self, step):
        for col, second, way, sign, index in self.each(step):
            where = self.torus.block(col, second, self.torus.wrap(col.first + sign))
            self.send(where, self.cols(col, 1 - way), R2, index, self.torus.peer1(col, sign))

    def relay(self, step):
        for col, second, way, sign, index in self.each(step):
            where = self.torus.block(col, second, self.torus.wrap(col.first + sign))
            self.add(where, self.cols(col, way), (R1, index))
            self.send(where, self.cols(col, way), R3, index, self.torus.peer1(col, sign))

    def end(self, step):
        for col, second, way, sign, index in self.each(step):
            where = self.torus.block(col, second, col.first)
            other = (col.index * 2 + 1 - way) * 4 + step
            self.add(where, self.cols(col, way), (R2, other), (R3, index))

    def far2(self):
        for col in self.torus.colours:
            for way, sign in enumerate(SIGNS):
                where = self.torus.block(col, self.torus.wrap(col.second + 2), col.first)
                self.send(where, self.cols(col, way), S1, col.index * 2 + way, self.torus.peer2(col, sign))

    def near2(self, way):
        for col in self.torus.colours:
            where = self.torus.block(col, self.torus.wrap(col.second + SIGNS[way]), col.first)
            self.send(where, self.cols(col, 1 - way), S2, col.index * 2 + way, self.torus.peer2(col, SIGNS[way]))

    def relay2(self, way):
        for col in self.torus.colours:
            index = col.index * 2 + way
            where = self.torus.block(col, self.torus.wrap(col.second + SIGNS[way]), col.first)
            self.add(where, self.cols(col, way), (S1, index))
            self.send(where, self.cols(col, way), S3, index, self.torus.peer2(col, SIGNS[way]))

    def end2(self):
        for col in self.torus.colours:
            where = self.torus.block(col, col.second, col.first)
            for way in PAIR:
                self.add(where, self.cols(col, way), (S2, col.index * 2 + 1 - way), (S3, col.index * 2 + way))

    def steps(self, fill):
        call = functools.partial
        return [call(fill, K2), call(self.far, K0), call(self.far, K1), call(fill, K1), call(fill, K3),
                call(self.near, K0), call(self.relay, K0), call(self.near, K1), call(self.far, K2), call(self.relay, K1),
                call(fill, K0), call(self.near, K2), call(self.far, K3), call(self.end, K0), self.far2,
                call(self.relay, K2), call(self.near, K3), call(self.end, K1), call(self.near2, K0), call(self.relay2, K0),
                call(self.relay, K3), call(self.end, K2), call(self.near2, K1), call(self.relay2, K1), call(self.end, K3),
                self.end2]

    def slow_steps(self, fill):
        call = functools.partial
        steps = range(self.torus.side)
        result = [call(fill, K2)] + [call(self.far, step) for step in steps] + [call(fill, K1), call(fill, K3)]
        for step in steps:
            result += [call(self.near, step), call(self.relay, step)]
        return result + [call(fill, K0), call(self.end, K0), self.far2, call(self.end, K1), call(self.near2, K0), call(self.relay2, K0),
                         call(self.end, K2), call(self.near2, K1), call(self.relay2, K1), call(self.end, K3), self.end2]


class AllGather:
    def __init__(self, torus, scr, by_rows):
        self.torus, self.gat, self.scr, self.by_rows, self.store = torus, scr.gat, scr, by_rows, None
        self.quarter = scr.gat.shape[2 if by_rows else 3] // 4
        self.back = (0, torus.side - 1, 1, 2)

    def sems(self, kind):
        return self.scr.out_sems[kind], self.scr.in_sems[kind]

    def piece(self, ref, where, first, count):
        at = pl.ds(first * self.quarter, count * self.quarter)
        return ref.at[(*where, at, slice(None))] if self.by_rows else ref.at[(*where, slice(None), at)]

    def half(self, col, where, half):
        return self.piece(self.gat, where, col.index * 2 + half, 1)

    def own2(self, turn):
        for col in self.torus.colours:
            where = self.torus.block(col, col.second, col.first)
            for way, sign in enumerate(SIGNS):
                at = self.half(col, where, way if turn == 0 else 1 - way)
                self.torus.send(at, at, self.sems(H1), (col.index * 2 + way) * 2 + turn, self.torus.peer2(col, sign))

    def send1(self, step, turn):
        for col in self.torus.colours:
            where = self.torus.block(col, self.torus.wrap(col.second + self.back[step]), col.first)
            for way, sign in enumerate(SIGNS):
                at = self.half(col, where, way if turn == 0 else 1 - way)
                self.torus.send(at, at, self.sems(H2), ((col.index * 2 + way) * 4 + step) * 2 + turn, self.torus.peer1(col, sign))

    def arrive2(self, way, turn):
        sign = SIGNS[way]
        for col in self.torus.colours:
            where = self.torus.block(col, self.torus.wrap(col.second - sign), col.first)
            at = self.half(col, where, way if turn == 0 else 1 - way)
            self.torus.arrive(at, self.sems(H1), (col.index * 2 + way) * 2 + turn)
            if turn == 0:
                self.torus.send(at, at, self.sems(F1), col.index * 2 + way, self.torus.peer2(col, sign))

    def relayed2(self):
        for col in self.torus.colours:
            where = self.torus.block(col, self.torus.wrap(col.second + 2), col.first)
            for way in PAIR:
                self.torus.arrive(self.half(col, where, way), self.sems(F1), col.index * 2 + way)

    def arrive1(self, step, turn):
        for col in self.torus.colours:
            second = self.torus.wrap(col.second + self.back[step])
            for way, sign in enumerate(SIGNS):
                where = self.torus.block(col, second, self.torus.wrap(col.first - sign))
                at = self.half(col, where, way if turn == 0 else 1 - way)
                self.torus.arrive(at, self.sems(H2), ((col.index * 2 + way) * 4 + step) * 2 + turn)
                if turn == 0:
                    self.torus.send(at, at, self.sems(F2), (col.index * 2 + way) * 4 + step, self.torus.peer1(col, sign))

    def relayed1(self, step):
        for col in self.torus.colours:
            second = self.torus.wrap(col.second + self.back[step])
            for way in PAIR:
                where = self.torus.block(col, second, self.torus.wrap(col.first + 2))
                self.torus.arrive(self.half(col, where, way), self.sems(F2), (col.index * 2 + way) * 4 + step)

    def keep(self, step, firsts):
        for col in self.torus.colours:
            for shift in firsts:
                where = self.torus.block(col, self.torus.wrap(col.second + self.back[step]), self.torus.wrap(col.first + shift))
                self.store.keep(where, col.index, lambda ref, where=where, col=col: self.piece(ref, where, col.index * 2, 2))

    def steps(self, whole=None):
        call = functools.partial
        whole = whole or (lambda step: None)
        here, beside, across = (K0,), (K1, self.torus.side - 1), (K2,)

        def rest(step):
            return [call(self.arrive1, step, K1), call(self.keep, step, beside), call(self.relayed1, step), call(self.keep, step, across), call(whole, step)]

        result = []
        for turn in PAIR:
            result += [call(self.own2, turn), call(self.send1, K0, turn)]
        result += [call(self.keep, K0, here), call(self.arrive2, K0, K0), call(self.arrive2, K1, K0), call(self.arrive1, K0, K0),
                   call(self.arrive2, K0, K1), call(self.send1, K1, K0), call(self.send1, K1, K1), call(self.keep, K1, here),
                   call(self.arrive2, K1, K1), call(self.send1, K2, K0), call(self.keep, K2, here),
                   call(self.arrive1, K1, K0), call(self.send1, K2, K1), self.relayed2, call(self.send1, K3, K0), call(self.keep, K3, here)]
        result += rest(K0) + [call(self.arrive1, K2, K0), call(self.send1, K3, K1)]
        return result + rest(K1) + [call(self.arrive1, K3, K0)] + rest(K2) + rest(K3)


class Store:
    def __init__(self, torus, scr, places, own=None):
        self.torus, self.scr, self.places, self.own = torus, scr, places, own
        self.stores = []

    def slot(self, where, colour, index):
        return ((index * 2 + colour) * self.torus.side + where[K0]) * self.torus.side + where[K1]

    def keep(self, where, colour, piece):
        for index, (src, dst) in enumerate(self.places(where, colour, self.torus.core)):
            slot = self.slot(where, colour, index)
            pairs = [(self.scr.full_sem, dst)]
            if self.own is not None:
                pairs.append((self.scr.own_sem, piece(self.own)))
            for sem, ref in pairs:
                store = pltpu.make_async_copy(src, ref, sem.at[slot])
                store.start()
                self.stores.append(store)
            self.torus.send(src, dst, self.scr.cross_sems, slot, self.torus.partner)

    def drain(self):
        for store in self.stores:
            store.wait()
        side = self.torus.side
        for colour in PAIR:
            for y_at in range(side):
                for x_at in range(side):
                    for index, (_, dst) in enumerate(self.places((y_at, x_at), colour, 1 - self.torus.core)):
                        self.torus.arrive(dst, self.scr.cross_sems, self.slot((y_at, x_at), colour, index))


def plain_places(gather, full):
    return lambda where, colour, half: [(gather.piece(gather.gat, where, colour * 2, 2), gather.piece(full.at[half], where, colour * 2, 2))]


def rs_scratch(side, rows, width):
    dma = pltpu.SemaphoreType.DMA
    return dict(
        part=pltpu.VMEM((side, side, rows, width), BF16),
        bufs=[pltpu.VMEM((count, rows, width // 4), BF16) for count in RS_COUNTS],
        out_sems=[dma((count,)) for count in RS_COUNTS],
        in_sems=[dma((count,)) for count in RS_COUNTS],
    )


def ag_scratch(side, rows, width, places=1):
    dma = pltpu.SemaphoreType.DMA
    blocks = 2 * side * side * places
    return dict(
        gat=pltpu.VMEM((side, side, rows, width), BF16),
        out_sems=[dma((count,)) for count in AG_COUNTS],
        in_sems=[dma((count,)) for count in AG_COUNTS],
        full_sem=dma((blocks,)),
        own_sem=dma((blocks,)),
        cross_sems=[dma((blocks,)), dma((blocks,))],
    )


class Weights:
    def __init__(self, refs, buf, sem, by_rows):
        self.refs, self.buf, self.sem, self.by_rows = refs, buf, sem, by_rows
        self.copies = [[], []]

    def start(self):
        for colour in PAIR:
            for index, ref in enumerate(self.refs):
                if self.by_rows:
                    half, depth = ref.shape[K0] // 2, ref.shape[K1]
                    rows, cols = pl.ds(colour * half, half), pl.ds(index * depth, depth)
                    copy = pltpu.make_async_copy(ref.at[rows, :], self.buf.at[rows, cols], self.sem.at[colour, index])
                else:
                    half, depth = ref.shape[K1] // 2, ref.shape[K0]
                    rows, cols = pl.ds(index * depth, depth), pl.ds(colour * half, half)
                    copy = pltpu.make_async_copy(ref.at[:, cols], self.buf.at[rows, cols], self.sem.at[colour, index])
                copy.start()
                self.copies[colour].append(copy)

    def wait(self, colour):
        for copy in self.copies[colour]:
            copy.wait()
        self.copies[colour] = []


def fill_partial(torus, part, lhs, weights):
    rows, width = part.shape[2:]
    tile = min(512, width // 2)

    def fill(shift):
        for col in torus.colours:
            weights.wait(col.index)
            first = torus.wrap(col.first + shift)
            left = []
            for ref in lhs:
                depth = ref.shape[K3]
                value = ref[:, first] if col.index == 0 else ref[first]
                left.append((value.reshape(torus.side * rows, depth), depth))

            def body(step, carry, col=col, first=first, left=left):
                at = pl.ds(pl.multiple_of(col.index * (width // 2) + step * tile, tile), tile)
                total = None
                base = 0
                for value, depth in left:
                    if weights.by_rows:
                        term = dot(value, weights.buf[at, base:base + depth], NT)
                    else:
                        term = dot(value, weights.buf[base:base + depth, at], NN)
                    total = term if total is None else total + term
                    base += depth
                total = total.astype(BF16).reshape(torus.side, rows, tile)
                if col.index == 0:
                    part[:, first, :, at] = total
                else:
                    part[first, :, :, at] = total
                return carry

            lax.fori_loop(0, (width // 2) // tile, body, 0)

    return fill


def run(*lists):
    keyed = []
    for order, steps in enumerate(lists):
        keyed += [((index + 0.5) / len(steps), order, step) for index, step in enumerate(steps)]
    for _, _, step in sorted(keyed, key=lambda item: item[:2]):
        step()


def swap_start(torus, sems, pairs):
    for index, (src, dst) in enumerate(pairs):
        torus.send(src, dst, sems, index, torus.partner)


def swap_end(torus, sems, pairs, first=0):
    for index, (_, dst) in enumerate(pairs):
        if index >= first:
            torus.arrive(dst, sems, index)


def row_tiles(rows):
    return [pl.ds(start, 16) for start in range(0, rows, 16)]


def rms_back(z_in, gain, grad):
    inv = lax.rsqrt(jnp.mean(z_in * z_in, axis=-1, keepdims=True) + EPS)
    normed = z_in * inv
    scaled = grad * gain
    back = inv * (scaled - normed * jnp.mean(scaled * normed, axis=-1, keepdims=True))
    return back, jnp.sum(grad * normed, axis=0, keepdims=True)


def bag(tree):
    if isinstance(tree, dict):
        return types.SimpleNamespace(**{key: bag(value) for key, value in tree.items()})
    return [bag(value) for value in tree] if isinstance(tree, list) else tree


class Staging:
    def __init__(self, loads, saves):
        self.loads, self.saves, self.left = loads, saves, {}

    def start(self):
        for load in self.loads:
            load.start()

    def wait(self):
        for load in self.loads:
            load.wait()

    def save(self, *refs):
        for ref, save in self.saves:
            if any(ref is one for one in refs):
                save.start()
                self.left[id(ref)] = save

    def finish(self):
        self.save(*[ref for ref, _ in self.saves if id(ref) not in self.left])
        for save in self.left.values():
            save.wait()


def call_kernel(name, body, ins, outs, scratch, flops, collective_id=None):
    is_leaf = lambda value: isinstance(value, tuple)
    in_leaves, in_tree = jax.tree.flatten(ins, is_leaf=is_leaf)
    out_leaves, out_tree = jax.tree.flatten(outs, is_leaf=is_leaf)
    scr_leaves, scr_tree = jax.tree.flatten(scratch)
    first_scr = len(in_leaves) + len(out_leaves)
    staged = [index for index, leaf in enumerate(in_leaves + out_leaves) if leaf[K1] is VMEM]
    stages = []
    for index in staged:
        leaf = (in_leaves + out_leaves)[index][K0]
        stages.append(pltpu.VMEM(leaf.shape, leaf.dtype))

    def kernel(*refs):
        refs = list(refs)
        own = refs[first_scr + len(scr_leaves):]
        sem = own.pop()
        loads, saves = [], []
        for slot, (index, ref) in enumerate(zip(staged, own)):
            if index < len(in_leaves):
                loads.append(pltpu.make_async_copy(refs[index], ref, sem.at[slot]))
            else:
                saves.append((ref, pltpu.make_async_copy(ref, refs[index], sem.at[slot])))
            refs[index] = ref
        staging = Staging(loads, saves)
        staging.start()
        body(bag(in_tree.unflatten(refs[:len(in_leaves)])), bag(out_tree.unflatten(refs[len(in_leaves):first_scr])), bag(scr_tree.unflatten(refs[first_scr:first_scr + len(scr_leaves)])), staging)
        staging.finish()

    results = pl.pallas_call(
        kernel,
        name=name,
        out_shape=[leaf[K0] for leaf in out_leaves],
        in_specs=[ANY] * len(in_leaves),
        out_specs=[ANY] * len(out_leaves),
        scratch_shapes=scr_leaves + stages + [pltpu.SemaphoreType.DMA((len(staged),))],
        compiler_params=pltpu.CompilerParams(collective_id=collective_id, has_side_effects=collective_id is not None, vmem_limit_bytes=LIMIT),
        cost_estimate=pl.CostEstimate(flops=int(flops), bytes_accessed=int(4e7), transcendentals=0),
    )(*[leaf[K0] for leaf in in_leaves])
    return bag(out_tree.unflatten(results))


def shape(dims, dtype=BF16):
    return jax.ShapeDtypeStruct(dims, dtype)


def sum_attention(side, attn, w_outs, hidden, grad_out, gain, w_gate, w_up, w_down):
    seq, depth = attn.ctx.shape
    width = gain.shape[K1]
    hidden_loc = w_gate.shape[K0]
    rows = seq // (side * side)

    def body(ins, outs, scr, staging):
        torus = Torus(side)
        weights = Weights(ins.w_outs, scr.w, scr.w_sem, False)
        weights.start()
        rows_at = pl.ds(pl.multiple_of(torus.chip * rows, rows), rows)
        x_load = pltpu.make_async_copy(ins.hidden.at[torus.core, rows_at, :], scr.x_rows, scr.x_sem.at[K0])
        x_load.start()

        def load_weight(src, slot):
            load = pltpu.make_async_copy(src, scr.w_mlp.at[slot], scr.w_mlp_sem.at[slot])
            load.start()
            return load

        loads = {slot: load_weight(src, slot) for slot, src in ((K0, ins.w_down), (K2, ins.w_gate), (K3, ins.w_up))}
        wait = torus.signal_all()
        part = scr.sum.part
        steps = ReduceScatter(torus, scr.sum).steps(fill_partial(torus, part, [ins.ctx], weights))
        staging.wait()
        steps[K0]()
        wait()
        other_ctx = ins.ctx.at[:, :, :, pl.ds(depth // 2, depth // 2)]
        swaps = [(ins.w_down, outs.w_down), (ins.w_gate, outs.w_gate), (ins.w_up, outs.w_up), (other_ctx, outs.ctx_other), (ins.normed, outs.normed_other)]
        swap_start(torus, scr.swap_sems, swaps)

        def dy_load(group):
            at = pl.ds(group * side * rows, side * rows)
            return pltpu.make_async_copy(ins.grad_out.at[torus.core, at, :], scr.dy.at[group % 2], scr.dy_sem.at[group % 2])

        def grad_act(group):
            if group == 0:
                torus.arrive(outs.w_down, scr.swap_sems, 0)
                loads[K1] = load_weight(outs.w_down, K1)
                for slot in PAIR:
                    loads[slot].wait()
            dy_load(group).wait()
            for slot in PAIR:
                product = dot(scr.dy[group % 2], scr.w_mlp[slot], NT)
                scr.grad_act[slot, group] = product.reshape(side, rows, hidden_loc)
            if group + 2 < side:
                dy_load(group + 2).start()

        dy_load(0).start()
        dy_load(1).start()
        half = len(steps) // 3
        run(steps[1:half])
        run(steps[half:], [functools.partial(grad_act, group) for group in range(side)])
        for index, (slot, out) in enumerate(((K0, outs.w_gate), (K1, outs.w_up))):
            torus.arrive(out, scr.swap_sems, index + 1)
            loads[slot] = load_weight(out, slot)
        scr.pre[...] = jnp.zeros_like(scr.pre)
        gat = scr.all.gat
        own = (torus.y, torus.x)
        x_load.wait()
        for at in row_tiles(rows):
            resid = (scr.x_rows[at, :].astype(F32) + part[(*own, at, slice(None))].astype(F32)).astype(BF16)
            outs.h_rows[at, :] = resid
            z_in = resid.astype(F32)
            inv = lax.rsqrt(jnp.mean(z_in * z_in, axis=-1, keepdims=True) + EPS)
            gat[(*own, at, slice(None))] = (z_in * inv * ins.gain[...]).astype(BF16)
        staging.save(outs.h_rows)
        gather = AllGather(torus, scr.all, False)
        gather.store = Store(torus, scr.all, plain_places(gather, outs.full))

        def products(step):
            if step == 0:
                for load in (loads[slot] for slot in (K0, K1, K2, K3)):
                    load.wait()
            for col in torus.colours:
                second = torus.wrap(col.second + gather.back[step])
                at_cols = pl.ds(col.index * (width // 2), width // 2)
                mixed = gat[second, :, :, at_cols] if col.index == 0 else gat[:, second, :, at_cols]
                mixed = mixed.reshape(side * rows, width // 2)

                def body(slot, carry, col=col, second=second, at_cols=at_cols, mixed=mixed):
                    term = dot(mixed, scr.w_mlp[slot, :, at_cols], NT).reshape(side, rows, hidden_loc)
                    if col.index == 0:
                        scr.pre[slot, second] += term
                    else:
                        scr.pre[slot, :, second] += term
                    return carry

                lax.fori_loop(0, 4, body, 0)
            for inner, count in ((0, step + 1), (1, step)):

                def block(index, carry, inner=inner):
                    shift = lax.rem(3 * index + 3 * lax.div(index * (index - 1), 2), side)
                    pair = (gather.back[step], shift) if inner == 0 else (shift, gather.back[step])
                    y_at, x_at = torus.wrap(torus.y + pair[K0]), torus.wrap(torus.x + pair[K1])
                    for core in PAIR:
                        gate, upper = scr.pre[2 - 2 * core, y_at, x_at], scr.pre[3 - 2 * core, y_at, x_at]
                        grad = scr.grad_act[core, y_at, x_at]
                        sigmoid_g = 1.0 / (1.0 + jnp.exp(-gate))
                        silu_g = gate * sigmoid_g
                        scr.results[core, y_at, x_at] = (silu_g * upper).astype(BF16)
                        scr.results[2 + core, y_at, x_at] = (grad * upper * sigmoid_g * (1.0 + gate * (1.0 - sigmoid_g))).astype(BF16)
                        scr.results[4 + core, y_at, x_at] = (grad * silu_g).astype(BF16)
                    for kind, out in enumerate(outs.acts + outs.gates + outs.ups):
                        pltpu.make_async_copy(scr.results.at[kind, y_at, x_at], out.at[y_at, x_at], scr.result_sem.at[kind]).start()
                    return carry

                lax.fori_loop(0, count, block, 0)

        run(gather.steps(products))
        for kind, out in enumerate(outs.acts + outs.gates + outs.ups):
            pltpu.make_async_copy(scr.results.at[kind], out, scr.result_sem.at[kind]).wait()
        gather.store.drain()
        swap_end(torus, scr.swap_sems, swaps, 3)
        torus.drain()

    dma = pltpu.SemaphoreType.DMA
    block = (side, side, rows, hidden_loc)
    ins = dict(ctx=(attn.ctx.reshape(side, side, rows, depth), VMEM), w_outs=[(weight, ANY) for weight in w_outs], hidden=(hidden, ANY), grad_out=(grad_out, ANY), gain=(gain, VMEM),
               normed=(attn.normed, ANY), w_gate=(w_gate, ANY), w_up=(w_up, ANY), w_down=(w_down, ANY))
    out, weight = (shape(block), ANY), (shape((hidden_loc, width)), ANY)
    outs = dict(full=(shape((2, side, side, rows, width)), ANY), h_rows=(shape((rows, width)), VMEM), ctx_other=(shape((side, side, rows, depth // 2)), ANY), normed_other=(shape((seq, width)), ANY),
                w_gate=weight, w_up=weight, w_down=weight, acts=[out, out], gates=[out, out], ups=[out, out])
    scratch = dict(sum=rs_scratch(side, rows, width), all=ag_scratch(side, rows, width), w=pltpu.VMEM((depth, width), BF16), w_sem=dma((K2, K2)), swap_sems=[dma((5,)), dma((5,))],
                   x_rows=pltpu.VMEM((rows, width), BF16), x_sem=dma((K1,)), w_mlp=pltpu.VMEM((4, hidden_loc, width), BF16), w_mlp_sem=dma((4,)),
                   dy=pltpu.VMEM((2, side * rows, width), BF16), dy_sem=dma((K2,)), pre=pltpu.VMEM((4, *block), F32), grad_act=pltpu.VMEM((2, *block), F32), results=pltpu.VMEM((6, *block), BF16), result_sem=dma((6,)))
    return call_kernel('sum_attention', body, ins, outs, scratch, 4e8, 1)


def sum_mlp(side, mlp, w_gates, w_ups, w_downs, grad_out, gain):
    depth = w_gates[K0].shape[K0]
    width = gain.shape[K1]
    rows = mlp.h_rows.shape[K0]
    seq = rows * side * side
    block = (side, side, rows, width)

    def body(ins, outs, scr, staging):
        torus = Torus(side)
        weights = Weights(ins.w_in, scr.w, scr.w_sem, False)
        weights.start()
        weights_p = Weights(ins.w_downs, scr.wd, scr.wd_sem, False)
        weights_p.start()
        rows_at = pl.ds(pl.multiple_of(torus.chip * rows, rows), rows)
        dy_load = pltpu.make_async_copy(ins.grad_out.at[torus.core, rows_at, :], scr.dy_rows, scr.dy_sem.at[K0])
        dy_load.start()
        wait = torus.signal_all()
        steps = ReduceScatter(torus, scr.sum).slow_steps(fill_partial(torus, scr.sum.part, ins.grads, weights))
        steps_p = ReduceScatter(torus, scr.sum_p).slow_steps(fill_partial(torus, scr.sum_p.part, ins.acts, weights_p))
        staging.wait()
        steps[K0]()
        wait()

        turned = []

        def half_at(half):
            return pl.ds(pl.multiple_of(half * seq, seq), seq)

        def turn(index):
            kind, core = index // 2, index % 2
            src = (ins.grads[2 * core], ins.grads[2 * core + 1], ins.acts[core])[kind]
            slot = index % 2
            if index >= 2:
                turned[index - 2]()
            scr.turn[slot] = src[...].reshape(seq, depth).T
            at = slice(None), half_at(torus.core)
            if core == 0:
                save = pltpu.make_async_copy(scr.turn.at[slot], outs.lefts[kind].at[at], scr.turn_sem.at[kind])
                save.start()
                turned.append(save.wait)
            else:
                torus.send(scr.turn.at[slot], outs.lefts[kind].at[at], scr.swap_sems, kind, torus.partner)
                turned.append(torus.pending.pop().wait_send)

        turns = [functools.partial(turn, index) for index in range(6)]
        late, begun = 18, 3
        run(steps[1:late])
        run(steps_p[:begun])
        run(steps[late:])
        own = (torus.y, torus.x)
        gain_total = jnp.zeros((1, width), F32)
        gat = scr.all.gat
        dy_load.wait()
        for at in row_tiles(rows):
            back, gain_part = rms_back(ins.h_rows[at, :].astype(F32), ins.gain[...], scr.sum.part[(*own, at, slice(None))].astype(F32))
            gain_total = gain_total + gain_part
            total = scr.dy_rows[at, :].astype(F32) + back
            outs.d_rows[at, :] = total
            gat[(*own, at, slice(None))] = total.astype(BF16)
        outs.gain[...] = gain_total
        staging.save(outs.d_rows, outs.gain)
        gather = AllGather(torus, scr.all, False)
        gather.store = Store(torus, scr.all, plain_places(gather, outs.full), outs.own)
        run(gather.steps(), steps_p[begun:], turns)
        for at in row_tiles(rows):
            outs.y_rows[at, :] = (ins.h_rows[at, :].astype(F32) + scr.sum_p.part[(*own, at, slice(None))].astype(F32)).astype(BF16)
        staging.save(outs.y_rows)
        turned[4]()
        turned[5]()
        for kind in range(3):
            torus.arrive(outs.lefts[kind].at[:, half_at(1 - torus.core)], scr.swap_sems, kind)
        gather.store.drain()
        torus.drain()

    dma = pltpu.SemaphoreType.DMA
    ins = dict(grads=[(grad, VMEM) for grad in (mlp.gates[K0], mlp.ups[K0], mlp.gates[K1], mlp.ups[K1])], acts=[(act, VMEM) for act in mlp.acts],
               w_in=[(weight, ANY) for weight in (w_gates[K0], w_ups[K0], w_gates[K1], w_ups[K1])], w_downs=[(weight, ANY) for weight in w_downs],
               h_rows=(mlp.h_rows, VMEM), grad_out=(grad_out, ANY), gain=(gain, VMEM))
    outs = dict(full=(shape((2, *block)), ANY), own=(shape(block), ANY), d_rows=(shape((rows, width), F32), VMEM), gain=(shape((1, width), F32), VMEM), y_rows=(shape((rows, width)), VMEM), lefts=[(shape((depth, 2 * seq)), ANY)] * 3)
    scratch = dict(sum=rs_scratch(side, rows, width), sum_p=rs_scratch(side, rows, width), all=ag_scratch(side, rows, width), dy_rows=pltpu.VMEM((rows, width), BF16), dy_sem=dma((K1,)),
                   w=pltpu.VMEM((4 * depth, width), BF16), w_sem=dma((K2, 4)), wd=pltpu.VMEM((2 * depth, width), BF16), wd_sem=dma((K2, K2)),
                   turn=pltpu.VMEM((2, depth, seq), BF16), turn_sem=dma((K3,)), swap_sems=[dma((K3,)), dma((K3,))])
    return call_kernel('sum_mlp', body, ins, outs, scratch, 6e8, 2)


def attention_backward(side, ins, outs, scr, staging):
    resid = scr.sum.part
    rows, width = resid.shape[2:]
    band = side * rows
    tile = min(256, side * band)
    loads = []
    for index in PAIR:
        at = pl.ds(index * HEAD_DIM, HEAD_DIM)
        loads.append(pltpu.make_async_copy(ins.w_outs[index], scr.w_out.at[at, :], scr.w_out_sem.at[index]))
    for index in range(side):
        loads.append(pltpu.make_async_copy(ins.resid.at[index], resid.at[index], scr.resid_sem.at[index]))
    for load in loads:
        load.start()
    for load in loads[:2]:
        load.wait()
    for index in range(side):
        loads[2 + index].wait()
        scr.grad_ctx[index * band:(index + 1) * band, :] = dot(resid[index].reshape(band, width), scr.w_out[...], NT).astype(BF16)
    staging.wait()
    seg_row, seg_col = segments(ins.seg)
    keys_t = ins.qkv[:, 2 * HEAD_DIM:3 * HEAD_DIM].T
    scr.grad_k[...] = jnp.zeros_like(scr.grad_k)
    scr.grad_v[...] = jnp.zeros_like(scr.grad_v)

    def put(first, count, cols, value):
        for start in range(first, first + count, 16):
            where = (start // band, start // rows % side, slice(start % rows, start % rows + 16), cols)
            outs.dqkv[where] = value[start - first:start - first + 16].astype(BF16)

    for head_index in PAIR:
        cols = slice(head_index * HEAD_DIM, (head_index + 1) * HEAD_DIM)
        for tile_index in range(side * band // tile):
            reach = (tile_index + 1) * tile
            probs, queries = scores_softmax(ins.qkv, seg_row, seg_col, head_index, tile_index, tile)
            grad_ctx = scr.grad_ctx[tile_index * tile:reach, cols]
            grad_probs = dot(ins.qkv[:reach, 3 * HEAD_DIM:], grad_ctx, NT)
            centre = jnp.sum(grad_probs * probs, axis=0, keepdims=True)
            grad_scores = (probs * (grad_probs - centre) * HEAD_DIM ** -0.5).astype(BF16)
            scr.grad_v[:reach, :] += dot(probs.astype(BF16), grad_ctx, NN)
            scr.grad_k[:reach, :] += dot(grad_scores, queries, NN)
            put(tile_index * tile, tile, cols, dot(keys_t[:, :reach], grad_scores, NN).T)
    for index, ref in ((2, scr.grad_k), (3, scr.grad_v)):
        put(0, side * band, slice(index * HEAD_DIM, (index + 1) * HEAD_DIM), ref[...])


def sum_input(side, qkv, seg_ids, w_outs, w_qs, w_k, w_v, hidden, second, gain, token):
    seq, depth = qkv.shape
    width = gain.shape[K1]
    rows = seq // (side * side)
    head = depth // 4
    half_side = side // 2
    tokens = seq // 2
    kv_width = w_k.shape[K1]
    per_kv = 2 * side * side * head // kv_width

    def body(ins, outs, scr, staging):
        torus = Torus(side)
        kv_col = pl.multiple_of(lax.div(torus.chip * 2, per_kv) * head, head)
        weights = Weights([*ins.w_qs, ins.w_k.at[:, pl.ds(kv_col, head)], ins.w_v.at[:, pl.ds(kv_col, head)]], scr.w, scr.w_sem, True)
        weights.start()
        wait = torus.signal_all()
        part = scr.sum.part
        steps = ReduceScatter(torus, scr.sum).steps(fill_partial(torus, part, [outs.dqkv], weights))
        own = (torus.y, torus.x)
        gat = scr.all.gat
        gather = AllGather(torus, scr.all, True)

        def places(where, colour, half):
            chip = where[K0] * side + where[K1]
            tokens_at = pl.ds(pl.multiple_of(lax.rem(chip, 2) * tokens + colour * (tokens // 2), tokens // 2), tokens // 2)
            at = lax.div(chip, 2) * head
            src = gather.piece(gat, where, colour * 2, 2)
            return [(src.at[:, pl.ds(index * head, head)], outs.kv.at[half, tokens_at, pl.ds(pl.multiple_of(at + index * kv_width, head), head)]) for index in PAIR]

        gather.store = Store(torus, scr.all, places)
        rows_at = pl.ds(pl.multiple_of(torus.chip * rows, rows), rows)
        x_load = pltpu.make_async_copy(ins.hidden.at[torus.core, rows_at, :], scr.x_rows, scr.x_sem.at[K0])
        x_load.start()
        place = lax.rem(torus.x, 2)
        mate = torus.at_chip(torus.y, torus.x + 1 - 2 * place)
        kv_cols = pl.ds(2 * head, 2 * head)

        def mate_add():
            torus.arrive(scr.mate, scr.mate_sems, 0)
            mine = outs.dqkv[pl.ds(place * half_side, half_side), :, :, kv_cols]
            gat[own] = (mine.astype(F32) + scr.mate[...].astype(F32)).astype(BF16).reshape(tokens, 2 * head)

        attention_backward(side, ins, outs, scr, staging)
        staging.save(outs.dqkv)
        steps[K0]()
        wait()
        swaps = [(outs.dqkv.at[:, :, :, pl.ds(head, head)], outs.q_other)]
        swap_start(torus, scr.swap_sems, swaps)
        torus.send(outs.dqkv.at[pl.ds((1 - place) * half_side, half_side), :, :, kv_cols], scr.mate, scr.mate_sems, 0, mate)
        for step in steps[1:5]:
            step()
        mate_add()
        run(steps[5:], gather.steps())
        x_load.wait()
        gain_total = jnp.zeros((1, width), F32)
        for at in row_tiles(rows):
            back, gain_part = rms_back(scr.x_rows[at, :].astype(F32), ins.gain[...], part[(*own, at, slice(None))].astype(F32))
            gain_total = gain_total + gain_part
            outs.rows[at, :] = (ins.d_rows[at, :] + back).astype(BF16)
        row = lax.broadcasted_iota(jnp.int32, (8, width), 0)
        extra = jnp.zeros((8, width), F32)
        for index, value in enumerate((gain_total, ins.gain_mlp[...])):
            for level in range(3):
                rounded = value.astype(BF16).astype(F32)
                extra = jnp.where(row == index * 3 + level, rounded, extra)
                value = value - rounded
        outs.rows[rows:rows + 8, :] = extra.astype(BF16)
        staging.save(outs.rows)
        gather.store.drain()
        swap_end(torus, scr.swap_sems, swaps)
        torus.drain()

    dma = pltpu.SemaphoreType.DMA
    ins = dict(qkv=(qkv, VMEM), seg=(seg_ids, VMEM), resid=(second.own, ANY), w_outs=[(weight, ANY) for weight in w_outs], token=(token, ANY), w_qs=[(weight, ANY) for weight in w_qs], w_k=(w_k, ANY), w_v=(w_v, ANY), hidden=(hidden, ANY), d_rows=(second.d_rows, VMEM),
               gain=(gain, VMEM), gain_mlp=(second.gain, VMEM))
    outs = dict(rows=(shape((rows + 8, width)), VMEM), kv=(shape((2, seq, 2 * kv_width)), ANY), q_other=(shape((side, side, rows, head)), ANY), dqkv=(shape((side, side, rows, depth)), VMEM))
    scratch = dict(w_out=pltpu.VMEM((2 * head, width), BF16), grad_ctx=pltpu.VMEM((seq, 2 * head), BF16), grad_k=pltpu.VMEM((seq, head), F32), grad_v=pltpu.VMEM((seq, head), F32), w_out_sem=dma((K2,)), resid_sem=dma((side,)),
                   sum=rs_scratch(side, rows, width), all=ag_scratch(side, tokens, 2 * head, 2), x_rows=pltpu.VMEM((rows, width), BF16), x_sem=dma((K1,)), w=pltpu.VMEM((width, depth), BF16), w_sem=dma((K2, 4)),
                   mate=pltpu.VMEM((half_side, side, rows, 2 * head), BF16), mate_sems=[dma((K1,)), dma((K1,))], swap_sems=[dma((K1,)), dma((K1,))])
    return call_kernel('sum_input', body, ins, outs, scratch, 3e8, 3)


def scores_softmax(qkv, seg_row, seg_col, head_index, tile_index, tile):
    reach = (tile_index + 1) * tile
    queries = qkv[tile_index * tile:reach, head_index * HEAD_DIM:(head_index + 1) * HEAD_DIM]
    scores = dot(qkv[:reach, 2 * HEAD_DIM:3 * HEAD_DIM], queries, NT) * HEAD_DIM ** -0.5
    key_at = lax.broadcasted_iota(jnp.int32, (reach, tile), 0)
    query_at = lax.broadcasted_iota(jnp.int32, (reach, tile), 1) + tile_index * tile
    allowed = (key_at <= query_at) & (seg_col[:reach, :] == seg_row[:, tile_index * tile:reach])
    scores = jnp.where(allowed, scores, -1e30)
    weights = jnp.exp(scores - jnp.max(scores, axis=0, keepdims=True))
    return weights * (1.0 / jnp.sum(weights, axis=0, keepdims=True)), queries


def segments(seg_ref):
    core = lax.rem(lax.axis_index('tp'), 2)
    seg_row = seg_ref[pl.ds(core, 1), :].astype(F32)
    return seg_row, jnp.broadcast_to(seg_row, (8, seg_row.shape[K1])).T[:, :1]


def attention_forward(hidden, seg_ids, gain, w_q, w_k, w_v, w_o, per_kv):
    seq, width = hidden.shape[1:]
    chunk = seq // 4
    tile = min(256, seq)
    depth = 4 * HEAD_DIM

    def body(ins, outs, scr, staging):
        tp_idx = lax.axis_index('tp')
        core = lax.rem(tp_idx, 2)
        kv_col = pl.multiple_of(lax.div(tp_idx, per_kv) * HEAD_DIM, HEAD_DIM)
        partner = dict(tp=tp_idx + 1 - 2 * core)
        barrier = pltpu.get_barrier_semaphore()
        pl.semaphore_signal(barrier, inc=1, device_id=partner, device_id_type=MESH)
        loads = []
        for index in range(4):
            at = pl.ds(index * chunk, chunk)
            loads.append(pltpu.make_async_copy(ins.hidden.at[core, at, :], scr.x.at[at, :], scr.x_sem.at[index]))

        def w_cols(index):
            return scr.w.at[:, pl.ds(index * HEAD_DIM, HEAD_DIM)]

        for index, ref in ((0, ins.w_q), (2, ins.w_k.at[:, pl.ds(kv_col, HEAD_DIM)]), (3, ins.w_v.at[:, pl.ds(kv_col, HEAD_DIM)])):
            loads.append(pltpu.make_async_copy(ref, w_cols(index), scr.w_sem.at[index]))
        for load in loads:
            load.start()
        pl.semaphore_wait(barrier, 1)
        swaps = [(ins.w_q, w_cols(1)), (ins.w_o, outs.w_o), (ins.w_q, outs.w_q)]
        copies = []
        for index, (src, dst) in enumerate(swaps):
            copies.append(pltpu.make_async_remote_copy(src, dst, scr.swap_sems[K0].at[index], scr.swap_sems[K1].at[index], device_id=partner, device_id_type=MESH))
            copies[index].start()
        stores = []
        for index in range(4):
            loads[index].wait()

            if index == 0:
                staging.wait()

            def square(step, carry, index=index):
                at = pl.ds(pl.multiple_of(index * chunk + step * 16, 16), 16)
                total = jnp.zeros((16, HEAD_DIM), F32)
                for lane in range(0, width, HEAD_DIM):
                    value = scr.x[at, lane:lane + HEAD_DIM].astype(F32)
                    total = total + value * value
                scr.squares[pl.ds(pl.multiple_of(step * 16, 16), 16), :] = total
                return carry

            lax.fori_loop(0, chunk // 16, square, 0)
            inv = lax.rsqrt(jnp.sum(scr.squares[...], axis=-1, keepdims=True) / width + EPS)
            scr.squares[...] = jnp.broadcast_to(inv, scr.squares.shape)

            def normalize(step, carry, index=index):
                at = pl.ds(pl.multiple_of(index * chunk + step * 16, 16), 16)
                scale = scr.squares[pl.ds(pl.multiple_of(step * 16, 16), 16), :]
                for lane in range(0, width, HEAD_DIM):
                    cols = slice(lane, lane + HEAD_DIM)
                    scr.normed[at, cols] = (scr.x[at, cols].astype(F32) * scale * ins.gain[:, cols]).astype(BF16)
                return carry

            lax.fori_loop(0, chunk // 16, normalize, 0)
            at = pl.ds(index * chunk, chunk)
            store = pltpu.make_async_copy(scr.normed.at[at, :], outs.normed.at[at, :], scr.out_sem.at[index])
            store.start()
            stores.append(store)
            if index == 0:
                for load in loads[4:]:
                    load.wait()
                copies[K0].wait_recv()
            outs.qkv[at, :] = dot(scr.normed[at, :], scr.w[...], NN).astype(BF16)
        staging.save(outs.qkv)
        seg_row, seg_col = segments(ins.seg)
        values_t = outs.qkv[:, 3 * HEAD_DIM:].T
        for head_index in PAIR:
            for tile_index in range(seq // tile):
                probs, _ = scores_softmax(outs.qkv, seg_row, seg_col, head_index, tile_index, tile)
                ctx_t = dot(values_t[:, :(tile_index + 1) * tile], probs.astype(BF16), NN)
                outs.ctx[tile_index * tile:(tile_index + 1) * tile, head_index * HEAD_DIM:(head_index + 1) * HEAD_DIM] = ctx_t.T.astype(BF16)
        for store in stores:
            store.wait()
        copies[K0].wait_send()
        copies[K1].wait()
        copies[K2].wait()

    dma = pltpu.SemaphoreType.DMA
    ins = dict(hidden=(hidden, ANY), seg=(seg_ids, VMEM), gain=(gain, VMEM), w_q=(w_q, ANY), w_o=(w_o, ANY), w_k=(w_k, ANY), w_v=(w_v, ANY))
    outs = dict(normed=(shape((seq, width)), ANY), qkv=(shape((seq, depth)), VMEM), ctx=(shape((seq, 2 * HEAD_DIM)), VMEM), w_q=(shape(w_q.shape), ANY), w_o=(shape(w_o.shape), ANY))
    scratch = dict(squares=pltpu.VMEM((chunk, HEAD_DIM), F32), swap_sems=[dma((K3,)), dma((K3,))], x=pltpu.VMEM((seq, width), BF16), normed=pltpu.VMEM((seq, width), BF16), w=pltpu.VMEM((width, depth), BF16), x_sem=dma((4,)), w_sem=dma((4,)), out_sem=dma((4,)))
    return call_kernel('attention_forward', body, ins, outs, scratch, 5e9, 4)


def weight_grads(name, groups, ctxs, tokens=()):
    seq, width = groups[K0][K1].shape[1:]
    head = ctxs[K1].shape[K1] if ctxs else 0
    tile = min(512, width)
    lefts = [left for left, _ in groups if left is not None]
    sizes = [head if left is None else left.shape[K0] for left, _ in groups]
    given = len(groups) + len(lefts) + len(ctxs)

    def kernel(*refs):
        rights, left_refs = refs[:len(groups)], list(refs[len(groups):len(groups) + len(lefts)])
        outs = refs[given + len(tokens):given + len(tokens) + len(groups)]
        if ctxs:
            core = lax.rem(lax.axis_index('tp'), 2)
            ctx_t = refs[-1]

            @pl.when(pl.program_id(0) == 0)
            def _():
                for half, ref in zip((core, 1 - core), refs[given - 2:given]):
                    ctx_t[:, pl.ds(pl.multiple_of(half * seq, seq), seq)] = ref[:, :head].T

        for (left, _), right, out in zip(groups, rights, outs):
            ref = ctx_t if left is None else left_refs.pop(0)
            out[...] = dot(ref[...], right[...].reshape(2 * seq, tile), NN)

    slab = pl.BlockSpec((2, seq, tile), lambda step: (0, 0, step))
    return pl.pallas_call(
        kernel,
        name=name,
        grid=(width // tile,),
        out_shape=[shape((size, width), F32) for size in sizes],
        in_specs=[slab] * len(groups) + [VMEM] * (len(lefts) + len(ctxs)) + [ANY] * len(tokens),
        out_specs=[pl.BlockSpec((size, tile), lambda step: (0, step)) for size in sizes],
        scratch_shapes=[pltpu.VMEM((head, 2 * seq), BF16)] if ctxs else [],
        compiler_params=pltpu.CompilerParams(vmem_limit_bytes=LIMIT),
        cost_estimate=pl.CostEstimate(flops=int(1e10), bytes_accessed=int(4e7), transcendentals=0),
    )(*[right for _, right in groups], *lefts, *ctxs, *tokens)


def weight_grads_pair(left_gate, left_up, mixed_full):
    seq, width = mixed_full.shape[1:]
    depth = left_gate.shape[K0]
    tile = min(512, width)

    def kernel(m_ref, gate_ref, up_ref, out_gate, out_up):
        mixed = m_ref[...].reshape(2 * seq, tile)
        out_gate[...] = dot(gate_ref[...], mixed, NN)
        out_up[...] = dot(up_ref[...], mixed, NN)

    out = pl.BlockSpec((depth, tile), lambda step: (0, step))
    return pl.pallas_call(
        kernel,
        name='weight_grads_pair',
        grid=(width // tile,),
        out_shape=[shape((depth, width), F32)] * 2,
        in_specs=[pl.BlockSpec((2, seq, tile), lambda step: (0, 0, step)), VMEM, VMEM],
        out_specs=[out, out],
        compiler_params=pltpu.CompilerParams(vmem_limit_bytes=LIMIT),
        cost_estimate=pl.CostEstimate(flops=int(1e10), bytes_accessed=int(4e7), transcendentals=0),
    )(mixed_full, left_gate, left_up)


def weight_grads_qkv(normeds, kv_full, grads_q):
    seq, width = normeds[K0].shape
    head = grads_q[K1].shape[K1]
    kv_width = kv_full.shape[K2] // 2
    tile = min(512, width)

    def kernel(a_own, a_other, kv_ref, q_own, q_other, out_q, out_k, out_v, left, q_both):
        core = lax.rem(lax.axis_index('tp'), 2)
        halves = [pl.ds(pl.multiple_of(half * seq, seq), seq) for half in (core, 1 - core)]

        @pl.when(pl.program_id(0) == 0)
        def _():
            q_both[halves[K0], :] = q_own[:, :head]
            q_both[halves[K1], :] = q_other[...]

        left[:, halves[K0]] = a_own[...].T
        left[:, halves[K1]] = a_other[...].T
        out_q[...] = dot(left[...], q_both[...], NN)
        for index, out in enumerate((out_k, out_v)):
            right = kv_ref[:, :, pl.ds(index * kv_width, kv_width)].reshape(2 * seq, kv_width)
            out[...] = dot(left[...], right, NN)

    slab = pl.BlockSpec((seq, tile), lambda step: (0, step))
    out = lambda size: pl.BlockSpec((tile, size), lambda step: (step, 0))
    return pl.pallas_call(
        kernel,
        name='weight_grads_qkv',
        grid=(width // tile,),
        out_shape=[shape((width, size), F32) for size in (head, kv_width, kv_width)],
        in_specs=[slab] * 2 + [VMEM] * 3,
        out_specs=[out(size) for size in (head, kv_width, kv_width)],
        scratch_shapes=[pltpu.VMEM((tile, 2 * seq), BF16), pltpu.VMEM((2 * seq, head), BF16)],
        compiler_params=pltpu.CompilerParams(vmem_limit_bytes=LIMIT),
        cost_estimate=pl.CostEstimate(flops=int(27e9), bytes_accessed=int(6e7), transcendentals=0),
    )(*normeds, kv_full, *grads_q)


def in_place(gathered, rows):
    blocks, held, width = gathered.shape
    slots = 24
    gains = 2 if held > rows else 0

    def kernel(src, dst, *refs):
        buf, extra, in_sem, out_sem, extra_sem = refs[gains:]

        def load(index):
            return pltpu.make_async_copy(src.at[index, pl.ds(0, rows), :], buf.at[index % slots], in_sem.at[index % slots])

        def store(index):
            return pltpu.make_async_copy(buf.at[index % slots], dst.at[index % 2, index // 2], out_sem.at[index % slots])

        ahead = slots // 2
        for index in range(blocks + ahead):
            if index < blocks:
                if index >= slots:
                    store(index - slots).wait()
                load(index).start()
            if index == ahead and gains:
                last = pltpu.make_async_copy(src.at[:, pl.ds(held - 8, 8), :], extra, extra_sem.at[K0])
                last.start()
            if index >= ahead:
                load(index - ahead).wait()
                store(index - ahead).start()
        if gains:
            last.wait()
            total = jnp.sum(extra[...].astype(F32), axis=0)
            for first, ref in zip((0, 3), refs):
                ref[...] = total[first:first + 1] + total[first + 1:first + 2] + total[first + 2:first + 3]
        for index in range(blocks - slots, blocks):
            store(index).wait()

    dma = pltpu.SemaphoreType.DMA
    return pl.pallas_call(
        kernel,
        name='in_place',
        out_shape=[shape((2, blocks // 2, rows, width))] + [shape((1, width), F32)] * gains,
        in_specs=[ANY],
        out_specs=[ANY] + [VMEM] * gains,
        scratch_shapes=[pltpu.VMEM((slots, rows, width), BF16), pltpu.VMEM((blocks, 8, width), BF16), dma((slots,)), dma((slots,)), dma((K1,))],
        compiler_params=pltpu.CompilerParams(vmem_limit_bytes=LIMIT),
        cost_estimate=pl.CostEstimate(flops=int(2e7), bytes_accessed=int(2e7), transcendentals=0),
    )(gathered)


def solution(mesh):
    tp_size = mesh.shape['tp']
    chips = tp_size // 2
    side = math.isqrt(chips)

    def device_step(hidden, seg_ids, grad_out, gain_attn, gain_mlp, w_q, w_k, w_v, w_o, w_gate, w_up, w_down):
        seq_len, width = hidden.shape[1:]
        kv_heads = w_k.shape[K1] // HEAD_DIM
        per_kv = tp_size // kv_heads
        rows = seq_len // chips

        def flat(value):
            return value.reshape(seq_len, value.shape[-1])

        gain_attn_row = gain_attn[None, :]
        gain_mlp_row = gain_mlp[None, :]

        attn = attention_forward(hidden, seg_ids, gain_attn_row, w_q, w_k, w_v, w_o, per_kv)
        w_qs, w_outs = (w_q, attn.w_q), (w_o, attn.w_o)
        mlp = sum_attention(side, attn, w_outs, hidden, grad_out, gain_mlp_row, w_gate.T, w_up.T, w_down)
        mixed_full = mlp.full.reshape(2, seq_len, width)
        second = sum_mlp(side, mlp, (w_gate.T, mlp.w_gate), (w_up.T, mlp.w_up), (w_down, mlp.w_down), grad_out, gain_mlp_row)
        resid_full = second.full.reshape(2, seq_len, width)

        (y_out,) = in_place(lax.all_gather(second.y_rows, 'tp'), rows)
        left_gate, left_up, left_act = second.lefts
        grad_gate_t, grad_up_t = weight_grads_pair(left_gate, left_up, mixed_full)
        third = sum_input(side, attn.qkv, seg_ids, w_outs, w_qs, w_k, w_v, hidden, second, gain_attn_row, grad_up_t)
        grad_in, grad_gain_attn, grad_gain_mlp = in_place(lax.all_gather(third.rows, 'tp'), rows)
        grad_w_down, grad_w_o = weight_grads('weight_grads_down', [(left_act, grad_out), (None, resid_full)], (attn.ctx, flat(mlp.ctx_other)), (third.q_other,))
        grad_w_q, grad_w_k, grad_w_v = weight_grads_qkv((attn.normed, mlp.normed_other), third.kv, (flat(third.dqkv), flat(third.q_other)))
        return (y_out.reshape(hidden.shape), grad_in.reshape(hidden.shape), grad_gain_attn[K0], grad_gain_mlp[K0], grad_w_q, grad_w_k, grad_w_v, grad_w_o, grad_gate_t.T, grad_up_t.T, grad_w_down)

    spec_act = P('data', None, None)
    spec_rows = P('data', None)
    spec_gain = P(None)
    spec_cols = P(None, 'tp')
    spec_tprows = P('tp', None)
    spec_whole = P(None, None)
    spec_stack = P(('data', 'tp'), None)
    in_specs = (spec_act, spec_rows, spec_act, spec_gain, spec_gain, spec_cols, spec_whole, spec_whole, spec_tprows, spec_cols, spec_cols, spec_tprows)
    out_specs = (spec_act, spec_act, P('data'), P('data'), P('data', 'tp'), spec_rows, spec_rows, spec_stack, P('data', 'tp'), P('data', 'tp'), spec_stack)
    return jax.shard_map(device_step, mesh=mesh, in_specs=in_specs, out_specs=out_specs, check_vma=False)
```

```python
import functools
import math
import types
import jax
import jax.numpy as jnp
from jax import lax
from jax.experimental import pallas as pl
from jax.experimental.pallas import tpu as pltpu
from jax.sharding import PartitionSpec as P

HEAD_DIM = 128
EPS = 1e-5
MESH = pl.DeviceIdType.MESH
F32 = jnp.float32
BF16 = jnp.bfloat16
LIMIT = 63 * 2 ** 20
K0, K1, K2, K3 = range(4)
PAIR = range(2)
ANY = pl.BlockSpec(memory_space=pl.ANY)
VMEM = pl.BlockSpec(memory_space=pltpu.VMEM)


def dot(lhs, rhs, dims):
    return lax.dot_general(lhs, rhs, (dims, ((), ())), preferred_element_type=F32)


NN = ((1,), (0,))
NT = ((1,), (1,))


SIGNS = (1, -1)


class Colour:
    def __init__(self, index, first, second):
        self.index, self.first, self.second = index, first, second


class Torus:
    def __init__(self, side):
        self.side = side
        tp_idx = lax.axis_index('tp')
        self.core = lax.rem(tp_idx, 2)
        self.chip = lax.div(tp_idx, 2)
        self.x = lax.rem(self.chip, side)
        self.y = lax.div(self.chip, side)
        self.partner = {'tp': self.chip * 2 + (1 - self.core)}
        self.colours = (Colour(0, self.x, self.y), Colour(1, self.y, self.x))
        self.pending = []

    def wrap(self, pos):
        return lax.rem(pos + 2 * self.side, self.side)

    def at_chip(self, y_at, x_at):
        return {'tp': (y_at * self.side + x_at) * 2 + self.core}

    def block(self, col, second, first):
        return (second, first) if col.index == 0 else (first, second)

    def peer1(self, col, shift):
        return self.at_chip(*self.block(col, col.second, self.wrap(col.first + shift)))

    def peer2(self, col, shift):
        return self.at_chip(*self.block(col, self.wrap(col.second + shift), col.first))

    def signal_all(self):
        barrier = pltpu.get_barrier_semaphore()
        peers = [self.partner]
        peers += [self.at_chip(self.y, self.wrap(self.x + shift)) for shift in SIGNS]
        peers += [self.at_chip(self.wrap(self.y + shift), self.x) for shift in SIGNS]
        for peer in peers:
            pl.semaphore_signal(barrier, inc=1, device_id=peer, device_id_type=MESH)
        return lambda: pl.semaphore_wait(barrier, len(peers))

    def send(self, src, dst, sems, index, device):
        copy = pltpu.make_async_remote_copy(src, dst, sems[K0].at[index], sems[K1].at[index], device_id=device, device_id_type=MESH)
        copy.start()
        self.pending.append(copy)

    def arrive(self, dst, sems, index):
        pltpu.make_async_remote_copy(dst, dst, sems[K0].at[index], sems[K1].at[index], device_id=self.partner, device_id_type=MESH).wait_recv()

    def drain(self):
        for copy in self.pending:
            copy.wait_send()


R1, R2, R3, S1, S2, S3 = range(6)
RS_COUNTS = (16, 16, 16, 4, 4, 4)
H1, H2, F1, F2 = range(4)
AG_COUNTS = (8, 32, 4, 16)


class ReduceScatter:
    SHIFTS = (2, 1, 3, 0)

    def __init__(self, torus, scr):
        self.torus, self.part, self.scr = torus, scr.part, scr
        self.quarter = scr.part.shape[K3] // 4

    def buf(self, kind, index):
        return self.scr.bufs[kind].at[index]

    def sems(self, kind):
        return self.scr.out_sems[kind], self.scr.in_sems[kind]

    def cols(self, col, half):
        return pl.ds((col.index * 2 + half) * self.quarter, self.quarter)

    def piece(self, where, at_cols):
        return self.part.at[(*where, slice(None), at_cols)]

    def send(self, where, at_cols, kind, index, peer):
        self.torus.send(self.piece(where, at_cols), self.buf(kind, index), self.sems(kind), index, peer)

    def add(self, where, at_cols, *kinds):
        total = self.part[(*where, slice(None), at_cols)].astype(F32)
        for kind, index in kinds:
            self.torus.arrive(self.buf(kind, index), self.sems(kind), index)
            total = total + self.buf(kind, index)[...].astype(F32)
        self.part[(*where, slice(None), at_cols)] = total.astype(BF16)

    def each(self, step):
        wrap = self.torus.wrap
        for col in self.torus.colours:
            second = wrap(col.second + self.SHIFTS[step])
            for way, sign in enumerate(SIGNS):
                yield col, second, way, sign, (col.index * 2 + way) * 4 + step

    def far(self, step):
        for col, second, way, sign, index in self.each(step):
            where = self.torus.block(col, second, self.torus.wrap(col.first + 2))
            self.send(where, self.cols(col, way), R1, index, self.torus.peer1(col, sign))

    def near(self, step):
        for col, second, way, sign, index in self.each(step):
            where = self.torus.block(col, second, self.torus.wrap(col.first + sign))
            self.send(where, self.cols(col, 1 - way), R2, index, self.torus.peer1(col, sign))

    def relay(self, step):
        for col, second, way, sign, index in self.each(step):
            where = self.torus.block(col, second, self.torus.wrap(col.first + sign))
            self.add(where, self.cols(col, way), (R1, index))
            self.send(where, self.cols(col, way), R3, index, self.torus.peer1(col, sign))

    def end(self, step):
        for col, second, way, sign, index in self.each(step):
            where = self.torus.block(col, second, col.first)
            other = (col.index * 2 + 1 - way) * 4 + step
            self.add(where, self.cols(col, way), (R2, other), (R3, index))

    def far2(self):
        for col in self.torus.colours:
            for way, sign in enumerate(SIGNS):
                where = self.torus.block(col, self.torus.wrap(col.second + 2), col.first)
                self.send(where, self.cols(col, way), S1, col.index * 2 + way, self.torus.peer2(col, sign))

    def near2(self, way):
        for col in self.torus.colours:
            where = self.torus.block(col, self.torus.wrap(col.second + SIGNS[way]), col.first)
            self.send(where, self.cols(col, 1 - way), S2, col.index * 2 + way, self.torus.peer2(col, SIGNS[way]))

    def relay2(self, way):
        for col in self.torus.colours:
            index = col.index * 2 + way
            where = self.torus.block(col, self.torus.wrap(col.second + SIGNS[way]), col.first)
            self.add(where, self.cols(col, way), (S1, index))
            self.send(where, self.cols(col, way), S3, index, self.torus.peer2(col, SIGNS[way]))

    def end2(self):
        for col in self.torus.colours:
            where = self.torus.block(col, col.second, col.first)
            for way in PAIR:
                self.add(where, self.cols(col, way), (S2, col.index * 2 + 1 - way), (S3, col.index * 2 + way))

    def steps(self, fill):
        call = functools.partial
        return [call(fill, K2), call(self.far, K0), call(self.far, K1), call(fill, K1), call(fill, K3),
                call(self.near, K0), call(self.relay, K0), call(self.near, K1), call(self.far, K2), call(self.relay, K1),
                call(fill, K0), call(self.near, K2), call(self.far, K3), call(self.end, K0), self.far2,
                call(self.relay, K2), call(self.near, K3), call(self.end, K1), call(self.near2, K0), call(self.relay2, K0),
                call(self.relay, K3), call(self.end, K2), call(self.near2, K1), call(self.relay2, K1), call(self.end, K3),
                self.end2]

    def slow_steps(self, fill):
        call = functools.partial
        steps = range(self.torus.side)
        result = [call(fill, K2)] + [call(self.far, step) for step in steps] + [call(fill, K1), call(fill, K3)]
        for step in steps:
            result += [call(self.near, step), call(self.relay, step)]
        return result + [call(fill, K0), call(self.end, K0), self.far2, call(self.end, K1), call(self.near2, K0), call(self.relay2, K0),
                         call(self.end, K2), call(self.near2, K1), call(self.relay2, K1), call(self.end, K3), self.end2]


class AllGather:
    def __init__(self, torus, scr, by_rows):
        self.torus, self.gat, self.scr, self.by_rows, self.store = torus, scr.gat, scr, by_rows, None
        self.quarter = scr.gat.shape[2 if by_rows else 3] // 4
        self.back = (0, torus.side - 1, 1, 2)

    def sems(self, kind):
        return self.scr.out_sems[kind], self.scr.in_sems[kind]

    def piece(self, ref, where, first, count):
        at = pl.ds(first * self.quarter, count * self.quarter)
        return ref.at[(*where, at, slice(None))] if self.by_rows else ref.at[(*where, slice(None), at)]

    def half(self, col, where, half):
        return self.piece(self.gat, where, col.index * 2 + half, 1)

    def own2(self, turn):
        for col in self.torus.colours:
            where = self.torus.block(col, col.second, col.first)
            for way, sign in enumerate(SIGNS):
                at = self.half(col, where, way if turn == 0 else 1 - way)
                self.torus.send(at, at, self.sems(H1), (col.index * 2 + way) * 2 + turn, self.torus.peer2(col, sign))

    def send1(self, step, turn):
        for col in self.torus.colours:
            where = self.torus.block(col, self.torus.wrap(col.second + self.back[step]), col.first)
            for way, sign in enumerate(SIGNS):
                at = self.half(col, where, way if turn == 0 else 1 - way)
                self.torus.send(at, at, self.sems(H2), ((col.index * 2 + way) * 4 + step) * 2 + turn, self.torus.peer1(col, sign))

    def arrive2(self, way, turn):
        sign = SIGNS[way]
        for col in self.torus.colours:
            where = self.torus.block(col, self.torus.wrap(col.second - sign), col.first)
            at = self.half(col, where, way if turn == 0 else 1 - way)
            self.torus.arrive(at, self.sems(H1), (col.index * 2 + way) * 2 + turn)
            if turn == 0:
                self.torus.send(at, at, self.sems(F1), col.index * 2 + way, self.torus.peer2(col, sign))

    def relayed2(self):
        for col in self.torus.colours:
            where = self.torus.block(col, self.torus.wrap(col.second + 2), col.first)
            for way in PAIR:
                self.torus.arrive(self.half(col, where, way), self.sems(F1), col.index * 2 + way)

    def arrive1(self, step, turn):
        for col in self.torus.colours:
            second = self.torus.wrap(col.second + self.back[step])
            for way, sign in enumerate(SIGNS):
                where = self.torus.block(col, second, self.torus.wrap(col.first - sign))
                at = self.half(col, where, way if turn == 0 else 1 - way)
                self.torus.arrive(at, self.sems(H2), ((col.index * 2 + way) * 4 + step) * 2 + turn)
                if turn == 0:
                    self.torus.send(at, at, self.sems(F2), (col.index * 2 + way) * 4 + step, self.torus.peer1(col, sign))

    def relayed1(self, step):
        for col in self.torus.colours:
            second = self.torus.wrap(col.second + self.back[step])
            for way in PAIR:
                where = self.torus.block(col, second, self.torus.wrap(col.first + 2))
                self.torus.arrive(self.half(col, where, way), self.sems(F2), (col.index * 2 + way) * 4 + step)

    def keep(self, step, firsts):
        for col in self.torus.colours:
            for shift in firsts:
                where = self.torus.block(col, self.torus.wrap(col.second + self.back[step]), self.torus.wrap(col.first + shift))
                self.store.keep(where, col.index, lambda ref, where=where, col=col: self.piece(ref, where, col.index * 2, 2))

    def steps(self, whole=None):
        call = functools.partial
        whole = whole or (lambda step: None)
        here, beside, across = (K0,), (K1, self.torus.side - 1), (K2,)

        def rest(step):
            return [call(self.arrive1, step, K1), call(self.keep, step, beside), call(self.relayed1, step), call(self.keep, step, across), call(whole, step)]

        result = []
        for turn in PAIR:
            result += [call(self.own2, turn), call(self.send1, K0, turn)]
        result += [call(self.keep, K0, here), call(self.arrive2, K0, K0), call(self.arrive2, K1, K0), call(self.arrive1, K0, K0),
                   call(self.arrive2, K0, K1), call(self.send1, K1, K0), call(self.send1, K1, K1), call(self.keep, K1, here),
                   call(self.arrive2, K1, K1), call(self.send1, K2, K0), call(self.keep, K2, here),
                   call(self.arrive1, K1, K0), call(self.send1, K2, K1), self.relayed2, call(self.send1, K3, K0), call(self.keep, K3, here)]
        result += rest(K0) + [call(self.arrive1, K2, K0), call(self.send1, K3, K1)]
        return result + rest(K1) + [call(self.arrive1, K3, K0)] + rest(K2) + rest(K3)


class Store:
    def __init__(self, torus, scr, places, own=None):
        self.torus, self.scr, self.places, self.own = torus, scr, places, own
        self.stores = []

    def slot(self, where, colour, index):
        return ((index * 2 + colour) * self.torus.side + where[K0]) * self.torus.side + where[K1]

    def keep(self, where, colour, piece):
        for index, (src, dst) in enumerate(self.places(where, colour, self.torus.core)):
            slot = self.slot(where, colour, index)
            pairs = [(self.scr.full_sem, dst)]
            if self.own is not None:
                pairs.append((self.scr.own_sem, piece(self.own)))
            for sem, ref in pairs:
                store = pltpu.make_async_copy(src, ref, sem.at[slot])
                store.start()
                self.stores.append(store)
            self.torus.send(src, dst, self.scr.cross_sems, slot, self.torus.partner)

    def drain(self):
        for store in self.stores:
            store.wait()
        side = self.torus.side
        for colour in PAIR:
            for y_at in range(side):
                for x_at in range(side):
                    for index, (_, dst) in enumerate(self.places((y_at, x_at), colour, 1 - self.torus.core)):
                        self.torus.arrive(dst, self.scr.cross_sems, self.slot((y_at, x_at), colour, index))


def plain_places(gather, full):
    return lambda where, colour, half: [(gather.piece(gather.gat, where, colour * 2, 2), gather.piece(full.at[half], where, colour * 2, 2))]


def rs_scratch(side, rows, width):
    dma = pltpu.SemaphoreType.DMA
    return dict(
        part=pltpu.VMEM((side, side, rows, width), BF16),
        bufs=[pltpu.VMEM((count, rows, width // 4), BF16) for count in RS_COUNTS],
        out_sems=[dma((count,)) for count in RS_COUNTS],
        in_sems=[dma((count,)) for count in RS_COUNTS],
    )


def ag_scratch(side, rows, width, places=1):
    dma = pltpu.SemaphoreType.DMA
    blocks = 2 * side * side * places
    return dict(
        gat=pltpu.VMEM((side, side, rows, width), BF16),
        out_sems=[dma((count,)) for count in AG_COUNTS],
        in_sems=[dma((count,)) for count in AG_COUNTS],
        full_sem=dma((blocks,)),
        own_sem=dma((blocks,)),
        cross_sems=[dma((blocks,)), dma((blocks,))],
    )


class Weights:
    def __init__(self, refs, buf, sem, by_rows):
        self.refs, self.buf, self.sem, self.by_rows = refs, buf, sem, by_rows
        self.copies = [[], []]

    def start(self):
        for colour in PAIR:
            for index, ref in enumerate(self.refs):
                if self.by_rows:
                    half, depth = ref.shape[K0] // 2, ref.shape[K1]
                    rows, cols = pl.ds(colour * half, half), pl.ds(index * depth, depth)
                    copy = pltpu.make_async_copy(ref.at[rows, :], self.buf.at[rows, cols], self.sem.at[colour, index])
                else:
                    half, depth = ref.shape[K1] // 2, ref.shape[K0]
                    rows, cols = pl.ds(index * depth, depth), pl.ds(colour * half, half)
                    copy = pltpu.make_async_copy(ref.at[:, cols], self.buf.at[rows, cols], self.sem.at[colour, index])
                copy.start()
                self.copies[colour].append(copy)

    def wait(self, colour):
        for copy in self.copies[colour]:
            copy.wait()
        self.copies[colour] = []


def fill_partial(torus, part, lhs, weights):
    rows, width = part.shape[2:]
    tile = min(512, width // 2)

    def fill(shift):
        for col in torus.colours:
            weights.wait(col.index)
            first = torus.wrap(col.first + shift)
            left = []
            for ref in lhs:
                depth = ref.shape[K3]
                value = ref[:, first] if col.index == 0 else ref[first]
                left.append((value.reshape(torus.side * rows, depth), depth))

            def body(step, carry, col=col, first=first, left=left):
                at = pl.ds(pl.multiple_of(col.index * (width // 2) + step * tile, tile), tile)
                total = None
                base = 0
                for value, depth in left:
                    if weights.by_rows:
                        term = dot(value, weights.buf[at, base:base + depth], NT)
                    else:
                        term = dot(value, weights.buf[base:base + depth, at], NN)
                    total = term if total is None else total + term
                    base += depth
                total = total.astype(BF16).reshape(torus.side, rows, tile)
                if col.index == 0:
                    part[:, first, :, at] = total
                else:
                    part[first, :, :, at] = total
                return carry

            lax.fori_loop(0, (width // 2) // tile, body, 0)

    return fill


def run(*lists):
    keyed = []
    for order, steps in enumerate(lists):
        keyed += [((index + 0.5) / len(steps), order, step) for index, step in enumerate(steps)]
    for _, _, step in sorted(keyed, key=lambda item: item[:2]):
        step()


def swap_start(torus, sems, pairs):
    for index, (src, dst) in enumerate(pairs):
        torus.send(src, dst, sems, index, torus.partner)


def swap_end(torus, sems, pairs, first=0):
    for index, (_, dst) in enumerate(pairs):
        if index >= first:
            torus.arrive(dst, sems, index)


def row_tiles(rows):
    return [pl.ds(start, 16) for start in range(0, rows, 16)]


def rms_back(z_in, gain, grad):
    inv = lax.rsqrt(jnp.mean(z_in * z_in, axis=-1, keepdims=True) + EPS)
    normed = z_in * inv
    scaled = grad * gain
    back = inv * (scaled - normed * jnp.mean(scaled * normed, axis=-1, keepdims=True))
    return back, jnp.sum(grad * normed, axis=0, keepdims=True)


def bag(tree):
    if isinstance(tree, dict):
        return types.SimpleNamespace(**{key: bag(value) for key, value in tree.items()})
    return [bag(value) for value in tree] if isinstance(tree, list) else tree


class Staging:
    def __init__(self, loads, saves):
        self.loads, self.saves, self.left = loads, saves, {}

    def start(self):
        for load in self.loads:
            load.start()

    def wait(self):
        for load in self.loads:
            load.wait()

    def save(self, *refs):
        for ref, save in self.saves:
            if any(ref is one for one in refs):
                save.start()
                self.left[id(ref)] = save

    def finish(self):
        self.save(*[ref for ref, _ in self.saves if id(ref) not in self.left])
        for save in self.left.values():
            save.wait()


def call_kernel(name, body, ins, outs, scratch, flops, collective_id=None):
    is_leaf = lambda value: isinstance(value, tuple)
    in_leaves, in_tree = jax.tree.flatten(ins, is_leaf=is_leaf)
    out_leaves, out_tree = jax.tree.flatten(outs, is_leaf=is_leaf)
    scr_leaves, scr_tree = jax.tree.flatten(scratch)
    first_scr = len(in_leaves) + len(out_leaves)
    staged = [index for index, leaf in enumerate(in_leaves + out_leaves) if leaf[K1] is VMEM]
    stages = []
    for index in staged:
        leaf = (in_leaves + out_leaves)[index][K0]
        stages.append(pltpu.VMEM(leaf.shape, leaf.dtype))

    def kernel(*refs):
        refs = list(refs)
        own = refs[first_scr + len(scr_leaves):]
        sem = own.pop()
        loads, saves = [], []
        for slot, (index, ref) in enumerate(zip(staged, own)):
            if index < len(in_leaves):
                loads.append(pltpu.make_async_copy(refs[index], ref, sem.at[slot]))
            else:
                saves.append((ref, pltpu.make_async_copy(ref, refs[index], sem.at[slot])))
            refs[index] = ref
        staging = Staging(loads, saves)
        staging.start()
        body(bag(in_tree.unflatten(refs[:len(in_leaves)])), bag(out_tree.unflatten(refs[len(in_leaves):first_scr])), bag(scr_tree.unflatten(refs[first_scr:first_scr + len(scr_leaves)])), staging)
        staging.finish()

    results = pl.pallas_call(
        kernel,
        name=name,
        out_shape=[leaf[K0] for leaf in out_leaves],
        in_specs=[ANY] * len(in_leaves),
        out_specs=[ANY] * len(out_leaves),
        scratch_shapes=scr_leaves + stages + [pltpu.SemaphoreType.DMA((len(staged),))],
        compiler_params=pltpu.CompilerParams(collective_id=collective_id, has_side_effects=collective_id is not None, vmem_limit_bytes=LIMIT),
        cost_estimate=pl.CostEstimate(flops=int(flops), bytes_accessed=int(4e7), transcendentals=0),
    )(*[leaf[K0] for leaf in in_leaves])
    return bag(out_tree.unflatten(results))


def shape(dims, dtype=BF16):
    return jax.ShapeDtypeStruct(dims, dtype)


def sum_attention(side, attn, w_outs, hidden, grad_out, gain, w_gate, w_up, w_down):
    seq, depth = attn.ctx.shape
    width = gain.shape[K1]
    hidden_loc = w_gate.shape[K0]
    rows = seq // (side * side)

    def body(ins, outs, scr, staging):
        torus = Torus(side)
        weights = Weights(ins.w_outs, scr.w, scr.w_sem, False)
        weights.start()
        rows_at = pl.ds(pl.multiple_of(torus.chip * rows, rows), rows)
        x_load = pltpu.make_async_copy(ins.hidden.at[torus.core, rows_at, :], scr.x_rows, scr.x_sem.at[K0])
        x_load.start()

        def load_weight(src, slot):
            load = pltpu.make_async_copy(src, scr.w_mlp.at[slot], scr.w_mlp_sem.at[slot])
            load.start()
            return load

        loads = {slot: load_weight(src, slot) for slot, src in ((K0, ins.w_down), (K2, ins.w_gate), (K3, ins.w_up))}
        wait = torus.signal_all()
        part = scr.sum.part
        steps = ReduceScatter(torus, scr.sum).steps(fill_partial(torus, part, [ins.ctx], weights))
        staging.wait()
        steps[K0]()
        wait()
        other_ctx = ins.ctx.at[:, :, :, pl.ds(depth // 2, depth // 2)]
        swaps = [(ins.w_down, outs.w_down), (ins.w_gate, outs.w_gate), (ins.w_up, outs.w_up), (other_ctx, outs.ctx_other), (ins.normed, outs.normed_other)]
        swap_start(torus, scr.swap_sems, swaps)

        def dy_load(group):
            at = pl.ds(group * side * rows, side * rows)
            return pltpu.make_async_copy(ins.grad_out.at[torus.core, at, :], scr.dy.at[group % 2], scr.dy_sem.at[group % 2])

        def grad_act(group):
            if group == 0:
                torus.arrive(outs.w_down, scr.swap_sems, 0)
                loads[K1] = load_weight(outs.w_down, K1)
                for slot in PAIR:
                    loads[slot].wait()
            dy_load(group).wait()
            for slot in PAIR:
                product = dot(scr.dy[group % 2], scr.w_mlp[slot], NT)
                scr.grad_act[slot, group] = product.reshape(side, rows, hidden_loc)
            if group + 2 < side:
                dy_load(group + 2).start()

        dy_load(0).start()
        dy_load(1).start()
        half = len(steps) // 3
        run(steps[1:half])
        run(steps[half:], [functools.partial(grad_act, group) for group in range(side)])
        for index, (slot, out) in enumerate(((K0, outs.w_gate), (K1, outs.w_up))):
            torus.arrive(out, scr.swap_sems, index + 1)
            loads[slot] = load_weight(out, slot)
        scr.pre[...] = jnp.zeros_like(scr.pre)
        gat = scr.all.gat
        own = (torus.y, torus.x)
        x_load.wait()
        for at in row_tiles(rows):
            resid = (scr.x_rows[at, :].astype(F32) + part[(*own, at, slice(None))].astype(F32)).astype(BF16)
            outs.h_rows[at, :] = resid
            z_in = resid.astype(F32)
            inv = lax.rsqrt(jnp.mean(z_in * z_in, axis=-1, keepdims=True) + EPS)
            gat[(*own, at, slice(None))] = (z_in * inv * ins.gain[...]).astype(BF16)
        staging.save(outs.h_rows)
        gather = AllGather(torus, scr.all, False)
        gather.store = Store(torus, scr.all, plain_places(gather, outs.full))

        def products(step):
            if step == 0:
                for load in (loads[slot] for slot in (K0, K1, K2, K3)):
                    load.wait()
            for col in torus.colours:
                second = torus.wrap(col.second + gather.back[step])
                at_cols = pl.ds(col.index * (width // 2), width // 2)
                mixed = gat[second, :, :, at_cols] if col.index == 0 else gat[:, second, :, at_cols]
                mixed = mixed.reshape(side * rows, width // 2)

                def body(slot, carry, col=col, second=second, at_cols=at_cols, mixed=mixed):
                    term = dot(mixed, scr.w_mlp[slot, :, at_cols], NT).reshape(side, rows, hidden_loc)
                    if col.index == 0:
                        scr.pre[slot, second] += term
                    else:
                        scr.pre[slot, :, second] += term
                    return carry

                lax.fori_loop(0, 4, body, 0)
            for inner, count in ((0, step + 1), (1, step)):

                def block(index, carry, inner=inner):
                    shift = lax.rem(3 * index + 3 * lax.div(index * (index - 1), 2), side)
                    pair = (gather.back[step], shift) if inner == 0 else (shift, gather.back[step])
                    y_at, x_at = torus.wrap(torus.y + pair[K0]), torus.wrap(torus.x + pair[K1])
                    for core in PAIR:
                        gate, upper = scr.pre[2 - 2 * core, y_at, x_at], scr.pre[3 - 2 * core, y_at, x_at]
                        grad = scr.grad_act[core, y_at, x_at]
                        sigmoid_g = 1.0 / (1.0 + jnp.exp(-gate))
                        silu_g = gate * sigmoid_g
                        scr.results[core, y_at, x_at] = (silu_g * upper).astype(BF16)
                        scr.results[2 + core, y_at, x_at] = (grad * upper * sigmoid_g * (1.0 + gate * (1.0 - sigmoid_g))).astype(BF16)
                        scr.results[4 + core, y_at, x_at] = (grad * silu_g).astype(BF16)
                    for kind, out in enumerate(outs.acts + outs.gates + outs.ups):
                        pltpu.make_async_copy(scr.results.at[kind, y_at, x_at], out.at[y_at, x_at], scr.result_sem.at[kind]).start()
                    return carry

                lax.fori_loop(0, count, block, 0)

        run(gather.steps(products))
        for kind, out in enumerate(outs.acts + outs.gates + outs.ups):
            pltpu.make_async_copy(scr.results.at[kind], out, scr.result_sem.at[kind]).wait()
        gather.store.drain()
        swap_end(torus, scr.swap_sems, swaps, 3)
        torus.drain()

    dma = pltpu.SemaphoreType.DMA
    block = (side, side, rows, hidden_loc)
    ins = dict(ctx=(attn.ctx.reshape(side, side, rows, depth), VMEM), w_outs=[(weight, ANY) for weight in w_outs], hidden=(hidden, ANY), grad_out=(grad_out, ANY), gain=(gain, VMEM),
               normed=(attn.normed, ANY), w_gate=(w_gate, ANY), w_up=(w_up, ANY), w_down=(w_down, ANY))
    out, weight = (shape(block), ANY), (shape((hidden_loc, width)), ANY)
    outs = dict(full=(shape((2, side, side, rows, width)), ANY), h_rows=(shape((rows, width)), VMEM), ctx_other=(shape((side, side, rows, depth // 2)), ANY), normed_other=(shape((seq, width)), ANY),
                w_gate=weight, w_up=weight, w_down=weight, acts=[out, out], gates=[out, out], ups=[out, out])
    scratch = dict(sum=rs_scratch(side, rows, width), all=ag_scratch(side, rows, width), w=pltpu.VMEM((depth, width), BF16), w_sem=dma((K2, K2)), swap_sems=[dma((5,)), dma((5,))],
                   x_rows=pltpu.VMEM((rows, width), BF16), x_sem=dma((K1,)), w_mlp=pltpu.VMEM((4, hidden_loc, width), BF16), w_mlp_sem=dma((4,)),
                   dy=pltpu.VMEM((2, side * rows, width), BF16), dy_sem=dma((K2,)), pre=pltpu.VMEM((4, *block), F32), grad_act=pltpu.VMEM((2, *block), F32), results=pltpu.VMEM((6, *block), BF16), result_sem=dma((6,)))
    return call_kernel('sum_attention', body, ins, outs, scratch, 4e8, 1)


def sum_mlp(side, mlp, w_gates, w_ups, grad_out, gain):
    depth = w_gates[K0].shape[K0]
    width = gain.shape[K1]
    rows = mlp.h_rows.shape[K0]
    seq = rows * side * side
    block = (side, side, rows, width)

    def body(ins, outs, scr, staging):
        torus = Torus(side)
        weights = Weights(ins.w_in, scr.w, scr.w_sem, False)
        weights.start()
        rows_at = pl.ds(pl.multiple_of(torus.chip * rows, rows), rows)
        dy_load = pltpu.make_async_copy(ins.grad_out.at[torus.core, rows_at, :], scr.dy_rows, scr.dy_sem.at[K0])
        dy_load.start()
        wait = torus.signal_all()
        steps = ReduceScatter(torus, scr.sum).slow_steps(fill_partial(torus, scr.sum.part, ins.grads, weights))
        staging.wait()
        steps[K0]()
        wait()

        turned = []

        def half_at(half):
            return pl.ds(pl.multiple_of(half * seq, seq), seq)

        def turn(index):
            kind, core = index // 2, index % 2
            src = (ins.grads[2 * core], ins.grads[2 * core + 1], ins.acts[core])[kind]
            slot = index % 2
            if index >= 2:
                turned[index - 2]()
            scr.turn[slot] = src[...].reshape(seq, depth).T
            at = slice(None), half_at(torus.core)
            if core == 0:
                save = pltpu.make_async_copy(scr.turn.at[slot], outs.lefts[kind].at[at], scr.turn_sem.at[kind])
                save.start()
                turned.append(save.wait)
            else:
                torus.send(scr.turn.at[slot], outs.lefts[kind].at[at], scr.swap_sems, kind, torus.partner)
                turned.append(torus.pending.pop().wait_send)

        turns = [functools.partial(turn, index) for index in range(6)]
        run(steps[1:])
        own = (torus.y, torus.x)
        gain_total = jnp.zeros((1, width), F32)
        gat = scr.all.gat
        dy_load.wait()
        for at in row_tiles(rows):
            back, gain_part = rms_back(ins.h_rows[at, :].astype(F32), ins.gain[...], scr.sum.part[(*own, at, slice(None))].astype(F32))
            gain_total = gain_total + gain_part
            total = scr.dy_rows[at, :].astype(F32) + back
            outs.d_rows[at, :] = total
            gat[(*own, at, slice(None))] = total.astype(BF16)
        outs.gain[...] = gain_total
        staging.save(outs.d_rows, outs.gain)
        gather = AllGather(torus, scr.all, False)
        gather.store = Store(torus, scr.all, plain_places(gather, outs.full), outs.own)
        run(gather.steps(), turns)
        turned[4]()
        turned[5]()
        for kind in range(3):
            torus.arrive(outs.lefts[kind].at[:, half_at(1 - torus.core)], scr.swap_sems, kind)
        gather.store.drain()
        torus.drain()

    dma = pltpu.SemaphoreType.DMA
    ins = dict(grads=[(grad, VMEM) for grad in (mlp.gates[K0], mlp.ups[K0], mlp.gates[K1], mlp.ups[K1])], acts=[(act, VMEM) for act in mlp.acts],
               w_in=[(weight, ANY) for weight in (w_gates[K0], w_ups[K0], w_gates[K1], w_ups[K1])],
               h_rows=(mlp.h_rows, VMEM), grad_out=(grad_out, ANY), gain=(gain, VMEM))
    outs = dict(full=(shape((2, *block)), ANY), own=(shape(block), ANY), d_rows=(shape((rows, width), F32), VMEM), gain=(shape((1, width), F32), VMEM), lefts=[(shape((depth, 2 * seq)), ANY)] * 3)
    scratch = dict(sum=rs_scratch(side, rows, width), all=ag_scratch(side, rows, width), dy_rows=pltpu.VMEM((rows, width), BF16), dy_sem=dma((K1,)),
                   w=pltpu.VMEM((4 * depth, width), BF16), w_sem=dma((K2, 4)),
                   turn=pltpu.VMEM((2, depth, seq), BF16), turn_sem=dma((K3,)), swap_sems=[dma((K3,)), dma((K3,))])
    return call_kernel('sum_mlp', body, ins, outs, scratch, 6e8, 2)


def attention_backward(side, ins, outs, scr):
    resid = scr.sum.part
    rows, width = resid.shape[2:]
    band = side * rows
    tile = min(256, side * band)
    loads, shared = [], []
    for index in PAIR:
        at = pl.ds(index * HEAD_DIM, HEAD_DIM)
        loads.append(pltpu.make_async_copy(ins.w_outs[index], scr.w_out.at[at, :], scr.w_out_sem.at[index]))
    for index in range(side):
        loads.append(pltpu.make_async_copy(ins.resid.at[index], resid.at[index], scr.resid_sem.at[index]))
    for load in loads:
        load.start()

    def context(index):
        if index == 0:
            for load in loads[:2]:
                load.wait()
        loads[2 + index].wait()
        scr.grad_ctx[index * band:(index + 1) * band, :] = dot(resid[index].reshape(band, width), scr.w_out[...], NT).astype(BF16)

    def begin():
        shared.extend([*segments(ins.seg), ins.qkv[:, 2 * HEAD_DIM:3 * HEAD_DIM].T])
        scr.grad_k[...] = jnp.zeros_like(scr.grad_k)
        scr.grad_v[...] = jnp.zeros_like(scr.grad_v)

    def put(first, count, cols, value):
        for start in range(first, first + count, 16):
            where = (start // band, start // rows % side, slice(start % rows, start % rows + 16), cols)
            outs.dqkv[where] = value[start - first:start - first + 16].astype(BF16)

    def head_tile(head_index, tile_index):
        cols = slice(head_index * HEAD_DIM, (head_index + 1) * HEAD_DIM)
        reach = (tile_index + 1) * tile
        probs, queries = scores_softmax(ins.qkv, *shared[:2], head_index, tile_index, tile)
        grad_ctx = scr.grad_ctx[tile_index * tile:reach, cols]
        grad_probs = dot(ins.qkv[:reach, 3 * HEAD_DIM:], grad_ctx, NT)
        centre = jnp.sum(grad_probs * probs, axis=0, keepdims=True)
        grad_scores = (probs * (grad_probs - centre) * HEAD_DIM ** -0.5).astype(BF16)
        scr.grad_v[:reach, :] += dot(probs.astype(BF16), grad_ctx, NN)
        scr.grad_k[:reach, :] += dot(grad_scores, queries, NN)
        put(tile_index * tile, tile, cols, dot(shared[K2][:, :reach], grad_scores, NN).T)

    def end():
        for index, ref in ((2, scr.grad_k), (3, scr.grad_v)):
            put(0, side * band, slice(index * HEAD_DIM, (index + 1) * HEAD_DIM), ref[...])

    call = functools.partial
    tiles = [call(head_tile, head_index, tile_index) for head_index in PAIR for tile_index in range(side * band // tile)]
    return [call(context, index) for index in range(side)] + [begin] + tiles + [end]


def sum_input(side, qkv, seg_ids, w_outs, w_qs, w_k, w_v, hidden, second, gain, mlp, w_downs):
    seq, depth = qkv.shape
    width = gain.shape[K1]
    rows = seq // (side * side)
    head = depth // 4
    half_side = side // 2
    tokens = seq // 2
    kv_width = w_k.shape[K1]
    per_kv = 2 * side * side * head // kv_width

    def body(ins, outs, scr, staging):
        torus = Torus(side)
        kv_col = pl.multiple_of(lax.div(torus.chip * 2, per_kv) * head, head)
        weights = Weights([*ins.w_qs, ins.w_k.at[:, pl.ds(kv_col, head)], ins.w_v.at[:, pl.ds(kv_col, head)]], scr.w, scr.w_sem, True)
        weights.start()
        weights_p = Weights(ins.w_downs, scr.wd, scr.wd_sem, False)
        weights_p.start()
        wait = torus.signal_all()
        part = scr.sum.part
        attention = attention_backward(side, ins, outs, scr)
        steps_p = ReduceScatter(torus, scr.sum_p).slow_steps(fill_partial(torus, scr.sum_p.part, ins.acts, weights_p))
        steps = ReduceScatter(torus, scr.sum).steps(fill_partial(torus, part, [outs.dqkv], weights))
        own = (torus.y, torus.x)
        gat = scr.all.gat
        gather = AllGather(torus, scr.all, True)

        def places(where, colour, half):
            chip = where[K0] * side + where[K1]
            tokens_at = pl.ds(pl.multiple_of(lax.rem(chip, 2) * tokens + colour * (tokens // 2), tokens // 2), tokens // 2)
            at = lax.div(chip, 2) * head
            src = gather.piece(gat, where, colour * 2, 2)
            return [(src.at[:, pl.ds(index * head, head)], outs.kv.at[half, tokens_at, pl.ds(pl.multiple_of(at + index * kv_width, head), head)]) for index in PAIR]

        gather.store = Store(torus, scr.all, places)
        rows_at = pl.ds(pl.multiple_of(torus.chip * rows, rows), rows)
        x_load = pltpu.make_async_copy(ins.hidden.at[torus.core, rows_at, :], scr.x_rows, scr.x_sem.at[K0])
        x_load.start()
        place = lax.rem(torus.x, 2)
        mate = torus.at_chip(torus.y, torus.x + 1 - 2 * place)
        kv_cols = pl.ds(2 * head, 2 * head)

        def mate_add():
            torus.arrive(scr.mate, scr.mate_sems, 0)
            mine = outs.dqkv[pl.ds(place * half_side, half_side), :, :, kv_cols]
            gat[own] = (mine.astype(F32) + scr.mate[...].astype(F32)).astype(BF16).reshape(tokens, 2 * head)

        staging.wait()
        steps_p[K0]()
        wait()
        sent, ringed = 5, 15
        run(steps_p[1:sent])
        run(attention, steps_p[sent:ringed])
        staging.save(outs.dqkv)
        steps[K0]()
        swaps = [(outs.dqkv.at[:, :, :, pl.ds(head, head)], outs.q_other)]
        swap_start(torus, scr.swap_sems, swaps)
        torus.send(outs.dqkv.at[pl.ds((1 - place) * half_side, half_side), :, :, kv_cols], scr.mate, scr.mate_sems, 0, mate)
        for step in steps[1:5]:
            step()
        mate_add()
        run(steps[5:], gather.steps(), steps_p[ringed:])
        x_load.wait()
        gain_total = jnp.zeros((1, width), F32)
        for at in row_tiles(rows):
            back, gain_part = rms_back(scr.x_rows[at, :].astype(F32), ins.gain[...], part[(*own, at, slice(None))].astype(F32))
            gain_total = gain_total + gain_part
            outs.rows[at, :] = (ins.d_rows[at, :] + back).astype(BF16)
            y_at = pl.ds(rows + at.start, at.size)
            outs.rows[y_at, :] = (ins.h_rows[at, :].astype(F32) + scr.sum_p.part[(*own, at, slice(None))].astype(F32)).astype(BF16)
        row = lax.broadcasted_iota(jnp.int32, (8, width), 0)
        extra = jnp.zeros((8, width), F32)
        for index, value in enumerate((gain_total, ins.gain_mlp[...])):
            for level in range(3):
                rounded = value.astype(BF16).astype(F32)
                extra = jnp.where(row == index * 3 + level, rounded, extra)
                value = value - rounded
        outs.rows[2 * rows:2 * rows + 8, :] = extra.astype(BF16)
        staging.save(outs.rows)
        gather.store.drain()
        swap_end(torus, scr.swap_sems, swaps)
        torus.drain()

    dma = pltpu.SemaphoreType.DMA
    ins = dict(qkv=(qkv, VMEM), seg=(seg_ids, VMEM), resid=(second.own, ANY), w_outs=[(weight, ANY) for weight in w_outs], acts=[(act, VMEM) for act in mlp.acts], w_downs=[(weight, ANY) for weight in w_downs], h_rows=(mlp.h_rows, VMEM), w_qs=[(weight, ANY) for weight in w_qs], w_k=(w_k, ANY), w_v=(w_v, ANY), hidden=(hidden, ANY), d_rows=(second.d_rows, VMEM),
               gain=(gain, VMEM), gain_mlp=(second.gain, VMEM))
    outs = dict(rows=(shape((2 * rows + 8, width)), VMEM), kv=(shape((2, seq, 2 * kv_width)), ANY), q_other=(shape((side, side, rows, head)), ANY), dqkv=(shape((side, side, rows, depth)), VMEM))
    scratch = dict(w_out=pltpu.VMEM((2 * head, width), BF16), grad_ctx=pltpu.VMEM((seq, 2 * head), BF16), grad_k=pltpu.VMEM((seq, head), F32), grad_v=pltpu.VMEM((seq, head), F32), w_out_sem=dma((K2,)), resid_sem=dma((side,)), sum_p=rs_scratch(side, rows, width), wd=pltpu.VMEM((2 * mlp.acts[K0].shape[K3], width), BF16), wd_sem=dma((K2, K2)),
                   sum=rs_scratch(side, rows, width), all=ag_scratch(side, tokens, 2 * head, 2), x_rows=pltpu.VMEM((rows, width), BF16), x_sem=dma((K1,)), w=pltpu.VMEM((width, depth), BF16), w_sem=dma((K2, 4)),
                   mate=pltpu.VMEM((half_side, side, rows, 2 * head), BF16), mate_sems=[dma((K1,)), dma((K1,))], swap_sems=[dma((K1,)), dma((K1,))])
    return call_kernel('sum_input', body, ins, outs, scratch, 3e8, 3)


def scores_softmax(qkv, seg_row, seg_col, head_index, tile_index, tile):
    reach = (tile_index + 1) * tile
    queries = qkv[tile_index * tile:reach, head_index * HEAD_DIM:(head_index + 1) * HEAD_DIM]
    scores = dot(qkv[:reach, 2 * HEAD_DIM:3 * HEAD_DIM], queries, NT) * HEAD_DIM ** -0.5
    key_at = lax.broadcasted_iota(jnp.int32, (reach, tile), 0)
    query_at = lax.broadcasted_iota(jnp.int32, (reach, tile), 1) + tile_index * tile
    allowed = (key_at <= query_at) & (seg_col[:reach, :] == seg_row[:, tile_index * tile:reach])
    scores = jnp.where(allowed, scores, -1e30)
    weights = jnp.exp(scores - jnp.max(scores, axis=0, keepdims=True))
    return weights * (1.0 / jnp.sum(weights, axis=0, keepdims=True)), queries


def segments(seg_ref):
    core = lax.rem(lax.axis_index('tp'), 2)
    seg_row = seg_ref[pl.ds(core, 1), :].astype(F32)
    return seg_row, jnp.broadcast_to(seg_row, (8, seg_row.shape[K1])).T[:, :1]


def attention_forward(hidden, seg_ids, gain, w_q, w_k, w_v, w_o, per_kv):
    seq, width = hidden.shape[1:]
    chunk = seq // 4
    tile = min(256, seq)
    depth = 4 * HEAD_DIM

    def body(ins, outs, scr, staging):
        tp_idx = lax.axis_index('tp')
        core = lax.rem(tp_idx, 2)
        kv_col = pl.multiple_of(lax.div(tp_idx, per_kv) * HEAD_DIM, HEAD_DIM)
        partner = dict(tp=tp_idx + 1 - 2 * core)
        barrier = pltpu.get_barrier_semaphore()
        pl.semaphore_signal(barrier, inc=1, device_id=partner, device_id_type=MESH)
        loads = []
        for index in range(4):
            at = pl.ds(index * chunk, chunk)
            loads.append(pltpu.make_async_copy(ins.hidden.at[core, at, :], scr.x.at[at, :], scr.x_sem.at[index]))

        def w_cols(index):
            return scr.w.at[:, pl.ds(index * HEAD_DIM, HEAD_DIM)]

        for index, ref in ((0, ins.w_q), (2, ins.w_k.at[:, pl.ds(kv_col, HEAD_DIM)]), (3, ins.w_v.at[:, pl.ds(kv_col, HEAD_DIM)])):
            loads.append(pltpu.make_async_copy(ref, w_cols(index), scr.w_sem.at[index]))
        for load in loads:
            load.start()
        pl.semaphore_wait(barrier, 1)
        swaps = [(ins.w_q, w_cols(1)), (ins.w_o, outs.w_o), (ins.w_q, outs.w_q)]
        copies = []
        for index, (src, dst) in enumerate(swaps):
            copies.append(pltpu.make_async_remote_copy(src, dst, scr.swap_sems[K0].at[index], scr.swap_sems[K1].at[index], device_id=partner, device_id_type=MESH))
            copies[index].start()
        stores = []
        for index in range(4):
            loads[index].wait()

            if index == 0:
                staging.wait()

            def square(step, carry, index=index):
                at = pl.ds(pl.multiple_of(index * chunk + step * 16, 16), 16)
                total = jnp.zeros((16, HEAD_DIM), F32)
                for lane in range(0, width, HEAD_DIM):
                    value = scr.x[at, lane:lane + HEAD_DIM].astype(F32)
                    total = total + value * value
                scr.squares[pl.ds(pl.multiple_of(step * 16, 16), 16), :] = total
                return carry

            lax.fori_loop(0, chunk // 16, square, 0)
            inv = lax.rsqrt(jnp.sum(scr.squares[...], axis=-1, keepdims=True) / width + EPS)
            scr.squares[...] = jnp.broadcast_to(inv, scr.squares.shape)

            def normalize(step, carry, index=index):
                at = pl.ds(pl.multiple_of(index * chunk + step * 16, 16), 16)
                scale = scr.squares[pl.ds(pl.multiple_of(step * 16, 16), 16), :]
                for lane in range(0, width, HEAD_DIM):
                    cols = slice(lane, lane + HEAD_DIM)
                    scr.normed[at, cols] = (scr.x[at, cols].astype(F32) * scale * ins.gain[:, cols]).astype(BF16)
                return carry

            lax.fori_loop(0, chunk // 16, normalize, 0)
            at = pl.ds(index * chunk, chunk)
            store = pltpu.make_async_copy(scr.normed.at[at, :], outs.normed.at[at, :], scr.out_sem.at[index])
            store.start()
            stores.append(store)
            if index == 0:
                for load in loads[4:]:
                    load.wait()
                copies[K0].wait_recv()
            outs.qkv[at, :] = dot(scr.normed[at, :], scr.w[...], NN).astype(BF16)
        staging.save(outs.qkv)
        seg_row, seg_col = segments(ins.seg)
        values_t = outs.qkv[:, 3 * HEAD_DIM:].T
        for head_index in PAIR:
            for tile_index in range(seq // tile):
                probs, _ = scores_softmax(outs.qkv, seg_row, seg_col, head_index, tile_index, tile)
                ctx_t = dot(values_t[:, :(tile_index + 1) * tile], probs.astype(BF16), NN)
                outs.ctx[tile_index * tile:(tile_index + 1) * tile, head_index * HEAD_DIM:(head_index + 1) * HEAD_DIM] = ctx_t.T.astype(BF16)
        for store in stores:
            store.wait()
        copies[K0].wait_send()
        copies[K1].wait()
        copies[K2].wait()

    dma = pltpu.SemaphoreType.DMA
    ins = dict(hidden=(hidden, ANY), seg=(seg_ids, VMEM), gain=(gain, VMEM), w_q=(w_q, ANY), w_o=(w_o, ANY), w_k=(w_k, ANY), w_v=(w_v, ANY))
    outs = dict(normed=(shape((seq, width)), ANY), qkv=(shape((seq, depth)), VMEM), ctx=(shape((seq, 2 * HEAD_DIM)), VMEM), w_q=(shape(w_q.shape), ANY), w_o=(shape(w_o.shape), ANY))
    scratch = dict(squares=pltpu.VMEM((chunk, HEAD_DIM), F32), swap_sems=[dma((K3,)), dma((K3,))], x=pltpu.VMEM((seq, width), BF16), normed=pltpu.VMEM((seq, width), BF16), w=pltpu.VMEM((width, depth), BF16), x_sem=dma((4,)), w_sem=dma((4,)), out_sem=dma((4,)))
    return call_kernel('attention_forward', body, ins, outs, scratch, 5e9, 4)


def weight_grads(name, groups, ctxs, tokens=()):
    seq, width = groups[K0][K1].shape[1:]
    head = ctxs[K1].shape[K1] if ctxs else 0
    tile = min(512, width)
    lefts = [left for left, _ in groups if left is not None]
    sizes = [head if left is None else left.shape[K0] for left, _ in groups]
    given = len(groups) + len(lefts) + len(ctxs)

    def kernel(*refs):
        rights, left_refs = refs[:len(groups)], list(refs[len(groups):len(groups) + len(lefts)])
        outs = refs[given + len(tokens):given + len(tokens) + len(groups)]
        if ctxs:
            core = lax.rem(lax.axis_index('tp'), 2)
            ctx_t = refs[-1]

            @pl.when(pl.program_id(0) == 0)
            def _():
                for half, ref in zip((core, 1 - core), refs[given - 2:given]):
                    ctx_t[:, pl.ds(pl.multiple_of(half * seq, seq), seq)] = ref[:, :head].T

        for (left, _), right, out in zip(groups, rights, outs):
            ref = ctx_t if left is None else left_refs.pop(0)
            out[...] = dot(ref[...], right[...].reshape(2 * seq, tile), NN)

    slab = pl.BlockSpec((2, seq, tile), lambda step: (0, 0, step))
    return pl.pallas_call(
        kernel,
        name=name,
        grid=(width // tile,),
        out_shape=[shape((size, width), F32) for size in sizes],
        in_specs=[slab] * len(groups) + [VMEM] * (len(lefts) + len(ctxs)) + [ANY] * len(tokens),
        out_specs=[pl.BlockSpec((size, tile), lambda step: (0, step)) for size in sizes],
        scratch_shapes=[pltpu.VMEM((head, 2 * seq), BF16)] if ctxs else [],
        compiler_params=pltpu.CompilerParams(vmem_limit_bytes=LIMIT),
        cost_estimate=pl.CostEstimate(flops=int(1e10), bytes_accessed=int(4e7), transcendentals=0),
    )(*[right for _, right in groups], *lefts, *ctxs, *tokens)


def weight_grads_pair(left_gate, left_up, mixed_full, token):
    seq, width = mixed_full.shape[1:]
    depth = left_gate.shape[K0]
    tile = min(512, width)

    def kernel(m_ref, gate_ref, up_ref, _, out_gate, out_up):
        mixed = m_ref[...].reshape(2 * seq, tile)
        out_gate[...] = dot(gate_ref[...], mixed, NN)
        out_up[...] = dot(up_ref[...], mixed, NN)

    out = pl.BlockSpec((depth, tile), lambda step: (0, step))
    return pl.pallas_call(
        kernel,
        name='weight_grads_pair',
        grid=(width // tile,),
        out_shape=[shape((depth, width), F32)] * 2,
        in_specs=[pl.BlockSpec((2, seq, tile), lambda step: (0, 0, step)), VMEM, VMEM, ANY],
        out_specs=[out, out],
        compiler_params=pltpu.CompilerParams(vmem_limit_bytes=LIMIT),
        cost_estimate=pl.CostEstimate(flops=int(1e10), bytes_accessed=int(4e7), transcendentals=0),
    )(mixed_full, left_gate, left_up, token)


def weight_grads_qkv(normeds, kv_full, grads_q):
    seq, width = normeds[K0].shape
    head = grads_q[K1].shape[K1]
    kv_width = kv_full.shape[K2] // 2
    tile = min(512, width)

    def kernel(a_own, a_other, kv_ref, q_own, q_other, out_q, out_k, out_v, left, q_both):
        core = lax.rem(lax.axis_index('tp'), 2)
        halves = [pl.ds(pl.multiple_of(half * seq, seq), seq) for half in (core, 1 - core)]

        @pl.when(pl.program_id(0) == 0)
        def _():
            q_both[halves[K0], :] = q_own[:, :head]
            q_both[halves[K1], :] = q_other[...]

        left[:, halves[K0]] = a_own[...].T
        left[:, halves[K1]] = a_other[...].T
        out_q[...] = dot(left[...], q_both[...], NN)
        for index, out in enumerate((out_k, out_v)):
            right = kv_ref[:, :, pl.ds(index * kv_width, kv_width)].reshape(2 * seq, kv_width)
            out[...] = dot(left[...], right, NN)

    slab = pl.BlockSpec((seq, tile), lambda step: (0, step))
    out = lambda size: pl.BlockSpec((tile, size), lambda step: (step, 0))
    return pl.pallas_call(
        kernel,
        name='weight_grads_qkv',
        grid=(width // tile,),
        out_shape=[shape((width, size), F32) for size in (head, kv_width, kv_width)],
        in_specs=[slab] * 2 + [VMEM] * 3,
        out_specs=[out(size) for size in (head, kv_width, kv_width)],
        scratch_shapes=[pltpu.VMEM((tile, 2 * seq), BF16), pltpu.VMEM((2 * seq, head), BF16)],
        compiler_params=pltpu.CompilerParams(vmem_limit_bytes=LIMIT),
        cost_estimate=pl.CostEstimate(flops=int(27e9), bytes_accessed=int(6e7), transcendentals=0),
    )(*normeds, kv_full, *grads_q)


def in_place(gathered, rows):
    blocks, _, width = gathered.shape
    slots = 24
    pieces = 2 * blocks

    def kernel(src, dx_ref, y_ref, gain_attn, gain_mlp, buf, extra, in_sem, out_sem, extra_sem):
        gains = pltpu.make_async_copy(src.at[:, pl.ds(2 * rows, 8), :], extra, extra_sem.at[K0])

        def load(index):
            at = pl.ds(index // blocks * rows, rows)
            return pltpu.make_async_copy(src.at[index % blocks, at, :], buf.at[index % slots], in_sem.at[index % slots])

        def store(index):
            dst, block = (dx_ref, y_ref)[index // blocks], index % blocks
            return pltpu.make_async_copy(buf.at[index % slots], dst.at[block % 2, block // 2], out_sem.at[index % slots])

        ahead = slots // 2
        for index in range(pieces + ahead):
            if index < pieces:
                if index >= slots:
                    store(index - slots).wait()
                load(index).start()
            if index == ahead:
                gains.start()
            if index >= ahead:
                load(index - ahead).wait()
                store(index - ahead).start()
        gains.wait()
        total = jnp.sum(extra[...].astype(F32), axis=0)
        for first, ref in ((0, gain_attn), (3, gain_mlp)):
            ref[...] = total[first:first + 1] + total[first + 1:first + 2] + total[first + 2:first + 3]
        for index in range(pieces - slots, pieces):
            store(index).wait()

    dma = pltpu.SemaphoreType.DMA
    whole = shape((2, blocks // 2, rows, width))
    return pl.pallas_call(
        kernel,
        name='in_place',
        out_shape=[whole, whole, shape((1, width), F32), shape((1, width), F32)],
        in_specs=[ANY],
        out_specs=[ANY, ANY, VMEM, VMEM],
        scratch_shapes=[pltpu.VMEM((slots, rows, width), BF16), pltpu.VMEM((blocks, 8, width), BF16), dma((slots,)), dma((slots,)), dma((K1,))],
        compiler_params=pltpu.CompilerParams(vmem_limit_bytes=LIMIT),
        cost_estimate=pl.CostEstimate(flops=int(2e7), bytes_accessed=int(2e7), transcendentals=0),
    )(gathered)


def solution(mesh):
    tp_size = mesh.shape['tp']
    chips = tp_size // 2
    side = math.isqrt(chips)

    def device_step(hidden, seg_ids, grad_out, gain_attn, gain_mlp, w_q, w_k, w_v, w_o, w_gate, w_up, w_down):
        seq_len, width = hidden.shape[1:]
        kv_heads = w_k.shape[K1] // HEAD_DIM
        per_kv = tp_size // kv_heads
        rows = seq_len // chips

        def flat(value):
            return value.reshape(seq_len, value.shape[-1])

        gain_attn_row = gain_attn[None, :]
        gain_mlp_row = gain_mlp[None, :]

        attn = attention_forward(hidden, seg_ids, gain_attn_row, w_q, w_k, w_v, w_o, per_kv)
        w_qs, w_outs = (w_q, attn.w_q), (w_o, attn.w_o)
        mlp = sum_attention(side, attn, w_outs, hidden, grad_out, gain_mlp_row, w_gate.T, w_up.T, w_down)
        mixed_full = mlp.full.reshape(2, seq_len, width)
        second = sum_mlp(side, mlp, (w_gate.T, mlp.w_gate), (w_up.T, mlp.w_up), grad_out, gain_mlp_row)
        resid_full = second.full.reshape(2, seq_len, width)

        third = sum_input(side, attn.qkv, seg_ids, w_outs, w_qs, w_k, w_v, hidden, second, gain_attn_row, mlp, (w_down, mlp.w_down))

        grad_in, y_out, grad_gain_attn, grad_gain_mlp = in_place(lax.all_gather(third.rows, 'tp'), rows)
        left_gate, left_up, left_act = second.lefts
        grad_gate_t, grad_up_t = weight_grads_pair(left_gate, left_up, mixed_full, third.q_other)
        grad_w_down, grad_w_o = weight_grads('weight_grads_down', [(left_act, grad_out), (None, resid_full)], (attn.ctx, flat(mlp.ctx_other)), (third.q_other,))
        grad_w_q, grad_w_k, grad_w_v = weight_grads_qkv((attn.normed, mlp.normed_other), third.kv, (flat(third.dqkv), flat(third.q_other)))
        return (y_out.reshape(hidden.shape), grad_in.reshape(hidden.shape), grad_gain_attn[K0], grad_gain_mlp[K0], grad_w_q, grad_w_k, grad_w_v, grad_w_o, grad_gate_t.T, grad_up_t.T, grad_w_down)

    spec_act = P('data', None, None)
    spec_rows = P('data', None)
    spec_gain = P(None)
    spec_cols = P(None, 'tp')
    spec_tprows = P('tp', None)
    spec_whole = P(None, None)
    spec_stack = P(('data', 'tp'), None)
    in_specs = (spec_act, spec_rows, spec_act, spec_gain, spec_gain, spec_cols, spec_whole, spec_whole, spec_tprows, spec_cols, spec_cols, spec_tprows)
    out_specs = (spec_act, spec_act, P('data'), P('data'), P('data', 'tp'), spec_rows, spec_rows, spec_stack, P('data', 'tp'), P('data', 'tp'), spec_stack)
    return jax.shard_map(device_step, mesh=mesh, in_specs=in_specs, out_specs=out_specs, check_vma=False)
```

```python
import functools
import math
import types
import jax
import jax.numpy as jnp
from jax import lax
from jax.experimental import pallas as pl
from jax.experimental.pallas import tpu as pltpu
from jax.sharding import PartitionSpec as P

HEAD_DIM = 128
EPS = 1e-5
MESH = pl.DeviceIdType.MESH
F32 = jnp.float32
BF16 = jnp.bfloat16
LIMIT = 63 * 2 ** 20
K0, K1, K2, K3 = range(4)
PAIR = range(2)
ANY = pl.BlockSpec(memory_space=pl.ANY)
VMEM = pl.BlockSpec(memory_space=pltpu.VMEM)


def dot(lhs, rhs, dims):
    return lax.dot_general(lhs, rhs, (dims, ((), ())), preferred_element_type=F32)


NN = ((1,), (0,))
NT = ((1,), (1,))


SIGNS = (1, -1)


class Colour:
    def __init__(self, index, first, second):
        self.index, self.first, self.second = index, first, second


class Torus:
    def __init__(self, side):
        self.side = side
        tp_idx = lax.axis_index('tp')
        self.core = lax.rem(tp_idx, 2)
        self.chip = lax.div(tp_idx, 2)
        self.x = lax.rem(self.chip, side)
        self.y = lax.div(self.chip, side)
        self.partner = {'tp': self.chip * 2 + (1 - self.core)}
        self.colours = (Colour(0, self.x, self.y), Colour(1, self.y, self.x))
        self.pending = []

    def wrap(self, pos):
        return lax.rem(pos + 2 * self.side, self.side)

    def at_chip(self, y_at, x_at):
        return {'tp': (y_at * self.side + x_at) * 2 + self.core}

    def block(self, col, second, first):
        return (second, first) if col.index == 0 else (first, second)

    def peer1(self, col, shift):
        return self.at_chip(*self.block(col, col.second, self.wrap(col.first + shift)))

    def peer2(self, col, shift):
        return self.at_chip(*self.block(col, self.wrap(col.second + shift), col.first))

    def signal_all(self):
        barrier = pltpu.get_barrier_semaphore()
        peers = [self.partner]
        peers += [self.at_chip(self.y, self.wrap(self.x + shift)) for shift in SIGNS]
        peers += [self.at_chip(self.wrap(self.y + shift), self.x) for shift in SIGNS]
        for peer in peers:
            pl.semaphore_signal(barrier, inc=1, device_id=peer, device_id_type=MESH)
        return lambda: pl.semaphore_wait(barrier, len(peers))

    def send(self, src, dst, sems, index, device):
        copy = pltpu.make_async_remote_copy(src, dst, sems[K0].at[index], sems[K1].at[index], device_id=device, device_id_type=MESH)
        copy.start()
        self.pending.append(copy)

    def arrive(self, dst, sems, index):
        pltpu.make_async_remote_copy(dst, dst, sems[K0].at[index], sems[K1].at[index], device_id=self.partner, device_id_type=MESH).wait_recv()

    def drain(self):
        for copy in self.pending:
            copy.wait_send()


R1, R2, R3, S1, S2, S3 = range(6)
RS_COUNTS = (16, 16, 16, 4, 4, 4)
H1, H2, F1, F2 = range(4)
AG_COUNTS = (8, 32, 4, 16)


class ReduceScatter:
    SHIFTS = (2, 1, 3, 0)

    def __init__(self, torus, scr):
        self.torus, self.part, self.scr = torus, scr.part, scr
        self.quarter = scr.part.shape[K3] // 4

    def buf(self, kind, index):
        return self.scr.bufs[kind].at[index]

    def sems(self, kind):
        return self.scr.out_sems[kind], self.scr.in_sems[kind]

    def cols(self, col, half):
        return pl.ds((col.index * 2 + half) * self.quarter, self.quarter)

    def piece(self, where, at_cols):
        return self.part.at[(*where, slice(None), at_cols)]

    def send(self, where, at_cols, kind, index, peer):
        self.torus.send(self.piece(where, at_cols), self.buf(kind, index), self.sems(kind), index, peer)

    def add(self, where, at_cols, *kinds):
        total = self.part[(*where, slice(None), at_cols)].astype(F32)
        for kind, index in kinds:
            self.torus.arrive(self.buf(kind, index), self.sems(kind), index)
            total = total + self.buf(kind, index)[...].astype(F32)
        self.part[(*where, slice(None), at_cols)] = total.astype(BF16)

    def each(self, step):
        wrap = self.torus.wrap
        for col in self.torus.colours:
            second = wrap(col.second + self.SHIFTS[step])
            for way, sign in enumerate(SIGNS):
                yield col, second, way, sign, (col.index * 2 + way) * 4 + step

    def far(self, step):
        for col, second, way, sign, index in self.each(step):
            where = self.torus.block(col, second, self.torus.wrap(col.first + 2))
            self.send(where, self.cols(col, way), R1, index, self.torus.peer1(col, sign))

    def near(self, step):
        for col, second, way, sign, index in self.each(step):
            where = self.torus.block(col, second, self.torus.wrap(col.first + sign))
            self.send(where, self.cols(col, 1 - way), R2, index, self.torus.peer1(col, sign))

    def relay(self, step):
        for col, second, way, sign, index in self.each(step):
            where = self.torus.block(col, second, self.torus.wrap(col.first + sign))
            self.add(where, self.cols(col, way), (R1, index))
            self.send(where, self.cols(col, way), R3, index, self.torus.peer1(col, sign))

    def end(self, step):
        for col, second, way, sign, index in self.each(step):
            where = self.torus.block(col, second, col.first)
            other = (col.index * 2 + 1 - way) * 4 + step
            self.add(where, self.cols(col, way), (R2, other), (R3, index))

    def far2(self):
        for col in self.torus.colours:
            for way, sign in enumerate(SIGNS):
                where = self.torus.block(col, self.torus.wrap(col.second + 2), col.first)
                self.send(where, self.cols(col, way), S1, col.index * 2 + way, self.torus.peer2(col, sign))

    def near2(self, way):
        for col in self.torus.colours:
            where = self.torus.block(col, self.torus.wrap(col.second + SIGNS[way]), col.first)
            self.send(where, self.cols(col, 1 - way), S2, col.index * 2 + way, self.torus.peer2(col, SIGNS[way]))

    def relay2(self, way):
        for col in self.torus.colours:
            index = col.index * 2 + way
            where = self.torus.block(col, self.torus.wrap(col.second + SIGNS[way]), col.first)
            self.add(where, self.cols(col, way), (S1, index))
            self.send(where, self.cols(col, way), S3, index, self.torus.peer2(col, SIGNS[way]))

    def end2(self):
        for col in self.torus.colours:
            where = self.torus.block(col, col.second, col.first)
            for way in PAIR:
                self.add(where, self.cols(col, way), (S2, col.index * 2 + 1 - way), (S3, col.index * 2 + way))

    def steps(self, fill):
        call = functools.partial
        return [call(fill, K2), call(self.far, K0), call(self.far, K1), call(fill, K1), call(fill, K3),
                call(self.near, K0), call(self.relay, K0), call(self.near, K1), call(self.far, K2), call(self.relay, K1),
                call(fill, K0), call(self.near, K2), call(self.far, K3), call(self.end, K0), self.far2,
                call(self.relay, K2), call(self.near, K3), call(self.end, K1), call(self.near2, K0), call(self.relay2, K0),
                call(self.relay, K3), call(self.end, K2), call(self.near2, K1), call(self.relay2, K1), call(self.end, K3),
                self.end2]

    def slow_steps(self, fill):
        call = functools.partial
        steps = range(self.torus.side)
        result = [call(fill, K2)] + [call(self.far, step) for step in steps] + [call(fill, K1), call(fill, K3)]
        for step in steps:
            result += [call(self.near, step), call(self.relay, step)]
        return result + [call(fill, K0), call(self.end, K0), self.far2, call(self.end, K1), call(self.near2, K0), call(self.relay2, K0),
                         call(self.end, K2), call(self.near2, K1), call(self.relay2, K1), call(self.end, K3), self.end2]


class AllGather:
    def __init__(self, torus, scr, by_rows):
        self.torus, self.gat, self.scr, self.by_rows, self.store = torus, scr.gat, scr, by_rows, None
        self.quarter = scr.gat.shape[2 if by_rows else 3] // 4
        self.back = (0, torus.side - 1, 1, 2)

    def sems(self, kind):
        return self.scr.out_sems[kind], self.scr.in_sems[kind]

    def piece(self, ref, where, first, count):
        at = pl.ds(first * self.quarter, count * self.quarter)
        return ref.at[(*where, at, slice(None))] if self.by_rows else ref.at[(*where, slice(None), at)]

    def half(self, col, where, half):
        return self.piece(self.gat, where, col.index * 2 + half, 1)

    def own2(self, turn):
        for col in self.torus.colours:
            where = self.torus.block(col, col.second, col.first)
            for way, sign in enumerate(SIGNS):
                at = self.half(col, where, way if turn == 0 else 1 - way)
                self.torus.send(at, at, self.sems(H1), (col.index * 2 + way) * 2 + turn, self.torus.peer2(col, sign))

    def send1(self, step, turn):
        for col in self.torus.colours:
            where = self.torus.block(col, self.torus.wrap(col.second + self.back[step]), col.first)
            for way, sign in enumerate(SIGNS):
                at = self.half(col, where, way if turn == 0 else 1 - way)
                self.torus.send(at, at, self.sems(H2), ((col.index * 2 + way) * 4 + step) * 2 + turn, self.torus.peer1(col, sign))

    def arrive2(self, way, turn):
        sign = SIGNS[way]
        for col in self.torus.colours:
            where = self.torus.block(col, self.torus.wrap(col.second - sign), col.first)
            at = self.half(col, where, way if turn == 0 else 1 - way)
            self.torus.arrive(at, self.sems(H1), (col.index * 2 + way) * 2 + turn)
            if turn == 0:
                self.torus.send(at, at, self.sems(F1), col.index * 2 + way, self.torus.peer2(col, sign))

    def relayed2(self):
        for col in self.torus.colours:
            where = self.torus.block(col, self.torus.wrap(col.second + 2), col.first)
            for way in PAIR:
                self.torus.arrive(self.half(col, where, way), self.sems(F1), col.index * 2 + way)

    def arrive1(self, step, turn):
        for col in self.torus.colours:
            second = self.torus.wrap(col.second + self.back[step])
            for way, sign in enumerate(SIGNS):
                where = self.torus.block(col, second, self.torus.wrap(col.first - sign))
                at = self.half(col, where, way if turn == 0 else 1 - way)
                self.torus.arrive(at, self.sems(H2), ((col.index * 2 + way) * 4 + step) * 2 + turn)
                if turn == 0:
                    self.torus.send(at, at, self.sems(F2), (col.index * 2 + way) * 4 + step, self.torus.peer1(col, sign))

    def relayed1(self, step):
        for col in self.torus.colours:
            second = self.torus.wrap(col.second + self.back[step])
            for way in PAIR:
                where = self.torus.block(col, second, self.torus.wrap(col.first + 2))
                self.torus.arrive(self.half(col, where, way), self.sems(F2), (col.index * 2 + way) * 4 + step)

    def keep(self, step, firsts):
        for col in self.torus.colours:
            for shift in firsts:
                where = self.torus.block(col, self.torus.wrap(col.second + self.back[step]), self.torus.wrap(col.first + shift))
                self.store.keep(where, col.index, lambda ref, where=where, col=col: self.piece(ref, where, col.index * 2, 2))

    def steps(self, whole=None):
        call = functools.partial
        whole = whole or (lambda step: None)
        here, beside, across = (K0,), (K1, self.torus.side - 1), (K2,)

        def rest(step):
            return [call(self.arrive1, step, K1), call(self.keep, step, beside), call(self.relayed1, step), call(self.keep, step, across), call(whole, step)]

        result = []
        for turn in PAIR:
            result += [call(self.own2, turn), call(self.send1, K0, turn)]
        result += [call(self.keep, K0, here), call(self.arrive2, K0, K0), call(self.arrive2, K1, K0), call(self.arrive1, K0, K0),
                   call(self.arrive2, K0, K1), call(self.send1, K1, K0), call(self.send1, K1, K1), call(self.keep, K1, here),
                   call(self.arrive2, K1, K1), call(self.send1, K2, K0), call(self.keep, K2, here),
                   call(self.arrive1, K1, K0), call(self.send1, K2, K1), self.relayed2, call(self.send1, K3, K0), call(self.keep, K3, here)]
        result += rest(K0) + [call(self.arrive1, K2, K0), call(self.send1, K3, K1)]
        return result + rest(K1) + [call(self.arrive1, K3, K0)] + rest(K2) + rest(K3)


class Store:
    def __init__(self, torus, scr, places, own=None):
        self.torus, self.scr, self.places, self.own = torus, scr, places, own
        self.stores = []

    def slot(self, where, colour, index):
        return ((index * 2 + colour) * self.torus.side + where[K0]) * self.torus.side + where[K1]

    def keep(self, where, colour, piece):
        for index, (src, dst) in enumerate(self.places(where, colour, self.torus.core)):
            slot = self.slot(where, colour, index)
            pairs = [(self.scr.full_sem, dst)]
            if self.own is not None:
                pairs.append((self.scr.own_sem, piece(self.own)))
            for sem, ref in pairs:
                store = pltpu.make_async_copy(src, ref, sem.at[slot])
                store.start()
                self.stores.append(store)
            self.torus.send(src, dst, self.scr.cross_sems, slot, self.torus.partner)

    def drain(self):
        for store in self.stores:
            store.wait()
        side = self.torus.side
        for colour in PAIR:
            for y_at in range(side):
                for x_at in range(side):
                    for index, (_, dst) in enumerate(self.places((y_at, x_at), colour, 1 - self.torus.core)):
                        self.torus.arrive(dst, self.scr.cross_sems, self.slot((y_at, x_at), colour, index))


def plain_places(gather, full):
    return lambda where, colour, half: [(gather.piece(gather.gat, where, colour * 2, 2), gather.piece(full.at[half], where, colour * 2, 2))]


def rs_scratch(side, rows, width):
    dma = pltpu.SemaphoreType.DMA
    return dict(
        part=pltpu.VMEM((side, side, rows, width), BF16),
        bufs=[pltpu.VMEM((count, rows, width // 4), BF16) for count in RS_COUNTS],
        out_sems=[dma((count,)) for count in RS_COUNTS],
        in_sems=[dma((count,)) for count in RS_COUNTS],
    )


def ag_scratch(side, rows, width, places=1):
    dma = pltpu.SemaphoreType.DMA
    blocks = 2 * side * side * places
    return dict(
        gat=pltpu.VMEM((side, side, rows, width), BF16),
        out_sems=[dma((count,)) for count in AG_COUNTS],
        in_sems=[dma((count,)) for count in AG_COUNTS],
        full_sem=dma((blocks,)),
        own_sem=dma((blocks,)),
        cross_sems=[dma((blocks,)), dma((blocks,))],
    )


class Weights:
    def __init__(self, refs, buf, sem, by_rows):
        self.refs, self.buf, self.sem, self.by_rows = refs, buf, sem, by_rows
        self.copies = [[], []]

    def start(self):
        for colour in PAIR:
            for index, ref in enumerate(self.refs):
                if self.by_rows:
                    half, depth = ref.shape[K0] // 2, ref.shape[K1]
                    rows, cols = pl.ds(colour * half, half), pl.ds(index * depth, depth)
                    copy = pltpu.make_async_copy(ref.at[rows, :], self.buf.at[rows, cols], self.sem.at[colour, index])
                else:
                    half, depth = ref.shape[K1] // 2, ref.shape[K0]
                    rows, cols = pl.ds(index * depth, depth), pl.ds(colour * half, half)
                    copy = pltpu.make_async_copy(ref.at[:, cols], self.buf.at[rows, cols], self.sem.at[colour, index])
                copy.start()
                self.copies[colour].append(copy)

    def wait(self, colour):
        for copy in self.copies[colour]:
            copy.wait()
        self.copies[colour] = []


def fill_partial(torus, part, lhs, weights):
    rows, width = part.shape[2:]
    tile = min(1024, width // 2)

    def fill(shift):
        for col in torus.colours:
            weights.wait(col.index)
            first = torus.wrap(col.first + shift)
            left = []
            for ref in lhs:
                depth = ref.shape[K3]
                value = ref[:, first] if col.index == 0 else ref[first]
                left.append((value.reshape(torus.side * rows, depth), depth))

            def body(step, carry, col=col, first=first, left=left):
                at = pl.ds(pl.multiple_of(col.index * (width // 2) + step * tile, tile), tile)
                total = None
                base = 0
                for value, depth in left:
                    if weights.by_rows:
                        term = dot(value, weights.buf[at, base:base + depth], NT)
                    else:
                        term = dot(value, weights.buf[base:base + depth, at], NN)
                    total = term if total is None else total + term
                    base += depth
                total = total.astype(BF16).reshape(torus.side, rows, tile)
                if col.index == 0:
                    part[:, first, :, at] = total
                else:
                    part[first, :, :, at] = total
                return carry

            lax.fori_loop(0, (width // 2) // tile, body, 0)

    return fill


def run(*lists):
    keyed = []
    for order, steps in enumerate(lists):
        keyed += [((index + 0.5) / len(steps), order, step) for index, step in enumerate(steps)]
    for _, _, step in sorted(keyed, key=lambda item: item[:2]):
        step()


def swap_start(torus, sems, pairs):
    for index, (src, dst) in enumerate(pairs):
        torus.send(src, dst, sems, index, torus.partner)


def swap_end(torus, sems, pairs, first=0):
    for index, (_, dst) in enumerate(pairs):
        if index >= first:
            torus.arrive(dst, sems, index)


def row_tiles(rows):
    return [pl.ds(start, 16) for start in range(0, rows, 16)]


def rms_back(z_in, gain, grad):
    inv = lax.rsqrt(jnp.mean(z_in * z_in, axis=-1, keepdims=True) + EPS)
    normed = z_in * inv
    scaled = grad * gain
    back = inv * (scaled - normed * jnp.mean(scaled * normed, axis=-1, keepdims=True))
    return back, jnp.sum(grad * normed, axis=0, keepdims=True)


def bag(tree):
    if isinstance(tree, dict):
        return types.SimpleNamespace(**{key: bag(value) for key, value in tree.items()})
    return [bag(value) for value in tree] if isinstance(tree, list) else tree


class Staging:
    def __init__(self, loads, saves):
        self.loads, self.saves, self.left = loads, saves, {}

    def start(self):
        for load in self.loads:
            load.start()

    def wait(self):
        for load in self.loads:
            load.wait()

    def save(self, *refs):
        for ref, save in self.saves:
            if any(ref is one for one in refs):
                save.start()
                self.left[id(ref)] = save

    def finish(self):
        self.save(*[ref for ref, _ in self.saves if id(ref) not in self.left])
        for save in self.left.values():
            save.wait()


def call_kernel(name, body, ins, outs, scratch, flops, collective_id=None):
    is_leaf = lambda value: isinstance(value, tuple)
    in_leaves, in_tree = jax.tree.flatten(ins, is_leaf=is_leaf)
    out_leaves, out_tree = jax.tree.flatten(outs, is_leaf=is_leaf)
    scr_leaves, scr_tree = jax.tree.flatten(scratch)
    first_scr = len(in_leaves) + len(out_leaves)
    staged = [index for index, leaf in enumerate(in_leaves + out_leaves) if leaf[K1] is VMEM]
    stages = []
    for index in staged:
        leaf = (in_leaves + out_leaves)[index][K0]
        stages.append(pltpu.VMEM(leaf.shape, leaf.dtype))

    def kernel(*refs):
        refs = list(refs)
        own = refs[first_scr + len(scr_leaves):]
        sem = own.pop()
        loads, saves = [], []
        for slot, (index, ref) in enumerate(zip(staged, own)):
            if index < len(in_leaves):
                loads.append(pltpu.make_async_copy(refs[index], ref, sem.at[slot]))
            else:
                saves.append((ref, pltpu.make_async_copy(ref, refs[index], sem.at[slot])))
            refs[index] = ref
        staging = Staging(loads, saves)
        staging.start()
        body(bag(in_tree.unflatten(refs[:len(in_leaves)])), bag(out_tree.unflatten(refs[len(in_leaves):first_scr])), bag(scr_tree.unflatten(refs[first_scr:first_scr + len(scr_leaves)])), staging)
        staging.finish()

    results = pl.pallas_call(
        kernel,
        name=name,
        out_shape=[leaf[K0] for leaf in out_leaves],
        in_specs=[ANY] * len(in_leaves),
        out_specs=[ANY] * len(out_leaves),
        scratch_shapes=scr_leaves + stages + [pltpu.SemaphoreType.DMA((len(staged),))],
        compiler_params=pltpu.CompilerParams(collective_id=collective_id, has_side_effects=collective_id is not None, vmem_limit_bytes=LIMIT),
        cost_estimate=pl.CostEstimate(flops=int(flops), bytes_accessed=int(4e7), transcendentals=0),
    )(*[leaf[K0] for leaf in in_leaves])
    return bag(out_tree.unflatten(results))


def shape(dims, dtype=BF16):
    return jax.ShapeDtypeStruct(dims, dtype)


def sum_attention(side, attn, w_outs, hidden, grad_out, gain, w_gate, w_up, w_down):
    seq, depth = attn.ctx.shape
    width = gain.shape[K1]
    hidden_loc = w_gate.shape[K0]
    rows = seq // (side * side)

    def body(ins, outs, scr, staging):
        torus = Torus(side)
        weights = Weights(ins.w_outs, scr.w, scr.w_sem, False)
        weights.start()
        rows_at = pl.ds(pl.multiple_of(torus.chip * rows, rows), rows)
        x_load = pltpu.make_async_copy(ins.hidden.at[torus.core, rows_at, :], scr.x_rows, scr.x_sem.at[K0])
        x_load.start()

        def load_weight(src, slot):
            load = pltpu.make_async_copy(src, scr.w_mlp.at[slot], scr.w_mlp_sem.at[slot])
            load.start()
            return load

        loads = {slot: load_weight(src, slot) for slot, src in ((K0, ins.w_down), (K2, ins.w_gate), (K3, ins.w_up))}
        wait = torus.signal_all()
        part = scr.sum.part
        steps = ReduceScatter(torus, scr.sum).steps(fill_partial(torus, part, [ins.ctx], weights))
        staging.wait()
        steps[K0]()
        wait()
        other_ctx = ins.ctx.at[:, :, :, pl.ds(depth // 2, depth // 2)]
        swaps = [(ins.w_down, outs.w_down), (ins.w_gate, outs.w_gate), (ins.w_up, outs.w_up), (other_ctx, outs.ctx_other), (ins.normed, outs.normed_other)]
        swap_start(torus, scr.swap_sems, swaps)

        def dy_load(group):
            at = pl.ds(group * side * rows, side * rows)
            return pltpu.make_async_copy(ins.grad_out.at[torus.core, at, :], scr.dy.at[group % 2], scr.dy_sem.at[group % 2])

        def grad_act(group):
            if group == 0:
                torus.arrive(outs.w_down, scr.swap_sems, 0)
                loads[K1] = load_weight(outs.w_down, K1)
                for slot in PAIR:
                    loads[slot].wait()
            dy_load(group).wait()
            for slot in PAIR:
                product = dot(scr.dy[group % 2], scr.w_mlp[slot], NT)
                scr.grad_act[slot, group] = product.reshape(side, rows, hidden_loc)
            if group + 2 < side:
                dy_load(group + 2).start()

        dy_load(0).start()
        dy_load(1).start()
        half = len(steps) // 3
        run(steps[1:half])
        run(steps[half:], [functools.partial(grad_act, group) for group in range(side)])
        for index, (slot, out) in enumerate(((K0, outs.w_gate), (K1, outs.w_up))):
            torus.arrive(out, scr.swap_sems, index + 1)
            loads[slot] = load_weight(out, slot)
        scr.pre[...] = jnp.zeros_like(scr.pre)
        gat = scr.all.gat
        own = (torus.y, torus.x)
        x_load.wait()
        for at in row_tiles(rows):
            resid = (scr.x_rows[at, :].astype(F32) + part[(*own, at, slice(None))].astype(F32)).astype(BF16)
            outs.h_rows[at, :] = resid
            z_in = resid.astype(F32)
            inv = lax.rsqrt(jnp.mean(z_in * z_in, axis=-1, keepdims=True) + EPS)
            gat[(*own, at, slice(None))] = (z_in * inv * ins.gain[...]).astype(BF16)
        staging.save(outs.h_rows)
        gather = AllGather(torus, scr.all, False)
        gather.store = Store(torus, scr.all, plain_places(gather, outs.full))

        def products(step):
            if step == 0:
                for load in (loads[slot] for slot in (K0, K1, K2, K3)):
                    load.wait()
            for col in torus.colours:
                second = torus.wrap(col.second + gather.back[step])
                at_cols = pl.ds(col.index * (width // 2), width // 2)
                mixed = gat[second, :, :, at_cols] if col.index == 0 else gat[:, second, :, at_cols]
                mixed = mixed.reshape(side * rows, width // 2)

                def body(slot, carry, col=col, second=second, at_cols=at_cols, mixed=mixed):
                    term = dot(mixed, scr.w_mlp[slot, :, at_cols], NT).reshape(side, rows, hidden_loc)
                    if col.index == 0:
                        scr.pre[slot, second] += term
                    else:
                        scr.pre[slot, :, second] += term
                    return carry

                lax.fori_loop(0, 4, body, 0)
            for inner, count in ((0, step + 1), (1, step)):

                def block(index, carry, inner=inner):
                    shift = lax.rem(3 * index + 3 * lax.div(index * (index - 1), 2), side)
                    pair = (gather.back[step], shift) if inner == 0 else (shift, gather.back[step])
                    y_at, x_at = torus.wrap(torus.y + pair[K0]), torus.wrap(torus.x + pair[K1])
                    for core in PAIR:
                        gate, upper = scr.pre[2 - 2 * core, y_at, x_at], scr.pre[3 - 2 * core, y_at, x_at]
                        grad = scr.grad_act[core, y_at, x_at]
                        sigmoid_g = 1.0 / (1.0 + jnp.exp(-gate))
                        silu_g = gate * sigmoid_g
                        scr.results[core, y_at, x_at] = (silu_g * upper).astype(BF16)
                        scr.results[2 + core, y_at, x_at] = (grad * upper * sigmoid_g * (1.0 + gate * (1.0 - sigmoid_g))).astype(BF16)
                        scr.results[4 + core, y_at, x_at] = (grad * silu_g).astype(BF16)
                    for kind, out in enumerate(outs.acts + outs.gates + outs.ups):
                        pltpu.make_async_copy(scr.results.at[kind, y_at, x_at], out.at[y_at, x_at], scr.result_sem.at[kind]).start()
                    return carry

                lax.fori_loop(0, count, block, 0)

        run(gather.steps(products))
        for kind, out in enumerate(outs.acts + outs.gates + outs.ups):
            pltpu.make_async_copy(scr.results.at[kind], out, scr.result_sem.at[kind]).wait()
        gather.store.drain()
        swap_end(torus, scr.swap_sems, swaps, 3)
        torus.drain()

    dma = pltpu.SemaphoreType.DMA
    block = (side, side, rows, hidden_loc)
    ins = dict(ctx=(attn.ctx.reshape(side, side, rows, depth), VMEM), w_outs=[(weight, ANY) for weight in w_outs], hidden=(hidden, ANY), grad_out=(grad_out, ANY), gain=(gain, VMEM),
               normed=(attn.normed, ANY), w_gate=(w_gate, ANY), w_up=(w_up, ANY), w_down=(w_down, ANY))
    out, weight = (shape(block), ANY), (shape((hidden_loc, width)), ANY)
    outs = dict(full=(shape((2, side, side, rows, width)), ANY), h_rows=(shape((rows, width)), VMEM), ctx_other=(shape((side, side, rows, depth // 2)), ANY), normed_other=(shape((seq, width)), ANY),
                w_gate=weight, w_up=weight, w_down=weight, acts=[out, out], gates=[out, out], ups=[out, out])
    scratch = dict(sum=rs_scratch(side, rows, width), all=ag_scratch(side, rows, width), w=pltpu.VMEM((depth, width), BF16), w_sem=dma((K2, K2)), swap_sems=[dma((5,)), dma((5,))],
                   x_rows=pltpu.VMEM((rows, width), BF16), x_sem=dma((K1,)), w_mlp=pltpu.VMEM((4, hidden_loc, width), BF16), w_mlp_sem=dma((4,)),
                   dy=pltpu.VMEM((2, side * rows, width), BF16), dy_sem=dma((K2,)), pre=pltpu.VMEM((4, *block), F32), grad_act=pltpu.VMEM((2, *block), F32), results=pltpu.VMEM((6, *block), BF16), result_sem=dma((6,)))
    return call_kernel('sum_attention', body, ins, outs, scratch, 4e8, 1)


def sum_mlp(side, mlp, w_gates, w_ups, grad_out, gain):
    depth = w_gates[K0].shape[K0]
    width = gain.shape[K1]
    rows = mlp.h_rows.shape[K0]
    seq = rows * side * side
    block = (side, side, rows, width)

    def body(ins, outs, scr, staging):
        torus = Torus(side)
        weights = Weights(ins.w_in, scr.w, scr.w_sem, False)
        weights.start()
        rows_at = pl.ds(pl.multiple_of(torus.chip * rows, rows), rows)
        dy_load = pltpu.make_async_copy(ins.grad_out.at[torus.core, rows_at, :], scr.dy_rows, scr.dy_sem.at[K0])
        dy_load.start()
        wait = torus.signal_all()
        steps = ReduceScatter(torus, scr.sum).slow_steps(fill_partial(torus, scr.sum.part, ins.grads, weights))
        staging.wait()
        steps[K0]()
        wait()

        turned = []

        def half_at(half):
            return pl.ds(pl.multiple_of(half * seq, seq), seq)

        def turn(index):
            kind, core = index // 2, index % 2
            src = (ins.grads[2 * core], ins.grads[2 * core + 1], ins.acts[core])[kind]
            slot = index % 2
            if index >= 2:
                turned[index - 2]()
            scr.turn[slot] = src[...].reshape(seq, depth).T
            at = slice(None), half_at(torus.core)
            if core == 0:
                save = pltpu.make_async_copy(scr.turn.at[slot], outs.lefts[kind].at[at], scr.turn_sem.at[kind])
                save.start()
                turned.append(save.wait)
            else:
                torus.send(scr.turn.at[slot], outs.lefts[kind].at[at], scr.swap_sems, kind, torus.partner)
                turned.append(torus.pending.pop().wait_send)

        turns = [functools.partial(turn, index) for index in range(6)]
        run(steps[1:])
        own = (torus.y, torus.x)
        gain_total = jnp.zeros((1, width), F32)
        gat = scr.all.gat
        dy_load.wait()
        for at in row_tiles(rows):
            back, gain_part = rms_back(ins.h_rows[at, :].astype(F32), ins.gain[...], scr.sum.part[(*own, at, slice(None))].astype(F32))
            gain_total = gain_total + gain_part
            total = scr.dy_rows[at, :].astype(F32) + back
            outs.d_rows[at, :] = total
            gat[(*own, at, slice(None))] = total.astype(BF16)
        outs.gain[...] = gain_total
        staging.save(outs.d_rows, outs.gain)
        gather = AllGather(torus, scr.all, False)
        gather.store = Store(torus, scr.all, plain_places(gather, outs.full), outs.own)
        run(gather.steps(), turns)
        turned[4]()
        turned[5]()
        for kind in range(3):
            torus.arrive(outs.lefts[kind].at[:, half_at(1 - torus.core)], scr.swap_sems, kind)
        gather.store.drain()
        torus.drain()

    dma = pltpu.SemaphoreType.DMA
    ins = dict(grads=[(grad, VMEM) for grad in (mlp.gates[K0], mlp.ups[K0], mlp.gates[K1], mlp.ups[K1])], acts=[(act, VMEM) for act in mlp.acts],
               w_in=[(weight, ANY) for weight in (w_gates[K0], w_ups[K0], w_gates[K1], w_ups[K1])],
               h_rows=(mlp.h_rows, VMEM), grad_out=(grad_out, ANY), gain=(gain, VMEM))
    outs = dict(full=(shape((2, *block)), ANY), own=(shape(block), ANY), d_rows=(shape((rows, width), F32), VMEM), gain=(shape((1, width), F32), VMEM), lefts=[(shape((depth, 2 * seq)), ANY)] * 3)
    scratch = dict(sum=rs_scratch(side, rows, width), all=ag_scratch(side, rows, width), dy_rows=pltpu.VMEM((rows, width), BF16), dy_sem=dma((K1,)),
                   w=pltpu.VMEM((4 * depth, width), BF16), w_sem=dma((K2, 4)),
                   turn=pltpu.VMEM((2, depth, seq), BF16), turn_sem=dma((K3,)), swap_sems=[dma((K3,)), dma((K3,))])
    return call_kernel('sum_mlp', body, ins, outs, scratch, 6e8, 2)


def attention_backward(side, ins, outs, scr):
    resid = scr.sum.part
    rows, width = resid.shape[2:]
    band = side * rows
    tile = min(256, side * band)
    loads, shared = [], []
    for index in PAIR:
        at = pl.ds(index * HEAD_DIM, HEAD_DIM)
        loads.append(pltpu.make_async_copy(ins.w_outs[index], scr.w_out.at[at, :], scr.w_out_sem.at[index]))
    for index in range(side):
        loads.append(pltpu.make_async_copy(ins.resid.at[index], resid.at[index], scr.resid_sem.at[index]))
    for load in loads:
        load.start()

    def context(index):
        if index == 0:
            for load in loads[:2]:
                load.wait()
        loads[2 + index].wait()
        scr.grad_ctx[index * band:(index + 1) * band, :] = dot(resid[index].reshape(band, width), scr.w_out[...], NT).astype(BF16)

    def begin():
        shared.extend([*segments(ins.seg), ins.qkv[:, 2 * HEAD_DIM:3 * HEAD_DIM].T])
        scr.grad_k[...] = jnp.zeros_like(scr.grad_k)
        scr.grad_v[...] = jnp.zeros_like(scr.grad_v)

    def put(first, count, cols, value):
        for start in range(first, first + count, 16):
            where = (start // band, start // rows % side, slice(start % rows, start % rows + 16), cols)
            outs.dqkv[where] = value[start - first:start - first + 16].astype(BF16)

    def head_tile(head_index, tile_index):
        cols = slice(head_index * HEAD_DIM, (head_index + 1) * HEAD_DIM)
        reach = (tile_index + 1) * tile
        probs, queries = scores_softmax(ins.qkv, *shared[:2], head_index, tile_index, tile)
        grad_ctx = scr.grad_ctx[tile_index * tile:reach, cols]
        grad_probs = dot(ins.qkv[:reach, 3 * HEAD_DIM:], grad_ctx, NT)
        centre = jnp.sum(grad_probs * probs, axis=0, keepdims=True)
        grad_scores = (probs * (grad_probs - centre) * HEAD_DIM ** -0.5).astype(BF16)
        scr.grad_v[:reach, :] += dot(probs.astype(BF16), grad_ctx, NN)
        scr.grad_k[:reach, :] += dot(grad_scores, queries, NN)
        put(tile_index * tile, tile, cols, dot(shared[K2][:, :reach], grad_scores, NN).T)

    def end():
        for index, ref in ((2, scr.grad_k), (3, scr.grad_v)):
            put(0, side * band, slice(index * HEAD_DIM, (index + 1) * HEAD_DIM), ref[...])

    call = functools.partial
    tiles = [call(head_tile, head_index, tile_index) for head_index in PAIR for tile_index in range(side * band // tile)]
    return [call(context, index) for index in range(side)] + [begin] + tiles + [end]


def sum_input(side, qkv, seg_ids, w_outs, w_qs, w_k, w_v, hidden, second, gain, mlp, w_downs):
    seq, depth = qkv.shape
    width = gain.shape[K1]
    rows = seq // (side * side)
    head = depth // 4
    half_side = side // 2
    tokens = seq // 2
    kv_width = w_k.shape[K1]
    per_kv = 2 * side * side * head // kv_width

    def body(ins, outs, scr, staging):
        torus = Torus(side)
        kv_col = pl.multiple_of(lax.div(torus.chip * 2, per_kv) * head, head)
        weights = Weights([*ins.w_qs, ins.w_k.at[:, pl.ds(kv_col, head)], ins.w_v.at[:, pl.ds(kv_col, head)]], scr.w, scr.w_sem, True)
        weights.start()
        weights_p = Weights(ins.w_downs, scr.wd, scr.wd_sem, False)
        weights_p.start()
        wait = torus.signal_all()
        part = scr.sum.part
        attention = attention_backward(side, ins, outs, scr)
        steps_p = ReduceScatter(torus, scr.sum_p).slow_steps(fill_partial(torus, scr.sum_p.part, ins.acts, weights_p))
        steps = ReduceScatter(torus, scr.sum).steps(fill_partial(torus, part, [outs.dqkv], weights))
        own = (torus.y, torus.x)
        gat = scr.all.gat
        gather = AllGather(torus, scr.all, True)

        def places(where, colour, half):
            chip = where[K0] * side + where[K1]
            tokens_at = pl.ds(pl.multiple_of(lax.rem(chip, 2) * tokens + colour * (tokens // 2), tokens // 2), tokens // 2)
            at = lax.div(chip, 2) * head
            src = gather.piece(gat, where, colour * 2, 2)
            return [(src.at[:, pl.ds(index * head, head)], outs.kv.at[half, tokens_at, pl.ds(pl.multiple_of(at + index * kv_width, head), head)]) for index in PAIR]

        gather.store = Store(torus, scr.all, places)
        rows_at = pl.ds(pl.multiple_of(torus.chip * rows, rows), rows)
        x_load = pltpu.make_async_copy(ins.hidden.at[torus.core, rows_at, :], scr.x_rows, scr.x_sem.at[K0])
        x_load.start()
        place = lax.rem(torus.x, 2)
        mate = torus.at_chip(torus.y, torus.x + 1 - 2 * place)
        kv_cols = pl.ds(2 * head, 2 * head)

        def mate_add():
            torus.arrive(scr.mate, scr.mate_sems, 0)
            mine = outs.dqkv[pl.ds(place * half_side, half_side), :, :, kv_cols]
            gat[own] = (mine.astype(F32) + scr.mate[...].astype(F32)).astype(BF16).reshape(tokens, 2 * head)

        staging.wait()
        steps_p[K0]()
        wait()
        sent, ringed = 5, 15
        run(steps_p[1:sent])
        run(attention, steps_p[sent:ringed])
        staging.save(outs.dqkv)
        steps[K0]()
        swaps = [(outs.dqkv.at[:, :, :, pl.ds(head, head)], outs.q_other)]
        swap_start(torus, scr.swap_sems, swaps)
        torus.send(outs.dqkv.at[pl.ds((1 - place) * half_side, half_side), :, :, kv_cols], scr.mate, scr.mate_sems, 0, mate)
        for step in steps[1:5]:
            step()
        mate_add()
        run(steps[5:], gather.steps(), steps_p[ringed:])
        x_load.wait()
        gain_total = jnp.zeros((1, width), F32)
        for at in row_tiles(rows):
            back, gain_part = rms_back(scr.x_rows[at, :].astype(F32), ins.gain[...], part[(*own, at, slice(None))].astype(F32))
            gain_total = gain_total + gain_part
            outs.rows[at, :] = (ins.d_rows[at, :] + back).astype(BF16)
            y_at = pl.ds(rows + at.start, at.size)
            outs.rows[y_at, :] = (ins.h_rows[at, :].astype(F32) + scr.sum_p.part[(*own, at, slice(None))].astype(F32)).astype(BF16)
        row = lax.broadcasted_iota(jnp.int32, (8, width), 0)
        extra = jnp.zeros((8, width), F32)
        for index, value in enumerate((gain_total, ins.gain_mlp[...])):
            for level in range(3):
                rounded = value.astype(BF16).astype(F32)
                extra = jnp.where(row == index * 3 + level, rounded, extra)
                value = value - rounded
        outs.rows[2 * rows:2 * rows + 8, :] = extra.astype(BF16)
        staging.save(outs.rows)
        gather.store.drain()
        swap_end(torus, scr.swap_sems, swaps)
        torus.drain()

    dma = pltpu.SemaphoreType.DMA
    ins = dict(qkv=(qkv, VMEM), seg=(seg_ids, VMEM), resid=(second.own, ANY), w_outs=[(weight, ANY) for weight in w_outs], acts=[(act, VMEM) for act in mlp.acts], w_downs=[(weight, ANY) for weight in w_downs], h_rows=(mlp.h_rows, VMEM), w_qs=[(weight, ANY) for weight in w_qs], w_k=(w_k, ANY), w_v=(w_v, ANY), hidden=(hidden, ANY), d_rows=(second.d_rows, VMEM),
               gain=(gain, VMEM), gain_mlp=(second.gain, VMEM))
    outs = dict(rows=(shape((2 * rows + 8, width)), VMEM), kv=(shape((2, seq, 2 * kv_width)), ANY), q_other=(shape((side, side, rows, head)), ANY), dqkv=(shape((side, side, rows, depth)), VMEM))
    scratch = dict(w_out=pltpu.VMEM((2 * head, width), BF16), grad_ctx=pltpu.VMEM((seq, 2 * head), BF16), grad_k=pltpu.VMEM((seq, head), F32), grad_v=pltpu.VMEM((seq, head), F32), w_out_sem=dma((K2,)), resid_sem=dma((side,)), sum_p=rs_scratch(side, rows, width), wd=pltpu.VMEM((2 * mlp.acts[K0].shape[K3], width), BF16), wd_sem=dma((K2, K2)),
                   sum=rs_scratch(side, rows, width), all=ag_scratch(side, tokens, 2 * head, 2), x_rows=pltpu.VMEM((rows, width), BF16), x_sem=dma((K1,)), w=pltpu.VMEM((width, depth), BF16), w_sem=dma((K2, 4)),
                   mate=pltpu.VMEM((half_side, side, rows, 2 * head), BF16), mate_sems=[dma((K1,)), dma((K1,))], swap_sems=[dma((K1,)), dma((K1,))])
    return call_kernel('sum_input', body, ins, outs, scratch, 3e8, 3)


def scores_softmax(qkv, seg_row, seg_col, head_index, tile_index, tile):
    reach = (tile_index + 1) * tile
    queries = qkv[tile_index * tile:reach, head_index * HEAD_DIM:(head_index + 1) * HEAD_DIM]
    scores = dot(qkv[:reach, 2 * HEAD_DIM:3 * HEAD_DIM], queries, NT) * HEAD_DIM ** -0.5
    key_at = lax.broadcasted_iota(jnp.int32, (reach, tile), 0)
    query_at = lax.broadcasted_iota(jnp.int32, (reach, tile), 1) + tile_index * tile
    allowed = (key_at <= query_at) & (seg_col[:reach, :] == seg_row[:, tile_index * tile:reach])
    scores = jnp.where(allowed, scores, -1e30)
    weights = jnp.exp(scores - jnp.max(scores, axis=0, keepdims=True))
    return weights * (1.0 / jnp.sum(weights, axis=0, keepdims=True)), queries


def segments(seg_ref):
    core = lax.rem(lax.axis_index('tp'), 2)
    seg_row = seg_ref[pl.ds(core, 1), :].astype(F32)
    return seg_row, jnp.broadcast_to(seg_row, (8, seg_row.shape[K1])).T[:, :1]


def attention_forward(hidden, seg_ids, gain, w_q, w_k, w_v, w_o, per_kv):
    seq, width = hidden.shape[1:]
    chunk = seq // 4
    group = 64
    tile = min(256, seq)
    depth = 4 * HEAD_DIM

    def body(ins, outs, scr, staging):
        tp_idx = lax.axis_index('tp')
        core = lax.rem(tp_idx, 2)
        kv_col = pl.multiple_of(lax.div(tp_idx, per_kv) * HEAD_DIM, HEAD_DIM)
        partner = dict(tp=tp_idx + 1 - 2 * core)
        barrier = pltpu.get_barrier_semaphore()
        pl.semaphore_signal(barrier, inc=1, device_id=partner, device_id_type=MESH)
        loads = []
        for index in range(4):
            at = pl.ds(index * chunk, chunk)
            loads.append(pltpu.make_async_copy(ins.hidden.at[core, at, :], scr.x.at[at, :], scr.x_sem.at[index]))

        def w_cols(index):
            return scr.w.at[:, pl.ds(index * HEAD_DIM, HEAD_DIM)]

        for index, ref in ((0, ins.w_q), (2, ins.w_k.at[:, pl.ds(kv_col, HEAD_DIM)]), (3, ins.w_v.at[:, pl.ds(kv_col, HEAD_DIM)])):
            loads.append(pltpu.make_async_copy(ref, w_cols(index), scr.w_sem.at[index]))
        for load in loads:
            load.start()
        pl.semaphore_wait(barrier, 1)
        swaps = [(ins.w_q, w_cols(1)), (ins.w_o, outs.w_o), (ins.w_q, outs.w_q)]
        copies = []
        for index, (src, dst) in enumerate(swaps):
            copies.append(pltpu.make_async_remote_copy(src, dst, scr.swap_sems[K0].at[index], scr.swap_sems[K1].at[index], device_id=partner, device_id_type=MESH))
            copies[index].start()
        stores = []
        for index in range(4):
            loads[index].wait()

            if index == 0:
                staging.wait()

            def square(step, carry, index=index):
                at = pl.ds(pl.multiple_of(index * chunk + step * group, group), group)
                total = jnp.zeros((group, HEAD_DIM), F32)
                for lane in range(0, width, HEAD_DIM):
                    value = scr.x[at, lane:lane + HEAD_DIM].astype(F32)
                    total = total + value * value
                scr.squares[pl.ds(pl.multiple_of(step * group, group), group), :] = total
                return carry

            lax.fori_loop(0, chunk // group, square, 0)
            inv = lax.rsqrt(jnp.sum(scr.squares[...], axis=-1, keepdims=True) / width + EPS)
            scr.squares[...] = jnp.broadcast_to(inv, scr.squares.shape)

            def normalize(step, carry, index=index):
                at = pl.ds(pl.multiple_of(index * chunk + step * group, group), group)
                scale = scr.squares[pl.ds(pl.multiple_of(step * group, group), group), :]
                for lane in range(0, width, HEAD_DIM):
                    cols = slice(lane, lane + HEAD_DIM)
                    scr.normed[at, cols] = (scr.x[at, cols].astype(F32) * scale * ins.gain[:, cols]).astype(BF16)
                return carry

            lax.fori_loop(0, chunk // group, normalize, 0)
            at = pl.ds(index * chunk, chunk)
            store = pltpu.make_async_copy(scr.normed.at[at, :], outs.normed.at[at, :], scr.out_sem.at[index])
            store.start()
            stores.append(store)
            if index == 0:
                for load in loads[4:]:
                    load.wait()
                copies[K0].wait_recv()
            outs.qkv[at, :] = dot(scr.normed[at, :], scr.w[...], NN).astype(BF16)
        staging.save(outs.qkv)
        seg_row, seg_col = segments(ins.seg)
        values_t = outs.qkv[:, 3 * HEAD_DIM:].T
        for head_index in PAIR:
            for tile_index in range(seq // tile):
                probs, _ = scores_softmax(outs.qkv, seg_row, seg_col, head_index, tile_index, tile)
                ctx_t = dot(values_t[:, :(tile_index + 1) * tile], probs.astype(BF16), NN)
                outs.ctx[tile_index * tile:(tile_index + 1) * tile, head_index * HEAD_DIM:(head_index + 1) * HEAD_DIM] = ctx_t.T.astype(BF16)
        for store in stores:
            store.wait()
        copies[K0].wait_send()
        copies[K1].wait()
        copies[K2].wait()

    dma = pltpu.SemaphoreType.DMA
    ins = dict(hidden=(hidden, ANY), seg=(seg_ids, VMEM), gain=(gain, VMEM), w_q=(w_q, ANY), w_o=(w_o, ANY), w_k=(w_k, ANY), w_v=(w_v, ANY))
    outs = dict(normed=(shape((seq, width)), ANY), qkv=(shape((seq, depth)), VMEM), ctx=(shape((seq, 2 * HEAD_DIM)), VMEM), w_q=(shape(w_q.shape), ANY), w_o=(shape(w_o.shape), ANY))
    scratch = dict(squares=pltpu.VMEM((chunk, HEAD_DIM), F32), swap_sems=[dma((K3,)), dma((K3,))], x=pltpu.VMEM((seq, width), BF16), normed=pltpu.VMEM((seq, width), BF16), w=pltpu.VMEM((width, depth), BF16), x_sem=dma((4,)), w_sem=dma((4,)), out_sem=dma((4,)))
    return call_kernel('attention_forward', body, ins, outs, scratch, 5e9, 4)


def weight_grads(name, groups, ctxs, tokens=()):
    seq, width = groups[K0][K1].shape[1:]
    head = ctxs[K1].shape[K1] if ctxs else 0
    tile = min(512, width)
    lefts = [left for left, _ in groups if left is not None]
    sizes = [head if left is None else left.shape[K0] for left, _ in groups]
    given = len(groups) + len(lefts) + len(ctxs)

    def kernel(*refs):
        rights, left_refs = refs[:len(groups)], list(refs[len(groups):len(groups) + len(lefts)])
        outs = refs[given + len(tokens):given + len(tokens) + len(groups)]
        if ctxs:
            core = lax.rem(lax.axis_index('tp'), 2)
            ctx_t = refs[-1]

            @pl.when(pl.program_id(0) == 0)
            def _():
                for half, ref in zip((core, 1 - core), refs[given - 2:given]):
                    ctx_t[:, pl.ds(pl.multiple_of(half * seq, seq), seq)] = ref[:, :head].T

        for (left, _), right, out in zip(groups, rights, outs):
            ref = ctx_t if left is None else left_refs.pop(0)
            out[...] = dot(ref[...], right[...].reshape(2 * seq, tile), NN)

    slab = pl.BlockSpec((2, seq, tile), lambda step: (0, 0, step))
    return pl.pallas_call(
        kernel,
        name=name,
        grid=(width // tile,),
        out_shape=[shape((size, width), F32) for size in sizes],
        in_specs=[slab] * len(groups) + [VMEM] * (len(lefts) + len(ctxs)) + [ANY] * len(tokens),
        out_specs=[pl.BlockSpec((size, tile), lambda step: (0, step)) for size in sizes],
        scratch_shapes=[pltpu.VMEM((head, 2 * seq), BF16)] if ctxs else [],
        compiler_params=pltpu.CompilerParams(vmem_limit_bytes=LIMIT),
        cost_estimate=pl.CostEstimate(flops=int(1e10), bytes_accessed=int(4e7), transcendentals=0),
    )(*[right for _, right in groups], *lefts, *ctxs, *tokens)


def weight_grads_pair(left_gate, left_up, mixed_full, token):
    seq, width = mixed_full.shape[1:]
    depth = left_gate.shape[K0]
    tile = min(512, width)

    def kernel(m_ref, gate_ref, up_ref, _, out_gate, out_up):
        mixed = m_ref[...].reshape(2 * seq, tile)
        out_gate[...] = dot(gate_ref[...], mixed, NN)
        out_up[...] = dot(up_ref[...], mixed, NN)

    out = pl.BlockSpec((depth, tile), lambda step: (0, step))
    return pl.pallas_call(
        kernel,
        name='weight_grads_pair',
        grid=(width // tile,),
        out_shape=[shape((depth, width), F32)] * 2,
        in_specs=[pl.BlockSpec((2, seq, tile), lambda step: (0, 0, step)), VMEM, VMEM, ANY],
        out_specs=[out, out],
        compiler_params=pltpu.CompilerParams(vmem_limit_bytes=LIMIT),
        cost_estimate=pl.CostEstimate(flops=int(1e10), bytes_accessed=int(4e7), transcendentals=0),
    )(mixed_full, left_gate, left_up, token)


def weight_grads_qkv(normeds, kv_full, grads_q):
    seq, width = normeds[K0].shape
    head = grads_q[K1].shape[K1]
    kv_width = kv_full.shape[K2] // 2
    tile = min(512, width)

    def kernel(a_own, a_other, kv_ref, q_own, q_other, out_q, out_k, out_v, left, q_both):
        core = lax.rem(lax.axis_index('tp'), 2)
        halves = [pl.ds(pl.multiple_of(half * seq, seq), seq) for half in (core, 1 - core)]

        @pl.when(pl.program_id(0) == 0)
        def _():
            q_both[halves[K0], :] = q_own[:, :head]
            q_both[halves[K1], :] = q_other[...]

        left[:, halves[K0]] = a_own[...].T
        left[:, halves[K1]] = a_other[...].T
        out_q[...] = dot(left[...], q_both[...], NN)
        for index, out in enumerate((out_k, out_v)):
            right = kv_ref[:, :, pl.ds(index * kv_width, kv_width)].reshape(2 * seq, kv_width)
            out[...] = dot(left[...], right, NN)

    slab = pl.BlockSpec((seq, tile), lambda step: (0, step))
    out = lambda size: pl.BlockSpec((tile, size), lambda step: (step, 0))
    return pl.pallas_call(
        kernel,
        name='weight_grads_qkv',
        grid=(width // tile,),
        out_shape=[shape((width, size), F32) for size in (head, kv_width, kv_width)],
        in_specs=[slab] * 2 + [VMEM] * 3,
        out_specs=[out(size) for size in (head, kv_width, kv_width)],
        scratch_shapes=[pltpu.VMEM((tile, 2 * seq), BF16), pltpu.VMEM((2 * seq, head), BF16)],
        compiler_params=pltpu.CompilerParams(vmem_limit_bytes=LIMIT),
        cost_estimate=pl.CostEstimate(flops=int(27e9), bytes_accessed=int(6e7), transcendentals=0),
    )(*normeds, kv_full, *grads_q)


def in_place(gathered, rows):
    blocks, _, width = gathered.shape
    slots = pieces = 2 * blocks

    def kernel(src, dx_ref, y_ref, gain_attn, gain_mlp, buf, extra, in_sem, out_sem, extra_sem):
        gains = pltpu.make_async_copy(src.at[:, pl.ds(2 * rows, 8), :], extra, extra_sem.at[K0])

        def load(index):
            at = pl.ds(index // blocks * rows, rows)
            return pltpu.make_async_copy(src.at[index % blocks, at, :], buf.at[index % slots], in_sem.at[index % slots])

        def store(index):
            dst, block = (dx_ref, y_ref)[index // blocks], index % blocks
            return pltpu.make_async_copy(buf.at[index % slots], dst.at[block % 2, block // 2], out_sem.at[index % slots])

        ahead = slots // 2
        for index in range(pieces + ahead):
            if index < pieces:
                if index >= slots:
                    store(index - slots).wait()
                load(index).start()
            if index == ahead:
                gains.start()
            if index >= ahead:
                load(index - ahead).wait()
                store(index - ahead).start()
        gains.wait()
        total = jnp.sum(extra[...].astype(F32), axis=0)
        for first, ref in ((0, gain_attn), (3, gain_mlp)):
            ref[...] = total[first:first + 1] + total[first + 1:first + 2] + total[first + 2:first + 3]
        for index in range(pieces - slots, pieces):
            store(index).wait()

    dma = pltpu.SemaphoreType.DMA
    whole = shape((2, blocks // 2, rows, width))
    return pl.pallas_call(
        kernel,
        name='in_place',
        out_shape=[whole, whole, shape((1, width), F32), shape((1, width), F32)],
        in_specs=[ANY],
        out_specs=[ANY, ANY, VMEM, VMEM],
        scratch_shapes=[pltpu.VMEM((slots, rows, width), BF16), pltpu.VMEM((blocks, 8, width), BF16), dma((slots,)), dma((slots,)), dma((K1,))],
        compiler_params=pltpu.CompilerParams(vmem_limit_bytes=LIMIT),
        cost_estimate=pl.CostEstimate(flops=int(2e7), bytes_accessed=int(2e7), transcendentals=0),
    )(gathered)


def solution(mesh):
    tp_size = mesh.shape['tp']
    chips = tp_size // 2
    side = math.isqrt(chips)

    def device_step(hidden, seg_ids, grad_out, gain_attn, gain_mlp, w_q, w_k, w_v, w_o, w_gate, w_up, w_down):
        seq_len, width = hidden.shape[1:]
        kv_heads = w_k.shape[K1] // HEAD_DIM
        per_kv = tp_size // kv_heads
        rows = seq_len // chips

        def flat(value):
            return value.reshape(seq_len, value.shape[-1])

        gain_attn_row = gain_attn[None, :]
        gain_mlp_row = gain_mlp[None, :]

        attn = attention_forward(hidden, seg_ids, gain_attn_row, w_q, w_k, w_v, w_o, per_kv)
        w_qs, w_outs = (w_q, attn.w_q), (w_o, attn.w_o)
        mlp = sum_attention(side, attn, w_outs, hidden, grad_out, gain_mlp_row, w_gate.T, w_up.T, w_down)
        mixed_full = mlp.full.reshape(2, seq_len, width)
        second = sum_mlp(side, mlp, (w_gate.T, mlp.w_gate), (w_up.T, mlp.w_up), grad_out, gain_mlp_row)
        resid_full = second.full.reshape(2, seq_len, width)

        third = sum_input(side, attn.qkv, seg_ids, w_outs, w_qs, w_k, w_v, hidden, second, gain_attn_row, mlp, (w_down, mlp.w_down))

        grad_in, y_out, grad_gain_attn, grad_gain_mlp = in_place(lax.all_gather(third.rows, 'tp'), rows)
        left_gate, left_up, left_act = second.lefts
        grad_gate_t, grad_up_t = weight_grads_pair(left_gate, left_up, mixed_full, third.q_other)
        grad_w_down, grad_w_o = weight_grads('weight_grads_down', [(left_act, grad_out), (None, resid_full)], (attn.ctx, flat(mlp.ctx_other)), (third.q_other,))
        grad_w_q, grad_w_k, grad_w_v = weight_grads_qkv((attn.normed, mlp.normed_other), third.kv, (flat(third.dqkv), flat(third.q_other)))
        return (y_out.reshape(hidden.shape), grad_in.reshape(hidden.shape), grad_gain_attn[K0], grad_gain_mlp[K0], grad_w_q, grad_w_k, grad_w_v, grad_w_o, grad_gate_t.T, grad_up_t.T, grad_w_down)

    spec_act = P('data', None, None)
    spec_rows = P('data', None)
    spec_gain = P(None)
    spec_cols = P(None, 'tp')
    spec_tprows = P('tp', None)
    spec_whole = P(None, None)
    spec_stack = P(('data', 'tp'), None)
    in_specs = (spec_act, spec_rows, spec_act, spec_gain, spec_gain, spec_cols, spec_whole, spec_whole, spec_tprows, spec_cols, spec_cols, spec_tprows)
    out_specs = (spec_act, spec_act, P('data'), P('data'), P('data', 'tp'), spec_rows, spec_rows, spec_stack, P('data', 'tp'), P('data', 'tp'), spec_stack)
    return jax.shard_map(device_step, mesh=mesh, in_specs=in_specs, out_specs=out_specs, check_vma=False)
```

```python
import functools
import math
import types
import jax
import jax.numpy as jnp
from jax import lax
from jax.experimental import pallas as pl
from jax.experimental.pallas import tpu as pltpu
from jax.sharding import PartitionSpec as P

HEAD_DIM = 128
EPS = 1e-5
MESH = pl.DeviceIdType.MESH
F32 = jnp.float32
BF16 = jnp.bfloat16
LIMIT = 63 * 2 ** 20
K0, K1, K2, K3 = range(4)
PAIR = range(2)
ANY = pl.BlockSpec(memory_space=pl.ANY)
VMEM = pl.BlockSpec(memory_space=pltpu.VMEM)


def dot(lhs, rhs, dims):
    return lax.dot_general(lhs, rhs, (dims, ((), ())), preferred_element_type=F32)


NN = ((1,), (0,))
NT = ((1,), (1,))


SIGNS = (1, -1)


class Colour:
    def __init__(self, index, first, second):
        self.index, self.first, self.second = index, first, second


class Torus:
    def __init__(self, side):
        self.side = side
        tp_idx = lax.axis_index('tp')
        self.core = lax.rem(tp_idx, 2)
        self.chip = lax.div(tp_idx, 2)
        self.x = lax.rem(self.chip, side)
        self.y = lax.div(self.chip, side)
        self.partner = {'tp': self.chip * 2 + (1 - self.core)}
        self.colours = (Colour(0, self.x, self.y), Colour(1, self.y, self.x))
        self.pending = []

    def wrap(self, pos):
        return lax.rem(pos + 2 * self.side, self.side)

    def at_chip(self, y_at, x_at):
        return {'tp': (y_at * self.side + x_at) * 2 + self.core}

    def block(self, col, second, first):
        return (second, first) if col.index == 0 else (first, second)

    def peer1(self, col, shift):
        return self.at_chip(*self.block(col, col.second, self.wrap(col.first + shift)))

    def peer2(self, col, shift):
        return self.at_chip(*self.block(col, self.wrap(col.second + shift), col.first))

    def signal_all(self):
        barrier = pltpu.get_barrier_semaphore()
        peers = [self.partner]
        peers += [self.at_chip(self.y, self.wrap(self.x + shift)) for shift in SIGNS]
        peers += [self.at_chip(self.wrap(self.y + shift), self.x) for shift in SIGNS]
        for peer in peers:
            pl.semaphore_signal(barrier, inc=1, device_id=peer, device_id_type=MESH)
        return lambda: pl.semaphore_wait(barrier, len(peers))

    def send(self, src, dst, sems, index, device):
        copy = pltpu.make_async_remote_copy(src, dst, sems[K0].at[index], sems[K1].at[index], device_id=device, device_id_type=MESH)
        copy.start()
        self.pending.append(copy)

    def arrive(self, dst, sems, index):
        pltpu.make_async_remote_copy(dst, dst, sems[K0].at[index], sems[K1].at[index], device_id=self.partner, device_id_type=MESH).wait_recv()

    def drain(self):
        for copy in self.pending:
            copy.wait_send()


R1, R2, R3, S1, S2, S3 = range(6)
RS_COUNTS = (16, 16, 16, 4, 4, 4)
H1, H2, F1, F2 = range(4)
AG_COUNTS = (8, 32, 4, 16)


class ReduceScatter:
    SHIFTS = (2, 1, 3, 0)

    def __init__(self, torus, scr):
        self.torus, self.part, self.scr = torus, scr.part, scr
        self.quarter = scr.part.shape[K3] // 4

    def buf(self, kind, index):
        return self.scr.bufs[kind].at[index]

    def sems(self, kind):
        return self.scr.out_sems[kind], self.scr.in_sems[kind]

    def cols(self, col, half):
        return pl.ds((col.index * 2 + half) * self.quarter, self.quarter)

    def piece(self, where, at_cols):
        return self.part.at[(*where, slice(None), at_cols)]

    def send(self, where, at_cols, kind, index, peer):
        self.torus.send(self.piece(where, at_cols), self.buf(kind, index), self.sems(kind), index, peer)

    def add(self, where, at_cols, *kinds):
        total = self.part[(*where, slice(None), at_cols)].astype(F32)
        for kind, index in kinds:
            self.torus.arrive(self.buf(kind, index), self.sems(kind), index)
            total = total + self.buf(kind, index)[...].astype(F32)
        self.part[(*where, slice(None), at_cols)] = total.astype(BF16)

    def each(self, step):
        wrap = self.torus.wrap
        for col in self.torus.colours:
            second = wrap(col.second + self.SHIFTS[step])
            for way, sign in enumerate(SIGNS):
                yield col, second, way, sign, (col.index * 2 + way) * 4 + step

    def far(self, step):
        for col, second, way, sign, index in self.each(step):
            where = self.torus.block(col, second, self.torus.wrap(col.first + 2))
            self.send(where, self.cols(col, way), R1, index, self.torus.peer1(col, sign))

    def near(self, step):
        for col, second, way, sign, index in self.each(step):
            where = self.torus.block(col, second, self.torus.wrap(col.first + sign))
            self.send(where, self.cols(col, 1 - way), R2, index, self.torus.peer1(col, sign))

    def relay(self, step):
        for col, second, way, sign, index in self.each(step):
            where = self.torus.block(col, second, self.torus.wrap(col.first + sign))
            self.add(where, self.cols(col, way), (R1, index))
            self.send(where, self.cols(col, way), R3, index, self.torus.peer1(col, sign))

    def end(self, step):
        for col, second, way, sign, index in self.each(step):
            where = self.torus.block(col, second, col.first)
            other = (col.index * 2 + 1 - way) * 4 + step
            self.add(where, self.cols(col, way), (R2, other), (R3, index))

    def far2(self):
        for col in self.torus.colours:
            for way, sign in enumerate(SIGNS):
                where = self.torus.block(col, self.torus.wrap(col.second + 2), col.first)
                self.send(where, self.cols(col, way), S1, col.index * 2 + way, self.torus.peer2(col, sign))

    def near2(self, way):
        for col in self.torus.colours:
            where = self.torus.block(col, self.torus.wrap(col.second + SIGNS[way]), col.first)
            self.send(where, self.cols(col, 1 - way), S2, col.index * 2 + way, self.torus.peer2(col, SIGNS[way]))

    def relay2(self, way):
        for col in self.torus.colours:
            index = col.index * 2 + way
            where = self.torus.block(col, self.torus.wrap(col.second + SIGNS[way]), col.first)
            self.add(where, self.cols(col, way), (S1, index))
            self.send(where, self.cols(col, way), S3, index, self.torus.peer2(col, SIGNS[way]))

    def end2(self):
        for col in self.torus.colours:
            where = self.torus.block(col, col.second, col.first)
            for way in PAIR:
                self.add(where, self.cols(col, way), (S2, col.index * 2 + 1 - way), (S3, col.index * 2 + way))

    def steps(self, fill):
        call = functools.partial
        return [call(fill, K2), call(self.far, K0), call(self.far, K1), call(fill, K1), call(fill, K3),
                call(self.near, K0), call(self.relay, K0), call(self.near, K1), call(self.far, K2), call(self.relay, K1),
                call(fill, K0), call(self.near, K2), call(self.far, K3), call(self.end, K0), self.far2,
                call(self.relay, K2), call(self.near, K3), call(self.end, K1), call(self.near2, K0), call(self.relay2, K0),
                call(self.relay, K3), call(self.end, K2), call(self.near2, K1), call(self.relay2, K1), call(self.end, K3),
                self.end2]

    def slow_steps(self, fill):
        call = functools.partial
        steps = range(self.torus.side)
        result = [call(fill, K2)] + [call(self.far, step) for step in steps] + [call(fill, K1), call(fill, K3)]
        for step in steps:
            result += [call(self.near, step), call(self.relay, step)]
        return result + [call(fill, K0), call(self.end, K0), self.far2, call(self.end, K1), call(self.near2, K0), call(self.relay2, K0),
                         call(self.end, K2), call(self.near2, K1), call(self.relay2, K1), call(self.end, K3), self.end2]


class AllGather:
    def __init__(self, torus, scr, by_rows):
        self.torus, self.gat, self.scr, self.by_rows, self.store = torus, scr.gat, scr, by_rows, None
        self.quarter = scr.gat.shape[2 if by_rows else 3] // 4
        self.back = (0, torus.side - 1, 1, 2)

    def sems(self, kind):
        return self.scr.out_sems[kind], self.scr.in_sems[kind]

    def piece(self, ref, where, first, count):
        at = pl.ds(first * self.quarter, count * self.quarter)
        return ref.at[(*where, at, slice(None))] if self.by_rows else ref.at[(*where, slice(None), at)]

    def half(self, col, where, half):
        return self.piece(self.gat, where, col.index * 2 + half, 1)

    def own2(self, turn):
        for col in self.torus.colours:
            where = self.torus.block(col, col.second, col.first)
            for way, sign in enumerate(SIGNS):
                at = self.half(col, where, way if turn == 0 else 1 - way)
                self.torus.send(at, at, self.sems(H1), (col.index * 2 + way) * 2 + turn, self.torus.peer2(col, sign))

    def send1(self, step, turn):
        for col in self.torus.colours:
            where = self.torus.block(col, self.torus.wrap(col.second + self.back[step]), col.first)
            for way, sign in enumerate(SIGNS):
                at = self.half(col, where, way if turn == 0 else 1 - way)
                self.torus.send(at, at, self.sems(H2), ((col.index * 2 + way) * 4 + step) * 2 + turn, self.torus.peer1(col, sign))

    def arrive2(self, way, turn):
        sign = SIGNS[way]
        for col in self.torus.colours:
            where = self.torus.block(col, self.torus.wrap(col.second - sign), col.first)
            at = self.half(col, where, way if turn == 0 else 1 - way)
            self.torus.arrive(at, self.sems(H1), (col.index * 2 + way) * 2 + turn)
            if turn == 0:
                self.torus.send(at, at, self.sems(F1), col.index * 2 + way, self.torus.peer2(col, sign))

    def relayed2(self):
        for col in self.torus.colours:
            where = self.torus.block(col, self.torus.wrap(col.second + 2), col.first)
            for way in PAIR:
                self.torus.arrive(self.half(col, where, way), self.sems(F1), col.index * 2 + way)

    def arrive1(self, step, turn):
        for col in self.torus.colours:
            second = self.torus.wrap(col.second + self.back[step])
            for way, sign in enumerate(SIGNS):
                where = self.torus.block(col, second, self.torus.wrap(col.first - sign))
                at = self.half(col, where, way if turn == 0 else 1 - way)
                self.torus.arrive(at, self.sems(H2), ((col.index * 2 + way) * 4 + step) * 2 + turn)
                if turn == 0:
                    self.torus.send(at, at, self.sems(F2), (col.index * 2 + way) * 4 + step, self.torus.peer1(col, sign))

    def relayed1(self, step):
        for col in self.torus.colours:
            second = self.torus.wrap(col.second + self.back[step])
            for way in PAIR:
                where = self.torus.block(col, second, self.torus.wrap(col.first + 2))
                self.torus.arrive(self.half(col, where, way), self.sems(F2), (col.index * 2 + way) * 4 + step)

    def keep(self, step, firsts):
        for col in self.torus.colours:
            for shift in firsts:
                where = self.torus.block(col, self.torus.wrap(col.second + self.back[step]), self.torus.wrap(col.first + shift))
                self.store.keep(where, col.index, lambda ref, where=where, col=col: self.piece(ref, where, col.index * 2, 2))

    def steps(self, whole=None):
        call = functools.partial
        whole = whole or (lambda step: None)
        here, beside, across = (K0,), (K1, self.torus.side - 1), (K2,)

        def rest(step):
            return [call(self.arrive1, step, K1), call(self.keep, step, beside), call(self.relayed1, step), call(self.keep, step, across), call(whole, step)]

        result = []
        for turn in PAIR:
            result += [call(self.own2, turn), call(self.send1, K0, turn)]
        result += [call(self.keep, K0, here), call(self.arrive2, K0, K0), call(self.arrive2, K1, K0), call(self.arrive1, K0, K0),
                   call(self.arrive2, K0, K1), call(self.send1, K1, K0), call(self.send1, K1, K1), call(self.keep, K1, here),
                   call(self.arrive2, K1, K1), call(self.send1, K2, K0), call(self.keep, K2, here),
                   call(self.arrive1, K1, K0), call(self.send1, K2, K1), self.relayed2, call(self.send1, K3, K0), call(self.keep, K3, here)]
        result += rest(K0) + [call(self.arrive1, K2, K0), call(self.send1, K3, K1)]
        return result + rest(K1) + [call(self.arrive1, K3, K0)] + rest(K2) + rest(K3)


class Store:
    def __init__(self, torus, scr, places, own=None):
        self.torus, self.scr, self.places, self.own = torus, scr, places, own
        self.stores = []

    def slot(self, where, colour, index):
        return ((index * 2 + colour) * self.torus.side + where[K0]) * self.torus.side + where[K1]

    def keep(self, where, colour, piece):
        for index, (src, dst) in enumerate(self.places(where, colour, self.torus.core)):
            slot = self.slot(where, colour, index)
            pairs = [(self.scr.full_sem, dst)]
            if self.own is not None:
                pairs.append((self.scr.own_sem, piece(self.own)))
            for sem, ref in pairs:
                store = pltpu.make_async_copy(src, ref, sem.at[slot])
                store.start()
                self.stores.append(store)
            self.torus.send(src, dst, self.scr.cross_sems, slot, self.torus.partner)

    def drain(self):
        for store in self.stores:
            store.wait()
        side = self.torus.side
        for colour in PAIR:
            for y_at in range(side):
                for x_at in range(side):
                    for index, (_, dst) in enumerate(self.places((y_at, x_at), colour, 1 - self.torus.core)):
                        self.torus.arrive(dst, self.scr.cross_sems, self.slot((y_at, x_at), colour, index))


def plain_places(gather, full):
    return lambda where, colour, half: [(gather.piece(gather.gat, where, colour * 2, 2), gather.piece(full.at[half], where, colour * 2, 2))]


def rs_scratch(side, rows, width):
    dma = pltpu.SemaphoreType.DMA
    return dict(
        part=pltpu.VMEM((side, side, rows, width), BF16),
        bufs=[pltpu.VMEM((count, rows, width // 4), BF16) for count in RS_COUNTS],
        out_sems=[dma((count,)) for count in RS_COUNTS],
        in_sems=[dma((count,)) for count in RS_COUNTS],
    )


def ag_scratch(side, rows, width, places=1):
    dma = pltpu.SemaphoreType.DMA
    blocks = 2 * side * side * places
    return dict(
        gat=pltpu.VMEM((side, side, rows, width), BF16),
        out_sems=[dma((count,)) for count in AG_COUNTS],
        in_sems=[dma((count,)) for count in AG_COUNTS],
        full_sem=dma((blocks,)),
        own_sem=dma((blocks,)),
        cross_sems=[dma((blocks,)), dma((blocks,))],
    )


class Weights:
    def __init__(self, refs, buf, sem, by_rows):
        self.refs, self.buf, self.sem, self.by_rows = refs, buf, sem, by_rows
        self.copies = [[], []]

    def start(self):
        for colour in PAIR:
            for index, ref in enumerate(self.refs):
                if self.by_rows:
                    half, depth = ref.shape[K0] // 2, ref.shape[K1]
                    rows, cols = pl.ds(colour * half, half), pl.ds(index * depth, depth)
                    copy = pltpu.make_async_copy(ref.at[rows, :], self.buf.at[rows, cols], self.sem.at[colour, index])
                else:
                    half, depth = ref.shape[K1] // 2, ref.shape[K0]
                    rows, cols = pl.ds(index * depth, depth), pl.ds(colour * half, half)
                    copy = pltpu.make_async_copy(ref.at[:, cols], self.buf.at[rows, cols], self.sem.at[colour, index])
                copy.start()
                self.copies[colour].append(copy)

    def wait(self, colour):
        for copy in self.copies[colour]:
            copy.wait()
        self.copies[colour] = []


def fill_partial(torus, part, lhs, weights):
    rows, width = part.shape[2:]
    tile = min(1024, width // 2)

    def fill(shift):
        for col in torus.colours:
            weights.wait(col.index)
            first = torus.wrap(col.first + shift)
            left = []
            for ref in lhs:
                depth = ref.shape[K3]
                value = ref[:, first] if col.index == 0 else ref[first]
                left.append((value.reshape(torus.side * rows, depth), depth))

            def body(step, carry, col=col, first=first, left=left):
                at = pl.ds(pl.multiple_of(col.index * (width // 2) + step * tile, tile), tile)
                total = None
                base = 0
                for value, depth in left:
                    if weights.by_rows:
                        term = dot(value, weights.buf[at, base:base + depth], NT)
                    else:
                        term = dot(value, weights.buf[base:base + depth, at], NN)
                    total = term if total is None else total + term
                    base += depth
                total = total.astype(BF16).reshape(torus.side, rows, tile)
                if col.index == 0:
                    part[:, first, :, at] = total
                else:
                    part[first, :, :, at] = total
                return carry

            lax.fori_loop(0, (width // 2) // tile, body, 0)

    return fill


def run(*lists):
    keyed = []
    for order, steps in enumerate(lists):
        keyed += [((index + 0.5) / len(steps), order, step) for index, step in enumerate(steps)]
    for _, _, step in sorted(keyed, key=lambda item: item[:2]):
        step()


def swap_start(torus, sems, pairs):
    for index, (src, dst) in enumerate(pairs):
        torus.send(src, dst, sems, index, torus.partner)


def swap_end(torus, sems, pairs, first=0):
    for index, (_, dst) in enumerate(pairs):
        if index >= first:
            torus.arrive(dst, sems, index)


def row_tiles(rows):
    return [pl.ds(start, 16) for start in range(0, rows, 16)]


def rms_back(z_in, gain, grad):
    inv = lax.rsqrt(jnp.mean(z_in * z_in, axis=-1, keepdims=True) + EPS)
    normed = z_in * inv
    scaled = grad * gain
    back = inv * (scaled - normed * jnp.mean(scaled * normed, axis=-1, keepdims=True))
    return back, jnp.sum(grad * normed, axis=0, keepdims=True)


def bag(tree):
    if isinstance(tree, dict):
        return types.SimpleNamespace(**{key: bag(value) for key, value in tree.items()})
    return [bag(value) for value in tree] if isinstance(tree, list) else tree


class Staging:
    def __init__(self, loads, saves):
        self.loads, self.saves, self.left = loads, saves, {}

    def start(self):
        for load in self.loads:
            load.start()

    def wait(self):
        for load in self.loads:
            load.wait()

    def save(self, *refs):
        for ref, save in self.saves:
            if any(ref is one for one in refs):
                save.start()
                self.left[id(ref)] = save

    def finish(self):
        self.save(*[ref for ref, _ in self.saves if id(ref) not in self.left])
        for save in self.left.values():
            save.wait()


def call_kernel(name, body, ins, outs, scratch, flops, collective_id=None):
    is_leaf = lambda value: isinstance(value, tuple)
    in_leaves, in_tree = jax.tree.flatten(ins, is_leaf=is_leaf)
    out_leaves, out_tree = jax.tree.flatten(outs, is_leaf=is_leaf)
    scr_leaves, scr_tree = jax.tree.flatten(scratch)
    first_scr = len(in_leaves) + len(out_leaves)
    staged = [index for index, leaf in enumerate(in_leaves + out_leaves) if leaf[K1] is VMEM]
    stages = []
    for index in staged:
        leaf = (in_leaves + out_leaves)[index][K0]
        stages.append(pltpu.VMEM(leaf.shape, leaf.dtype))

    def kernel(*refs):
        refs = list(refs)
        own = refs[first_scr + len(scr_leaves):]
        sem = own.pop()
        loads, saves = [], []
        for slot, (index, ref) in enumerate(zip(staged, own)):
            if index < len(in_leaves):
                loads.append(pltpu.make_async_copy(refs[index], ref, sem.at[slot]))
            else:
                saves.append((ref, pltpu.make_async_copy(ref, refs[index], sem.at[slot])))
            refs[index] = ref
        staging = Staging(loads, saves)
        staging.start()
        body(bag(in_tree.unflatten(refs[:len(in_leaves)])), bag(out_tree.unflatten(refs[len(in_leaves):first_scr])), bag(scr_tree.unflatten(refs[first_scr:first_scr + len(scr_leaves)])), staging)
        staging.finish()

    results = pl.pallas_call(
        kernel,
        name=name,
        out_shape=[leaf[K0] for leaf in out_leaves],
        in_specs=[ANY] * len(in_leaves),
        out_specs=[ANY] * len(out_leaves),
        scratch_shapes=scr_leaves + stages + [pltpu.SemaphoreType.DMA((len(staged),))],
        compiler_params=pltpu.CompilerParams(collective_id=collective_id, has_side_effects=collective_id is not None, vmem_limit_bytes=LIMIT),
        cost_estimate=pl.CostEstimate(flops=int(flops), bytes_accessed=int(4e7), transcendentals=0),
    )(*[leaf[K0] for leaf in in_leaves])
    return bag(out_tree.unflatten(results))


def shape(dims, dtype=BF16):
    return jax.ShapeDtypeStruct(dims, dtype)


def sum_attention(side, attn, w_outs, hidden, grad_out, gain, w_gate, w_up, w_down):
    seq, depth = attn.ctx.shape
    width = gain.shape[K1]
    hidden_loc = w_gate.shape[K0]
    rows = seq // (side * side)

    def body(ins, outs, scr, staging):
        torus = Torus(side)
        weights = Weights(ins.w_outs, scr.w, scr.w_sem, False)
        weights.start()
        rows_at = pl.ds(pl.multiple_of(torus.chip * rows, rows), rows)
        x_load = pltpu.make_async_copy(ins.hidden.at[torus.core, rows_at, :], scr.x_rows, scr.x_sem.at[K0])
        x_load.start()

        def load_weight(src, slot):
            load = pltpu.make_async_copy(src, scr.w_mlp.at[slot], scr.w_mlp_sem.at[slot])
            load.start()
            return load

        loads = {slot: load_weight(src, slot) for slot, src in ((K0, ins.w_down), (K2, ins.w_gate), (K3, ins.w_up))}
        wait = torus.signal_all()
        part = scr.sum.part
        steps = ReduceScatter(torus, scr.sum).steps(fill_partial(torus, part, [ins.ctx], weights))
        staging.wait()
        steps[K0]()
        wait()
        other_ctx = ins.ctx.at[:, :, :, pl.ds(depth // 2, depth // 2)]
        swaps = [(ins.w_down, outs.w_down), (ins.w_gate, outs.w_gate), (ins.w_up, outs.w_up), (other_ctx, outs.ctx_other), (ins.normed, outs.normed_other)]
        swap_start(torus, scr.swap_sems, swaps)

        def dy_load(group):
            at = pl.ds(group * side * rows, side * rows)
            return pltpu.make_async_copy(ins.grad_out.at[torus.core, at, :], scr.dy.at[group % 2], scr.dy_sem.at[group % 2])

        def grad_act(group):
            if group == 0:
                torus.arrive(outs.w_down, scr.swap_sems, 0)
                loads[K1] = load_weight(outs.w_down, K1)
                for slot in PAIR:
                    loads[slot].wait()
            dy_load(group).wait()
            for slot in PAIR:
                product = dot(scr.dy[group % 2], scr.w_mlp[slot], NT)
                scr.grad_act[slot, group] = product.reshape(side, rows, hidden_loc)
            if group + 2 < side:
                dy_load(group + 2).start()

        dy_load(0).start()
        dy_load(1).start()
        half = len(steps) // 3
        run(steps[1:half])
        run(steps[half:], [functools.partial(grad_act, group) for group in range(side)])
        for index, (slot, out) in enumerate(((K0, outs.w_gate), (K1, outs.w_up))):
            torus.arrive(out, scr.swap_sems, index + 1)
            loads[slot] = load_weight(out, slot)
        scr.pre[...] = jnp.zeros_like(scr.pre)
        gat = scr.all.gat
        own = (torus.y, torus.x)
        x_load.wait()
        for at in row_tiles(rows):
            resid = (scr.x_rows[at, :].astype(F32) + part[(*own, at, slice(None))].astype(F32)).astype(BF16)
            outs.h_rows[at, :] = resid
            z_in = resid.astype(F32)
            inv = lax.rsqrt(jnp.mean(z_in * z_in, axis=-1, keepdims=True) + EPS)
            gat[(*own, at, slice(None))] = (z_in * inv * ins.gain[...]).astype(BF16)
        staging.save(outs.h_rows)
        gather = AllGather(torus, scr.all, False)
        gather.store = Store(torus, scr.all, plain_places(gather, outs.full))

        def products(step):
            if step == 0:
                for load in (loads[slot] for slot in (K0, K1, K2, K3)):
                    load.wait()
            for col in torus.colours:
                second = torus.wrap(col.second + gather.back[step])
                at_cols = pl.ds(col.index * (width // 2), width // 2)
                mixed = gat[second, :, :, at_cols] if col.index == 0 else gat[:, second, :, at_cols]
                mixed = mixed.reshape(side * rows, width // 2)

                def body(slot, carry, col=col, second=second, at_cols=at_cols, mixed=mixed):
                    term = dot(mixed, scr.w_mlp[slot, :, at_cols], NT).reshape(side, rows, hidden_loc)
                    if col.index == 0:
                        scr.pre[slot, second] += term
                    else:
                        scr.pre[slot, :, second] += term
                    return carry

                lax.fori_loop(0, 4, body, 0)
            for inner, count in ((0, step + 1), (1, step)):

                def block(index, carry, inner=inner):
                    shift = lax.rem(3 * index + 3 * lax.div(index * (index - 1), 2), side)
                    pair = (gather.back[step], shift) if inner == 0 else (shift, gather.back[step])
                    y_at, x_at = torus.wrap(torus.y + pair[K0]), torus.wrap(torus.x + pair[K1])
                    for core in PAIR:
                        gate, upper = scr.pre[2 - 2 * core, y_at, x_at], scr.pre[3 - 2 * core, y_at, x_at]
                        grad = scr.grad_act[core, y_at, x_at]
                        sigmoid_g = 1.0 / (1.0 + jnp.exp(-gate))
                        silu_g = gate * sigmoid_g
                        scr.results[core, y_at, x_at] = (silu_g * upper).astype(BF16)
                        scr.results[2 + core, y_at, x_at] = (grad * upper * sigmoid_g * (1.0 + gate * (1.0 - sigmoid_g))).astype(BF16)
                        scr.results[4 + core, y_at, x_at] = (grad * silu_g).astype(BF16)
                    for kind, out in enumerate(outs.acts + outs.gates + outs.ups):
                        pltpu.make_async_copy(scr.results.at[kind, y_at, x_at], out.at[y_at, x_at], scr.result_sem.at[kind]).start()
                    return carry

                lax.fori_loop(0, count, block, 0)

        run(gather.steps(products))
        for kind, out in enumerate(outs.acts + outs.gates + outs.ups):
            pltpu.make_async_copy(scr.results.at[kind], out, scr.result_sem.at[kind]).wait()
        gather.store.drain()
        swap_end(torus, scr.swap_sems, swaps, 3)
        torus.drain()

    dma = pltpu.SemaphoreType.DMA
    block = (side, side, rows, hidden_loc)
    ins = dict(ctx=(attn.ctx.reshape(side, side, rows, depth), VMEM), w_outs=[(weight, ANY) for weight in w_outs], hidden=(hidden, ANY), grad_out=(grad_out, ANY), gain=(gain, VMEM),
               normed=(attn.normed, ANY), w_gate=(w_gate, ANY), w_up=(w_up, ANY), w_down=(w_down, ANY))
    out, weight = (shape(block), ANY), (shape((hidden_loc, width)), ANY)
    outs = dict(full=(shape((2, side, side, rows, width)), ANY), h_rows=(shape((rows, width)), VMEM), ctx_other=(shape((side, side, rows, depth // 2)), ANY), normed_other=(shape((seq, width)), ANY),
                w_gate=weight, w_up=weight, w_down=weight, acts=[out, out], gates=[out, out], ups=[out, out])
    scratch = dict(sum=rs_scratch(side, rows, width), all=ag_scratch(side, rows, width), w=pltpu.VMEM((depth, width), BF16), w_sem=dma((K2, K2)), swap_sems=[dma((5,)), dma((5,))],
                   x_rows=pltpu.VMEM((rows, width), BF16), x_sem=dma((K1,)), w_mlp=pltpu.VMEM((4, hidden_loc, width), BF16), w_mlp_sem=dma((4,)),
                   dy=pltpu.VMEM((2, side * rows, width), BF16), dy_sem=dma((K2,)), pre=pltpu.VMEM((4, *block), F32), grad_act=pltpu.VMEM((2, *block), F32), results=pltpu.VMEM((6, *block), BF16), result_sem=dma((6,)))
    return call_kernel('sum_attention', body, ins, outs, scratch, 4e8, 1)


def sum_mlp(side, mlp, w_gates, w_ups, grad_out, gain):
    depth = w_gates[K0].shape[K0]
    width = gain.shape[K1]
    rows = mlp.h_rows.shape[K0]
    seq = rows * side * side
    block = (side, side, rows, width)

    def body(ins, outs, scr, staging):
        torus = Torus(side)
        weights = Weights(ins.w_in, scr.w, scr.w_sem, False)
        weights.start()
        rows_at = pl.ds(pl.multiple_of(torus.chip * rows, rows), rows)
        dy_load = pltpu.make_async_copy(ins.grad_out.at[torus.core, rows_at, :], scr.dy_rows, scr.dy_sem.at[K0])
        dy_load.start()
        wait = torus.signal_all()
        steps = ReduceScatter(torus, scr.sum).slow_steps(fill_partial(torus, scr.sum.part, ins.grads, weights))
        staging.wait()
        steps[K0]()
        wait()

        turned = []

        def half_at(half):
            return pl.ds(pl.multiple_of(half * seq, seq), seq)

        def turn(index):
            kind, core = index // 2, index % 2
            src = (ins.grads[2 * core], ins.grads[2 * core + 1], ins.acts[core])[kind]
            slot = index % 2
            if index >= 2:
                turned[index - 2]()
            scr.turn[slot] = src[...].reshape(seq, depth).T
            at = slice(None), half_at(torus.core)
            if core == 0:
                save = pltpu.make_async_copy(scr.turn.at[slot], outs.lefts[kind].at[at], scr.turn_sem.at[kind])
                save.start()
                turned.append(save.wait)
            else:
                torus.send(scr.turn.at[slot], outs.lefts[kind].at[at], scr.swap_sems, kind, torus.partner)
                turned.append(torus.pending.pop().wait_send)

        turns = [functools.partial(turn, index) for index in range(6)]
        run(steps[1:])
        own = (torus.y, torus.x)
        gain_total = jnp.zeros((1, width), F32)
        gat = scr.all.gat
        dy_load.wait()
        for at in row_tiles(rows):
            back, gain_part = rms_back(ins.h_rows[at, :].astype(F32), ins.gain[...], scr.sum.part[(*own, at, slice(None))].astype(F32))
            gain_total = gain_total + gain_part
            total = scr.dy_rows[at, :].astype(F32) + back
            outs.d_rows[at, :] = total
            gat[(*own, at, slice(None))] = total.astype(BF16)
        outs.gain[...] = gain_total
        staging.save(outs.d_rows, outs.gain)
        gather = AllGather(torus, scr.all, False)
        gather.store = Store(torus, scr.all, plain_places(gather, outs.full), outs.own)
        run(gather.steps(), turns)
        turned[4]()
        turned[5]()
        for kind in range(3):
            torus.arrive(outs.lefts[kind].at[:, half_at(1 - torus.core)], scr.swap_sems, kind)
        gather.store.drain()
        torus.drain()

    dma = pltpu.SemaphoreType.DMA
    ins = dict(grads=[(grad, VMEM) for grad in (mlp.gates[K0], mlp.ups[K0], mlp.gates[K1], mlp.ups[K1])], acts=[(act, VMEM) for act in mlp.acts],
               w_in=[(weight, ANY) for weight in (w_gates[K0], w_ups[K0], w_gates[K1], w_ups[K1])],
               h_rows=(mlp.h_rows, VMEM), grad_out=(grad_out, ANY), gain=(gain, VMEM))
    outs = dict(full=(shape((2, *block)), ANY), own=(shape(block), ANY), d_rows=(shape((rows, width), F32), VMEM), gain=(shape((1, width), F32), VMEM), lefts=[(shape((depth, 2 * seq)), ANY)] * 3)
    scratch = dict(sum=rs_scratch(side, rows, width), all=ag_scratch(side, rows, width), dy_rows=pltpu.VMEM((rows, width), BF16), dy_sem=dma((K1,)),
                   w=pltpu.VMEM((4 * depth, width), BF16), w_sem=dma((K2, 4)),
                   turn=pltpu.VMEM((2, depth, seq), BF16), turn_sem=dma((K3,)), swap_sems=[dma((K3,)), dma((K3,))])
    return call_kernel('sum_mlp', body, ins, outs, scratch, 6e8, 2)


def attention_backward(side, ins, outs, scr):
    resid = scr.sum.part
    rows, width = resid.shape[2:]
    band = side * rows
    tile = min(256, side * band)
    loads, shared = [], []
    for index in PAIR:
        at = pl.ds(index * HEAD_DIM, HEAD_DIM)
        loads.append(pltpu.make_async_copy(ins.w_outs[index], scr.w_out.at[at, :], scr.w_out_sem.at[index]))
    for index in range(side):
        loads.append(pltpu.make_async_copy(ins.resid.at[index], resid.at[index], scr.resid_sem.at[index]))
    for load in loads:
        load.start()

    def context(index):
        if index == 0:
            for load in loads[:2]:
                load.wait()
        loads[2 + index].wait()
        scr.grad_ctx[index * band:(index + 1) * band, :] = dot(resid[index].reshape(band, width), scr.w_out[...], NT).astype(BF16)

    def begin():
        shared.extend([*segments(ins.seg), ins.qkv[:, 2 * HEAD_DIM:3 * HEAD_DIM].T])
        scr.grad_k[...] = jnp.zeros_like(scr.grad_k)
        scr.grad_v[...] = jnp.zeros_like(scr.grad_v)

    def put(first, count, cols, value):
        for start in range(first, first + count, 16):
            where = (start // band, start // rows % side, slice(start % rows, start % rows + 16), cols)
            outs.dqkv[where] = value[start - first:start - first + 16].astype(BF16)

    def head_tile(head_index, tile_index):
        cols = slice(head_index * HEAD_DIM, (head_index + 1) * HEAD_DIM)
        reach = (tile_index + 1) * tile
        probs, queries = scores_softmax(ins.qkv, *shared[:2], head_index, tile_index, tile)
        grad_ctx = scr.grad_ctx[tile_index * tile:reach, cols]
        grad_probs = dot(ins.qkv[:reach, 3 * HEAD_DIM:], grad_ctx, NT)
        centre = jnp.sum(grad_probs * probs, axis=0, keepdims=True)
        grad_scores = (probs * (grad_probs - centre) * HEAD_DIM ** -0.5).astype(BF16)
        scr.grad_v[:reach, :] += dot(probs.astype(BF16), grad_ctx, NN)
        scr.grad_k[:reach, :] += dot(grad_scores, queries, NN)
        put(tile_index * tile, tile, cols, dot(shared[K2][:, :reach], grad_scores, NN).T)

    def end():
        for index, ref in ((2, scr.grad_k), (3, scr.grad_v)):
            put(0, side * band, slice(index * HEAD_DIM, (index + 1) * HEAD_DIM), ref[...])

    call = functools.partial
    tiles = [call(head_tile, head_index, tile_index) for head_index in PAIR for tile_index in range(side * band // tile)]
    return [call(context, index) for index in range(side)] + [begin] + tiles + [end]


def sum_input(side, qkv, seg_ids, w_outs, w_qs, w_k, w_v, hidden, second, gain, mlp, w_downs):
    seq, depth = qkv.shape
    width = gain.shape[K1]
    rows = seq // (side * side)
    head = depth // 4
    half_side = side // 2
    tokens = seq // 2
    kv_width = w_k.shape[K1]
    per_kv = 2 * side * side * head // kv_width

    def body(ins, outs, scr, staging):
        torus = Torus(side)
        kv_col = pl.multiple_of(lax.div(torus.chip * 2, per_kv) * head, head)
        weights = Weights([*ins.w_qs, ins.w_k.at[:, pl.ds(kv_col, head)], ins.w_v.at[:, pl.ds(kv_col, head)]], scr.w, scr.w_sem, True)
        weights.start()
        weights_p = Weights(ins.w_downs, scr.wd, scr.wd_sem, False)
        weights_p.start()
        wait = torus.signal_all()
        part = scr.sum.part
        attention = attention_backward(side, ins, outs, scr)
        steps_p = ReduceScatter(torus, scr.sum_p).slow_steps(fill_partial(torus, scr.sum_p.part, ins.acts, weights_p))
        steps = ReduceScatter(torus, scr.sum).steps(fill_partial(torus, part, [outs.dqkv], weights))
        own = (torus.y, torus.x)
        gat = scr.all.gat
        gather = AllGather(torus, scr.all, True)

        def places(where, colour, half):
            chip = where[K0] * side + where[K1]
            tokens_at = pl.ds(pl.multiple_of(lax.rem(chip, 2) * tokens + colour * (tokens // 2), tokens // 2), tokens // 2)
            at = lax.div(chip, 2) * head
            src = gather.piece(gat, where, colour * 2, 2)
            return [(src.at[:, pl.ds(index * head, head)], outs.kv.at[half, tokens_at, pl.ds(pl.multiple_of(at + index * kv_width, head), head)]) for index in PAIR]

        gather.store = Store(torus, scr.all, places)
        rows_at = pl.ds(pl.multiple_of(torus.chip * rows, rows), rows)
        x_load = pltpu.make_async_copy(ins.hidden.at[torus.core, rows_at, :], scr.x_rows, scr.x_sem.at[K0])
        x_load.start()
        place = lax.rem(torus.x, 2)
        mate = torus.at_chip(torus.y, torus.x + 1 - 2 * place)
        kv_cols = pl.ds(2 * head, 2 * head)

        def mate_add():
            torus.arrive(scr.mate, scr.mate_sems, 0)
            mine = outs.dqkv[pl.ds(place * half_side, half_side), :, :, kv_cols]
            gat[own] = (mine.astype(F32) + scr.mate[...].astype(F32)).astype(BF16).reshape(tokens, 2 * head)

        staging.wait()
        steps_p[K0]()
        wait()
        sent, ringed = 5, 18
        run(steps_p[1:sent])
        run(attention, steps_p[sent:ringed])
        staging.save(outs.dqkv)
        steps[K0]()
        swaps = [(outs.dqkv.at[:, :, :, pl.ds(head, head)], outs.q_other)]
        swap_start(torus, scr.swap_sems, swaps)
        torus.send(outs.dqkv.at[pl.ds((1 - place) * half_side, half_side), :, :, kv_cols], scr.mate, scr.mate_sems, 0, mate)
        for step in steps[1:5]:
            step()
        mate_add()
        run(steps[5:], gather.steps(), steps_p[ringed:])
        x_load.wait()
        gain_total = jnp.zeros((1, width), F32)
        for at in row_tiles(rows):
            back, gain_part = rms_back(scr.x_rows[at, :].astype(F32), ins.gain[...], part[(*own, at, slice(None))].astype(F32))
            gain_total = gain_total + gain_part
            outs.rows[at, :] = (ins.d_rows[at, :] + back).astype(BF16)
            y_at = pl.ds(rows + at.start, at.size)
            outs.rows[y_at, :] = (ins.h_rows[at, :].astype(F32) + scr.sum_p.part[(*own, at, slice(None))].astype(F32)).astype(BF16)
        row = lax.broadcasted_iota(jnp.int32, (8, width), 0)
        extra = jnp.zeros((8, width), F32)
        for index, value in enumerate((gain_total, ins.gain_mlp[...])):
            for level in range(3):
                rounded = value.astype(BF16).astype(F32)
                extra = jnp.where(row == index * 3 + level, rounded, extra)
                value = value - rounded
        outs.rows[2 * rows:2 * rows + 8, :] = extra.astype(BF16)
        staging.save(outs.rows)
        gather.store.drain()
        swap_end(torus, scr.swap_sems, swaps)
        torus.drain()

    dma = pltpu.SemaphoreType.DMA
    ins = dict(qkv=(qkv, VMEM), seg=(seg_ids, VMEM), resid=(second.own, ANY), w_outs=[(weight, ANY) for weight in w_outs], acts=[(act, VMEM) for act in mlp.acts], w_downs=[(weight, ANY) for weight in w_downs], h_rows=(mlp.h_rows, VMEM), w_qs=[(weight, ANY) for weight in w_qs], w_k=(w_k, ANY), w_v=(w_v, ANY), hidden=(hidden, ANY), d_rows=(second.d_rows, VMEM),
               gain=(gain, VMEM), gain_mlp=(second.gain, VMEM))
    outs = dict(rows=(shape((2 * rows + 8, width)), VMEM), kv=(shape((2, seq, 2 * kv_width)), ANY), q_other=(shape((side, side, rows, head)), ANY), dqkv=(shape((side, side, rows, depth)), VMEM))
    scratch = dict(w_out=pltpu.VMEM((2 * head, width), BF16), grad_ctx=pltpu.VMEM((seq, 2 * head), BF16), grad_k=pltpu.VMEM((seq, head), F32), grad_v=pltpu.VMEM((seq, head), F32), w_out_sem=dma((K2,)), resid_sem=dma((side,)), sum_p=rs_scratch(side, rows, width), wd=pltpu.VMEM((2 * mlp.acts[K0].shape[K3], width), BF16), wd_sem=dma((K2, K2)),
                   sum=rs_scratch(side, rows, width), all=ag_scratch(side, tokens, 2 * head, 2), x_rows=pltpu.VMEM((rows, width), BF16), x_sem=dma((K1,)), w=pltpu.VMEM((width, depth), BF16), w_sem=dma((K2, 4)),
                   mate=pltpu.VMEM((half_side, side, rows, 2 * head), BF16), mate_sems=[dma((K1,)), dma((K1,))], swap_sems=[dma((K1,)), dma((K1,))])
    return call_kernel('sum_input', body, ins, outs, scratch, 3e8, 3)


def scores_softmax(qkv, seg_row, seg_col, head_index, tile_index, tile):
    reach = (tile_index + 1) * tile
    queries = qkv[tile_index * tile:reach, head_index * HEAD_DIM:(head_index + 1) * HEAD_DIM]
    scores = dot(qkv[:reach, 2 * HEAD_DIM:3 * HEAD_DIM], queries, NT) * HEAD_DIM ** -0.5
    key_at = lax.broadcasted_iota(jnp.int32, (reach, tile), 0)
    query_at = lax.broadcasted_iota(jnp.int32, (reach, tile), 1) + tile_index * tile
    allowed = (key_at <= query_at) & (seg_col[:reach, :] == seg_row[:, tile_index * tile:reach])
    scores = jnp.where(allowed, scores, -1e30)
    weights = jnp.exp(scores - jnp.max(scores, axis=0, keepdims=True))
    return weights * (1.0 / jnp.sum(weights, axis=0, keepdims=True)), queries


def segments(seg_ref):
    core = lax.rem(lax.axis_index('tp'), 2)
    seg_row = seg_ref[pl.ds(core, 1), :].astype(F32)
    return seg_row, jnp.broadcast_to(seg_row, (8, seg_row.shape[K1])).T[:, :1]


def attention_forward(hidden, seg_ids, gain, w_q, w_k, w_v, w_o, per_kv):
    seq, width = hidden.shape[1:]
    chunk = seq // 4
    group = 64
    tile = min(256, seq)
    depth = 4 * HEAD_DIM

    def body(ins, outs, scr, staging):
        tp_idx = lax.axis_index('tp')
        core = lax.rem(tp_idx, 2)
        kv_col = pl.multiple_of(lax.div(tp_idx, per_kv) * HEAD_DIM, HEAD_DIM)
        partner = dict(tp=tp_idx + 1 - 2 * core)
        barrier = pltpu.get_barrier_semaphore()
        pl.semaphore_signal(barrier, inc=1, device_id=partner, device_id_type=MESH)
        loads = []
        for index in range(4):
            at = pl.ds(index * chunk, chunk)
            loads.append(pltpu.make_async_copy(ins.hidden.at[core, at, :], scr.x.at[at, :], scr.x_sem.at[index]))

        def w_cols(index):
            return scr.w.at[:, pl.ds(index * HEAD_DIM, HEAD_DIM)]

        for index, ref in ((0, ins.w_q), (2, ins.w_k.at[:, pl.ds(kv_col, HEAD_DIM)]), (3, ins.w_v.at[:, pl.ds(kv_col, HEAD_DIM)])):
            loads.append(pltpu.make_async_copy(ref, w_cols(index), scr.w_sem.at[index]))
        for load in loads[4:] + loads[:4]:
            load.start()
        pl.semaphore_wait(barrier, 1)
        swaps = [(ins.w_q, w_cols(1)), (ins.w_o, outs.w_o), (ins.w_q, outs.w_q)]
        copies = []
        for index, (src, dst) in enumerate(swaps):
            copies.append(pltpu.make_async_remote_copy(src, dst, scr.swap_sems[K0].at[index], scr.swap_sems[K1].at[index], device_id=partner, device_id_type=MESH))
            copies[index].start()
        stores = []
        for index in range(4):
            loads[index].wait()

            if index == 0:
                staging.wait()

            def square(step, carry, index=index):
                at = pl.ds(pl.multiple_of(index * chunk + step * group, group), group)
                total = jnp.zeros((group, HEAD_DIM), F32)
                for lane in range(0, width, HEAD_DIM):
                    value = scr.x[at, lane:lane + HEAD_DIM].astype(F32)
                    total = total + value * value
                scr.squares[pl.ds(pl.multiple_of(step * group, group), group), :] = total
                return carry

            lax.fori_loop(0, chunk // group, square, 0)
            inv = lax.rsqrt(jnp.sum(scr.squares[...], axis=-1, keepdims=True) / width + EPS)
            scr.squares[...] = jnp.broadcast_to(inv, scr.squares.shape)

            def normalize(step, carry, index=index):
                at = pl.ds(pl.multiple_of(index * chunk + step * group, group), group)
                scale = scr.squares[pl.ds(pl.multiple_of(step * group, group), group), :]
                for lane in range(0, width, HEAD_DIM):
                    cols = slice(lane, lane + HEAD_DIM)
                    scr.normed[at, cols] = (scr.x[at, cols].astype(F32) * scale * ins.gain[:, cols]).astype(BF16)
                return carry

            lax.fori_loop(0, chunk // group, normalize, 0)
            at = pl.ds(index * chunk, chunk)
            store = pltpu.make_async_copy(scr.normed.at[at, :], outs.normed.at[at, :], scr.out_sem.at[index])
            store.start()
            stores.append(store)
            if index == 0:
                for load in loads[4:]:
                    load.wait()
                copies[K0].wait_recv()
            outs.qkv[at, :] = dot(scr.normed[at, :], scr.w[...], NN).astype(BF16)
        staging.save(outs.qkv)
        seg_row, seg_col = segments(ins.seg)
        values_t = outs.qkv[:, 3 * HEAD_DIM:].T
        for head_index in PAIR:
            for tile_index in range(seq // tile):
                probs, _ = scores_softmax(outs.qkv, seg_row, seg_col, head_index, tile_index, tile)
                ctx_t = dot(values_t[:, :(tile_index + 1) * tile], probs.astype(BF16), NN)
                outs.ctx[tile_index * tile:(tile_index + 1) * tile, head_index * HEAD_DIM:(head_index + 1) * HEAD_DIM] = ctx_t.T.astype(BF16)
        for store in stores:
            store.wait()
        copies[K0].wait_send()
        copies[K1].wait()
        copies[K2].wait()

    dma = pltpu.SemaphoreType.DMA
    ins = dict(hidden=(hidden, ANY), seg=(seg_ids, VMEM), gain=(gain, VMEM), w_q=(w_q, ANY), w_o=(w_o, ANY), w_k=(w_k, ANY), w_v=(w_v, ANY))
    outs = dict(normed=(shape((seq, width)), ANY), qkv=(shape((seq, depth)), VMEM), ctx=(shape((seq, 2 * HEAD_DIM)), VMEM), w_q=(shape(w_q.shape), ANY), w_o=(shape(w_o.shape), ANY))
    scratch = dict(squares=pltpu.VMEM((chunk, HEAD_DIM), F32), swap_sems=[dma((K3,)), dma((K3,))], x=pltpu.VMEM((seq, width), BF16), normed=pltpu.VMEM((seq, width), BF16), w=pltpu.VMEM((width, depth), BF16), x_sem=dma((4,)), w_sem=dma((4,)), out_sem=dma((4,)))
    return call_kernel('attention_forward', body, ins, outs, scratch, 5e9, 4)


def weight_grads(name, groups, ctxs, tokens=()):
    seq, width = groups[K0][K1].shape[1:]
    head = ctxs[K1].shape[K1] if ctxs else 0
    tile = min(512, width)
    lefts = [left for left, _ in groups if left is not None]
    sizes = [head if left is None else left.shape[K0] for left, _ in groups]
    given = len(groups) + len(lefts) + len(ctxs)

    def kernel(*refs):
        rights, left_refs = refs[:len(groups)], list(refs[len(groups):len(groups) + len(lefts)])
        outs = refs[given + len(tokens):given + len(tokens) + len(groups)]
        if ctxs:
            core = lax.rem(lax.axis_index('tp'), 2)
            ctx_t = refs[-1]

            @pl.when(pl.program_id(0) == 0)
            def _():
                for half, ref in zip((core, 1 - core), refs[given - 2:given]):
                    ctx_t[:, pl.ds(pl.multiple_of(half * seq, seq), seq)] = ref[:, :head].T

        for (left, _), right, out in zip(groups, rights, outs):
            ref = ctx_t if left is None else left_refs.pop(0)
            out[...] = dot(ref[...], right[...].reshape(2 * seq, tile), NN)

    slab = pl.BlockSpec((2, seq, tile), lambda step: (0, 0, step))
    return pl.pallas_call(
        kernel,
        name=name,
        grid=(width // tile,),
        out_shape=[shape((size, width), F32) for size in sizes],
        in_specs=[slab] * len(groups) + [VMEM] * (len(lefts) + len(ctxs)) + [ANY] * len(tokens),
        out_specs=[pl.BlockSpec((size, tile), lambda step: (0, step)) for size in sizes],
        scratch_shapes=[pltpu.VMEM((head, 2 * seq), BF16)] if ctxs else [],
        compiler_params=pltpu.CompilerParams(vmem_limit_bytes=LIMIT),
        cost_estimate=pl.CostEstimate(flops=int(1e10), bytes_accessed=int(4e7), transcendentals=0),
    )(*[right for _, right in groups], *lefts, *ctxs, *tokens)


def weight_grads_pair(left_gate, left_up, mixed_full, token):
    seq, width = mixed_full.shape[1:]
    depth = left_gate.shape[K0]
    tile = min(512, width)

    def kernel(m_ref, gate_ref, up_ref, _, out_gate, out_up):
        mixed = m_ref[...].reshape(2 * seq, tile)
        out_gate[...] = dot(gate_ref[...], mixed, NN)
        out_up[...] = dot(up_ref[...], mixed, NN)

    out = pl.BlockSpec((depth, tile), lambda step: (0, step))
    return pl.pallas_call(
        kernel,
        name='weight_grads_pair',
        grid=(width // tile,),
        out_shape=[shape((depth, width), F32)] * 2,
        in_specs=[pl.BlockSpec((2, seq, tile), lambda step: (0, 0, step)), VMEM, VMEM, ANY],
        out_specs=[out, out],
        compiler_params=pltpu.CompilerParams(vmem_limit_bytes=LIMIT),
        cost_estimate=pl.CostEstimate(flops=int(1e10), bytes_accessed=int(4e7), transcendentals=0),
    )(mixed_full, left_gate, left_up, token)


def weight_grads_qkv(normeds, kv_full, grads_q):
    seq, width = normeds[K0].shape
    head = grads_q[K1].shape[K1]
    kv_width = kv_full.shape[K2] // 2
    tile = min(512, width)

    def kernel(a_own, a_other, kv_ref, q_own, q_other, out_q, out_k, out_v, left, q_both):
        core = lax.rem(lax.axis_index('tp'), 2)
        halves = [pl.ds(pl.multiple_of(half * seq, seq), seq) for half in (core, 1 - core)]

        @pl.when(pl.program_id(0) == 0)
        def _():
            q_both[halves[K0], :] = q_own[:, :head]
            q_both[halves[K1], :] = q_other[...]

        left[:, halves[K0]] = a_own[...].T
        left[:, halves[K1]] = a_other[...].T
        out_q[...] = dot(left[...], q_both[...], NN)
        for index, out in enumerate((out_k, out_v)):
            right = kv_ref[:, :, pl.ds(index * kv_width, kv_width)].reshape(2 * seq, kv_width)
            out[...] = dot(left[...], right, NN)

    slab = pl.BlockSpec((seq, tile), lambda step: (0, step))
    out = lambda size: pl.BlockSpec((tile, size), lambda step: (step, 0))
    return pl.pallas_call(
        kernel,
        name='weight_grads_qkv',
        grid=(width // tile,),
        out_shape=[shape((width, size), F32) for size in (head, kv_width, kv_width)],
        in_specs=[slab] * 2 + [VMEM] * 3,
        out_specs=[out(size) for size in (head, kv_width, kv_width)],
        scratch_shapes=[pltpu.VMEM((tile, 2 * seq), BF16), pltpu.VMEM((2 * seq, head), BF16)],
        compiler_params=pltpu.CompilerParams(vmem_limit_bytes=LIMIT),
        cost_estimate=pl.CostEstimate(flops=int(27e9), bytes_accessed=int(6e7), transcendentals=0),
    )(*normeds, kv_full, *grads_q)


def in_place(gathered, rows):
    blocks, _, width = gathered.shape
    slots = 24
    pieces = 2 * blocks

    def kernel(src, dx_ref, y_ref, gain_attn, gain_mlp, buf, extra, in_sem, out_sem, extra_sem):
        gains = pltpu.make_async_copy(src.at[:, pl.ds(2 * rows, 8), :], extra, extra_sem.at[K0])

        def load(index):
            at = pl.ds(index // blocks * rows, rows)
            return pltpu.make_async_copy(src.at[index % blocks, at, :], buf.at[index % slots], in_sem.at[index % slots])

        def store(index):
            dst, block = (dx_ref, y_ref)[index // blocks], index % blocks
            return pltpu.make_async_copy(buf.at[index % slots], dst.at[block % 2, block // 2], out_sem.at[index % slots])

        ahead = slots // 2
        for index in range(pieces + ahead):
            if index < pieces:
                if index >= slots:
                    store(index - slots).wait()
                load(index).start()
            if index == ahead:
                gains.start()
            if index >= ahead:
                load(index - ahead).wait()
                store(index - ahead).start()
        gains.wait()
        total = jnp.sum(extra[...].astype(F32), axis=0)
        for first, ref in ((0, gain_attn), (3, gain_mlp)):
            ref[...] = total[first:first + 1] + total[first + 1:first + 2] + total[first + 2:first + 3]
        for index in range(pieces - slots, pieces):
            store(index).wait()

    dma = pltpu.SemaphoreType.DMA
    whole = shape((2, blocks // 2, rows, width))
    return pl.pallas_call(
        kernel,
        name='in_place',
        out_shape=[whole, whole, shape((1, width), F32), shape((1, width), F32)],
        in_specs=[ANY],
        out_specs=[ANY, ANY, VMEM, VMEM],
        scratch_shapes=[pltpu.VMEM((slots, rows, width), BF16), pltpu.VMEM((blocks, 8, width), BF16), dma((slots,)), dma((slots,)), dma((K1,))],
        compiler_params=pltpu.CompilerParams(vmem_limit_bytes=LIMIT),
        cost_estimate=pl.CostEstimate(flops=int(2e7), bytes_accessed=int(2e7), transcendentals=0),
    )(gathered)


def solution(mesh):
    tp_size = mesh.shape['tp']
    chips = tp_size // 2
    side = math.isqrt(chips)

    def device_step(hidden, seg_ids, grad_out, gain_attn, gain_mlp, w_q, w_k, w_v, w_o, w_gate, w_up, w_down):
        seq_len, width = hidden.shape[1:]
        kv_heads = w_k.shape[K1] // HEAD_DIM
        per_kv = tp_size // kv_heads
        rows = seq_len // chips

        def flat(value):
            return value.reshape(seq_len, value.shape[-1])

        gain_attn_row = gain_attn[None, :]
        gain_mlp_row = gain_mlp[None, :]

        attn = attention_forward(hidden, seg_ids, gain_attn_row, w_q, w_k, w_v, w_o, per_kv)
        w_qs, w_outs = (w_q, attn.w_q), (w_o, attn.w_o)
        mlp = sum_attention(side, attn, w_outs, hidden, grad_out, gain_mlp_row, w_gate.T, w_up.T, w_down)
        mixed_full = mlp.full.reshape(2, seq_len, width)
        second = sum_mlp(side, mlp, (w_gate.T, mlp.w_gate), (w_up.T, mlp.w_up), grad_out, gain_mlp_row)
        resid_full = second.full.reshape(2, seq_len, width)

        third = sum_input(side, attn.qkv, seg_ids, w_outs, w_qs, w_k, w_v, hidden, second, gain_attn_row, mlp, (w_down, mlp.w_down))

        grad_in, y_out, grad_gain_attn, grad_gain_mlp = in_place(lax.all_gather(third.rows, 'tp'), rows)
        left_gate, left_up, left_act = second.lefts
        grad_gate_t, grad_up_t = weight_grads_pair(left_gate, left_up, mixed_full, third.q_other)
        grad_w_down, grad_w_o = weight_grads('weight_grads_down', [(left_act, grad_out), (None, resid_full)], (attn.ctx, flat(mlp.ctx_other)), (third.q_other,))
        grad_w_q, grad_w_k, grad_w_v = weight_grads_qkv((attn.normed, mlp.normed_other), third.kv, (flat(third.dqkv), flat(third.q_other)))
        return (y_out.reshape(hidden.shape), grad_in.reshape(hidden.shape), grad_gain_attn[K0], grad_gain_mlp[K0], grad_w_q, grad_w_k, grad_w_v, grad_w_o, grad_gate_t.T, grad_up_t.T, grad_w_down)

    spec_act = P('data', None, None)
    spec_rows = P('data', None)
    spec_gain = P(None)
    spec_cols = P(None, 'tp')
    spec_tprows = P('tp', None)
    spec_whole = P(None, None)
    spec_stack = P(('data', 'tp'), None)
    in_specs = (spec_act, spec_rows, spec_act, spec_gain, spec_gain, spec_cols, spec_whole, spec_whole, spec_tprows, spec_cols, spec_cols, spec_tprows)
    out_specs = (spec_act, spec_act, P('data'), P('data'), P('data', 'tp'), spec_rows, spec_rows, spec_stack, P('data', 'tp'), P('data', 'tp'), spec_stack)
    return jax.shard_map(device_step, mesh=mesh, in_specs=in_specs, out_specs=out_specs, check_vma=False)
```
